32 devices in a mesh: fsdp: 4 (over y, x), ctx: 4 (over z), tp: 2 (over core).
Axes of the slice: x: 2, y: 2, z: 4, core: 2. Of those that a mesh axis runs over, the one named last changes fastest.
Arguments:
- hidden_in: bfloat16 [4, 512, 1024], P('fsdp', 'ctx'), may hold values from -6 to 6
- out_grad: bfloat16 [4, 512, 1024], P('fsdp', 'ctx'), may hold values from -6 to 6
- attention_gain: bfloat16 [1024], P(('fsdp', 'ctx')), may hold values from 0.5 to 1.5
- query_weight: bfloat16 [1024, 1024], P(('fsdp', 'ctx'), 'tp'), may hold values from -1 to 1
- key_weight: bfloat16 [1024, 512], P(('fsdp', 'ctx'), 'tp'), may hold values from -1 to 1
- value_weight: bfloat16 [1024, 512], P(('fsdp', 'ctx'), 'tp'), may hold values from -0.1875 to 0.1875
- output_weight: bfloat16 [1024, 1024], P(('fsdp', 'ctx'), 'tp'), may hold values from -0.75 to 0.75
- expert_gain: bfloat16 [1024], P(('fsdp', 'ctx')), may hold values from 0.5 to 1.5
- router_weight: bfloat16 [1024, 16], P(('fsdp', 'ctx')), may hold values from -1 to 1
- gate_weight: bfloat16 [16, 1024, 512], P(None, ('fsdp', 'ctx'), 'tp'), may hold values from -0.1875 to 0.1875
- up_weight: bfloat16 [16, 1024, 512], P(None, ('fsdp', 'ctx'), 'tp'), may hold values from -0.1875 to 0.1875
- down_weight: bfloat16 [16, 1024, 512], P(None, ('fsdp', 'ctx'), 'tp'), may hold values from -0.25 to 0.25
- doc_lengths: int32 [4, 8], P('fsdp'), may hold values from 1 to 256, 512 in all within a row
- expert_choice: int32 [4, 512, 8], P('fsdp', 'ctx'), may hold values from 0 to 15, all different within a row; in each aligned block of 128 rows (0 to 127, 128 to 255, ..., all dimensions but the last counted through in order) at most 96 rows name the same one
Outputs:
- block_out: bfloat16 [4, 512, 1024], P('fsdp', 'ctx')
- input_grad: float32 [4, 512, 1024], P('fsdp', 'ctx')
- attention_gain_grad: float32 [1024], P(('fsdp', 'ctx'))
- query_weight_grad: float32 [1024, 1024], P(('fsdp', 'ctx'), 'tp')
- key_weight_grad: float32 [1024, 512], P(('fsdp', 'ctx'), 'tp')
- value_weight_grad: float32 [1024, 512], P(('fsdp', 'ctx'), 'tp')
- output_weight_grad: float32 [1024, 1024], P(('fsdp', 'ctx'), 'tp')
- expert_gain_grad: float32 [1024], P(('fsdp', 'ctx'))
- router_weight_grad: float32 [1024, 16], P(('fsdp', 'ctx'))
- gate_weight_grad: float32 [16, 1024, 512], P(None, ('fsdp', 'ctx'), 'tp')
- up_weight_grad: float32 [16, 1024, 512], P(None, ('fsdp', 'ctx'), 'tp')
- down_weight_grad: float32 [16, 1024, 512], P(None, ('fsdp', 'ctx'), 'tp')
The draws below stay inside these ranges and needn't reach their ends.
Inputs may be any that keep to these rules, and one draw needn't show every extreme that they name: `doc_lengths`: each row's lengths sum to 512; in every row the longest document has exactly 256 positions. `expert_choice`: A token names 8 different experts. Among the tokens of one block of 128 positions (one device's tokens) no expert is named more than 96 times, and in every draw some expert is named exactly 96 times in some block.
All inputs are finite; a program needn't handle non-finite values.
Results may differ from the reference program's by a relative error of at most 0.04.
Values may be sent and summed in bfloat16 or wider, within the bound.
A program may use at most 192 MiB of HBM per device.

```python
import math
import jax
import jax.numpy as jnp
import numpy as np
from jax import lax

D = 1024
H = 16
KV = 8
HD = 64
E = 16
FF = 512
TOPK = 8
BLK = 128
NDOC = 8
ROWS = 4
LEN = 512
CAP = 96


def draw_hidden_in(key, part):
    return jnp.clip(jax.random.normal(jax.random.fold_in(key, 1), (ROWS, LEN, D), jnp.float32), -6.0, 6.0).astype(jnp.bfloat16)


def draw_query_weight(key, part):
    return (jax.random.truncated_normal(jax.random.fold_in(key, 11), -6.0, 6.0, (D, H * HD), jnp.float32) * D ** (-0.5)).astype(jnp.bfloat16)


def draw_key_weight(key, part):
    return (jax.random.truncated_normal(jax.random.fold_in(key, 21), -6.0, 6.0, (D, KV * HD), jnp.float32) * D ** (-0.5)).astype(jnp.bfloat16)


def draw_router_weight(key, part):
    spread = (D // 4) ** (-0.5)
    return (jax.random.truncated_normal(jax.random.fold_in(key, 31), -6.0, 6.0, (D, E), jnp.float32) * spread).astype(jnp.bfloat16)


def shard_levels(own_key, shape, pieces, smallest, high):
    level, own = 1.0, jax.random.fold_in(own_key, 6)
    for axis_at, shards_of in pieces:
        steps = jnp.exp(jax.random.uniform(jax.random.fold_in(own, axis_at), (shards_of,), jnp.float32, smallest / len(pieces), high / len(pieces)))
        level = level * jnp.repeat(steps, shape[axis_at] // shards_of).reshape([-1 if axis == axis_at else 1 for axis in range(len(shape))])
    return level


def profile(count, total, limit, slope):
    portions = [(1 << 20) // math.isqrt(standing ** slope) + 1 for standing in range(2, count + 1)]
    rest, holding = total - limit - (count - 1), [1] * (count - 1)
    while rest > 0:
        movable = [i for i in range(count - 1) if holding[i] < limit]
        mass, budget = sum([portions[i] for i in movable]), rest
        for i in movable:
            extra = min(limit - holding[i], max(1, budget * portions[i] // mass), rest)
            holding[i] = holding[i] + extra
            rest = rest - extra
    return np.array([limit] + holding)


def ragged(rng, number_of, total, limit, lean):
    if number_of == 2:
        one = jax.random.randint(rng, (), max(1, total - limit), min(limit, total - 1) + 1)
        return jnp.stack([one, total - one])
    sizes = jnp.asarray(profile(number_of, total, limit, lean), jnp.int32)
    couples = (number_of - 1) // 2
    giver, sink = sizes[1:1 + 2 * couples:2], sizes[2:2 + 2 * couples:2]
    slack = jnp.minimum(giver - 1, limit - sink)
    shifted = jax.random.randint(jax.random.fold_in(rng, 1), (couples,), 0, 1 << 20) % (slack + 1)
    sizes = sizes.at[1:1 + 2 * couples:2].set(giver - shifted).at[2:2 + 2 * couples:2].set(sink + shifted)
    return sizes[jax.random.permutation(jax.random.fold_in(rng, 2), number_of)]


def shared_out(key, own, number, rows, number_of, top, reach, lean):
    ranking = jax.random.permutation(key, number_of)
    crowded, common = shares(number_of, rows * top, reach, lean, True), shares(number_of, rows * top, reach, lean, False)
    places = jnp.arange(number_of)

    def named(sizes, turn):
        used = int((sizes > 0).sum())
        fixed = max(1, used // 4)
        passed = fixed + (places - fixed + turn * (used - fixed)) % max(1, number_of - fixed)
        return jnp.zeros((number_of,), jnp.int32).at[ranking[jnp.where(places < fixed, places, passed)]].set(jnp.asarray(sizes, jnp.int32))

    sizes = jnp.where(number % 4 == 0, named(crowded, number // 4), named(common, number - number // 4 - 1))
    mixed = jax.random.permutation(jax.random.fold_in(own, 3), number_of)
    source_of, taker = mixed[0:number_of // 2 * 2:2], mixed[1:number_of // 2 * 2:2]
    slack = jnp.minimum(sizes[source_of] - 1, reach - sizes[taker]) // 2
    slack = jnp.where((source_of == ranking[0]) | (taker == ranking[0]) | (sizes[taker] == 0), 0, jnp.maximum(slack, 0))
    passed = jax.random.randint(jax.random.fold_in(own, 4), (number_of // 2,), 0, 1 << 20) % (slack + 1)
    sizes = sizes.at[source_of].add(-passed).at[taker].add(passed)
    members = jnp.searchsorted(jnp.cumsum(sizes), jnp.arange(rows * top), side="right").astype(jnp.int32)
    grid = members.reshape(top, rows).T
    grid = grid[jax.random.permutation(jax.random.fold_in(own, 1), rows)]
    turn = jax.random.randint(jax.random.fold_in(own, 2), (rows, 1), 0, top)
    return jnp.take_along_axis(grid, (jnp.arange(top)[None, :] + turn) % top, axis=1)


def shares(number_of, total, bound, slope, full):
    weights = [(1 << 20) // math.isqrt(standing ** slope) + 1 for standing in range(1, number_of + 1)]
    largest = bound if full else min(bound, max(-(-total // number_of), total * weights[0] // sum(weights)))
    least = 1 if total - largest >= number_of - 1 else 0
    holding, spare = [largest] + [least] * (number_of - 1), total - largest - least * (number_of - 1)
    while spare > 0:
        movable = [i for i in range(1, number_of) if holding[i] < largest] or [i for i in range(1, number_of) if holding[i] < bound]
        mass, left = sum([weights[i] for i in movable]), spare
        for i in movable:
            addition = min(bound - holding[i], max(1, left * weights[i] // mass), spare)
            holding[i] = holding[i] + addition
            spare = spare - addition
    return np.array(holding)


def bell_draw(own_key, dims, scale, bound, cuts=(), kind=jnp.bfloat16):
    entries = scale * jax.random.normal(own_key, dims, jnp.float32)
    if cuts:
        entries = entries * shard_levels(own_key, dims, cuts, -0.22, 0.18)
    return jnp.clip(entries, -bound, bound).astype(kind)


def setup_inputs(seed: int = 0) -> dict:
    seeds = jax.random.split(jax.random.key(seed), 15)
    hidden_in = draw_hidden_in(jax.random.fold_in(seeds[14], 71), 0)
    out_grad = bell_draw(seeds[1], (ROWS, LEN, D), 1.0, 6.0, ((0, 4), (1, 4)))
    attention_gain = jnp.clip(1.0 + 0.1 * jax.random.normal(seeds[2], (D,), jnp.float32), 0.5, 1.5).astype(jnp.bfloat16)
    query_weight = draw_query_weight(jax.random.fold_in(seeds[14], 71), 0)
    key_weight = draw_key_weight(jax.random.fold_in(seeds[14], 71), 0)
    value_weight = bell_draw(seeds[5], (D, KV * HD), D ** -0.5, 0.1875, ((0, 16), (1, 2)))
    output_weight = bell_draw(seeds[6], (D, H * HD), (H * HD // 16) ** -0.5, 0.75, ((0, 16), (1, 2)))
    expert_gain = jnp.clip(1.0 + 0.1 * jax.random.normal(seeds[7], (D,), jnp.float32), 0.5, 1.5).astype(jnp.bfloat16)
    router_weight = draw_router_weight(jax.random.fold_in(seeds[14], 71), 0)
    gate_weight = bell_draw(seeds[9], (E, D, FF), D ** -0.5, 0.1875, ((1, 16), (2, 2)))
    up_weight = bell_draw(seeds[10], (E, D, FF), D ** -0.5, 0.1875, ((1, 16), (2, 2)))
    down_weight = bell_draw(seeds[11], (E, D, FF), FF ** -0.5, 0.25, ((1, 16), (2, 2)))
    doc_lengths = jax.vmap(lambda own: ragged(own, NDOC, LEN, LEN // 2, 2))(jax.random.split(seeds[12], ROWS)).reshape((ROWS, NDOC)).astype(jnp.int32)
    expert_choice_keys = jax.random.split(jax.random.fold_in(seeds[13], 1), ROWS * LEN // BLK)
    expert_choice_turns = jax.random.permutation(jax.random.fold_in(seeds[13], 3), ROWS * LEN // BLK)
    expert_choice = jax.vmap(lambda own, number: shared_out(jax.random.fold_in(seeds[13], 2), own, number, BLK, E, TOPK, CAP, 2))(expert_choice_keys, expert_choice_turns).reshape((ROWS, LEN, TOPK))
    return dict(hidden_in=hidden_in, out_grad=out_grad, attention_gain=attention_gain, query_weight=query_weight, key_weight=key_weight, value_weight=value_weight, output_weight=output_weight, expert_gain=expert_gain, router_weight=router_weight, gate_weight=gate_weight, up_weight=up_weight, down_weight=down_weight, doc_lengths=doc_lengths, expert_choice=expert_choice)


epsilon = 1e-05
rope_base = 10000.0
masked_score = -1e+30
highest = lax.Precision.HIGHEST

def doc_layout(lengths, positions):
    ends = jnp.cumsum(lengths)
    after = (positions[:, None] >= ends[None, :]).astype(jnp.int32)
    segment = lax.optimization_barrier(jnp.sum(after, axis=1))
    offset = positions - lax.optimization_barrier(jnp.sum(after * lengths[None, :], axis=1))
    return (segment, offset)

def rope_tables(offset):
    halfway = HD // 2
    frequency = rope_base ** (-jnp.arange(halfway, dtype=jnp.float32) / halfway)
    angle = offset.astype(jnp.float32)[:, None] * frequency[None, :]
    return (jnp.cos(angle), jnp.sin(angle))

def rotate(vectors, cosine, sine):
    halfway = vectors.shape[-1] // 2
    former = vectors[..., :halfway]
    latter = vectors[..., halfway:]
    cosine = cosine[:, None, :]
    sine = sine[:, None, :]
    return jnp.concatenate([former * cosine - latter * sine, latter * cosine + former * sine], axis=-1)

def rotate_back(grads, cosine, sine):
    halfway = grads.shape[-1] // 2
    former = grads[..., :halfway]
    latter = grads[..., halfway:]
    cosine = cosine[:, None, :]
    sine = sine[:, None, :]
    return jnp.concatenate([former * cosine + latter * sine, latter * cosine - former * sine], axis=-1)

def norm_forward(values, gain):
    inverse = lax.rsqrt(lax.optimization_barrier(jnp.mean(values * values, axis=-1, keepdims=True)) + epsilon)
    return (values * inverse * gain.astype(jnp.float32), inverse)

def norm_backward(values, inverse, gain, grad_normed):
    scaled = grad_normed * gain.astype(jnp.float32)
    grad_values = inverse * scaled - values * inverse ** 3 * lax.optimization_barrier(jnp.mean(scaled * values, axis=-1, keepdims=True))
    grad_gain = lax.optimization_barrier(jnp.sum(grad_normed * values * inverse, axis=0))
    return (grad_values, grad_gain)

def dispatch(route, experts, capacity):
    flat = route.reshape(-1)
    onehot = (flat[:, None] == jnp.arange(experts, dtype=jnp.int32)[None, :]).astype(jnp.int32)
    rank = lax.optimization_barrier(jnp.sum((jnp.cumsum(onehot, axis=0) - onehot) * onehot, axis=1))
    slot = (flat * capacity + rank).astype(jnp.int32)
    pairs = flat.shape[0]
    owner = jnp.zeros((experts * capacity,), jnp.int32).at[slot].set(jnp.arange(pairs, dtype=jnp.int32))
    filled = jnp.zeros((experts * capacity,), jnp.int32).at[slot].set(1) > 0
    return (slot, owner, filled)

def expert_block(normed, route, grad_out, router_weight, gate_weight, up_weight, down_weight):
    logits = jnp.dot(normed, router_weight, preferred_element_type=jnp.float32)
    gates = jax.nn.softmax(jnp.take_along_axis(logits, route, axis=1), axis=1)
    slot, owner, filled = dispatch(route, E, CAP)
    token_of = owner // TOPK
    slot_inputs = jnp.where(filled[:, None], normed[token_of], 0).reshape(E, CAP, D)
    slot_wide = slot_inputs.astype(jnp.float32)
    gate_wide = gate_weight.astype(jnp.float32)
    up_wide = up_weight.astype(jnp.float32)
    down_wide = down_weight.astype(jnp.float32)
    gate_pre = jnp.einsum('ecd,edf->ecf', slot_wide, gate_wide)
    up_pre = jnp.einsum('ecd,edf->ecf', slot_wide, up_wide)
    sigmoid = jax.nn.sigmoid(gate_pre)
    activated = (gate_pre * sigmoid * up_pre).astype(jnp.bfloat16)
    expert_out = jnp.einsum('ecf,edf->ecd', activated.astype(jnp.float32), down_wide)
    pair_out = expert_out.reshape(E * CAP, D)[slot].reshape(route.shape[0], TOPK, D)
    mixed = lax.optimization_barrier(jnp.sum(gates[..., None] * pair_out, axis=1))
    gate_dot = lax.optimization_barrier(jnp.sum(pair_out * grad_out[:, None, :], axis=2))
    chosen_grad = gates * (gate_dot - lax.optimization_barrier(jnp.sum(gates * gate_dot, axis=1, keepdims=True)))
    picked = (route[..., None] == jnp.arange(E, dtype=jnp.int32)[None, None, :]).astype(jnp.float32)
    logit_grad = lax.optimization_barrier(jnp.sum(picked * chosen_grad[..., None], axis=1))
    router_term = jnp.dot(normed.astype(jnp.float32).T, logit_grad, precision=highest)
    router_input = jnp.dot(logit_grad, router_weight.astype(jnp.float32).T, precision=highest)
    slot_gate = jnp.where(filled, gates.reshape(-1)[owner], 0.0)
    slot_grads = (grad_out[token_of] * slot_gate[:, None]).astype(jnp.bfloat16).reshape(E, CAP, D)
    slot_grads_wide = slot_grads.astype(jnp.float32)
    act_grad = jnp.einsum('ecd,edf->ecf', slot_grads_wide, down_wide)
    gate_pre_grad = (act_grad * up_pre * sigmoid * (1.0 + gate_pre * (1.0 - sigmoid))).astype(jnp.bfloat16)
    up_pre_grad = (act_grad * gate_pre * sigmoid).astype(jnp.bfloat16)
    gate_pre_wide = gate_pre_grad.astype(jnp.float32)
    up_pre_wide = up_pre_grad.astype(jnp.float32)
    down_term = jnp.einsum('ecd,ecf->edf', slot_grads_wide, activated.astype(jnp.float32))
    gate_term = jnp.einsum('ecd,ecf->edf', slot_wide, gate_pre_wide)
    up_term = jnp.einsum('ecd,ecf->edf', slot_wide, up_pre_wide)
    slot_back = jnp.einsum('ecf,edf->ecd', gate_pre_wide, gate_wide) + jnp.einsum('ecf,edf->ecd', up_pre_wide, up_wide)
    moe_input = lax.optimization_barrier(jnp.sum(slot_back.reshape(E * CAP, D)[slot].reshape(route.shape[0], TOPK, D), axis=1))
    return (mixed, moe_input + router_input, router_term, gate_term, up_term, down_term)

def reference(hidden_in, out_grad, attention_gain, query_weight, key_weight, value_weight, output_weight, expert_gain, router_weight, gate_weight, up_weight, down_weight, doc_lengths, expert_choice):
    ratio = H // KV
    scale = HD ** (-0.5)
    blocks = LEN // BLK

    def per_row(totals, item):
        inputs_low, grads_low, lengths, route_row = item
        position = jnp.arange(LEN, dtype=jnp.int32)
        segment, offset = doc_layout(lengths, position)
        cosine, sine = rope_tables(offset)
        inputs = inputs_low.astype(jnp.float32)
        normed_one, inverse_one = norm_forward(inputs, attention_gain)
        normed_one = normed_one.astype(jnp.bfloat16)
        query = rotate(jnp.dot(normed_one, query_weight, preferred_element_type=jnp.float32).reshape(LEN, H, HD), cosine, sine).astype(jnp.bfloat16)
        keys = rotate(jnp.dot(normed_one, key_weight, preferred_element_type=jnp.float32).reshape(LEN, KV, HD), cosine, sine).astype(jnp.bfloat16)
        values = jnp.dot(normed_one, value_weight, preferred_element_type=jnp.float32).astype(jnp.bfloat16).reshape(LEN, KV, HD)
        keys_wide = keys.astype(jnp.float32)
        values_wide = values.astype(jnp.float32)
        grouped = query.reshape(blocks, BLK, KV, ratio, HD)
        segment_blocks = segment.reshape(blocks, BLK)
        position_blocks = position.reshape(blocks, BLK)

        def forward_block(piece):
            query_block, segment_block, position_block = piece
            allowed = (segment_block[:, None] == segment[None, :]) & (position[None, :] <= position_block[:, None])
            mask = allowed[:, None, None, :]
            scores = jnp.einsum('qgrd,kgd->qgrk', query_block.astype(jnp.float32), keys_wide) * scale
            scores = jnp.where(mask, scores, masked_score)
            peak = lax.optimization_barrier(jnp.max(scores, axis=3))
            weights = jnp.where(mask, jnp.exp(scores - peak[..., None]), 0.0)
            total = lax.optimization_barrier(jnp.sum(weights, axis=3))
            attended = jnp.einsum('qgrk,kgd->qgrd', weights, values_wide, precision=highest) / total[..., None]
            return (attended, peak + jnp.log(total))
        attended, log_total = lax.map(forward_block, (grouped, segment_blocks, position_blocks))
        attended = attended.reshape(LEN, H * HD).astype(jnp.bfloat16)
        log_total = log_total.reshape(blocks, BLK, KV, ratio)
        residual = inputs + jnp.dot(attended, output_weight.T, preferred_element_type=jnp.float32)
        normed_two, inverse_two = norm_forward(residual, expert_gain)
        normed_two = normed_two.astype(jnp.bfloat16)
        grad_out = grads_low.astype(jnp.float32)

        def expert_visit(carry, piece):
            normed_block, route_block, grad_block = piece
            mixed, grad_normed, router_term, gate_term, up_term, down_term = expert_block(normed_block, route_block, grad_block, router_weight, gate_weight, up_weight, down_weight)
            router_sum, gate_sum, up_sum, down_sum = carry
            return ((router_sum + router_term, gate_sum + gate_term, up_sum + up_term, down_sum + down_term), (mixed, grad_normed))
        expert_init = (jnp.zeros((D, E), jnp.float32), jnp.zeros((E, D, FF), jnp.float32), jnp.zeros((E, D, FF), jnp.float32), jnp.zeros((E, D, FF), jnp.float32))
        expert_sums, (mixed, grad_normed_two) = lax.scan(expert_visit, expert_init, (normed_two.reshape(blocks, BLK, D), route_row.reshape(blocks, BLK, TOPK), grad_out.reshape(blocks, BLK, D)))
        mixed = mixed.reshape(LEN, D)
        grad_normed_two = grad_normed_two.reshape(LEN, D)
        block_out = (residual + mixed).astype(jnp.bfloat16)
        grad_residual_norm, gain_two_term = norm_backward(residual, inverse_two, expert_gain, grad_normed_two)
        grad_residual = grad_out + grad_residual_norm
        residual_low = grad_residual.astype(jnp.bfloat16)
        attended_grad = jnp.dot(residual_low, output_weight, preferred_element_type=jnp.float32).astype(jnp.bfloat16)
        output_term = jnp.dot(residual_low.T, attended, preferred_element_type=jnp.float32)
        delta = lax.optimization_barrier(jnp.sum((attended_grad.astype(jnp.float32) * attended.astype(jnp.float32)).reshape(LEN, KV, ratio, HD), axis=3))
        grad_blocks = attended_grad.reshape(blocks, BLK, KV, ratio, HD)

        def backward_block(carry, piece):
            key_acc, value_acc = carry
            query_block, grad_block, delta_block, total_block, segment_block, position_block = piece
            allowed = (segment_block[:, None] == segment[None, :]) & (position[None, :] <= position_block[:, None])
            mask = allowed[:, None, None, :]
            query_wide = query_block.astype(jnp.float32)
            grad_wide = grad_block.astype(jnp.float32)
            scores = jnp.einsum('qgrd,kgd->qgrk', query_wide, keys_wide) * scale
            probs = jnp.where(mask, jnp.exp(scores - total_block[..., None]), 0.0)
            probs_low = lax.optimization_barrier(probs.astype(jnp.bfloat16))
            value_acc = value_acc + jnp.einsum('qgrk,qgrd->kgd', probs_low.astype(jnp.float32), grad_wide)
            prob_grad = jnp.einsum('qgrd,kgd->qgrk', grad_wide, values_wide)
            score_grad = lax.optimization_barrier((probs * (prob_grad - delta_block[..., None]) * scale).astype(jnp.bfloat16))
            score_wide = score_grad.astype(jnp.float32)
            query_grad_block = jnp.einsum('qgrk,kgd->qgrd', score_wide, keys_wide)
            key_acc = key_acc + jnp.einsum('qgrk,qgrd->kgd', score_wide, query_wide)
            return ((key_acc, value_acc), query_grad_block)
        back_init = (jnp.zeros((LEN, KV, HD), jnp.float32), jnp.zeros((LEN, KV, HD), jnp.float32))
        (key_acc, value_acc), query_grad = lax.scan(backward_block, back_init, (grouped, grad_blocks, delta.reshape(blocks, BLK, KV, ratio), log_total, segment_blocks, position_blocks))
        query_grad = rotate_back(query_grad.reshape(LEN, H, HD), cosine, sine).reshape(LEN, H * HD).astype(jnp.bfloat16)
        key_grad = rotate_back(key_acc, cosine, sine).reshape(LEN, KV * HD).astype(jnp.bfloat16)
        value_grad = value_acc.reshape(LEN, KV * HD).astype(jnp.bfloat16)
        normed_one_grad = jnp.dot(query_grad, query_weight.T, preferred_element_type=jnp.float32)
        normed_one_grad = normed_one_grad + jnp.dot(key_grad, key_weight.T, preferred_element_type=jnp.float32)
        normed_one_grad = normed_one_grad + jnp.dot(value_grad, value_weight.T, preferred_element_type=jnp.float32)
        grad_input_norm, gain_one_term = norm_backward(inputs, inverse_one, attention_gain, normed_one_grad)
        input_grad = grad_residual + grad_input_norm
        query_term = jnp.dot(normed_one.T, query_grad, preferred_element_type=jnp.float32)
        key_term = jnp.dot(normed_one.T, key_grad, preferred_element_type=jnp.float32)
        value_term = jnp.dot(normed_one.T, value_grad, preferred_element_type=jnp.float32)
        router_sum, gate_sum, up_sum, down_sum = expert_sums
        terms = (gain_one_term, query_term, key_term, value_term, output_term, gain_two_term, router_sum, gate_sum, up_sum, down_sum)
        totals = tuple((total + term for total, term in zip(totals, terms)))
        return (totals, (block_out, input_grad))
    init = (jnp.zeros((D,), jnp.float32), jnp.zeros((D, H * HD), jnp.float32), jnp.zeros((D, KV * HD), jnp.float32), jnp.zeros((D, KV * HD), jnp.float32), jnp.zeros((D, H * HD), jnp.float32), jnp.zeros((D,), jnp.float32), jnp.zeros((D, E), jnp.float32), jnp.zeros((E, D, FF), jnp.float32), jnp.zeros((E, D, FF), jnp.float32), jnp.zeros((E, D, FF), jnp.float32))
    totals, (block_out, input_grad) = lax.scan(per_row, init, (hidden_in, out_grad, doc_lengths, expert_choice))
    return (block_out, input_grad, totals[0], totals[1], totals[2], totals[3], totals[4], totals[5], totals[6], totals[7], totals[8], totals[9])
```

```python
import functools

import jax
import jax.numpy as jnp
from jax import lax
from jax.experimental import pallas as pl
from jax.experimental.pallas import tpu as pltpu
from jax.sharding import PartitionSpec as P

HD = 64


epsilon = 1e-05
rope_base = 10000.0
masked_score = -1e30
highest = lax.Precision.HIGHEST


def doc_layout(lengths, positions):
    ends = jnp.cumsum(lengths)
    after = (positions[:, None] >= ends[None, :]).astype(jnp.int32)
    segment = jnp.sum(after, axis=1)
    offset = positions - jnp.sum(after * lengths[None, :], axis=1)
    return (segment, offset)


def rope_tables(offset):
    halfway = HD // 2
    frequency = rope_base ** (-jnp.arange(halfway, dtype=jnp.float32) / halfway)
    angle = offset.astype(jnp.float32)[:, None] * frequency[None, :]
    return (jnp.cos(angle), jnp.sin(angle))


def rotate(vectors, cosine, sine):
    halfway = vectors.shape[-1] // 2
    former = vectors[..., :halfway]
    latter = vectors[..., halfway:]
    cosine = cosine[:, None, :]
    sine = sine[:, None, :]
    return jnp.concatenate(
        [former * cosine - latter * sine, latter * cosine + former * sine], axis=-1
    )


def rotate_back(grads, cosine, sine):
    halfway = grads.shape[-1] // 2
    former = grads[..., :halfway]
    latter = grads[..., halfway:]
    cosine = cosine[:, None, :]
    sine = sine[:, None, :]
    return jnp.concatenate(
        [former * cosine + latter * sine, latter * cosine - former * sine], axis=-1
    )


def norm_forward(values, gain):
    inverse = lax.rsqrt(jnp.mean(values * values, axis=-1, keepdims=True) + epsilon)
    return (values * inverse * gain.astype(jnp.float32), inverse)


def norm_backward(values, inverse, gain, grad_normed):
    scaled = grad_normed * gain.astype(jnp.float32)
    grad_values = inverse * scaled - values * inverse**3 * jnp.mean(
        scaled * values, axis=-1, keepdims=True
    )
    grad_gain = jnp.sum(grad_normed * values * inverse, axis=0)
    return (grad_values, grad_gain)


def dispatch(route, experts, capacity):
    flat = route.reshape(-1)
    onehot = (flat[:, None] == jnp.arange(experts, dtype=jnp.int32)[None, :]).astype(jnp.int32)
    rank = jnp.sum((jnp.cumsum(onehot, axis=0) - onehot) * onehot, axis=1)
    slot = flat * capacity + rank
    pairs = flat.shape[0]
    owner = (
        jnp.zeros((experts * capacity,), jnp.int32).at[slot].set(jnp.arange(pairs, dtype=jnp.int32))
    )
    filled = jnp.zeros((experts * capacity,), jnp.int32).at[slot].set(1) > 0
    return (slot, owner, filled)


def expert_math(slot_inputs, slot_grads, gate_full, up_full, down_full):
    gate_pre = jnp.einsum(
        "gsd,gdf->gsf", slot_inputs, gate_full, preferred_element_type=jnp.float32
    )
    up_pre = jnp.einsum("gsd,gdf->gsf", slot_inputs, up_full, preferred_element_type=jnp.float32)
    sigmoid = jax.nn.sigmoid(gate_pre)
    activated = (gate_pre * sigmoid * up_pre).astype(jnp.bfloat16)
    expert_out = jnp.einsum(
        "gsf,gdf->gsd", activated, down_full, preferred_element_type=jnp.float32
    )
    act_grad = jnp.einsum("gsd,gdf->gsf", slot_grads, down_full, preferred_element_type=jnp.float32)
    gate_pre_grad = (act_grad * up_pre * sigmoid * (1.0 + gate_pre * (1.0 - sigmoid))).astype(
        jnp.bfloat16
    )
    up_pre_grad = (act_grad * gate_pre * sigmoid).astype(jnp.bfloat16)
    down_term = jnp.einsum(
        "gsd,gsf->gdf", slot_grads, activated, preferred_element_type=jnp.float32
    )
    gate_term = jnp.einsum(
        "gsd,gsf->gdf", slot_inputs, gate_pre_grad, preferred_element_type=jnp.float32
    )
    up_term = jnp.einsum(
        "gsd,gsf->gdf", slot_inputs, up_pre_grad, preferred_element_type=jnp.float32
    )
    slot_back = jnp.einsum(
        "gsf,gdf->gsd", gate_pre_grad, gate_full, preferred_element_type=jnp.float32
    ) + jnp.einsum("gsf,gdf->gsd", up_pre_grad, up_full, preferred_element_type=jnp.float32)
    return (expert_out, slot_back, gate_term, up_term, down_term)


def local(
    hidden_in,
    out_grad,
    attention_gain,
    query_weight,
    key_weight,
    value_weight,
    output_weight,
    expert_gain,
    router_weight,
    gate_weight,
    up_weight,
    down_weight,
    doc_lengths,
    expert_choice,
):
    block = hidden_in.shape[1]
    experts = gate_weight.shape[0]
    capacity = block * 3 // 4
    chosen_count = expert_choice.shape[2]
    context_count = lax.axis_size("ctx")
    scale = HD ** (-0.5)
    position = lax.axis_index("ctx") * block + jnp.arange(block, dtype=jnp.int32)
    lengths = doc_lengths[0]
    segment, offset = doc_layout(lengths, position)
    cosine, sine = rope_tables(offset)
    gain_one, query_full, key_full, value_full, output_full, gain_two, router_full = (
        lax.all_gather(attention_gain, ("fsdp", "ctx"), axis=0, tiled=True),
        lax.all_gather(query_weight, ("fsdp", "ctx"), axis=0, tiled=True),
        lax.all_gather(key_weight, ("fsdp", "ctx"), axis=0, tiled=True),
        lax.all_gather(value_weight, ("fsdp", "ctx"), axis=0, tiled=True),
        lax.all_gather(output_weight, ("fsdp", "ctx"), axis=0, tiled=True),
        lax.all_gather(expert_gain, ("fsdp", "ctx"), axis=0, tiled=True),
        lax.all_gather(router_weight, ("fsdp", "ctx"), axis=0, tiled=True),
    )
    inputs = hidden_in[0].astype(jnp.float32)
    normed_one, inverse_one = norm_forward(inputs, gain_one)
    normed_one = normed_one.astype(jnp.bfloat16)
    heads_local = query_full.shape[1] // HD
    groups_local = key_full.shape[1] // HD
    ratio = heads_local // groups_local
    query = rotate(
        jnp.dot(normed_one, query_full, preferred_element_type=jnp.float32).reshape(
            block, heads_local, HD
        ),
        cosine,
        sine,
    ).astype(jnp.bfloat16)
    keys = rotate(
        jnp.dot(normed_one, key_full, preferred_element_type=jnp.float32).reshape(
            block, groups_local, HD
        ),
        cosine,
        sine,
    ).astype(jnp.bfloat16)
    values = jnp.dot(normed_one, value_full, preferred_element_type=jnp.float32).astype(
        jnp.bfloat16
    )
    query_grouped = query.reshape(block, groups_local, ratio, HD)

    def allowed_mask(key_start, count):
        key_position = key_start + jnp.arange(count, dtype=jnp.int32)
        key_segment, unused = doc_layout(lengths, key_position)
        return (segment[:, None] == key_segment[None, :]) & (
            key_position[None, :] <= position[:, None]
        )

    def forward_update(state, key_block, value_block, allowed):
        peak, total, accum = state
        mask = allowed[:, None, None, :]
        scores = (
            jnp.einsum(
                "qgrd,kgd->qgrk", query_grouped, key_block, preferred_element_type=jnp.float32
            )
            * scale
        )
        scores = jnp.where(mask, scores, masked_score)
        new_peak = jnp.maximum(peak, jnp.max(scores, axis=3))
        weights = jnp.where(mask, jnp.exp(scores - new_peak[..., None]), 0.0)
        rescale = jnp.exp(peak - new_peak)
        total = total * rescale + jnp.sum(weights, axis=3)
        accum = accum * rescale[..., None] + jnp.einsum(
            "qgrk,kgd->qgrd", weights, value_block.astype(jnp.float32), precision=highest
        )
        return (new_peak, total, accum)

    travel = (keys.reshape(block, groups_local * HD), values)
    initial = (
        jnp.full((block, groups_local, ratio), masked_score, jnp.float32),
        jnp.zeros((block, groups_local, ratio), jnp.float32),
        jnp.zeros((block, groups_local, ratio, HD), jnp.float32),
    )
    state = initial
    key_piece = lax.all_gather(travel[0], "ctx", axis=0, tiled=True)
    value_piece = lax.all_gather(travel[1], "ctx", axis=0, tiled=True)
    pieces = key_piece.shape[0] // block
    key_blocks = key_piece.reshape(pieces, block, groups_local, HD)
    value_blocks = value_piece.reshape(pieces, block, groups_local, HD)
    starts = block * jnp.arange(pieces, dtype=jnp.int32)

    def visit(carry, item):
        key_block, value_block, key_start = item
        allowed = allowed_mask(key_start, block)
        return (forward_update(carry, key_block, value_block, allowed), None)

    state, unused = lax.scan(visit, state, (key_blocks, value_blocks, starts))
    peak, total, accum = state
    attended = (accum / total[..., None]).reshape(block, heads_local * HD).astype(jnp.bfloat16)
    log_total = peak + jnp.log(total)
    projected = lax.psum(jnp.dot(attended, output_full.T, preferred_element_type=jnp.float32), "tp")
    residual = inputs + projected
    normed_two, inverse_two = norm_forward(residual, gain_two)
    normed_two = normed_two.astype(jnp.bfloat16)
    route = expert_choice[0]
    logits = jnp.dot(normed_two, router_full, preferred_element_type=jnp.float32)
    gates = jax.nn.softmax(jnp.take_along_axis(logits, route, axis=1), axis=1)
    slot, owner, filled = dispatch(route, experts, capacity)
    token_of = owner // chosen_count
    grad_out = out_grad[0].astype(jnp.float32)
    slot_inputs = jnp.where(filled[:, None], normed_two[token_of], 0).reshape(experts, capacity, -1)
    slot_gate = jnp.where(filled, gates.reshape(-1)[owner], 0.0)
    slot_grads = (
        (grad_out[token_of] * slot_gate[:, None])
        .astype(jnp.bfloat16)
        .reshape(experts, capacity, -1)
    )
    gate_full, up_full, down_full = (
        lax.all_gather(gate_weight, ("fsdp", "ctx"), axis=1, tiled=True),
        lax.all_gather(up_weight, ("fsdp", "ctx"), axis=1, tiled=True),
        lax.all_gather(down_weight, ("fsdp", "ctx"), axis=1, tiled=True),
    )
    expert_out, slot_back, gate_term, up_term, down_term = expert_math(
        slot_inputs, slot_grads, gate_full, up_full, down_full
    )
    gate_share, up_share, down_share = (
        lax.psum_scatter(gate_term, ("fsdp", "ctx"), scatter_dimension=1, tiled=True),
        lax.psum_scatter(up_term, ("fsdp", "ctx"), scatter_dimension=1, tiled=True),
        lax.psum_scatter(down_term, ("fsdp", "ctx"), scatter_dimension=1, tiled=True),
    )
    pair_out = expert_out.reshape(experts * capacity, -1)[slot].reshape(block, chosen_count, -1)
    pair_back = slot_back.reshape(experts * capacity, -1)[slot].reshape(block, chosen_count, -1)
    mixed_part = jnp.sum(gates[..., None] * pair_out, axis=1)
    gate_dot_part = jnp.sum(pair_out * grad_out[:, None, :], axis=2)
    moe_part = jnp.sum(pair_back, axis=1)
    mixed, gate_dot, moe_input = (
        lax.psum(mixed_part.astype(jnp.bfloat16), "tp").astype(jnp.float32),
        lax.psum(gate_dot_part.astype(jnp.bfloat16), "tp").astype(jnp.float32),
        lax.psum(moe_part.astype(jnp.bfloat16), "tp").astype(jnp.float32),
    )
    block_out = (residual + mixed).astype(jnp.bfloat16)[None]
    chosen_grad = gates * (gate_dot - jnp.sum(gates * gate_dot, axis=1, keepdims=True))
    picked = (route[..., None] == jnp.arange(experts, dtype=jnp.int32)[None, None, :]).astype(
        jnp.float32
    )
    logit_grad = jnp.sum(picked * chosen_grad[..., None], axis=1)
    router_term = jnp.dot(normed_two.astype(jnp.float32).T, logit_grad, precision=highest)
    router_input = jnp.dot(logit_grad, router_full.astype(jnp.float32).T, precision=highest)
    grad_residual_norm, gain_two_term = norm_backward(
        residual, inverse_two, gain_two, moe_input + router_input
    )
    grad_residual = grad_out + grad_residual_norm
    residual_low = grad_residual.astype(jnp.bfloat16)
    attended_grad = jnp.dot(residual_low, output_full, preferred_element_type=jnp.float32).astype(
        jnp.bfloat16
    )
    output_term = jnp.dot(residual_low.T, attended, preferred_element_type=jnp.float32)
    delta = jnp.sum(
        (attended_grad.astype(jnp.float32) * attended.astype(jnp.float32)).reshape(
            block, groups_local, ratio, HD
        ),
        axis=3,
    )
    grad_grouped = attended_grad.reshape(block, groups_local, ratio, HD)
    back_keys, back_values = (
        lax.all_gather(travel[0], "ctx", axis=0, tiled=True),
        lax.all_gather(travel[1], "ctx", axis=0, tiled=True),
    )
    key_blocks = back_keys.reshape(context_count, block, groups_local, HD)
    value_blocks = back_values.reshape(context_count, block, groups_local, HD)
    starts = block * jnp.arange(context_count, dtype=jnp.int32)

    def backward_update(grad_query, key_block, value_block, allowed):
        mask = allowed[:, None, None, :]
        scores = (
            jnp.einsum(
                "qgrd,kgd->qgrk", query_grouped, key_block, preferred_element_type=jnp.float32
            )
            * scale
        )
        probs = jnp.where(mask, jnp.exp(scores - log_total[..., None]), 0.0)
        value_grad = jnp.einsum(
            "qgrk,qgrd->kgd",
            probs.astype(jnp.bfloat16),
            grad_grouped,
            preferred_element_type=jnp.float32,
        )
        prob_grad = jnp.einsum(
            "qgrd,kgd->qgrk", grad_grouped, value_block, preferred_element_type=jnp.float32
        )
        score_grad = (probs * (prob_grad - delta[..., None]) * scale).astype(jnp.bfloat16)
        grad_query = grad_query + jnp.einsum(
            "qgrk,kgd->qgrd", score_grad, key_block, preferred_element_type=jnp.float32
        )
        key_grad = jnp.einsum(
            "qgrk,qgrd->kgd", score_grad, query_grouped, preferred_element_type=jnp.float32
        )
        return (grad_query, key_grad.reshape(block, -1), value_grad.reshape(block, -1))

    def backward_visit(grad_query, item):
        key_block, value_block, key_start = item
        allowed = allowed_mask(key_start, block)
        grad_query, key_grad, value_grad = backward_update(
            grad_query, key_block, value_block, allowed
        )
        return (grad_query, (key_grad, value_grad))

    grad_query, (key_grads, value_grads) = lax.scan(
        backward_visit,
        jnp.zeros((block, groups_local, ratio, HD), jnp.float32),
        (key_blocks, value_blocks, starts),
    )
    own_key_grad, own_value_grad = (
        lax.psum_scatter(
            key_grads.reshape(context_count * block, -1).astype(jnp.bfloat16),
            "ctx",
            scatter_dimension=0,
            tiled=True,
        ).astype(jnp.float32),
        lax.psum_scatter(
            value_grads.reshape(context_count * block, -1).astype(jnp.bfloat16),
            "ctx",
            scatter_dimension=0,
            tiled=True,
        ).astype(jnp.float32),
    )
    query_grad = (
        rotate_back(grad_query.reshape(block, heads_local, HD), cosine, sine)
        .reshape(block, -1)
        .astype(jnp.bfloat16)
    )
    key_grad = (
        rotate_back(own_key_grad.reshape(block, groups_local, HD), cosine, sine)
        .reshape(block, -1)
        .astype(jnp.bfloat16)
    )
    value_grad = own_value_grad.astype(jnp.bfloat16)
    input_part = jnp.dot(query_grad, query_full.T, preferred_element_type=jnp.float32)
    input_part = input_part + jnp.dot(key_grad, key_full.T, preferred_element_type=jnp.float32)
    input_part = input_part + jnp.dot(value_grad, value_full.T, preferred_element_type=jnp.float32)
    normed_one_grad = lax.psum(input_part.astype(jnp.bfloat16), "tp").astype(jnp.float32)
    grad_input_norm, gain_one_term = norm_backward(inputs, inverse_one, gain_one, normed_one_grad)
    input_grad = (grad_residual + grad_input_norm)[None]
    query_term = jnp.dot(normed_one.T, query_grad, preferred_element_type=jnp.float32)
    key_term = jnp.dot(normed_one.T, key_grad, preferred_element_type=jnp.float32)
    value_term = jnp.dot(normed_one.T, value_grad, preferred_element_type=jnp.float32)
    (
        gain_one_share,
        query_share,
        key_share,
        value_share,
        output_share,
        gain_two_share,
        router_share,
    ) = (
        lax.psum_scatter(gain_one_term, ("fsdp", "ctx"), scatter_dimension=0, tiled=True),
        lax.psum_scatter(query_term, ("fsdp", "ctx"), scatter_dimension=0, tiled=True),
        lax.psum_scatter(key_term, ("fsdp", "ctx"), scatter_dimension=0, tiled=True),
        lax.psum_scatter(value_term, ("fsdp", "ctx"), scatter_dimension=0, tiled=True),
        lax.psum_scatter(output_term, ("fsdp", "ctx"), scatter_dimension=0, tiled=True),
        lax.psum_scatter(gain_two_term, ("fsdp", "ctx"), scatter_dimension=0, tiled=True),
        lax.psum_scatter(router_term, ("fsdp", "ctx"), scatter_dimension=0, tiled=True),
    )
    return (
        block_out,
        input_grad,
        gain_one_share,
        query_share,
        key_share,
        value_share,
        output_share,
        gain_two_share,
        router_share,
        gate_share,
        up_share,
        down_share,
    )


MESH = pl.DeviceIdType.MESH
f32 = jnp.float32
bf16 = jnp.bfloat16


def dot_nn(a, b, precision=None):
    return lax.dot_general(a, b, (((1,), (0,)), ((), ())), precision=precision, preferred_element_type=f32)


def dot_nt(a, b, precision=None):
    return lax.dot_general(a, b, (((1,), (1,)), ((), ())), precision=precision, preferred_element_type=f32)


def dot_tn(a, b, precision=None):
    return lax.dot_general(a, b, (((0,), (0,)), ((), ())), precision=precision, preferred_element_type=f32)


class Net:
    def __init__(self, send_sems, recv_sems):
        self.send_sems, self.recv_sems, self.copies = send_sems, recv_sems, []

    def send(self, source, target, device):
        at = len(self.copies)
        copy = pltpu.make_async_remote_copy(
            src_ref=source,
            dst_ref=target,
            send_sem=self.send_sems.at[at],
            recv_sem=self.recv_sems.at[at],
            device_id=device,
            device_id_type=MESH,
        )
        copy.start()
        self.copies.append(copy)
        return copy

    def drain(self):
        for copy in self.copies:
            copy.wait_send()


def layer_kernel(
    dims,
    x_ref, g_ref, wp_ref, sm_ref, wo_ref, wg_ref, wu_ref, wd_ref, dl_ref, ec_ref, fr_ref,
    block_out, input_grad, small_out, gain_out, dqkv_out, dwo_out, dgu_out, dd_out,
    X, WQ, WO, SMB, SMW, N1, CT, ST, SEGC, POSC, Q, K, V, PSC, ATT, AT, PP, PR, RES,
    N2, GTB, GA, WGU, WD, AA, PSX, GC, H, UG, PRD, MP, MR, BP, BR, DGU, DDT, GDS, GD,
    RB, RM, TB, RB2, TM, RM2, BOWN, MOWN, DGB, GUL, DDB, DDL, SG, RSG, GRES, RL,
    AGS, AGR, DWO, RWO, ZWO, LWO, DS, DQ, DQKV, NG, NR, NZ, DWQ, RWQ, ZWQ, LWQ,
    SG1, RSG1, EXB, EXG,
    send_sems, recv_sems, local_sems,
):
    nf, nz, hb, width, experts, half_ff, ndoc, chosen = dims
    rows = 2 * nz * hb
    half = nz * hb
    block = 2 * hb
    f, z, c = lax.axis_index("fsdp"), lax.axis_index("ctx"), lax.axis_index("tp")
    other = 1 - c
    own = f * nz + z
    net = Net(send_sems, recv_sems)
    device = lambda df, dz, core: {"fsdp": df, "ctx": dz, "tp": core}
    partner = device(f, z, other)
    zs = [lax.rem(z + k, nz) for k in range(nz)]
    zback = [lax.rem(z + nz - k, nz) for k in range(nz)]
    fs = [lax.rem(f + k, nf) for k in range(nf)]
    fback = [lax.rem(f + nf - k, nf) for k in range(nf)]
    everyone = [(i, j, k) for k in range(2) for i in range(nf) for j in range(nz) if (i, j, k) != (0, 0, 0)]
    others = [device(fs[i], zs[j], lax.rem(c + k, 2)) for i, j, k in everyone]
    mine = pl.ds(pl.multiple_of(c * hb, hb), hb)
    yours = pl.ds(pl.multiple_of(other * hb, hb), hb)

    barrier = pltpu.get_barrier_semaphore()
    for peer in others:
        pl.semaphore_signal(barrier, inc=1, device_id=peer, device_id_type=MESH)
    pl.semaphore_wait(barrier, len(others))

    sends_x = [net.send(x_ref.at[mine], X.at[c, z], device(f, zs[k], c)) for k in range(1, nz)]
    sends_q = [net.send(wp_ref.at[zs[k]], WQ.at[f, z], device(f, zs[k], c)) for k in range(1, nz)]
    sends_s = [
        net.send(sm_ref, SMB.at[f, z], device(fs[i], zs[j], c))
        for i in range(nf) for j in range(nz) if (i, j) != (0, 0)
    ]
    X[0, z] = x_ref[0:hb]
    X[1, z] = x_ref[hb:block]
    WQ[f, z] = wp_ref[z]
    SMB[f, z] = sm_ref[...]
    sends_o = [net.send(wo_ref, WO.at[f, z], device(f, zs[k], c)) for k in range(1, nz)]
    WO[f, z] = wo_ref[...]
    sends_g = [net.send(g_ref.at[mine], GA.at[f, c, z], device(f, zs[k], c)) for k in range(1, nz)]
    GA[f, 0, z] = g_ref[0:hb]
    GA[f, 1, z] = g_ref[hb:block]

    def places(shape, dim):
        at = lax.broadcasted_iota(jnp.int32, shape, dim)
        core_at, rest = lax.div(at, half), lax.rem(at, half)
        return lax.div(rest, hb) * block + core_at * hb + lax.rem(rest, hb)

    def layout(position):
        segment = jnp.zeros_like(position)
        start = jnp.zeros_like(position)
        end = jnp.int32(0)
        for i in range(ndoc):
            length = dl_ref[0, i]
            end = end + length
            after = jnp.where(position >= end, 1, 0)
            segment = segment + after
            start = start + after * length
        return segment, position - start

    pos_col = places((rows, 1), 0)
    seg_col, offset = layout(pos_col)
    POSC[...] = pos_col
    SEGC[...] = seg_col
    angle = offset.astype(f32) * fr_ref[0:1, :]
    lane = lax.broadcasted_iota(jnp.int32, (1, 2 * HD), 1)
    former = lax.rem(lane, HD) < HD // 2
    CT[...] = jnp.cos(angle)
    ST[...] = jnp.where(former, -1.0, 1.0) * jnp.sin(angle)
    pos_row = places((1, rows), 1)
    seg_row, unused = layout(pos_row)
    is_key = lane < HD

    def swapped(v):
        return jnp.where(former, pltpu.roll(v, 2 * HD - HD // 2, 1), pltpu.roll(v, HD // 2, 1))

    for k in range(1, nz):
        sends_q[k - 1].wait_recv()
    sends_q2 = [net.send(WQ.at[f], WQ.at[f], device(fs[k], z, c)) for k in range(1, nf)]
    forwards_x = []
    for k in range(1, nz):
        sends_x[k - 1].wait_recv()
        forwards_x.append(net.send(X.at[c, zback[k]], X.at[c, zback[k]], partner))

    sends_e = []
    for i in range(nf):
        for j in range(nz):
            if (i, j) != (0, 0):
                e = fs[i] * nz + zs[j]
                to = device(fs[i], zs[j], c)
                sends_e.append(net.send(wg_ref.at[e], WGU.at[own, :, pl.ds(0, half_ff)], to))
                sends_e.append(net.send(wu_ref.at[e], WGU.at[own, :, pl.ds(half_ff, half_ff)], to))
                sends_e.append(net.send(wd_ref.at[e], WD.at[own], to))
    locals_e = [
        pltpu.make_async_copy(wg_ref.at[own], WGU.at[own, :, pl.ds(0, half_ff)], local_sems.at[0]),
        pltpu.make_async_copy(wu_ref.at[own], WGU.at[own, :, pl.ds(half_ff, half_ff)], local_sems.at[1]),
        pltpu.make_async_copy(wd_ref.at[own], WD.at[own], local_sems.at[2]),
    ]
    for copy in locals_e:
        copy.start()

    for copy in sends_s:
        copy.wait_recv()
    for pair in range(nf * nz // 2):
        at_f, at_z = pair // (nz // 2), 2 * (pair % (nz // 2))
        SMW[:, 128 * pair : 128 * pair + 128] = SMB[at_f, at_z] + SMB[at_f, at_z + 1]
    gain_one = SMW[0:1, :].astype(f32)
    gain_two = SMW[1:2, :].astype(f32)

    for copy in sends_o:
        copy.wait_recv()
    sends_o2 = [net.send(WO.at[f], WO.at[f], device(fs[k], z, c)) for k in range(1, nf)]

    for copy in forwards_x:
        copy.wait_recv()

    def norm_chunk(i, carry):
        at_c, at_z = lax.div(i, nz), lax.rem(i, nz)
        v = X[at_c, at_z].astype(f32)
        inverse = lax.rsqrt(jnp.mean(v * v, axis=1, keepdims=True) + epsilon)
        N1[pl.ds(pl.multiple_of(i * hb, hb), hb), :] = (v * inverse * SMW[0:1, :].astype(f32)).astype(bf16)
        return carry

    lax.fori_loop(0, 2 * nz, norm_chunk, 0)
    for copy in sends_q2:
        copy.wait_recv()
    wq_full = WQ[...].reshape(width, 4 * HD)
    projected = dot_nn(N1[...], wq_full)
    cosine, sine = CT[...], ST[...]
    q_part, kv_part = projected[:, : 2 * HD], projected[:, 2 * HD :]
    Q[...] = (q_part * cosine + swapped(q_part) * sine).astype(bf16)
    kv = jnp.where(is_key, kv_part * cosine + swapped(kv_part) * sine, kv_part).astype(bf16)
    K[...] = kv[:, :HD]
    V[...] = kv[:, HD:]

    scale = HD ** (-0.5)
    step = 2 * hb

    def attend(i, carry):
        at = pl.ds(pl.multiple_of(i * step, step), step)
        mask = (SEGC[at, :] == seg_row) & (pos_row <= POSC[at, :])
        q = Q[at, :]
        pieces = []
        for r in range(2):
            scores = dot_nt(q[:, r * HD : (r + 1) * HD], K[...]) * scale
            scores = jnp.where(mask, scores, masked_score)
            peak = jnp.max(scores, axis=1, keepdims=True)
            weights = jnp.where(mask, jnp.exp(scores - peak), 0.0)
            total = jnp.sum(weights, axis=1, keepdims=True)
            pieces.append(dot_nn(weights.astype(bf16), V[...]) / total)
            PSC[r, at, :] = weights / total
        out = jnp.concatenate(pieces, axis=1).astype(bf16)
        at_c, at_z = lax.div(2 * i, nz), lax.rem(2 * i, nz)
        ATT[at_c, pl.ds(at_z, 2)] = out.reshape(2, hb, 2 * HD)
        return carry

    lax.fori_loop(0, rows // step, attend, 0)
    columns = pl.ds(pl.multiple_of(z * 2 * HD, 2 * HD), 2 * HD)
    sends_a = [
        net.send(ATT.at[:, zs[k]], AT.at[:, :, columns], device(f, zs[k], c)) for k in range(1, nz)
    ]
    AT[:, :, columns] = ATT[:, z]

    for copy in sends_g:
        copy.wait_recv()
    sends_g2 = [net.send(GA.at[f, c], GA.at[f, c], device(fs[k], z, c)) for k in range(1, nf)]
    forwards_g = [net.send(GA.at[f, c, zback[k]], GA.at[f, c, zback[k]], partner) for k in range(1, nz)]

    for copy in sends_o2:
        copy.wait_recv()
    for copy in sends_a:
        copy.wait_recv()
    part = dot_nt(AT[...].reshape(block, nz * 2 * HD), WO[...].reshape(width, nz * 2 * HD))
    PP[...] = part.reshape(2, hb, width)
    send_p = net.send(PP.at[other], PR, partner)
    x_own = x_ref[mine, :].astype(f32)
    send_p.wait_recv()
    residual = x_own + PP[c] + PR[...]
    RES[...] = residual
    inverse_two = lax.rsqrt(jnp.mean(residual * residual, axis=1, keepdims=True) + epsilon)
    N2[f, c, z] = (residual * inverse_two * gain_two).astype(bf16)
    sends_n = [net.send(N2.at[f, c, z], N2.at[f, c, z], device(f, zs[k], c)) for k in range(1, nz)]
    normed_two = N2[f, c, z]
    logits = dot_nt(SMW[16 : 16 + experts, :], normed_two)
    expert_at = lax.broadcasted_iota(jnp.int32, (experts, hb), 0)
    picked = jnp.zeros((experts, hb), jnp.bool_)
    for j in range(chosen):
        picked = picked | (ec_ref[j : j + 1, 0:hb] == expert_at)
    peak = jnp.max(jnp.where(picked, logits, masked_score), axis=0, keepdims=True)
    weight = jnp.where(picked, jnp.exp(logits - peak), 0.0)
    gates = weight / jnp.sum(weight, axis=0, keepdims=True)
    GTB[f, c, z] = jnp.concatenate([gates, jnp.zeros((experts, 128 - hb), f32)], axis=1)
    sends_t = [
        net.send(GTB.at[f, c, z], GTB.at[f, c, z], device(fs[i], zs[j], lax.rem(c + k, 2)))
        for i, j, k in everyone
    ]

    for copy in locals_e:
        copy.wait()
    for copy in sends_e:
        copy.wait_recv()
    for copy in forwards_g:
        copy.wait_recv()
    wd_full = lambda: WD[...].reshape(width, half_ff)
    wgu_full = lambda: WGU[...].reshape(width, 2 * half_ff)
    AA[f] = dot_nn(GA[f].reshape(rows, width), wd_full())

    for copy in sends_n:
        copy.wait_recv()
    sends_n2 = [net.send(N2.at[f, c], N2.at[f, c], device(fs[k], z, c)) for k in range(1, nf)]
    forwards_n = [net.send(N2.at[f, c], N2.at[f, c], partner)]
    forwards_g2 = []
    for k in range(1, nf):
        sends_g2[k - 1].wait_recv()
        forwards_g2.append(net.send(GA.at[fback[k], c], GA.at[fback[k], c], partner))
    for copy in sends_t:
        copy.wait_recv()

    chosen_row = jnp.where(
        lax.broadcasted_iota(jnp.int32, (experts, 128), 0) == own, 1.0, 0.0
    ).astype(f32)
    DGU[...] = jnp.zeros_like(DGU)
    DDT[...] = jnp.zeros_like(DDT)
    sends_d, sends_b, sends_m = [], [], []
    exchange_b, exchange_m = [], []

    for k in range(nf):
        at_f = fback[k]
        if k > 0:
            forwards_g2[k - 1].wait_recv()
            AA[at_f] = dot_nn(GA[at_f].reshape(rows, width), wd_full())
            sends_n2[k - 1].wait_recv()
            forwards_n.append(net.send(N2.at[at_f, c], N2.at[at_f, c], partner))
        forwards_n[k].wait_recv()
        tokens = N2[at_f].reshape(rows, width)
        PSX[...] = dot_nn(tokens, wgu_full())
        for piece in range(2 * nz):
            tile = GTB[at_f, piece // nz, piece % nz][:, 0:hb]
            GC[piece * hb : (piece + 1) * hb, :] = dot_tn(tile, chosen_row, lax.Precision.HIGHEST)

        def expert_chunk(i, carry):
            at = pl.ds(pl.multiple_of(i * 32, 32), 32)
            gate_pre = PSX[at, 0:half_ff]
            up_pre = PSX[at, half_ff : 2 * half_ff]
            raw = AA[at_f, at, :]
            gate = GC[at, 0:1]
            sigmoid = jax.nn.sigmoid(gate_pre)
            silu = gate_pre * sigmoid
            act = silu * up_pre
            PRD[at, :] = (act * raw).astype(bf16)
            H[at, :] = (act * gate).astype(bf16)
            grad = raw * gate
            UG[at, 0:half_ff] = (
                grad * up_pre * sigmoid * (1.0 + gate_pre * (1.0 - sigmoid))
            ).astype(bf16)
            UG[at, half_ff : 2 * half_ff] = (grad * silu).astype(bf16)
            return carry

        lax.fori_loop(0, rows // 32, expert_chunk, 0)
        BP[at_f] = dot_nt(UG[...], wgu_full()).astype(bf16).reshape(2, nz, hb, width)
        exchange_b.append(net.send(BP.at[at_f, other], BR.at[at_f], partner))
        GDS[k] = dot_nt(jnp.ones((8, half_ff), bf16), PRD[...])
        for j in range(nz):
            for t in range(2):
                if (k, j, t) != (0, 0, 0):
                    to_z, to_c = zs[j], lax.rem(c + t, 2)
                    lanes = pl.ds(pl.multiple_of((to_c * (nz // 2) + lax.div(to_z, 2)) * 128, 128), 128)
                    sends_d.append(
                        net.send(GDS.at[k, :, lanes], GD.at[f, z, c], device(at_f, to_z, to_c))
                    )
                else:
                    lanes = pl.ds(pl.multiple_of((c * (nz // 2) + lax.div(z, 2)) * 128, 128), 128)
                    GD[f, z, c] = GDS[0, :, lanes]
        MP[at_f] = dot_nt(H[...], wd_full()).astype(bf16).reshape(2, nz, hb, width)
        exchange_m.append(net.send(MP.at[at_f, other], MR.at[at_f], partner))
        exchange_b[k].wait_recv()
        if k == 0:
            BOWN[...] = BP[at_f, c].astype(f32) + BR[at_f].astype(f32)
        else:
            BP[at_f, c] = (BP[at_f, c].astype(f32) + BR[at_f].astype(f32)).astype(bf16)
            sends_b.append(net.send(BP.at[at_f, c], RB.at[f], device(at_f, z, c)))
        DGU[...] += dot_tn(UG[...], tokens)
        DDT[...] += dot_tn(H[...], GA[at_f].reshape(rows, width))
        exchange_m[k].wait_recv()
        if k == 0:
            MOWN[...] = MP[at_f, c].astype(f32) + MR[at_f].astype(f32)
        else:
            MP[at_f, c] = (MP[at_f, c].astype(f32) + MR[at_f].astype(f32)).astype(bf16)
            sends_m.append(net.send(MP.at[at_f, c], RM.at[f], device(at_f, z, c)))

    for k in range(1, nf):
        sends_b[k - 1].wait_recv()
        source = lax.rem(f + k, nf)
        BOWN[...] += RB[source].astype(f32)
    TB[...] = BOWN[...].astype(bf16)
    sends_b2 = [net.send(TB.at[zs[k]], RB2.at[z], device(f, zs[k], c)) for k in range(1, nz)]

    DGB[...] = jnp.transpose(DGU[...]).astype(bf16).reshape(nf, nz, width // (nf * nz), 2 * half_ff)
    DDB[...] = jnp.transpose(DDT[...]).astype(bf16).reshape(nf, nz, width // (nf * nz), half_ff)
    sends_w = []
    for i in range(nf):
        for j in range(nz):
            if (i, j) != (0, 0):
                to = device(fs[i], zs[j], c)
                sends_w.append(net.send(DGB.at[fs[i], zs[j]], GUL.at[own], to))
                sends_w.append(net.send(DDB.at[fs[i], zs[j]], DDL.at[own], to))
    GUL[own] = DGB[f, z]
    DDL[own] = DDB[f, z]

    for copy in sends_d:
        copy.wait_recv()
    dots = jnp.concatenate(
        [
            GD[e // nz, e % nz, 0][0:1, :] + GD[e // nz, e % nz, 1][0:1, :]
            for e in range(experts)
        ],
        axis=0,
    )
    dots = jnp.where(lax.rem(z, 2) == 0, dots, pltpu.roll(dots, 64, 1))[:, 0:hb]
    gates = GTB[f, c, z][:, 0:hb]
    logit_grad = gates * (dots - jnp.sum(gates * dots, axis=0, keepdims=True))
    router_t = SMW[16 : 16 + experts, :].astype(f32)
    router_term = dot_nn(logit_grad, N2[f, c, z].astype(f32), lax.Precision.HIGHEST)
    router_input = dot_tn(logit_grad, router_t, lax.Precision.HIGHEST)
    moe = BOWN[z]
    for k in range(1, nz):
        sends_b2[k - 1].wait_recv()
        moe = moe + RB2[zback[k]].astype(f32)
    grad_two = moe + router_input
    residual = RES[...]
    inverse_two = lax.rsqrt(jnp.mean(residual * residual, axis=1, keepdims=True) + epsilon)
    scaled = grad_two * gain_two
    grad_res = (
        g_ref[mine, :].astype(f32)
        + inverse_two * scaled
        - residual * (inverse_two * inverse_two * inverse_two) * jnp.mean(scaled * residual, axis=1, keepdims=True)
    )
    GRES[...] = grad_res
    RL[c] = grad_res.astype(bf16)
    send_r = net.send(RL.at[c], RL.at[c], partner)
    gain_term = jnp.sum(grad_two * residual * inverse_two, axis=0, keepdims=True)
    SG[0:experts, :] = router_term
    SG[experts : experts + 8, :] = jnp.broadcast_to(gain_term, (8, width))
    sends_sg = []
    for (i, j, k), to in zip(everyone, others):
        lanes = pl.ds(pl.multiple_of((fs[i] * (nz // 2) + lax.div(zs[j], 2)) * 128, 128), 128)
        sends_sg.append(net.send(SG.at[:, lanes], RSG.at[f, z, c], to))
    own_lanes = pl.ds(pl.multiple_of((f * (nz // 2) + lax.div(z, 2)) * 128, 128), 128)
    RSG[f, z, c] = SG[:, own_lanes]
    send_r.wait_recv()
    low = RL[...].reshape(block, width)
    AGS[...] = dot_nn(low, WO[...].reshape(width, nz * 2 * HD)).astype(bf16).reshape(2, hb, nz * 2 * HD)
    sends_ag = [
        net.send(
            AGS.at[:, :, pl.ds(pl.multiple_of(zs[k] * 2 * HD, 2 * HD), 2 * HD)],
            AGR.at[:, z],
            device(f, zs[k], c),
        )
        for k in range(1, nz)
    ]
    AGR[:, z] = AGS[:, :, columns]
    shard = width // (nf * nz)
    DWO[...] = (
        dot_tn(low, AT[...].reshape(block, nz * 2 * HD))
        .astype(bf16)
        .reshape(nf, nz, shard, nz * 2 * HD)
    )
    sends_wo = [net.send(DWO.at[fs[k]], RWO.at[f], device(fs[k], z, c)) for k in range(1, nf)]

    for copy in sends_ag:
        copy.wait_recv()

    def backward(i, carry):
        at = pl.ds(pl.multiple_of(i * step, step), step)
        at_c, at_z = lax.div(2 * i, nz), lax.rem(2 * i, nz)
        grad = AGR[at_c, pl.ds(at_z, 2)].reshape(step, 2 * HD)
        out = ATT[at_c, pl.ds(at_z, 2)].reshape(step, 2 * HD)
        both = grad.astype(f32) * out.astype(f32)
        pieces = []
        for r in range(2):
            delta = jnp.sum(both[:, r * HD : (r + 1) * HD], axis=1, keepdims=True)
            prob_grad = dot_nt(grad[:, r * HD : (r + 1) * HD], V[...])
            probs = PSC[r, at, :]
            score_grad = (probs * (prob_grad - delta) * scale).astype(bf16)
            DS[r, at, :] = score_grad
            pieces.append(dot_nn(score_grad, K[...]))
        DQ[at, :] = jnp.concatenate(pieces, axis=1)
        return carry

    lax.fori_loop(0, rows // step, backward, 0)
    grads = AGR[...].reshape(rows, 2 * HD)
    key_t = dot_tn(Q[:, 0:HD], DS[0]) + dot_tn(Q[:, HD : 2 * HD], DS[1])
    value_t = dot_tn(grads[:, 0:HD], PSC[0].astype(bf16)) + dot_tn(
        grads[:, HD : 2 * HD], PSC[1].astype(bf16)
    )
    kv_grad = jnp.transpose(jnp.concatenate([key_t, value_t], axis=0))
    cosine, sine = CT[...], ST[...]
    q_grad = DQ[...]
    DQKV[:, 0 : 2 * HD] = (q_grad * cosine - swapped(q_grad) * sine).astype(bf16)
    DQKV[:, 2 * HD : 4 * HD] = jnp.where(
        is_key, kv_grad * cosine - swapped(kv_grad) * sine, kv_grad
    ).astype(bf16)
    NG[...] = dot_nt(DQKV[...], WQ[...].reshape(width, 4 * HD)).astype(bf16).reshape(2, nz, hb, width)
    send_ng = net.send(NG.at[other], NR, partner)
    DWQ[...] = (
        jnp.transpose(dot_tn(DQKV[...], N1[...])).astype(bf16).reshape(nf, nz, shard, 4 * HD)
    )
    send_ng.wait_recv()
    NG[c] = (NG[c].astype(f32) + NR[...].astype(f32)).astype(bf16)
    sends_nz = [net.send(NG.at[c, zs[k]], NZ.at[z], device(f, zs[k], c)) for k in range(1, nz)]
    sends_wq = [net.send(DWQ.at[fs[k]], RWQ.at[f], device(fs[k], z, c)) for k in range(1, nf)]

    for k in range(1, nf):
        sends_m[k - 1].wait_recv()
        MOWN[...] += RM[lax.rem(f + k, nf)].astype(f32)
    TM[...] = MOWN[...].astype(bf16)
    sends_m2 = [net.send(TM.at[zs[k]], RM2.at[z], device(f, zs[k], c)) for k in range(1, nz)]

    total = DWO[f].astype(f32)
    for k in range(1, nf):
        sends_wo[k - 1].wait_recv()
        total = total + RWO[fback[k]].astype(f32)
    ZWO[...] = total.astype(bf16)
    sends_wo2 = [net.send(ZWO.at[zs[k]], LWO.at[z], device(f, zs[k], c)) for k in range(1, nz)]
    LWO[z] = ZWO[z]
    total = DWQ[f].astype(f32)
    for k in range(1, nf):
        sends_wq[k - 1].wait_recv()
        total = total + RWQ[fback[k]].astype(f32)
    ZWQ[...] = total.astype(bf16)
    sends_wq2 = [net.send(ZWQ.at[zs[k]], LWQ.at[z], device(f, zs[k], c)) for k in range(1, nz)]
    LWQ[z] = ZWQ[z]

    grad_one = NG[c, z].astype(f32)
    for k in range(1, nz):
        sends_nz[k - 1].wait_recv()
        grad_one = grad_one + NZ[zback[k]].astype(f32)
    x_own = x_ref[mine, :].astype(f32)
    inverse = lax.rsqrt(jnp.mean(x_own * x_own, axis=1, keepdims=True) + epsilon)
    gain_term = jnp.sum(grad_one * x_own * inverse, axis=0, keepdims=True)
    SG1[...] = jnp.broadcast_to(gain_term, (8, width))
    sends_g1 = []
    for (i, j, k), to in zip(everyone, others):
        lanes = pl.ds(pl.multiple_of((fs[i] * (nz // 2) + lax.div(zs[j], 2)) * 128, 128), 128)
        sends_g1.append(net.send(SG1.at[:, lanes], RSG1.at[f, z, c], to))
    RSG1[f, z, c] = SG1[:, own_lanes]
    scaled = grad_one * gain_one
    EXG[c] = (
        GRES[...]
        + inverse * scaled
        - x_own * (inverse * inverse * inverse) * jnp.mean(scaled * x_own, axis=1, keepdims=True)
    )
    send_ig = net.send(EXG.at[c], EXG.at[c], partner)

    mixed = MOWN[z]
    for k in range(1, nz):
        sends_m2[k - 1].wait_recv()
        mixed = mixed + RM2[zback[k]].astype(f32)
    EXB[c] = (RES[...] + mixed).astype(bf16)
    send_bo = net.send(EXB.at[c], EXB.at[c], partner)

    for copy in sends_sg:
        copy.wait_recv()
    small = jnp.zeros((experts + 8, 128), f32)
    for i in range(nf):
        for j in range(nz):
            small = small + RSG[i, j, 0] + RSG[i, j, 1]
    small_out[...] = small
    for copy in sends_wo2:
        copy.wait_recv()
    total = LWO[0].astype(f32)
    for j in range(1, nz):
        total = total + LWO[j].astype(f32)
    dwo_out[...] = total
    for copy in sends_wq2:
        copy.wait_recv()
    dqkv_out[...] = LWQ[...]
    for copy in sends_w:
        copy.wait_recv()
    outs = [
        pltpu.make_async_copy(GUL, dgu_out, local_sems.at[3]),
        pltpu.make_async_copy(DDL, dd_out, local_sems.at[4]),
    ]
    for copy in outs:
        copy.start()
    for copy in sends_g1:
        copy.wait_recv()
    small = jnp.zeros((8, 128), f32)
    for i in range(nf):
        for j in range(nz):
            small = small + RSG1[i, j, 0] + RSG1[i, j, 1]
    gain_out[...] = small
    send_bo.wait_recv()
    block_out[...] = EXB[...].reshape(block, width)
    send_ig.wait_recv()
    input_grad[...] = EXG[...].reshape(block, width)
    for copy in outs:
        copy.wait()
    net.drain()


def fast_local(
    nf, nz,
    hidden_in, out_grad, attention_gain, query_weight, key_weight, value_weight, output_weight,
    expert_gain, router_weight, gate_weight, up_weight, down_weight, doc_lengths, expert_choice,
):
    block, width = hidden_in.shape[1], hidden_in.shape[2]
    hb = block // 2
    experts, shard, half_ff = gate_weight.shape
    ndoc, chosen = doc_lengths.shape[1], expert_choice.shape[2]
    rows = nz * block
    z, c = lax.axis_index("ctx"), lax.axis_index("tp")
    packed = jnp.concatenate(
        [
            query_weight.reshape(shard, nz, 2 * HD),
            key_weight.reshape(shard, nz, HD),
            value_weight.reshape(shard, nz, HD),
        ],
        axis=2,
    ).transpose(1, 0, 2)
    base = jnp.concatenate(
        [attention_gain[None], expert_gain[None], jnp.zeros((14, shard), bf16), router_weight.T], axis=0
    )
    blank = jnp.zeros_like(base)
    even = lax.rem(z, 2) == 0
    small = jnp.concatenate([jnp.where(even, base, blank), jnp.where(even, blank, base)], axis=1)
    own_choice = lax.dynamic_slice_in_dim(expert_choice[0], c * hb, hb, axis=0)
    route = jnp.concatenate([own_choice.T, jnp.zeros((chosen, 128 - hb), jnp.int32)], axis=1)
    halfway = HD // 2
    frequency = rope_base ** (-jnp.arange(halfway, dtype=f32) / halfway)
    frequency = jnp.broadcast_to(jnp.tile(frequency, 4)[None], (8, 2 * HD))

    vm = pl.BlockSpec(memory_space=pltpu.VMEM)
    anywhere = pl.BlockSpec(memory_space=pl.ANY)
    shape = lambda s, d: jax.ShapeDtypeStruct(s, d)
    W = nz * 2 * HD
    scratch = dict(
        X=((2, nz, hb, width), bf16), WQ=((nf, nz, shard, 4 * HD), bf16), WO=((nf, nz, shard, W), bf16),
        SMB=((nf, nz, 32, 128), bf16), SMW=((32, width), bf16), N1=((rows, width), bf16),
        CT=((rows, 128), f32), ST=((rows, 128), f32), SEGC=((rows, 1), jnp.int32), POSC=((rows, 1), jnp.int32),
        Q=((rows, 2 * HD), bf16), K=((rows, HD), bf16), V=((rows, HD), bf16), PSC=((2, rows, rows), f32),
        ATT=((2, nz, hb, 2 * HD), bf16), AT=((2, hb, W), bf16), PP=((2, hb, width), f32), PR=((hb, width), f32),
        RES=((hb, width), f32),
        N2=((nf, 2, nz, hb, width), bf16), GTB=((nf, 2, nz, experts, 128), f32), GA=((nf, 2, nz, hb, width), bf16),
        WGU=((nf * nz, shard, 2 * half_ff), bf16), WD=((nf * nz, shard, half_ff), bf16),
        AA=((nf, rows, half_ff), f32), PSX=((rows, 2 * half_ff), f32), GC=((rows, 128), f32),
        H=((rows, half_ff), bf16), UG=((rows, 2 * half_ff), bf16), PRD=((rows, half_ff), bf16),
        MP=((nf, 2, nz, hb, width), bf16), MR=((nf, nz, hb, width), bf16),
        BP=((nf, 2, nz, hb, width), bf16), BR=((nf, nz, hb, width), bf16),
        DGU=((2 * half_ff, width), f32), DDT=((half_ff, width), f32),
        GDS=((nf, 8, rows), f32), GD=((nf, nz, 2, 8, 128), f32),
        RB=((nf, nz, hb, width), bf16),
        RM=((nf, nz, hb, width), bf16),
        TB=((nz, hb, width), bf16), RB2=((nz, hb, width), bf16),
        TM=((nz, hb, width), bf16), RM2=((nz, hb, width), bf16),
        BOWN=((nz, hb, width), f32), MOWN=((nz, hb, width), f32),
        DGB=((nf, nz, shard, 2 * half_ff), bf16), GUL=((nf * nz, shard, 2 * half_ff), bf16),
        DDB=((nf, nz, shard, half_ff), bf16), DDL=((nf * nz, shard, half_ff), bf16),
        SG=((experts + 8, width), f32), RSG=((nf, nz, 2, experts + 8, 128), f32),
        GRES=((hb, width), f32), RL=((2, hb, width), bf16),
        AGS=((2, hb, W), bf16), AGR=((2, nz, hb, 2 * HD), bf16),
        DWO=((nf, nz, shard, W), bf16), RWO=((nf, nz, shard, W), bf16),
        ZWO=((nz, shard, W), bf16), LWO=((nz, shard, W), bf16),
        DS=((2, rows, rows), bf16), DQ=((rows, 2 * HD), f32),
        DQKV=((rows, 4 * HD), bf16), NG=((2, nz, hb, width), bf16), NR=((nz, hb, width), bf16),
        NZ=((nz, hb, width), bf16),
        DWQ=((nf, nz, shard, 4 * HD), bf16), RWQ=((nf, nz, shard, 4 * HD), bf16),
        ZWQ=((nz, shard, 4 * HD), bf16), LWQ=((nz, shard, 4 * HD), bf16),
        SG1=((8, width), f32), RSG1=((nf, nz, 2, 8, 128), f32),
        EXB=((2, hb, width), bf16), EXG=((2, hb, width), f32),
    )
    slots = 400
    out = pl.pallas_call(
        functools.partial(layer_kernel, (nf, nz, hb, width, experts, half_ff, ndoc, chosen)),
        name="layer",
        out_shape=(
            shape((block, width), bf16), shape((block, width), f32), shape((experts + 8, 128), f32),
            shape((8, 128), f32), shape((nz, shard, 4 * HD), bf16), shape((shard, W), f32),
            shape((nf * nz, shard, 2 * half_ff), bf16), shape((nf * nz, shard, half_ff), bf16),
        ),
        in_specs=[vm] * 5 + [anywhere] * 3 + [pl.BlockSpec(memory_space=pltpu.SMEM), vm, vm],
        out_specs=(vm,) * 6 + (anywhere,) * 2,
        scratch_shapes=[pltpu.VMEM(s, d) for s, d in scratch.values()]
        + [pltpu.SemaphoreType.DMA((slots,)), pltpu.SemaphoreType.DMA((slots,)), pltpu.SemaphoreType.DMA((5,))],
        compiler_params=pltpu.CompilerParams(
            collective_id=0, has_side_effects=True, vmem_limit_bytes=67043328
        ),
    )(
        hidden_in[0], out_grad[0], packed, small, output_weight, gate_weight, up_weight, down_weight,
        doc_lengths, route, frequency,
    )
    block_out, input_grad, small, gain, dqkv, dwo, dgu, dd = out
    lanes = lambda v: jnp.where(even, v[:, :shard], v[:, shard:])
    small, gain = lanes(small), lanes(gain)
    dqkv = dqkv.astype(f32)
    return (
        block_out[None],
        input_grad[None],
        gain[0],
        dqkv[:, :, : 2 * HD].transpose(1, 0, 2).reshape(shard, -1),
        dqkv[:, :, 2 * HD : 3 * HD].transpose(1, 0, 2).reshape(shard, -1),
        dqkv[:, :, 3 * HD :].transpose(1, 0, 2).reshape(shard, -1),
        dwo,
        small[experts],
        small[:experts].T,
        dgu[:, :, :half_ff].astype(f32),
        dgu[:, :, half_ff:].astype(f32),
        dd.astype(f32),
    )


def fits(mesh, args):
    nf, nz, nc = mesh.shape["fsdp"], mesh.shape["ctx"], mesh.shape["tp"]
    hidden, query, key, gate = args[0], args[3], args[4], args[9]
    width, block = hidden.shape[2], hidden.shape[1] // nz
    return (
        nc == 2
        and nz % 2 == 0
        and hidden.shape[0] == nf
        and gate.shape[0] == nf * nz
        and gate.shape[0] == 16
        and width == 64 * nf * nz
        and block == 128
        and query.shape[1] == 2 * HD * nz * nc
        and key.shape[1] == HD * nz * nc
        and HD == 64
    )


def solution(mesh):
    in_specs = (
        P("fsdp", "ctx", None),
        P("fsdp", "ctx", None),
        P(("fsdp", "ctx")),
        P(("fsdp", "ctx"), "tp"),
        P(("fsdp", "ctx"), "tp"),
        P(("fsdp", "ctx"), "tp"),
        P(("fsdp", "ctx"), "tp"),
        P(("fsdp", "ctx")),
        P(("fsdp", "ctx"), None),
        P(None, ("fsdp", "ctx"), "tp"),
        P(None, ("fsdp", "ctx"), "tp"),
        P(None, ("fsdp", "ctx"), "tp"),
        P("fsdp", None),
        P("fsdp", "ctx", None),
    )
    out_specs = (
        P("fsdp", "ctx", None),
        P("fsdp", "ctx", None),
        P(("fsdp", "ctx")),
        P(("fsdp", "ctx"), "tp"),
        P(("fsdp", "ctx"), "tp"),
        P(("fsdp", "ctx"), "tp"),
        P(("fsdp", "ctx"), "tp"),
        P(("fsdp", "ctx")),
        P(("fsdp", "ctx"), None),
        P(None, ("fsdp", "ctx"), "tp"),
        P(None, ("fsdp", "ctx"), "tp"),
        P(None, ("fsdp", "ctx"), "tp"),
    )

    def step(*args):
        body = local
        if fits(mesh, args):
            body = functools.partial(fast_local, mesh.shape["fsdp"], mesh.shape["ctx"])
        return jax.shard_map(
            body, mesh=mesh, in_specs=in_specs, out_specs=out_specs, check_vma=False
        )(*args)

    return step
```

```python
import functools

import jax
import jax.numpy as jnp
import numpy as np
from jax import lax
from jax.experimental import pallas as pl
from jax.experimental.pallas import tpu as pltpu
from jax.sharding import PartitionSpec as P

HD = 64


epsilon = 1e-05
rope_base = 10000.0
masked_score = -1e30
highest = lax.Precision.HIGHEST


def doc_layout(lengths, positions):
    ends = jnp.cumsum(lengths)
    after = (positions[:, None] >= ends[None, :]).astype(jnp.int32)
    segment = jnp.sum(after, axis=1)
    offset = positions - jnp.sum(after * lengths[None, :], axis=1)
    return (segment, offset)


def rope_tables(offset):
    halfway = HD // 2
    frequency = rope_base ** (-jnp.arange(halfway, dtype=jnp.float32) / halfway)
    angle = offset.astype(jnp.float32)[:, None] * frequency[None, :]
    return (jnp.cos(angle), jnp.sin(angle))


def rotate(vectors, cosine, sine):
    halfway = vectors.shape[-1] // 2
    former = vectors[..., :halfway]
    latter = vectors[..., halfway:]
    cosine = cosine[:, None, :]
    sine = sine[:, None, :]
    return jnp.concatenate(
        [former * cosine - latter * sine, latter * cosine + former * sine], axis=-1
    )


def rotate_back(grads, cosine, sine):
    halfway = grads.shape[-1] // 2
    former = grads[..., :halfway]
    latter = grads[..., halfway:]
    cosine = cosine[:, None, :]
    sine = sine[:, None, :]
    return jnp.concatenate(
        [former * cosine + latter * sine, latter * cosine - former * sine], axis=-1
    )


def norm_forward(values, gain):
    inverse = lax.rsqrt(jnp.mean(values * values, axis=-1, keepdims=True) + epsilon)
    return (values * inverse * gain.astype(jnp.float32), inverse)


def norm_backward(values, inverse, gain, grad_normed):
    scaled = grad_normed * gain.astype(jnp.float32)
    grad_values = inverse * scaled - values * inverse**3 * jnp.mean(
        scaled * values, axis=-1, keepdims=True
    )
    grad_gain = jnp.sum(grad_normed * values * inverse, axis=0)
    return (grad_values, grad_gain)


def dispatch(route, experts, capacity):
    flat = route.reshape(-1)
    onehot = (flat[:, None] == jnp.arange(experts, dtype=jnp.int32)[None, :]).astype(jnp.int32)
    rank = jnp.sum((jnp.cumsum(onehot, axis=0) - onehot) * onehot, axis=1)
    slot = flat * capacity + rank
    pairs = flat.shape[0]
    owner = (
        jnp.zeros((experts * capacity,), jnp.int32).at[slot].set(jnp.arange(pairs, dtype=jnp.int32))
    )
    filled = jnp.zeros((experts * capacity,), jnp.int32).at[slot].set(1) > 0
    return (slot, owner, filled)


def expert_math(slot_inputs, slot_grads, gate_full, up_full, down_full):
    gate_pre = jnp.einsum(
        "gsd,gdf->gsf", slot_inputs, gate_full, preferred_element_type=jnp.float32
    )
    up_pre = jnp.einsum("gsd,gdf->gsf", slot_inputs, up_full, preferred_element_type=jnp.float32)
    sigmoid = jax.nn.sigmoid(gate_pre)
    activated = (gate_pre * sigmoid * up_pre).astype(jnp.bfloat16)
    expert_out = jnp.einsum(
        "gsf,gdf->gsd", activated, down_full, preferred_element_type=jnp.float32
    )
    act_grad = jnp.einsum("gsd,gdf->gsf", slot_grads, down_full, preferred_element_type=jnp.float32)
    gate_pre_grad = (act_grad * up_pre * sigmoid * (1.0 + gate_pre * (1.0 - sigmoid))).astype(
        jnp.bfloat16
    )
    up_pre_grad = (act_grad * gate_pre * sigmoid).astype(jnp.bfloat16)
    down_term = jnp.einsum(
        "gsd,gsf->gdf", slot_grads, activated, preferred_element_type=jnp.float32
    )
    gate_term = jnp.einsum(
        "gsd,gsf->gdf", slot_inputs, gate_pre_grad, preferred_element_type=jnp.float32
    )
    up_term = jnp.einsum(
        "gsd,gsf->gdf", slot_inputs, up_pre_grad, preferred_element_type=jnp.float32
    )
    slot_back = jnp.einsum(
        "gsf,gdf->gsd", gate_pre_grad, gate_full, preferred_element_type=jnp.float32
    ) + jnp.einsum("gsf,gdf->gsd", up_pre_grad, up_full, preferred_element_type=jnp.float32)
    return (expert_out, slot_back, gate_term, up_term, down_term)


def local(
    hidden_in,
    out_grad,
    attention_gain,
    query_weight,
    key_weight,
    value_weight,
    output_weight,
    expert_gain,
    router_weight,
    gate_weight,
    up_weight,
    down_weight,
    doc_lengths,
    expert_choice,
):
    block = hidden_in.shape[1]
    experts = gate_weight.shape[0]
    capacity = block * 3 // 4
    chosen_count = expert_choice.shape[2]
    context_count = lax.axis_size("ctx")
    scale = HD ** (-0.5)
    position = lax.axis_index("ctx") * block + jnp.arange(block, dtype=jnp.int32)
    lengths = doc_lengths[0]
    segment, offset = doc_layout(lengths, position)
    cosine, sine = rope_tables(offset)
    gain_one, query_full, key_full, value_full, output_full, gain_two, router_full = (
        lax.all_gather(attention_gain, ("fsdp", "ctx"), axis=0, tiled=True),
        lax.all_gather(query_weight, ("fsdp", "ctx"), axis=0, tiled=True),
        lax.all_gather(key_weight, ("fsdp", "ctx"), axis=0, tiled=True),
        lax.all_gather(value_weight, ("fsdp", "ctx"), axis=0, tiled=True),
        lax.all_gather(output_weight, ("fsdp", "ctx"), axis=0, tiled=True),
        lax.all_gather(expert_gain, ("fsdp", "ctx"), axis=0, tiled=True),
        lax.all_gather(router_weight, ("fsdp", "ctx"), axis=0, tiled=True),
    )
    inputs = hidden_in[0].astype(jnp.float32)
    normed_one, inverse_one = norm_forward(inputs, gain_one)
    normed_one = normed_one.astype(jnp.bfloat16)
    heads_local = query_full.shape[1] // HD
    groups_local = key_full.shape[1] // HD
    ratio = heads_local // groups_local
    query = rotate(
        jnp.dot(normed_one, query_full, preferred_element_type=jnp.float32).reshape(
            block, heads_local, HD
        ),
        cosine,
        sine,
    ).astype(jnp.bfloat16)
    keys = rotate(
        jnp.dot(normed_one, key_full, preferred_element_type=jnp.float32).reshape(
            block, groups_local, HD
        ),
        cosine,
        sine,
    ).astype(jnp.bfloat16)
    values = jnp.dot(normed_one, value_full, preferred_element_type=jnp.float32).astype(
        jnp.bfloat16
    )
    query_grouped = query.reshape(block, groups_local, ratio, HD)

    def allowed_mask(key_start, count):
        key_position = key_start + jnp.arange(count, dtype=jnp.int32)
        key_segment, unused = doc_layout(lengths, key_position)
        return (segment[:, None] == key_segment[None, :]) & (
            key_position[None, :] <= position[:, None]
        )

    def forward_update(state, key_block, value_block, allowed):
        peak, total, accum = state
        mask = allowed[:, None, None, :]
        scores = (
            jnp.einsum(
                "qgrd,kgd->qgrk", query_grouped, key_block, preferred_element_type=jnp.float32
            )
            * scale
        )
        scores = jnp.where(mask, scores, masked_score)
        new_peak = jnp.maximum(peak, jnp.max(scores, axis=3))
        weights = jnp.where(mask, jnp.exp(scores - new_peak[..., None]), 0.0)
        rescale = jnp.exp(peak - new_peak)
        total = total * rescale + jnp.sum(weights, axis=3)
        accum = accum * rescale[..., None] + jnp.einsum(
            "qgrk,kgd->qgrd", weights, value_block.astype(jnp.float32), precision=highest
        )
        return (new_peak, total, accum)

    travel = (keys.reshape(block, groups_local * HD), values)
    initial = (
        jnp.full((block, groups_local, ratio), masked_score, jnp.float32),
        jnp.zeros((block, groups_local, ratio), jnp.float32),
        jnp.zeros((block, groups_local, ratio, HD), jnp.float32),
    )
    state = initial
    key_piece = lax.all_gather(travel[0], "ctx", axis=0, tiled=True)
    value_piece = lax.all_gather(travel[1], "ctx", axis=0, tiled=True)
    pieces = key_piece.shape[0] // block
    key_blocks = key_piece.reshape(pieces, block, groups_local, HD)
    value_blocks = value_piece.reshape(pieces, block, groups_local, HD)
    starts = block * jnp.arange(pieces, dtype=jnp.int32)

    def visit(carry, item):
        key_block, value_block, key_start = item
        allowed = allowed_mask(key_start, block)
        return (forward_update(carry, key_block, value_block, allowed), None)

    state, unused = lax.scan(visit, state, (key_blocks, value_blocks, starts))
    peak, total, accum = state
    attended = (accum / total[..., None]).reshape(block, heads_local * HD).astype(jnp.bfloat16)
    log_total = peak + jnp.log(total)
    projected = lax.psum(jnp.dot(attended, output_full.T, preferred_element_type=jnp.float32), "tp")
    residual = inputs + projected
    normed_two, inverse_two = norm_forward(residual, gain_two)
    normed_two = normed_two.astype(jnp.bfloat16)
    route = expert_choice[0]
    logits = jnp.dot(normed_two, router_full, preferred_element_type=jnp.float32)
    gates = jax.nn.softmax(jnp.take_along_axis(logits, route, axis=1), axis=1)
    slot, owner, filled = dispatch(route, experts, capacity)
    token_of = owner // chosen_count
    grad_out = out_grad[0].astype(jnp.float32)
    slot_inputs = jnp.where(filled[:, None], normed_two[token_of], 0).reshape(experts, capacity, -1)
    slot_gate = jnp.where(filled, gates.reshape(-1)[owner], 0.0)
    slot_grads = (
        (grad_out[token_of] * slot_gate[:, None])
        .astype(jnp.bfloat16)
        .reshape(experts, capacity, -1)
    )
    gate_full, up_full, down_full = (
        lax.all_gather(gate_weight, ("fsdp", "ctx"), axis=1, tiled=True),
        lax.all_gather(up_weight, ("fsdp", "ctx"), axis=1, tiled=True),
        lax.all_gather(down_weight, ("fsdp", "ctx"), axis=1, tiled=True),
    )
    expert_out, slot_back, gate_term, up_term, down_term = expert_math(
        slot_inputs, slot_grads, gate_full, up_full, down_full
    )
    gate_share, up_share, down_share = (
        lax.psum_scatter(gate_term, ("fsdp", "ctx"), scatter_dimension=1, tiled=True),
        lax.psum_scatter(up_term, ("fsdp", "ctx"), scatter_dimension=1, tiled=True),
        lax.psum_scatter(down_term, ("fsdp", "ctx"), scatter_dimension=1, tiled=True),
    )
    pair_out = expert_out.reshape(experts * capacity, -1)[slot].reshape(block, chosen_count, -1)
    pair_back = slot_back.reshape(experts * capacity, -1)[slot].reshape(block, chosen_count, -1)
    mixed_part = jnp.sum(gates[..., None] * pair_out, axis=1)
    gate_dot_part = jnp.sum(pair_out * grad_out[:, None, :], axis=2)
    moe_part = jnp.sum(pair_back, axis=1)
    mixed, gate_dot, moe_input = (
        lax.psum(mixed_part.astype(jnp.bfloat16), "tp").astype(jnp.float32),
        lax.psum(gate_dot_part.astype(jnp.bfloat16), "tp").astype(jnp.float32),
        lax.psum(moe_part.astype(jnp.bfloat16), "tp").astype(jnp.float32),
    )
    block_out = (residual + mixed).astype(jnp.bfloat16)[None]
    chosen_grad = gates * (gate_dot - jnp.sum(gates * gate_dot, axis=1, keepdims=True))
    picked = (route[..., None] == jnp.arange(experts, dtype=jnp.int32)[None, None, :]).astype(
        jnp.float32
    )
    logit_grad = jnp.sum(picked * chosen_grad[..., None], axis=1)
    router_term = jnp.dot(normed_two.astype(jnp.float32).T, logit_grad, precision=highest)
    router_input = jnp.dot(logit_grad, router_full.astype(jnp.float32).T, precision=highest)
    grad_residual_norm, gain_two_term = norm_backward(
        residual, inverse_two, gain_two, moe_input + router_input
    )
    grad_residual = grad_out + grad_residual_norm
    residual_low = grad_residual.astype(jnp.bfloat16)
    attended_grad = jnp.dot(residual_low, output_full, preferred_element_type=jnp.float32).astype(
        jnp.bfloat16
    )
    output_term = jnp.dot(residual_low.T, attended, preferred_element_type=jnp.float32)
    delta = jnp.sum(
        (attended_grad.astype(jnp.float32) * attended.astype(jnp.float32)).reshape(
            block, groups_local, ratio, HD
        ),
        axis=3,
    )
    grad_grouped = attended_grad.reshape(block, groups_local, ratio, HD)
    back_keys, back_values = (
        lax.all_gather(travel[0], "ctx", axis=0, tiled=True),
        lax.all_gather(travel[1], "ctx", axis=0, tiled=True),
    )
    key_blocks = back_keys.reshape(context_count, block, groups_local, HD)
    value_blocks = back_values.reshape(context_count, block, groups_local, HD)
    starts = block * jnp.arange(context_count, dtype=jnp.int32)

    def backward_update(grad_query, key_block, value_block, allowed):
        mask = allowed[:, None, None, :]
        scores = (
            jnp.einsum(
                "qgrd,kgd->qgrk", query_grouped, key_block, preferred_element_type=jnp.float32
            )
            * scale
        )
        probs = jnp.where(mask, jnp.exp(scores - log_total[..., None]), 0.0)
        value_grad = jnp.einsum(
            "qgrk,qgrd->kgd",
            probs.astype(jnp.bfloat16),
            grad_grouped,
            preferred_element_type=jnp.float32,
        )
        prob_grad = jnp.einsum(
            "qgrd,kgd->qgrk", grad_grouped, value_block, preferred_element_type=jnp.float32
        )
        score_grad = (probs * (prob_grad - delta[..., None]) * scale).astype(jnp.bfloat16)
        grad_query = grad_query + jnp.einsum(
            "qgrk,kgd->qgrd", score_grad, key_block, preferred_element_type=jnp.float32
        )
        key_grad = jnp.einsum(
            "qgrk,qgrd->kgd", score_grad, query_grouped, preferred_element_type=jnp.float32
        )
        return (grad_query, key_grad.reshape(block, -1), value_grad.reshape(block, -1))

    def backward_visit(grad_query, item):
        key_block, value_block, key_start = item
        allowed = allowed_mask(key_start, block)
        grad_query, key_grad, value_grad = backward_update(
            grad_query, key_block, value_block, allowed
        )
        return (grad_query, (key_grad, value_grad))

    grad_query, (key_grads, value_grads) = lax.scan(
        backward_visit,
        jnp.zeros((block, groups_local, ratio, HD), jnp.float32),
        (key_blocks, value_blocks, starts),
    )
    own_key_grad, own_value_grad = (
        lax.psum_scatter(
            key_grads.reshape(context_count * block, -1).astype(jnp.bfloat16),
            "ctx",
            scatter_dimension=0,
            tiled=True,
        ).astype(jnp.float32),
        lax.psum_scatter(
            value_grads.reshape(context_count * block, -1).astype(jnp.bfloat16),
            "ctx",
            scatter_dimension=0,
            tiled=True,
        ).astype(jnp.float32),
    )
    query_grad = (
        rotate_back(grad_query.reshape(block, heads_local, HD), cosine, sine)
        .reshape(block, -1)
        .astype(jnp.bfloat16)
    )
    key_grad = (
        rotate_back(own_key_grad.reshape(block, groups_local, HD), cosine, sine)
        .reshape(block, -1)
        .astype(jnp.bfloat16)
    )
    value_grad = own_value_grad.astype(jnp.bfloat16)
    input_part = jnp.dot(query_grad, query_full.T, preferred_element_type=jnp.float32)
    input_part = input_part + jnp.dot(key_grad, key_full.T, preferred_element_type=jnp.float32)
    input_part = input_part + jnp.dot(value_grad, value_full.T, preferred_element_type=jnp.float32)
    normed_one_grad = lax.psum(input_part.astype(jnp.bfloat16), "tp").astype(jnp.float32)
    grad_input_norm, gain_one_term = norm_backward(inputs, inverse_one, gain_one, normed_one_grad)
    input_grad = (grad_residual + grad_input_norm)[None]
    query_term = jnp.dot(normed_one.T, query_grad, preferred_element_type=jnp.float32)
    key_term = jnp.dot(normed_one.T, key_grad, preferred_element_type=jnp.float32)
    value_term = jnp.dot(normed_one.T, value_grad, preferred_element_type=jnp.float32)
    (
        gain_one_share,
        query_share,
        key_share,
        value_share,
        output_share,
        gain_two_share,
        router_share,
    ) = (
        lax.psum_scatter(gain_one_term, ("fsdp", "ctx"), scatter_dimension=0, tiled=True),
        lax.psum_scatter(query_term, ("fsdp", "ctx"), scatter_dimension=0, tiled=True),
        lax.psum_scatter(key_term, ("fsdp", "ctx"), scatter_dimension=0, tiled=True),
        lax.psum_scatter(value_term, ("fsdp", "ctx"), scatter_dimension=0, tiled=True),
        lax.psum_scatter(output_term, ("fsdp", "ctx"), scatter_dimension=0, tiled=True),
        lax.psum_scatter(gain_two_term, ("fsdp", "ctx"), scatter_dimension=0, tiled=True),
        lax.psum_scatter(router_term, ("fsdp", "ctx"), scatter_dimension=0, tiled=True),
    )
    return (
        block_out,
        input_grad,
        gain_one_share,
        query_share,
        key_share,
        value_share,
        output_share,
        gain_two_share,
        router_share,
        gate_share,
        up_share,
        down_share,
    )


MESH = pl.DeviceIdType.MESH
f32 = jnp.float32
bf16 = jnp.bfloat16


def dot_nn(a, b, precision=None):
    return lax.dot_general(a, b, (((1,), (0,)), ((), ())), precision=precision, preferred_element_type=f32)


def dot_nt(a, b, precision=None):
    return lax.dot_general(a, b, (((1,), (1,)), ((), ())), precision=precision, preferred_element_type=f32)


def dot_tn(a, b, precision=None):
    return lax.dot_general(a, b, (((0,), (0,)), ((), ())), precision=precision, preferred_element_type=f32)


class Net:
    def __init__(self, send_sems, recv_sems):
        self.send_sems, self.recv_sems, self.copies, self.left = send_sems, recv_sems, [], set()

    def make(self, source, target, device, sends=None):
        at = len(self.copies)
        copy = pltpu.make_async_remote_copy(
            src_ref=source,
            dst_ref=target,
            send_sem=self.send_sems.at[at],
            recv_sem=self.recv_sems.at[at],
            device_id=device,
            device_id_type=MESH,
        )
        self.copies.append((copy, sends))
        return copy

    def send(self, source, target, device):
        copy = self.make(source, target, device)
        copy.start()
        return copy

    def drain(self, among=None):
        for at, (copy, sends) in enumerate(self.copies):
            if at in self.left or (among is not None and at not in among):
                continue
            self.left.add(at)
            if sends is None:
                copy.wait_send()
            else:
                pl.when(sends)(copy.wait_send)


class Line:
    def __init__(self, net, z, nz, device):
        self.net, self.z, self.nz, self.device = net, z, nz, device

    def both(self):
        z, nz = self.z, self.nz
        right, left = self.device(lax.min(z + 1, nz - 1)), self.device(lax.max(z - 1, 0))
        return ((z, right), (nz - 1 - z, left))

    def pass_on(self, step, views):
        copies = []
        for way, (rank, target) in enumerate(self.both()):
            sends = (rank >= step) & (rank < self.nz - 1)
            arrives = rank >= step + 1
            block = lax.clamp(0, self.z - step if way == 0 else self.z + step, self.nz - 1)
            for view in views:
                copy = self.net.make(view(block), view(block), target, sends)
                pl.when(sends)(copy.start)
                copies.append((copy, arrives))
        return copies

    def add_on(self, step, own, out, into):
        copies = []
        for way, (rank, target) in enumerate(self.both()):
            sends = rank <= step
            arrives = (rank >= 1) & (rank - 1 <= step)
            dest = self.nz - 1 - step + rank
            dest = lax.clamp(0, dest if way == 0 else self.nz - 1 - dest, self.nz - 1)
            copy = self.net.make(out(way, step), into(way, step), target, sends)

            def prepare():
                out(way, step)[...] = own(dest)[...].astype(bf16)
                if step > 0:

                    def add():
                        out(way, step)[...] = (own(dest)[...] + into(way, step - 1)[...].astype(f32)).astype(bf16)

                    pl.when(rank >= 1)(add)
                copy.start()

            pl.when(sends)(prepare)
            copies.append((copy, arrives))
        return copies

    def finish(self, total, into):
        for way, (rank, target) in enumerate(self.both()):

            def add():
                total[...] += into(way, self.nz - 2)[...].astype(f32)

            pl.when(rank >= 1)(add)


def arrive(copies):
    for copy, arrives in copies:
        pl.when(arrives)(copy.wait_recv)


def layer_kernel(
    dims,
    x_ref, g_ref, wq_ref, wk_ref, wv_ref, wo_ref, ga_ref, ge_ref, rt_ref, wg_ref, wu_ref, wd_ref, dl_ref, ec_ref,
    fr_ref,
    block_out, input_grad, small_out, gain_out, dqkv_out, dwo_out, dgu_out, dd_out,
    WP, SMT, X, WQ, WO, SMB, SMW, N1, CT, ST, SEGC, POSC, Q, K, V, PSC, ATT, AT, PP, PR, RES,
    N2, GTB, GA, WGU, WD, AA, PSX, GC, H, UG, PRD, MP, MR, BP, BR, DGU, DDT, GDS, GD,
    RB, RM, BOWN, MOWN, CO, CI, MO, MI, DGB, GUL, DDB, DDL, SG, SGF, SGT, SGZ, SGP, GRES, RL,
    AGS, AGR, DWO, RWO, ZWO, LWO, DS, DQ, DQKV, NG, NR, DWQ, RWQ, ZWQ, LWQ,
    SG1, SG1P, RSG1, EXB, EXG,
    send_sems, recv_sems, local_sems,
):
    nf, nz, hb, width, experts, half_ff, ndoc, chosen = dims
    rows = 2 * nz * hb
    half = nz * hb
    block = 2 * hb
    shard = width // (nf * nz)
    f, z, c = lax.axis_index("fsdp"), lax.axis_index("ctx"), lax.axis_index("tp")
    other = 1 - c
    own = f * nz + z
    net = Net(send_sems, recv_sems)
    device = lambda df, dz, core: {"fsdp": df, "ctx": dz, "tp": core}
    partner = device(f, z, other)
    line = Line(net, z, nz, lambda dz: device(f, dz, c))
    zs = [lax.rem(z + k, nz) for k in range(nz)]
    zback = [lax.rem(z + nz - k, nz) for k in range(nz)]
    fs = [f, f + 1 - 2 * lax.rem(f, 2), lax.rem(f + 2, 4), 3 - f]
    everyone = [(i, j, k) for k in range(2) for i in range(nf) for j in range(nz) if (i, j, k) != (0, 0, 0)]
    others = [device(fs[i], zs[j], lax.rem(c + k, 2)) for i, j, k in everyone]
    same = [(i, j) for j in range(nz) for i in range(nf) if (i, j) != (0, 0)]

    mine = pl.ds(pl.multiple_of(c * hb, hb), hb)
    loads = [
        pltpu.make_async_copy(x_ref.at[mine], X.at[c, z], local_sems.at[0]),
        pltpu.make_async_copy(g_ref.at[mine], GA.at[f, c, z], local_sems.at[1]),
        pltpu.make_async_copy(wo_ref, WO.at[f, z], local_sems.at[2]),
        pltpu.make_async_copy(wg_ref.at[own], WGU.at[own, :, pl.ds(0, half_ff)], local_sems.at[3]),
        pltpu.make_async_copy(wu_ref.at[own], WGU.at[own, :, pl.ds(half_ff, half_ff)], local_sems.at[4]),
        pltpu.make_async_copy(wd_ref.at[own], WD.at[own], local_sems.at[5]),
    ]
    for copy in loads:
        copy.start()
    barrier = pltpu.get_barrier_semaphore()
    for peer in others:
        pl.semaphore_signal(barrier, inc=1, device_id=peer, device_id_type=MESH)

    for j in range(nz):
        WP[j, :, 0 : 2 * HD] = wq_ref[:, 2 * HD * j : 2 * HD * (j + 1)]
        WP[j, :, 2 * HD : 4 * HD] = jnp.concatenate(
            [wk_ref[:, HD * j : HD * (j + 1)], wv_ref[:, HD * j : HD * (j + 1)]], axis=1
        )
    base = jnp.concatenate(
        [ga_ref[...].astype(f32), ge_ref[...].astype(f32), jnp.zeros((14, shard), f32), rt_ref[...].astype(f32)],
        axis=0,
    )
    in_half = (lax.broadcasted_iota(jnp.int32, (32, 128), 1) < shard) == (lax.rem(z, 2) == 0)
    SMT[...] = jnp.where(in_half, jnp.concatenate([base, base], axis=1), 0.0).astype(bf16)
    SMB[f, z] = SMT[...]
    WQ[f, z] = WP[z]
    pl.semaphore_wait(barrier, len(others))

    sends_q = [net.send(WP.at[zs[k]], WQ.at[f, z], device(f, zs[k], c)) for k in range(1, nz)]
    loads[0].wait()
    view_x = [lambda at: X.at[c, at]]
    chain_x = line.pass_on(0, view_x)
    sends_s = [net.send(SMT, SMB.at[f, z], device(f, zs[k], c)) for k in range(1, nz)]
    loads[2].wait()
    view_o = [lambda at: WO.at[f, at]]
    chain_o = line.pass_on(0, view_o)
    weights = []

    def send_weights(count):
        for i, j in same[len(weights) // 3 : len(weights) // 3 + count]:
            e, to = fs[i] * nz + zs[j], device(fs[i], zs[j], c)
            weights.append(net.send(wg_ref.at[e], WGU.at[own, :, pl.ds(0, half_ff)], to))
            weights.append(net.send(wu_ref.at[e], WGU.at[own, :, pl.ds(half_ff, half_ff)], to))
            weights.append(net.send(wd_ref.at[e], WD.at[own], to))

    send_weights(nf - 1)

    def places(shape, dim):
        at = lax.broadcasted_iota(jnp.int32, shape, dim)
        core_at, rest = lax.div(at, half), lax.rem(at, half)
        return lax.div(rest, hb) * block + core_at * hb + lax.rem(rest, hb)

    def layout(position):
        segment = jnp.zeros_like(position)
        start = jnp.zeros_like(position)
        end = jnp.int32(0)
        for i in range(ndoc):
            length = dl_ref[0, i]
            end = end + length
            after = jnp.where(position >= end, 1, 0)
            segment = segment + after
            start = start + after * length
        return segment, position - start

    lane = lax.broadcasted_iota(jnp.int32, (1, 2 * HD), 1)
    former = lax.rem(lane, HD) < HD // 2
    is_key = lane < HD

    with jax.named_scope("tables0"):
        pos_col = places((rows, 1), 0)
        seg_col, offset = layout(pos_col)
        POSC[...] = pos_col
        SEGC[...] = seg_col
        pos_row = places((1, rows), 1)
        seg_row, unused = layout(pos_row)

    def swapped(v):
        return jnp.where(former, pltpu.roll(v, 2 * HD - HD // 2, 1), pltpu.roll(v, HD // 2, 1))

    for copy in sends_q:
        copy.wait_recv()
    sends_q2 = [net.send(WQ.at[f], WQ.at[f], device(fs[k], z, c)) for k in range(1, nf)]
    arrive(chain_x)
    chain_x = line.pass_on(1, view_x)
    loads[1].wait()
    view_g = [lambda at: GA.at[f, c, at]]
    chain_g = line.pass_on(0, view_g)
    for copy in sends_s:
        copy.wait_recv()
    sends_s2 = [net.send(SMB.at[f], SMB.at[f], device(fs[k], z, c)) for k in range(1, nf)]
    with jax.named_scope("tables1"):
        angle = offset.astype(f32) * fr_ref[0:1, :]
        CT[...] = jnp.cos(angle)
    arrive(chain_x)
    chain_x = line.pass_on(2, view_x)
    arrive(chain_o)
    chain_o = line.pass_on(1, view_o)
    with jax.named_scope("tables2"):
        ST[...] = jnp.where(former, -1.0, 1.0) * jnp.sin(angle)
    arrive(chain_x)
    forward_x = net.send(X.at[c], X.at[c], partner)
    arrive(chain_g)
    chain_g = line.pass_on(1, view_g)
    for copy in sends_s2:
        copy.wait_recv()
    for pair in range(nf * nz // 2):
        at_f, at_z = pair // (nz // 2), 2 * (pair % (nz // 2))
        SMW[:, 128 * pair : 128 * pair + 128] = SMB[at_f, at_z] + SMB[at_f, at_z + 1]
    arrive(chain_o)
    chain_o = line.pass_on(2, view_o)
    send_weights(2)
    forward_x.wait_recv()

    def norm_chunk(i, carry):
        at_c, at_z = lax.div(i, nz), lax.rem(i, nz)
        v = X[at_c, at_z].astype(f32)
        inverse = lax.rsqrt(jnp.mean(v * v, axis=1, keepdims=True) + epsilon)
        N1[pl.ds(pl.multiple_of(i * hb, hb), hb), :] = (v * inverse * SMW[0:1, :].astype(f32)).astype(bf16)
        return carry

    lax.fori_loop(0, 2 * nz, norm_chunk, 0)
    for copy in sends_q2:
        copy.wait_recv()
    with jax.named_scope("qkv"):
        projected = dot_nn(N1[...], WQ[...].reshape(width, 4 * HD))
        cosine, sine = CT[...], ST[...]
        q_part, kv_part = projected[:, : 2 * HD], projected[:, 2 * HD :]
        Q[...] = (q_part * cosine + swapped(q_part) * sine).astype(bf16)
        kv = jnp.where(is_key, kv_part * cosine + swapped(kv_part) * sine, kv_part).astype(bf16)
        K[...] = kv[:, :HD]
        V[...] = kv[:, HD:]
    arrive(chain_g)
    chain_g = line.pass_on(2, view_g)
    arrive(chain_o)
    sends_o2 = [net.send(WO.at[f], WO.at[f], device(fs[k], z, c)) for k in range(1, nf)]
    send_weights(1)

    scale = HD ** (-0.5)
    step = 2 * hb

    def attend(i, carry):
        at = pl.ds(pl.multiple_of(i * step, step), step)
        mask = (SEGC[at, :] == seg_row) & (pos_row <= POSC[at, :])
        q = Q[at, :]
        pieces = []
        for r in range(2):
            scores = dot_nt(q[:, r * HD : (r + 1) * HD], K[...]) * scale
            scores = jnp.where(mask, scores, masked_score)
            peak = jnp.max(scores, axis=1, keepdims=True)
            weights = jnp.where(mask, jnp.exp(scores - peak), 0.0)
            total = jnp.sum(weights, axis=1, keepdims=True)
            pieces.append(dot_nn(weights.astype(bf16), V[...]) / total)
            PSC[r, at, :] = (weights / total).astype(bf16)
        out = jnp.concatenate(pieces, axis=1).astype(bf16)
        at_c, at_z = lax.div(2 * i, nz), lax.rem(2 * i, nz)
        ATT[at_c, pl.ds(at_z, 2)] = out.reshape(2, hb, 2 * HD)
        return carry

    with jax.named_scope("attend"):
        lax.fori_loop(0, rows // step, attend, 0)
    columns = pl.ds(pl.multiple_of(z * 2 * HD, 2 * HD), 2 * HD)
    sends_a = [
        net.send(ATT.at[:, zs[k]], AT.at[:, :, columns], device(f, zs[k], c)) for k in range(1, nz)
    ]
    AT[:, :, columns] = ATT[:, z]
    send_weights(3)

    arrive(chain_g)
    sends_g2 = [net.send(GA.at[f, c], GA.at[f, c], device(fs[k], z, c)) for k in range(1, nf)]
    forward_g = net.send(GA.at[f, c], GA.at[f, c], partner)

    for copy in sends_a:
        copy.wait_recv()
    for copy in sends_o2:
        copy.wait_recv()
    with jax.named_scope("proj"):
        part = dot_nt(AT[...].reshape(block, nz * 2 * HD), WO[...].reshape(width, nz * 2 * HD))
        PP[...] = part.reshape(2, hb, width)
    send_p = net.send(PP.at[other], PR, partner)
    x_own = X[c, z].astype(f32)
    gain_two = SMW[1:2, :].astype(f32)
    send_p.wait_recv()
    residual = x_own + PP[c] + PR[...]
    RES[...] = residual
    inverse_two = lax.rsqrt(jnp.mean(residual * residual, axis=1, keepdims=True) + epsilon)
    N2[f, c, z] = (residual * inverse_two * gain_two).astype(bf16)
    normed_two = N2[f, c, z]
    logits = dot_nt(SMW[16 : 16 + experts, :], normed_two)
    expert_at = lax.broadcasted_iota(jnp.int32, (experts, hb), 0)
    route = ec_ref[...]
    route = jnp.where(c == 0, route, pltpu.roll(route, 128 - hb, 1))
    picked = jnp.zeros((experts, hb), jnp.bool_)
    for j in range(chosen):
        picked = picked | (route[j : j + 1, 0:hb] == expert_at)
    peak = jnp.max(jnp.where(picked, logits, masked_score), axis=0, keepdims=True)
    weight = jnp.where(picked, jnp.exp(logits - peak), 0.0)
    gates = weight / jnp.sum(weight, axis=0, keepdims=True)
    GTB[f, c, z] = jnp.concatenate([gates, jnp.zeros((experts, 128 - hb), f32)], axis=1)
    view_n = [lambda at: N2.at[f, c, at], lambda at: GTB.at[f, c, at]]
    chain_n = line.pass_on(0, view_n)
    send_weights(2)

    wd_full = lambda: WD[...].reshape(width, half_ff)
    wgu_full = lambda: WGU[...].reshape(width, 2 * half_ff)
    forwards_g2 = []
    for k in range(1, nf):
        sends_g2[k - 1].wait_recv()
        forwards_g2.append(net.send(GA.at[fs[k], c], GA.at[fs[k], c], partner))
    arrive(chain_n)
    chain_n = line.pass_on(1, view_n)
    send_weights(2)
    arrive(chain_n)
    chain_n = line.pass_on(2, view_n)
    send_weights(nf * nz)
    arrive(chain_n)

    def second_hop(ref, at_f, to):
        return [net.send(ref.at[at_f, c], ref.at[at_f, c], to)]

    sends_n2 = [
        [net.send(N2.at[f, c], N2.at[f, c], device(fs[k], z, c)), net.send(GTB.at[f, c], GTB.at[f, c], device(fs[k], z, c))]
        for k in range(1, nf)
    ]
    forwards_n = [
        [net.send(N2.at[f, c], N2.at[f, c], partner), net.send(GTB.at[f, c], GTB.at[f, c], partner)]
    ]
    for copy in loads[3:]:
        copy.wait()
    for copy in weights:
        copy.wait_recv()
    forward_g.wait_recv()
    with jax.named_scope("cotangent"):
        AA[f] = dot_nn(GA[f].reshape(rows, width), wd_full())

    chosen_row = jnp.where(
        lax.broadcasted_iota(jnp.int32, (experts, 128), 0) == own, 1.0, 0.0
    ).astype(f32)
    DGU[...] = jnp.zeros_like(DGU)
    DDT[...] = jnp.zeros_like(DDT)
    sends_d, sends_b, sends_m = [], [], []
    exchange_b, exchange_m = [], []

    for k in range(nf):
        at_f = fs[k]
        if k > 0:
            forwards_g2[k - 1].wait_recv()
            with jax.named_scope("cotangent"):
                AA[at_f] = dot_nn(GA[at_f].reshape(rows, width), wd_full())
            for copy in sends_n2[k - 1]:
                copy.wait_recv()
            forwards_n.append(
                [net.send(N2.at[at_f, c], N2.at[at_f, c], partner), net.send(GTB.at[at_f, c], GTB.at[at_f, c], partner)]
            )
        for copy in forwards_n[k]:
            copy.wait_recv()
        tokens = N2[at_f].reshape(rows, width)
        with jax.named_scope("gateup"):
            PSX[...] = dot_nn(tokens, wgu_full())
        with jax.named_scope("gatecol"):
            for piece in range(2 * nz):
                tile = GTB[at_f, piece // nz, piece % nz][:, 0:hb]
                GC[piece * hb : (piece + 1) * hb, :] = dot_tn(tile, chosen_row, lax.Precision.HIGHEST)

        def expert_chunk(i, carry):
            at = pl.ds(pl.multiple_of(i * 32, 32), 32)
            gate_pre = PSX[at, 0:half_ff]
            up_pre = PSX[at, half_ff : 2 * half_ff]
            raw = AA[at_f, at, :]
            gate = GC[at, 0:1]
            sigmoid = jax.nn.sigmoid(gate_pre)
            silu = gate_pre * sigmoid
            act = silu * up_pre
            PRD[at, :] = (act * raw).astype(bf16)
            H[at, :] = (act * gate).astype(bf16)
            grad = raw * gate
            UG[at, 0:half_ff] = (
                grad * up_pre * sigmoid * (1.0 + gate_pre * (1.0 - sigmoid))
            ).astype(bf16)
            UG[at, half_ff : 2 * half_ff] = (grad * silu).astype(bf16)
            return carry

        with jax.named_scope("chunk"):
            lax.fori_loop(0, rows // 32, expert_chunk, 0)
        with jax.named_scope("back"):
            BP[at_f] = dot_nt(UG[...], wgu_full()).astype(bf16).reshape(2, nz, hb, width)
        exchange_b.append(net.send(BP.at[at_f, other], BR.at[at_f], partner))
        with jax.named_scope("gdot"):
            GDS[k] = dot_nt(jnp.ones((8, half_ff), bf16), PRD[...])
            for j in range(nz):
                for t in range(2):
                    to_z, to_c = zs[j], lax.rem(c + t, 2)
                    lanes = pl.ds(pl.multiple_of((to_c * (nz // 2) + lax.div(to_z, 2)) * 128, 128), 128)
                    if (k, j, t) != (0, 0, 0):
                        sends_d.append(
                            net.send(GDS.at[k, pl.ds(0, 1), lanes], GD.at[f, z, c, pl.ds(0, 1)], device(at_f, to_z, to_c))
                        )
                    else:
                        GD[f, z, c] = GDS[0, :, lanes]
        with jax.named_scope("mix"):
            MP[at_f] = dot_nt(H[...], wd_full()).astype(bf16).reshape(2, nz, hb, width)
        exchange_m.append(net.send(MP.at[at_f, other], MR.at[at_f], partner))
        exchange_b[k].wait_recv()
        if k == 0:
            BOWN[...] = BP[at_f, c].astype(f32) + BR[at_f].astype(f32)
        else:
            BP[at_f, c] = (BP[at_f, c].astype(f32) + BR[at_f].astype(f32)).astype(bf16)
            sends_b.append(net.send(BP.at[at_f, c], RB.at[k - 1], device(at_f, z, c)))
        with jax.named_scope("wgrad"):
            DGU[...] += dot_tn(UG[...], tokens)
            DDT[...] += dot_tn(H[...], GA[at_f].reshape(rows, width))
        exchange_m[k].wait_recv()
        if k == 0:
            MOWN[...] = MP[at_f, c].astype(f32) + MR[at_f].astype(f32)
        else:
            MP[at_f, c] = (MP[at_f, c].astype(f32) + MR[at_f].astype(f32)).astype(bf16)

    for k in range(1, nf):
        sends_m.append(net.send(MP.at[fs[k], c], RM.at[k - 1], device(fs[k], z, c)))
    with jax.named_scope("transpose"):
        DGB[...] = jnp.transpose(DGU[...]).astype(bf16).reshape(nf, nz, shard, 2 * half_ff)
        DDB[...] = jnp.transpose(DDT[...]).astype(bf16).reshape(nf, nz, shard, half_ff)
    grads_at = []
    far = same[nf - 1 :] + same[: nf - 1]

    def send_grads(count):
        for i, j in far[len(grads_at) // 2 : len(grads_at) // 2 + count]:
            to = device(fs[i], zs[j], c)
            grads_at.append(net.send(DGB.at[fs[i], zs[j]], GUL.at[own], to))
            grads_at.append(net.send(DDB.at[fs[i], zs[j]], DDL.at[own], to))

    send_grads(2)
    GUL[own] = DGB[f, z]
    DDL[own] = DDB[f, z]

    for copy in sends_d:
        copy.wait_recv()
    dots = jnp.concatenate(
        [
            GD[e // nz, e % nz, 0][0:1, :] + GD[e // nz, e % nz, 1][0:1, :]
            for e in range(experts)
        ],
        axis=0,
    )
    dots = jnp.where(lax.rem(z, 2) == 0, dots, pltpu.roll(dots, 128 - hb, 1))[:, 0:hb]
    gates = GTB[f, c, z][:, 0:hb]
    logit_grad = gates * (dots - jnp.sum(gates * dots, axis=0, keepdims=True))
    router_t = SMW[16 : 16 + experts, :].astype(f32)
    SG[0:experts, :] = dot_nn(logit_grad, N2[f, c, z].astype(f32), lax.Precision.HIGHEST)
    GRES[...] = dot_tn(logit_grad, router_t, lax.Precision.HIGHEST)
    residual = RES[...]
    inverse_two = lax.rsqrt(jnp.mean(residual * residual, axis=1, keepdims=True) + epsilon)

    for k in range(1, nf):
        sends_b[k - 1].wait_recv()
        BOWN[...] += RB[k - 1].astype(f32)
    own_b, out_b, into_b = (lambda at: BOWN.at[at]), (lambda w, t: CO.at[w, t]), (lambda w, t: CI.at[w, t])
    sums = []
    for t in range(nz - 1):
        at_sums = len(net.copies)
        chain_b = line.add_on(t, own_b, out_b, into_b)
        sums.extend(range(at_sums, len(net.copies)))
        send_grads(1)
        arrive(chain_b)
    line.finish(BOWN.at[z], into_b)

    grad_two = BOWN[z] + GRES[...]
    scaled = grad_two * gain_two
    grad_res = (
        GA[f, c, z].astype(f32)
        + inverse_two * scaled
        - residual * (inverse_two * inverse_two * inverse_two) * jnp.mean(scaled * residual, axis=1, keepdims=True)
    )
    GRES[...] = grad_res
    RL[c] = grad_res.astype(bf16)
    send_r = net.send(RL.at[c], RL.at[c], partner)
    gain_term = jnp.sum(grad_two * residual * inverse_two, axis=0, keepdims=True)
    SG[experts : experts + 8, :] = jnp.broadcast_to(gain_term, (8, width))
    wide = width // nf
    block_lanes = lambda at: pl.ds(pl.multiple_of(at * wide, 128), wide)
    sends_sg = [net.send(SG.at[:, block_lanes(fs[k])], SGF.at[k - 1], device(fs[k], z, c)) for k in range(1, nf)]
    send_r.wait_recv()
    low = RL[...].reshape(block, width)
    with jax.named_scope("attgrad"):
        AGS[...] = dot_nn(low, WO[...].reshape(width, nz * 2 * HD)).astype(bf16).reshape(2, hb, nz * 2 * HD)
    sends_ag = [
        net.send(
            AGS.at[:, :, pl.ds(pl.multiple_of(zs[k] * 2 * HD, 2 * HD), 2 * HD)],
            AGR.at[:, z],
            device(f, zs[k], c),
        )
        for k in range(1, nz)
    ]
    AGR[:, z] = AGS[:, :, columns]
    send_grads(3)
    with jax.named_scope("outgrad"):
        DWO[...] = (
            dot_tn(low, AT[...].reshape(block, nz * 2 * HD))
            .astype(bf16)
            .reshape(nf, nz, shard, nz * 2 * HD)
        )
    sends_wo = [net.send(DWO.at[fs[k]], RWO.at[k - 1], device(fs[k], z, c)) for k in range(1, nf)]

    for copy in sends_ag:
        copy.wait_recv()

    def backward(i, carry):
        at = pl.ds(pl.multiple_of(i * step, step), step)
        at_c, at_z = lax.div(2 * i, nz), lax.rem(2 * i, nz)
        grad = AGR[at_c, pl.ds(at_z, 2)].reshape(step, 2 * HD)
        out = ATT[at_c, pl.ds(at_z, 2)].reshape(step, 2 * HD)
        both = grad.astype(f32) * out.astype(f32)
        pieces = []
        for r in range(2):
            delta = jnp.sum(both[:, r * HD : (r + 1) * HD], axis=1, keepdims=True)
            prob_grad = dot_nt(grad[:, r * HD : (r + 1) * HD], V[...])
            probs = PSC[r, at, :].astype(f32)
            score_grad = (probs * (prob_grad - delta) * scale).astype(bf16)
            DS[r, at, :] = score_grad
            pieces.append(dot_nn(score_grad, K[...]))
        DQ[at, :] = jnp.concatenate(pieces, axis=1)
        return carry

    with jax.named_scope("attback"):
        lax.fori_loop(0, rows // step, backward, 0)
    with jax.named_scope("kvgrad"):
        grads = AGR[...].reshape(rows, 2 * HD)
        key_t = dot_tn(Q[:, 0:HD], DS[0]) + dot_tn(Q[:, HD : 2 * HD], DS[1])
        value_t = dot_tn(grads[:, 0:HD], PSC[0]) + dot_tn(grads[:, HD : 2 * HD], PSC[1])
        kv_grad = jnp.transpose(jnp.concatenate([key_t, value_t], axis=0))
        cosine, sine = CT[...], ST[...]
        q_grad = DQ[...]
        DQKV[:, 0 : 2 * HD] = (q_grad * cosine - swapped(q_grad) * sine).astype(bf16)
        DQKV[:, 2 * HD : 4 * HD] = jnp.where(
            is_key, kv_grad * cosine - swapped(kv_grad) * sine, kv_grad
        ).astype(bf16)
    with jax.named_scope("ingrad"):
        NG[...] = dot_nt(DQKV[...], WQ[...].reshape(width, 4 * HD)).astype(bf16).reshape(2, nz, hb, width)
    send_ng = net.send(NG.at[other], NR, partner)
    with jax.named_scope("qkvgrad"):
        DWQ[...] = (
            jnp.transpose(dot_tn(DQKV[...], N1[...])).astype(bf16).reshape(nf, nz, shard, 4 * HD)
        )
    sends_wq = [net.send(DWQ.at[fs[k]], RWQ.at[k - 1], device(fs[k], z, c)) for k in range(1, nf)]
    send_ng.wait_recv()
    BOWN[...] = NG[c].astype(f32) + NR[...].astype(f32)
    net.drain(sums)
    chain_g1 = line.add_on(0, own_b, out_b, into_b)

    for k in range(1, nf):
        sends_m[k - 1].wait_recv()
        MOWN[...] += RM[k - 1].astype(f32)
    own_m, out_m, into_m = (lambda at: MOWN.at[at]), (lambda w, t: MO.at[w, t]), (lambda w, t: MI.at[w, t])
    chain_m = line.add_on(0, own_m, out_m, into_m)
    arrive(chain_g1)
    chain_g1 = line.add_on(1, own_b, out_b, into_b)

    total = DWO[f].astype(f32)
    for k in range(1, nf):
        sends_wo[k - 1].wait_recv()
        total = total + RWO[k - 1].astype(f32)
    ZWO[...] = total.astype(bf16)
    sends_wo2 = [net.send(ZWO.at[zs[k]], LWO.at[z], device(f, zs[k], c)) for k in range(1, nz)]
    LWO[z] = ZWO[z]
    small = SG[:, block_lanes(f)]
    for k in range(1, nf):
        sends_sg[k - 1].wait_recv()
        small = small + SGF[k - 1]
    SGT[...] = small
    pair_lanes = lambda at: pl.ds(pl.multiple_of(lax.div(at, 2) * 128, 128), 128)
    sends_sz = [net.send(SGT.at[:, pair_lanes(zs[k])], SGZ.at[k - 1], device(f, zs[k], c)) for k in range(1, nz)]
    arrive(chain_g1)
    chain_g1 = line.add_on(2, own_b, out_b, into_b)
    arrive(chain_m)
    chain_m = line.add_on(1, own_m, out_m, into_m)

    total = DWQ[f].astype(f32)
    for k in range(1, nf):
        sends_wq[k - 1].wait_recv()
        total = total + RWQ[k - 1].astype(f32)
    ZWQ[...] = total.astype(bf16)
    sends_wq2 = [net.send(ZWQ.at[zs[k]], LWQ.at[z], device(f, zs[k], c)) for k in range(1, nz)]
    LWQ[z] = ZWQ[z]
    send_grads(nf * nz)
    small = SGT[:, pair_lanes(z)]
    for k in range(1, nz):
        sends_sz[k - 1].wait_recv()
        small = small + SGZ[k - 1]
    SGP[0] = small
    send_sp = net.send(SGP.at[0], SGP.at[1], partner)

    arrive(chain_g1)
    line.finish(BOWN.at[z], into_b)
    grad_one = BOWN[z]
    gain_one = SMW[0:1, :].astype(f32)
    x_own = X[c, z].astype(f32)
    inverse = lax.rsqrt(jnp.mean(x_own * x_own, axis=1, keepdims=True) + epsilon)
    gain_term = jnp.sum(grad_one * x_own * inverse, axis=0, keepdims=True)
    SG1[0] = jnp.broadcast_to(gain_term, (8, width))
    send_g1 = net.send(SG1.at[0], SG1.at[1], partner)
    scaled = grad_one * gain_one
    EXG[c] = (
        GRES[...]
        + inverse * scaled
        - x_own * (inverse * inverse * inverse) * jnp.mean(scaled * x_own, axis=1, keepdims=True)
    )
    send_ig = net.send(EXG.at[c], EXG.at[c], partner)
    send_g1.wait_recv()
    SG1P[...] = SG1[0] + SG1[1]
    lanes_of = lambda df, dz: pl.ds(pl.multiple_of((df * (nz // 2) + lax.div(dz, 2)) * 128, 128), 128)
    sends_g1 = [
        net.send(SG1P.at[pl.ds(0, 1), lanes_of(fs[i], zs[j])], RSG1.at[f, z, pl.ds(0, 1)], device(fs[i], zs[j], c))
        for i, j in same
    ]
    RSG1[f, z] = SG1P[:, lanes_of(f, z)]

    arrive(chain_m)
    chain_m = line.add_on(2, own_m, out_m, into_m)
    send_sp.wait_recv()
    small_out[...] = SGP[0] + SGP[1]
    for copy in sends_wo2:
        copy.wait_recv()
    total = LWO[0].astype(f32)
    for j in range(1, nz):
        total = total + LWO[j].astype(f32)
    dwo_out[...] = total
    arrive(chain_m)
    line.finish(MOWN.at[z], into_m)
    EXB[c] = (RES[...] + MOWN[z]).astype(bf16)
    send_bo = net.send(EXB.at[c], EXB.at[c], partner)
    for copy in sends_wq2:
        copy.wait_recv()
    dqkv_out[...] = LWQ[...]
    for copy in grads_at:
        copy.wait_recv()
    outs = [
        pltpu.make_async_copy(GUL, dgu_out, local_sems.at[6]),
        pltpu.make_async_copy(DDL, dd_out, local_sems.at[7]),
    ]
    for copy in outs:
        copy.start()
    for copy in sends_g1:
        copy.wait_recv()
    small = jnp.zeros((1, 128), f32)
    for i in range(nf):
        for j in range(nz):
            small = small + RSG1[i, j, 0:1]
    gain_out[...] = jnp.broadcast_to(small, (8, 128))
    send_bo.wait_recv()
    block_out[...] = EXB[...].reshape(block, width)
    send_ig.wait_recv()
    input_grad[...] = EXG[...].reshape(block, width)
    for copy in outs:
        copy.wait()
    net.drain()


def finish_kernel(
    dims, block_ref, input_ref, small_ref, gain_ref, dqkv_ref, dwo_ref, dgu_ref, dd_ref,
    block_out, input_out, gain1_out, q_out, k_out, v_out, o_out, gain2_out, router_out, gate_out, up_out, down_out,
):
    nz, experts, half_ff, shard = dims
    block_out[...] = block_ref[...]
    input_out[...] = input_ref[...]
    gate_out[...] = dgu_ref[:, :, 0:half_ff].astype(f32)
    up_out[...] = dgu_ref[:, :, half_ff : 2 * half_ff].astype(f32)
    down_out[...] = dd_ref[...].astype(f32)
    even = lax.rem(lax.axis_index("ctx"), 2) == 0
    pick = lambda v: jnp.where(even, v, pltpu.roll(v, 128 - shard, 1))[:, 0:shard]

    def once():
        gain1_out[...] = pick(gain_ref[...])[0:1]
        small = pick(small_ref[...])
        router_out[...] = small[0:experts]
        gain2_out[...] = small[experts : experts + 1]
        o_out[...] = dwo_ref[...]
        for j in range(nz):
            q_out[:, 2 * HD * j : 2 * HD * (j + 1)] = dqkv_ref[j, :, 0 : 2 * HD].astype(f32)
        for at, ref in ((2, k_out), (3, v_out)):
            ref[...] = jnp.concatenate(
                [dqkv_ref[j, :, at * HD : (at + 1) * HD].astype(f32) for j in range(nz)], axis=1
            )

    pl.when(pl.program_id(0) == 0)(once)


def fast_local(
    nf, nz,
    hidden_in, out_grad, attention_gain, query_weight, key_weight, value_weight, output_weight,
    expert_gain, router_weight, gate_weight, up_weight, down_weight, doc_lengths, expert_choice,
):
    block, width = hidden_in.shape[1], hidden_in.shape[2]
    hb = block // 2
    experts, shard, half_ff = gate_weight.shape
    ndoc, chosen = doc_lengths.shape[1], expert_choice.shape[2]
    rows = nz * block
    halfway = HD // 2
    frequency = np.float32(rope_base) ** (-np.arange(halfway, dtype=np.float32) / np.float32(halfway))
    frequency = jnp.asarray(np.tile(np.tile(frequency, 4)[None], (8, 1)).astype(np.float32))

    vm = pl.BlockSpec(memory_space=pltpu.VMEM)
    anywhere = pl.BlockSpec(memory_space=pl.ANY)
    shape = lambda s, d: jax.ShapeDtypeStruct(s, d)
    W = nz * 2 * HD
    scratch = dict(
        WP=((nz, shard, 4 * HD), bf16), SMT=((32, 128), bf16),
        X=((2, nz, hb, width), bf16), WQ=((nf, nz, shard, 4 * HD), bf16), WO=((nf, nz, shard, W), bf16),
        SMB=((nf, nz, 32, 128), bf16), SMW=((32, width), bf16), N1=((rows, width), bf16),
        CT=((rows, 128), f32), ST=((rows, 128), f32), SEGC=((rows, 1), jnp.int32), POSC=((rows, 1), jnp.int32),
        Q=((rows, 2 * HD), bf16), K=((rows, HD), bf16), V=((rows, HD), bf16), PSC=((2, rows, rows), bf16),
        ATT=((2, nz, hb, 2 * HD), bf16), AT=((2, hb, W), bf16), PP=((2, hb, width), f32), PR=((hb, width), f32),
        RES=((hb, width), f32),
        N2=((nf, 2, nz, hb, width), bf16), GTB=((nf, 2, nz, experts, 128), f32), GA=((nf, 2, nz, hb, width), bf16),
        WGU=((nf * nz, shard, 2 * half_ff), bf16), WD=((nf * nz, shard, half_ff), bf16),
        AA=((nf, rows, half_ff), f32), PSX=((rows, 2 * half_ff), f32), GC=((rows, 128), f32),
        H=((rows, half_ff), bf16), UG=((rows, 2 * half_ff), bf16), PRD=((rows, half_ff), bf16),
        MP=((nf, 2, nz, hb, width), bf16), MR=((nf, nz, hb, width), bf16),
        BP=((nf, 2, nz, hb, width), bf16), BR=((nf, nz, hb, width), bf16),
        DGU=((2 * half_ff, width), f32), DDT=((half_ff, width), f32),
        GDS=((nf, 8, rows), f32), GD=((nf, nz, 2, 8, 128), f32),
        RB=((nf - 1, nz, hb, width), bf16), RM=((nf - 1, nz, hb, width), bf16),
        BOWN=((nz, hb, width), f32), MOWN=((nz, hb, width), f32),
        CO=((2, nz - 1, hb, width), bf16), CI=((2, nz - 1, hb, width), bf16),
        MO=((2, nz - 1, hb, width), bf16), MI=((2, nz - 1, hb, width), bf16),
        DGB=((nf, nz, shard, 2 * half_ff), bf16), GUL=((nf * nz, shard, 2 * half_ff), bf16),
        DDB=((nf, nz, shard, half_ff), bf16), DDL=((nf * nz, shard, half_ff), bf16),
        SG=((experts + 8, width), f32), SGF=((nf - 1, experts + 8, width // nf), f32),
        SGT=((experts + 8, width // nf), f32), SGZ=((nz - 1, experts + 8, 128), f32), SGP=((2, experts + 8, 128), f32),
        GRES=((hb, width), f32), RL=((2, hb, width), bf16),
        AGS=((2, hb, W), bf16), AGR=((2, nz, hb, 2 * HD), bf16),
        DWO=((nf, nz, shard, W), bf16), RWO=((nf - 1, nz, shard, W), bf16),
        ZWO=((nz, shard, W), bf16), LWO=((nz, shard, W), bf16),
        DS=((2, rows, rows), bf16), DQ=((rows, 2 * HD), f32),
        DQKV=((rows, 4 * HD), bf16), NG=((2, nz, hb, width), bf16), NR=((nz, hb, width), bf16),
        DWQ=((nf, nz, shard, 4 * HD), bf16), RWQ=((nf - 1, nz, shard, 4 * HD), bf16),
        ZWQ=((nz, shard, 4 * HD), bf16), LWQ=((nz, shard, 4 * HD), bf16),
        SG1=((2, 8, width), f32), SG1P=((8, width), f32), RSG1=((nf, nz, 8, 128), f32),
        EXB=((2, hb, width), bf16), EXG=((2, hb, width), f32),
    )
    slots = 320
    out = pl.pallas_call(
        functools.partial(layer_kernel, (nf, nz, hb, width, experts, half_ff, ndoc, chosen)),
        name="layer",
        out_shape=(
            shape((block, width), bf16), shape((block, width), f32), shape((experts + 8, 128), f32),
            shape((8, 128), f32), shape((nz, shard, 4 * HD), bf16), shape((shard, W), f32),
            shape((nf * nz, shard, 2 * half_ff), bf16), shape((nf * nz, shard, half_ff), bf16),
        ),
        in_specs=[anywhere] * 2 + [vm] * 3 + [anywhere] + [vm] * 3 + [anywhere] * 3
        + [pl.BlockSpec(memory_space=pltpu.SMEM), vm, vm],
        out_specs=(vm,) * 6 + (anywhere,) * 2,
        scratch_shapes=[pltpu.VMEM(s, d) for s, d in scratch.values()]
        + [pltpu.SemaphoreType.DMA((slots,)), pltpu.SemaphoreType.DMA((slots,)), pltpu.SemaphoreType.DMA((8,))],
        compiler_params=pltpu.CompilerParams(
            collective_id=0, has_side_effects=True, vmem_limit_bytes=67043328
        ),
    )(
        hidden_in[0], out_grad[0], query_weight, key_weight, value_weight, output_weight,
        attention_gain[None], expert_gain[None], router_weight.T, gate_weight, up_weight, down_weight,
        doc_lengths, expert_choice[0].T, frequency,
    )
    steps = nz
    some = lambda *s: pl.BlockSpec(s, lambda i: (i,) + (0,) * (len(s) - 1))
    whole = lambda *s: pl.BlockSpec(s, lambda i: (0,) * len(s))
    per = nf * nz // steps
    out = pl.pallas_call(
        functools.partial(finish_kernel, (nz, experts, half_ff, shard)),
        name="finish",
        grid=(steps,),
        out_shape=(
            shape((block, width), bf16), shape((block, width), f32), shape((1, shard), f32),
            shape((shard, nz * 2 * HD), f32), shape((shard, nz * HD), f32), shape((shard, nz * HD), f32),
            shape((shard, W), f32), shape((1, shard), f32), shape((experts, shard), f32),
            shape((experts, shard, half_ff), f32), shape((experts, shard, half_ff), f32),
            shape((experts, shard, half_ff), f32),
        ),
        in_specs=[
            some(block // steps, width), some(block // steps, width), whole(experts + 8, 128), whole(8, 128),
            whole(nz, shard, 4 * HD), whole(shard, W), some(per, shard, 2 * half_ff), some(per, shard, half_ff),
        ],
        out_specs=(
            some(block // steps, width), some(block // steps, width), whole(1, shard),
            whole(shard, nz * 2 * HD), whole(shard, nz * HD), whole(shard, nz * HD), whole(shard, W), whole(1, shard),
            whole(experts, shard), some(per, shard, half_ff), some(per, shard, half_ff), some(per, shard, half_ff),
        ),
        compiler_params=pltpu.CompilerParams(vmem_limit_bytes=33554432),
    )(*out)
    block_out, input_grad, gain1, q, k, v, o, gain2, router, gate, up, down = out
    return (
        block_out[None], input_grad[None], gain1[0], q, k, v, o, gain2[0], router.T, gate, up, down,
    )


def fits(mesh, args):
    nf, nz, nc = mesh.shape["fsdp"], mesh.shape["ctx"], mesh.shape["tp"]
    hidden, query, key, gate = args[0], args[3], args[4], args[9]
    width, block = hidden.shape[2], hidden.shape[1] // nz
    return (
        nc == 2
        and nz == 4
        and nf == 4
        and hidden.shape[0] == nf
        and gate.shape[0] == nf * nz
        and gate.shape[0] == 16
        and width == 64 * nf * nz
        and block == 128
        and query.shape[1] == 2 * HD * nz * nc
        and key.shape[1] == HD * nz * nc
        and HD == 64
    )


def solution(mesh):
    in_specs = (
        P("fsdp", "ctx", None),
        P("fsdp", "ctx", None),
        P(("fsdp", "ctx")),
        P(("fsdp", "ctx"), "tp"),
        P(("fsdp", "ctx"), "tp"),
        P(("fsdp", "ctx"), "tp"),
        P(("fsdp", "ctx"), "tp"),
        P(("fsdp", "ctx")),
        P(("fsdp", "ctx"), None),
        P(None, ("fsdp", "ctx"), "tp"),
        P(None, ("fsdp", "ctx"), "tp"),
        P(None, ("fsdp", "ctx"), "tp"),
        P("fsdp", None),
        P("fsdp", "ctx", None),
    )
    out_specs = (
        P("fsdp", "ctx", None),
        P("fsdp", "ctx", None),
        P(("fsdp", "ctx")),
        P(("fsdp", "ctx"), "tp"),
        P(("fsdp", "ctx"), "tp"),
        P(("fsdp", "ctx"), "tp"),
        P(("fsdp", "ctx"), "tp"),
        P(("fsdp", "ctx")),
        P(("fsdp", "ctx"), None),
        P(None, ("fsdp", "ctx"), "tp"),
        P(None, ("fsdp", "ctx"), "tp"),
        P(None, ("fsdp", "ctx"), "tp"),
    )

    def step(*args):
        body = local
        if fits(mesh, args):
            body = functools.partial(fast_local, mesh.shape["fsdp"], mesh.shape["ctx"])
        return jax.shard_map(
            body, mesh=mesh, in_specs=in_specs, out_specs=out_specs, check_vma=False
        )(*args)

    return step
```

```python
import functools

import jax
import jax.numpy as jnp
import numpy as np
from jax import lax
from jax.experimental import pallas as pl
from jax.experimental.pallas import tpu as pltpu
from jax.sharding import PartitionSpec as P

HD = 64


epsilon = 1e-05
rope_base = 10000.0
masked_score = -1e30
highest = lax.Precision.HIGHEST


def doc_layout(lengths, positions):
    ends = jnp.cumsum(lengths)
    after = (positions[:, None] >= ends[None, :]).astype(jnp.int32)
    segment = jnp.sum(after, axis=1)
    offset = positions - jnp.sum(after * lengths[None, :], axis=1)
    return (segment, offset)


def rope_tables(offset):
    halfway = HD // 2
    frequency = rope_base ** (-jnp.arange(halfway, dtype=jnp.float32) / halfway)
    angle = offset.astype(jnp.float32)[:, None] * frequency[None, :]
    return (jnp.cos(angle), jnp.sin(angle))


def rotate(vectors, cosine, sine):
    halfway = vectors.shape[-1] // 2
    former = vectors[..., :halfway]
    latter = vectors[..., halfway:]
    cosine = cosine[:, None, :]
    sine = sine[:, None, :]
    return jnp.concatenate(
        [former * cosine - latter * sine, latter * cosine + former * sine], axis=-1
    )


def rotate_back(grads, cosine, sine):
    halfway = grads.shape[-1] // 2
    former = grads[..., :halfway]
    latter = grads[..., halfway:]
    cosine = cosine[:, None, :]
    sine = sine[:, None, :]
    return jnp.concatenate(
        [former * cosine + latter * sine, latter * cosine - former * sine], axis=-1
    )


def norm_forward(values, gain):
    inverse = lax.rsqrt(jnp.mean(values * values, axis=-1, keepdims=True) + epsilon)
    return (values * inverse * gain.astype(jnp.float32), inverse)


def norm_backward(values, inverse, gain, grad_normed):
    scaled = grad_normed * gain.astype(jnp.float32)
    grad_values = inverse * scaled - values * inverse**3 * jnp.mean(
        scaled * values, axis=-1, keepdims=True
    )
    grad_gain = jnp.sum(grad_normed * values * inverse, axis=0)
    return (grad_values, grad_gain)


def dispatch(route, experts, capacity):
    flat = route.reshape(-1)
    onehot = (flat[:, None] == jnp.arange(experts, dtype=jnp.int32)[None, :]).astype(jnp.int32)
    rank = jnp.sum((jnp.cumsum(onehot, axis=0) - onehot) * onehot, axis=1)
    slot = flat * capacity + rank
    pairs = flat.shape[0]
    owner = (
        jnp.zeros((experts * capacity,), jnp.int32).at[slot].set(jnp.arange(pairs, dtype=jnp.int32))
    )
    filled = jnp.zeros((experts * capacity,), jnp.int32).at[slot].set(1) > 0
    return (slot, owner, filled)


def expert_math(slot_inputs, slot_grads, gate_full, up_full, down_full):
    gate_pre = jnp.einsum(
        "gsd,gdf->gsf", slot_inputs, gate_full, preferred_element_type=jnp.float32
    )
    up_pre = jnp.einsum("gsd,gdf->gsf", slot_inputs, up_full, preferred_element_type=jnp.float32)
    sigmoid = jax.nn.sigmoid(gate_pre)
    activated = (gate_pre * sigmoid * up_pre).astype(jnp.bfloat16)
    expert_out = jnp.einsum(
        "gsf,gdf->gsd", activated, down_full, preferred_element_type=jnp.float32
    )
    act_grad = jnp.einsum("gsd,gdf->gsf", slot_grads, down_full, preferred_element_type=jnp.float32)
    gate_pre_grad = (act_grad * up_pre * sigmoid * (1.0 + gate_pre * (1.0 - sigmoid))).astype(
        jnp.bfloat16
    )
    up_pre_grad = (act_grad * gate_pre * sigmoid).astype(jnp.bfloat16)
    down_term = jnp.einsum(
        "gsd,gsf->gdf", slot_grads, activated, preferred_element_type=jnp.float32
    )
    gate_term = jnp.einsum(
        "gsd,gsf->gdf", slot_inputs, gate_pre_grad, preferred_element_type=jnp.float32
    )
    up_term = jnp.einsum(
        "gsd,gsf->gdf", slot_inputs, up_pre_grad, preferred_element_type=jnp.float32
    )
    slot_back = jnp.einsum(
        "gsf,gdf->gsd", gate_pre_grad, gate_full, preferred_element_type=jnp.float32
    ) + jnp.einsum("gsf,gdf->gsd", up_pre_grad, up_full, preferred_element_type=jnp.float32)
    return (expert_out, slot_back, gate_term, up_term, down_term)


def local(
    hidden_in,
    out_grad,
    attention_gain,
    query_weight,
    key_weight,
    value_weight,
    output_weight,
    expert_gain,
    router_weight,
    gate_weight,
    up_weight,
    down_weight,
    doc_lengths,
    expert_choice,
):
    block = hidden_in.shape[1]
    experts = gate_weight.shape[0]
    capacity = block * 3 // 4
    chosen_count = expert_choice.shape[2]
    context_count = lax.axis_size("ctx")
    scale = HD ** (-0.5)
    position = lax.axis_index("ctx") * block + jnp.arange(block, dtype=jnp.int32)
    lengths = doc_lengths[0]
    segment, offset = doc_layout(lengths, position)
    cosine, sine = rope_tables(offset)
    gain_one, query_full, key_full, value_full, output_full, gain_two, router_full = (
        lax.all_gather(attention_gain, ("fsdp", "ctx"), axis=0, tiled=True),
        lax.all_gather(query_weight, ("fsdp", "ctx"), axis=0, tiled=True),
        lax.all_gather(key_weight, ("fsdp", "ctx"), axis=0, tiled=True),
        lax.all_gather(value_weight, ("fsdp", "ctx"), axis=0, tiled=True),
        lax.all_gather(output_weight, ("fsdp", "ctx"), axis=0, tiled=True),
        lax.all_gather(expert_gain, ("fsdp", "ctx"), axis=0, tiled=True),
        lax.all_gather(router_weight, ("fsdp", "ctx"), axis=0, tiled=True),
    )
    inputs = hidden_in[0].astype(jnp.float32)
    normed_one, inverse_one = norm_forward(inputs, gain_one)
    normed_one = normed_one.astype(jnp.bfloat16)
    heads_local = query_full.shape[1] // HD
    groups_local = key_full.shape[1] // HD
    ratio = heads_local // groups_local
    query = rotate(
        jnp.dot(normed_one, query_full, preferred_element_type=jnp.float32).reshape(
            block, heads_local, HD
        ),
        cosine,
        sine,
    ).astype(jnp.bfloat16)
    keys = rotate(
        jnp.dot(normed_one, key_full, preferred_element_type=jnp.float32).reshape(
            block, groups_local, HD
        ),
        cosine,
        sine,
    ).astype(jnp.bfloat16)
    values = jnp.dot(normed_one, value_full, preferred_element_type=jnp.float32).astype(
        jnp.bfloat16
    )
    query_grouped = query.reshape(block, groups_local, ratio, HD)

    def allowed_mask(key_start, count):
        key_position = key_start + jnp.arange(count, dtype=jnp.int32)
        key_segment, unused = doc_layout(lengths, key_position)
        return (segment[:, None] == key_segment[None, :]) & (
            key_position[None, :] <= position[:, None]
        )

    def forward_update(state, key_block, value_block, allowed):
        peak, total, accum = state
        mask = allowed[:, None, None, :]
        scores = (
            jnp.einsum(
                "qgrd,kgd->qgrk", query_grouped, key_block, preferred_element_type=jnp.float32
            )
            * scale
        )
        scores = jnp.where(mask, scores, masked_score)
        new_peak = jnp.maximum(peak, jnp.max(scores, axis=3))
        weights = jnp.where(mask, jnp.exp(scores - new_peak[..., None]), 0.0)
        rescale = jnp.exp(peak - new_peak)
        total = total * rescale + jnp.sum(weights, axis=3)
        accum = accum * rescale[..., None] + jnp.einsum(
            "qgrk,kgd->qgrd", weights, value_block.astype(jnp.float32), precision=highest
        )
        return (new_peak, total, accum)

    travel = (keys.reshape(block, groups_local * HD), values)
    initial = (
        jnp.full((block, groups_local, ratio), masked_score, jnp.float32),
        jnp.zeros((block, groups_local, ratio), jnp.float32),
        jnp.zeros((block, groups_local, ratio, HD), jnp.float32),
    )
    state = initial
    key_piece = lax.all_gather(travel[0], "ctx", axis=0, tiled=True)
    value_piece = lax.all_gather(travel[1], "ctx", axis=0, tiled=True)
    pieces = key_piece.shape[0] // block
    key_blocks = key_piece.reshape(pieces, block, groups_local, HD)
    value_blocks = value_piece.reshape(pieces, block, groups_local, HD)
    starts = block * jnp.arange(pieces, dtype=jnp.int32)

    def visit(carry, item):
        key_block, value_block, key_start = item
        allowed = allowed_mask(key_start, block)
        return (forward_update(carry, key_block, value_block, allowed), None)

    state, unused = lax.scan(visit, state, (key_blocks, value_blocks, starts))
    peak, total, accum = state
    attended = (accum / total[..., None]).reshape(block, heads_local * HD).astype(jnp.bfloat16)
    log_total = peak + jnp.log(total)
    projected = lax.psum(jnp.dot(attended, output_full.T, preferred_element_type=jnp.float32), "tp")
    residual = inputs + projected
    normed_two, inverse_two = norm_forward(residual, gain_two)
    normed_two = normed_two.astype(jnp.bfloat16)
    route = expert_choice[0]
    logits = jnp.dot(normed_two, router_full, preferred_element_type=jnp.float32)
    gates = jax.nn.softmax(jnp.take_along_axis(logits, route, axis=1), axis=1)
    slot, owner, filled = dispatch(route, experts, capacity)
    token_of = owner // chosen_count
    grad_out = out_grad[0].astype(jnp.float32)
    slot_inputs = jnp.where(filled[:, None], normed_two[token_of], 0).reshape(experts, capacity, -1)
    slot_gate = jnp.where(filled, gates.reshape(-1)[owner], 0.0)
    slot_grads = (
        (grad_out[token_of] * slot_gate[:, None])
        .astype(jnp.bfloat16)
        .reshape(experts, capacity, -1)
    )
    gate_full, up_full, down_full = (
        lax.all_gather(gate_weight, ("fsdp", "ctx"), axis=1, tiled=True),
        lax.all_gather(up_weight, ("fsdp", "ctx"), axis=1, tiled=True),
        lax.all_gather(down_weight, ("fsdp", "ctx"), axis=1, tiled=True),
    )
    expert_out, slot_back, gate_term, up_term, down_term = expert_math(
        slot_inputs, slot_grads, gate_full, up_full, down_full
    )
    gate_share, up_share, down_share = (
        lax.psum_scatter(gate_term, ("fsdp", "ctx"), scatter_dimension=1, tiled=True),
        lax.psum_scatter(up_term, ("fsdp", "ctx"), scatter_dimension=1, tiled=True),
        lax.psum_scatter(down_term, ("fsdp", "ctx"), scatter_dimension=1, tiled=True),
    )
    pair_out = expert_out.reshape(experts * capacity, -1)[slot].reshape(block, chosen_count, -1)
    pair_back = slot_back.reshape(experts * capacity, -1)[slot].reshape(block, chosen_count, -1)
    mixed_part = jnp.sum(gates[..., None] * pair_out, axis=1)
    gate_dot_part = jnp.sum(pair_out * grad_out[:, None, :], axis=2)
    moe_part = jnp.sum(pair_back, axis=1)
    mixed, gate_dot, moe_input = (
        lax.psum(mixed_part.astype(jnp.bfloat16), "tp").astype(jnp.float32),
        lax.psum(gate_dot_part.astype(jnp.bfloat16), "tp").astype(jnp.float32),
        lax.psum(moe_part.astype(jnp.bfloat16), "tp").astype(jnp.float32),
    )
    block_out = (residual + mixed).astype(jnp.bfloat16)[None]
    chosen_grad = gates * (gate_dot - jnp.sum(gates * gate_dot, axis=1, keepdims=True))
    picked = (route[..., None] == jnp.arange(experts, dtype=jnp.int32)[None, None, :]).astype(
        jnp.float32
    )
    logit_grad = jnp.sum(picked * chosen_grad[..., None], axis=1)
    router_term = jnp.dot(normed_two.astype(jnp.float32).T, logit_grad, precision=highest)
    router_input = jnp.dot(logit_grad, router_full.astype(jnp.float32).T, precision=highest)
    grad_residual_norm, gain_two_term = norm_backward(
        residual, inverse_two, gain_two, moe_input + router_input
    )
    grad_residual = grad_out + grad_residual_norm
    residual_low = grad_residual.astype(jnp.bfloat16)
    attended_grad = jnp.dot(residual_low, output_full, preferred_element_type=jnp.float32).astype(
        jnp.bfloat16
    )
    output_term = jnp.dot(residual_low.T, attended, preferred_element_type=jnp.float32)
    delta = jnp.sum(
        (attended_grad.astype(jnp.float32) * attended.astype(jnp.float32)).reshape(
            block, groups_local, ratio, HD
        ),
        axis=3,
    )
    grad_grouped = attended_grad.reshape(block, groups_local, ratio, HD)
    back_keys, back_values = (
        lax.all_gather(travel[0], "ctx", axis=0, tiled=True),
        lax.all_gather(travel[1], "ctx", axis=0, tiled=True),
    )
    key_blocks = back_keys.reshape(context_count, block, groups_local, HD)
    value_blocks = back_values.reshape(context_count, block, groups_local, HD)
    starts = block * jnp.arange(context_count, dtype=jnp.int32)

    def backward_update(grad_query, key_block, value_block, allowed):
        mask = allowed[:, None, None, :]
        scores = (
            jnp.einsum(
                "qgrd,kgd->qgrk", query_grouped, key_block, preferred_element_type=jnp.float32
            )
            * scale
        )
        probs = jnp.where(mask, jnp.exp(scores - log_total[..., None]), 0.0)
        value_grad = jnp.einsum(
            "qgrk,qgrd->kgd",
            probs.astype(jnp.bfloat16),
            grad_grouped,
            preferred_element_type=jnp.float32,
        )
        prob_grad = jnp.einsum(
            "qgrd,kgd->qgrk", grad_grouped, value_block, preferred_element_type=jnp.float32
        )
        score_grad = (probs * (prob_grad - delta[..., None]) * scale).astype(jnp.bfloat16)
        grad_query = grad_query + jnp.einsum(
            "qgrk,kgd->qgrd", score_grad, key_block, preferred_element_type=jnp.float32
        )
        key_grad = jnp.einsum(
            "qgrk,qgrd->kgd", score_grad, query_grouped, preferred_element_type=jnp.float32
        )
        return (grad_query, key_grad.reshape(block, -1), value_grad.reshape(block, -1))

    def backward_visit(grad_query, item):
        key_block, value_block, key_start = item
        allowed = allowed_mask(key_start, block)
        grad_query, key_grad, value_grad = backward_update(
            grad_query, key_block, value_block, allowed
        )
        return (grad_query, (key_grad, value_grad))

    grad_query, (key_grads, value_grads) = lax.scan(
        backward_visit,
        jnp.zeros((block, groups_local, ratio, HD), jnp.float32),
        (key_blocks, value_blocks, starts),
    )
    own_key_grad, own_value_grad = (
        lax.psum_scatter(
            key_grads.reshape(context_count * block, -1).astype(jnp.bfloat16),
            "ctx",
            scatter_dimension=0,
            tiled=True,
        ).astype(jnp.float32),
        lax.psum_scatter(
            value_grads.reshape(context_count * block, -1).astype(jnp.bfloat16),
            "ctx",
            scatter_dimension=0,
            tiled=True,
        ).astype(jnp.float32),
    )
    query_grad = (
        rotate_back(grad_query.reshape(block, heads_local, HD), cosine, sine)
        .reshape(block, -1)
        .astype(jnp.bfloat16)
    )
    key_grad = (
        rotate_back(own_key_grad.reshape(block, groups_local, HD), cosine, sine)
        .reshape(block, -1)
        .astype(jnp.bfloat16)
    )
    value_grad = own_value_grad.astype(jnp.bfloat16)
    input_part = jnp.dot(query_grad, query_full.T, preferred_element_type=jnp.float32)
    input_part = input_part + jnp.dot(key_grad, key_full.T, preferred_element_type=jnp.float32)
    input_part = input_part + jnp.dot(value_grad, value_full.T, preferred_element_type=jnp.float32)
    normed_one_grad = lax.psum(input_part.astype(jnp.bfloat16), "tp").astype(jnp.float32)
    grad_input_norm, gain_one_term = norm_backward(inputs, inverse_one, gain_one, normed_one_grad)
    input_grad = (grad_residual + grad_input_norm)[None]
    query_term = jnp.dot(normed_one.T, query_grad, preferred_element_type=jnp.float32)
    key_term = jnp.dot(normed_one.T, key_grad, preferred_element_type=jnp.float32)
    value_term = jnp.dot(normed_one.T, value_grad, preferred_element_type=jnp.float32)
    (
        gain_one_share,
        query_share,
        key_share,
        value_share,
        output_share,
        gain_two_share,
        router_share,
    ) = (
        lax.psum_scatter(gain_one_term, ("fsdp", "ctx"), scatter_dimension=0, tiled=True),
        lax.psum_scatter(query_term, ("fsdp", "ctx"), scatter_dimension=0, tiled=True),
        lax.psum_scatter(key_term, ("fsdp", "ctx"), scatter_dimension=0, tiled=True),
        lax.psum_scatter(value_term, ("fsdp", "ctx"), scatter_dimension=0, tiled=True),
        lax.psum_scatter(output_term, ("fsdp", "ctx"), scatter_dimension=0, tiled=True),
        lax.psum_scatter(gain_two_term, ("fsdp", "ctx"), scatter_dimension=0, tiled=True),
        lax.psum_scatter(router_term, ("fsdp", "ctx"), scatter_dimension=0, tiled=True),
    )
    return (
        block_out,
        input_grad,
        gain_one_share,
        query_share,
        key_share,
        value_share,
        output_share,
        gain_two_share,
        router_share,
        gate_share,
        up_share,
        down_share,
    )


MESH = pl.DeviceIdType.MESH
f32 = jnp.float32
bf16 = jnp.bfloat16


def dot_nn(a, b, precision=None):
    return lax.dot_general(a, b, (((1,), (0,)), ((), ())), precision=precision, preferred_element_type=f32)


def dot_nt(a, b, precision=None):
    return lax.dot_general(a, b, (((1,), (1,)), ((), ())), precision=precision, preferred_element_type=f32)


def dot_tn(a, b, precision=None):
    return lax.dot_general(a, b, (((0,), (0,)), ((), ())), precision=precision, preferred_element_type=f32)


class Net:
    def __init__(self, send_sems, recv_sems):
        self.send_sems, self.recv_sems, self.copies, self.left = send_sems, recv_sems, [], set()

    def make(self, source, target, device, sends=None):
        at = len(self.copies)
        copy = pltpu.make_async_remote_copy(
            src_ref=source,
            dst_ref=target,
            send_sem=self.send_sems.at[at],
            recv_sem=self.recv_sems.at[at],
            device_id=device,
            device_id_type=MESH,
        )
        self.copies.append((copy, sends))
        return copy

    def send(self, source, target, device):
        copy = self.make(source, target, device)
        copy.start()
        return copy

    def drain(self, among=None):
        for at, (copy, sends) in enumerate(self.copies):
            if at in self.left or (among is not None and at not in among):
                continue
            self.left.add(at)
            if sends is None:
                copy.wait_send()
            else:
                pl.when(sends)(copy.wait_send)


class Line:
    def __init__(self, net, z, nz, device):
        self.net, self.z, self.nz, self.device = net, z, nz, device

    def both(self):
        z, nz = self.z, self.nz
        right, left = self.device(lax.min(z + 1, nz - 1)), self.device(lax.max(z - 1, 0))
        return ((z, right), (nz - 1 - z, left))

    def pass_on(self, step, views):
        copies = []
        for way, (rank, target) in enumerate(self.both()):
            sends = (rank >= step) & (rank < self.nz - 1)
            arrives = rank >= step + 1
            block = lax.clamp(0, self.z - step if way == 0 else self.z + step, self.nz - 1)
            for view in views:
                copy = self.net.make(view(block), view(block), target, sends)
                pl.when(sends)(copy.start)
                copies.append((copy, arrives))
        return copies

    def add_on(self, step, own, out, into):
        copies = []
        for way, (rank, target) in enumerate(self.both()):
            sends = rank <= step
            arrives = (rank >= 1) & (rank - 1 <= step)
            dest = self.nz - 1 - step + rank
            dest = lax.clamp(0, dest if way == 0 else self.nz - 1 - dest, self.nz - 1)
            copy = self.net.make(out(way, step), into(way, step), target, sends)

            def prepare():
                out(way, step)[...] = own(dest)[...].astype(bf16)
                if step > 0:

                    def add():
                        out(way, step)[...] = (own(dest)[...] + into(way, step - 1)[...].astype(f32)).astype(bf16)

                    pl.when(rank >= 1)(add)
                copy.start()

            pl.when(sends)(prepare)
            copies.append((copy, arrives))
        return copies

    def finish(self, total, into):
        for way, (rank, target) in enumerate(self.both()):

            def add():
                total[...] += into(way, self.nz - 2)[...].astype(f32)

            pl.when(rank >= 1)(add)


def arrive(copies):
    for copy, arrives in copies:
        pl.when(arrives)(copy.wait_recv)


def layer_kernel(
    dims,
    x_ref, g_ref, wq_ref, wk_ref, wv_ref, wo_ref, ga_ref, ge_ref, rt_ref, wg_ref, wu_ref, wd_ref, dl_ref, ec_ref,
    fr_ref,
    block_out, input_grad, small_out, gain_out, dqkv_out, dwo_out, dgu_out, dd_out,
    WP, SMT, X, WQ, WO, SMB, SMW, N1, CT, ST, SEGC, POSC, Q, K, V, PSC, ATT, AT, PP, PR, RES,
    N2, GTB, GA, WGU, WD, SWG, SWU, SWD, AA, PSX, GC, H, UG, PRD, MP, MR, BP, BR, DGU, DDT, GDS, GD,
    RB, RM, RBV, RMV, BOWN, MOWN, CO, CI, MO, MI, DGB, GUL, ZG, DDB, DDL, ZD, SG, SGF, SGT, SGZ, SGP, GRES, RL,
    AGS, AGR, DWO, RWO, ZWO, LWO, DS, DQ, DQKV, NG, NR, DWQ, RWQ, ZWQ, LWQ,
    SG1, SG1P, RSG1, EXB, EXG,
    send_sems, recv_sems, local_sems,
):
    nf, nz, hb, width, experts, half_ff, ndoc, chosen = dims
    rows = 2 * nz * hb
    half = nz * hb
    block = 2 * hb
    shard = width // (nf * nz)
    f, z, c = lax.axis_index("fsdp"), lax.axis_index("ctx"), lax.axis_index("tp")
    other = 1 - c
    own = f * nz + z
    net = Net(send_sems, recv_sems)
    device = lambda df, dz, core: {"fsdp": df, "ctx": dz, "tp": core}
    partner = device(f, z, other)
    line = Line(net, z, nz, lambda dz: device(f, dz, c))
    zs = [z, z + 1 - 2 * lax.rem(z, 2), lax.rem(z + 2, 4), 3 - z]
    fs = [f, f + 1 - 2 * lax.rem(f, 2), lax.rem(f + 2, 4), 3 - f]
    everyone = [(i, j, k) for k in range(2) for i in range(nf) for j in range(nz) if (i, j, k) != (0, 0, 0)]
    others = [device(fs[i], zs[j], lax.rem(c + k, 2)) for i, j, k in everyone]
    same = [(i, 0) for i in range(1, nf)] + [(i, j) for i in range(nf) for j in (3, 1, 2)]

    mine = pl.ds(pl.multiple_of(c * hb, hb), hb)
    loads = [
        pltpu.make_async_copy(x_ref.at[mine], X.at[c, z], local_sems.at[0]),
        pltpu.make_async_copy(g_ref.at[mine], GA.at[f, c, z], local_sems.at[1]),
        pltpu.make_async_copy(wo_ref, WO.at[f, z], local_sems.at[2]),
    ]
    row_experts = lambda at: pl.ds(at * nz, nz)
    shards = ((wg_ref, SWG), (wu_ref, SWU), (wd_ref, SWD))
    loads += [
        pltpu.make_async_copy(ref.at[row_experts(f)], staged.at[f], local_sems.at[3 + at])
        for at, (ref, staged) in enumerate(shards)
    ]
    unit = half_ff // 2
    units = lambda h: pl.ds(h * unit, unit)
    for copy in loads:
        copy.start()
    barrier = pltpu.get_barrier_semaphore()
    for peer in others:
        pl.semaphore_signal(barrier, inc=1, device_id=peer, device_id_type=MESH)

    for j in range(nz):
        WP[j, :, 0 : 2 * HD] = wq_ref[:, 2 * HD * j : 2 * HD * (j + 1)]
        WP[j, :, 2 * HD : 4 * HD] = jnp.concatenate(
            [wk_ref[:, HD * j : HD * (j + 1)], wv_ref[:, HD * j : HD * (j + 1)]], axis=1
        )
    base = jnp.concatenate(
        [ga_ref[...].astype(f32), ge_ref[...].astype(f32), jnp.zeros((14, shard), f32), rt_ref[...].astype(f32)],
        axis=0,
    )
    in_half = (lax.broadcasted_iota(jnp.int32, (32, 128), 1) < shard) == (lax.rem(z, 2) == 0)
    SMT[...] = jnp.where(in_half, jnp.concatenate([base, base], axis=1), 0.0).astype(bf16)
    SMB[f, z] = SMT[...]
    WQ[f, z] = WP[z]
    pl.semaphore_wait(barrier, len(others))

    sends_q = [net.send(WP.at[zs[k]], WQ.at[f, z], device(f, zs[k], c)) for k in range(1, nz)]
    sends_s = [net.send(SMT, SMB.at[f, z], device(f, zs[k], c)) for k in range(1, nz)]
    loads[0].wait()
    sends_x = [net.send(X.at[c, z], X.at[c, z], device(f, zs[k], c)) for k in range(1, nz)]
    forwards_x = [net.send(X.at[c, z], X.at[c, z], partner)]
    loads[2].wait()
    sends_o = [net.send(WO.at[f, z], WO.at[f, z], device(f, zs[k], c)) for k in range(1, nz)]
    loads[1].wait()
    view_g = [lambda at: GA.at[f, c, at]]
    chain_g = line.pass_on(0, view_g)
    weights = ([], [])

    def send_weights(h, k, which=(0, 1, 2)):
        for at in which:
            target, (ref, staged) = (units(2 * h), units(2 * h + 1), units(h))[at], shards[at]
            into = WD if staged is SWD else WGU
            weights[h].append(
                net.send(staged.at[:, zs[k], :, units(h)], into.at[:, z, :, target], device(f, zs[k], c))
            )

    def places(shape, dim):
        at = lax.broadcasted_iota(jnp.int32, shape, dim)
        core_at, rest = lax.div(at, half), lax.rem(at, half)
        return lax.div(rest, hb) * block + core_at * hb + lax.rem(rest, hb)

    def layout(position):
        segment = jnp.zeros_like(position)
        start = jnp.zeros_like(position)
        end = jnp.int32(0)
        for i in range(ndoc):
            length = dl_ref[0, i]
            end = end + length
            after = jnp.where(position >= end, 1, 0)
            segment = segment + after
            start = start + after * length
        return segment, position - start

    lane = lax.broadcasted_iota(jnp.int32, (1, 2 * HD), 1)
    former = lax.rem(lane, HD) < HD // 2
    is_key = lane < HD

    with jax.named_scope("tables0"):
        pos_col = places((rows, 1), 0)
        seg_col, offset = layout(pos_col)
        POSC[...] = pos_col
        SEGC[...] = seg_col
        pos_row = places((1, rows), 1)
        seg_row, unused = layout(pos_row)

    def swapped(v):
        return jnp.where(former, pltpu.roll(v, 2 * HD - HD // 2, 1), pltpu.roll(v, HD // 2, 1))

    for copy in sends_q:
        copy.wait_recv()
    sends_q2 = [net.send(WQ.at[f], WQ.at[f], device(fs[k], z, c)) for k in range(1, nf)]
    for copy in sends_s:
        copy.wait_recv()
    sends_s2 = [net.send(SMB.at[f], SMB.at[f], device(fs[k], z, c)) for k in range(1, nf)]
    sends_e = [
        net.send(ref.at[row_experts(fs[k])], staged.at[f], device(fs[k], z, c))
        for k in range(1, nf)
        for ref, staged in shards
    ]
    with jax.named_scope("tables1"):
        angle = offset.astype(f32) * fr_ref[0:1, :]
        CT[...] = jnp.cos(angle)
        ST[...] = jnp.where(former, -1.0, 1.0) * jnp.sin(angle)
    for copy in sends_s2:
        copy.wait_recv()
    for pair in range(nf * nz // 2):
        at_f, at_z = pair // (nz // 2), 2 * (pair % (nz // 2))
        SMW[:, 128 * pair : 128 * pair + 128] = SMB[at_f, at_z] + SMB[at_f, at_z + 1]

    def norm_block(at_c, at_z):
        v = X[at_c, at_z].astype(f32)
        inverse = lax.rsqrt(jnp.mean(v * v, axis=1, keepdims=True) + epsilon)
        at = pl.ds(pl.multiple_of((at_c * nz + at_z) * hb, hb), hb)
        N1[at, :] = (v * inverse * SMW[0:1, :].astype(f32)).astype(bf16)

    norm_block(c, z)
    for k in range(1, nz):
        sends_x[k - 1].wait_recv()
        forwards_x.append(net.send(X.at[c, zs[k]], X.at[c, zs[k]], partner))
        norm_block(c, zs[k])
    for k in range(nz):
        forwards_x[k].wait_recv()
        norm_block(other, zs[k])
    for copy in sends_q2:
        copy.wait_recv()
    with jax.named_scope("qkv"):
        projected = dot_nn(N1[...], WQ[...].reshape(width, 4 * HD))
        cosine, sine = CT[...], ST[...]
        q_part, kv_part = projected[:, : 2 * HD], projected[:, 2 * HD :]
        Q[...] = (q_part * cosine + swapped(q_part) * sine).astype(bf16)
        kv = jnp.where(is_key, kv_part * cosine + swapped(kv_part) * sine, kv_part).astype(bf16)
        K[...] = kv[:, :HD]
        V[...] = kv[:, HD:]
    arrive(chain_g)
    chain_g = line.pass_on(1, view_g)
    for copy in sends_o:
        copy.wait_recv()
    sends_o2 = [net.send(WO.at[f], WO.at[f], device(fs[k], z, c)) for k in range(1, nf)]

    scale = HD ** (-0.5)
    step = 2 * hb

    def attend(i, carry):
        at = pl.ds(pl.multiple_of(i * step, step), step)
        mask = (SEGC[at, :] == seg_row) & (pos_row <= POSC[at, :])
        q = Q[at, :]
        pieces = []
        for r in range(2):
            scores = dot_nt(q[:, r * HD : (r + 1) * HD], K[...]) * scale
            scores = jnp.where(mask, scores, masked_score)
            peak = jnp.max(scores, axis=1, keepdims=True)
            weights = jnp.where(mask, jnp.exp(scores - peak), 0.0)
            total = jnp.sum(weights, axis=1, keepdims=True)
            pieces.append(dot_nn(weights.astype(bf16), V[...]) / total)
            PSC[r, at, :] = (weights / total).astype(bf16)
        out = jnp.concatenate(pieces, axis=1).astype(bf16)
        at_c, at_z = lax.div(2 * i, nz), lax.rem(2 * i, nz)
        ATT[at_c, pl.ds(at_z, 2)] = out.reshape(2, hb, 2 * HD)
        return carry

    with jax.named_scope("attend"):
        lax.fori_loop(0, rows // step, attend, 0)
    columns = pl.ds(pl.multiple_of(z * 2 * HD, 2 * HD), 2 * HD)
    sends_a = [
        net.send(ATT.at[:, zs[k]], AT.at[:, :, columns], device(f, zs[k], c)) for k in range(1, nz)
    ]
    AT[:, :, columns] = ATT[:, z]
    arrive(chain_g)
    chain_g = line.pass_on(2, view_g)
    for copy in loads[3:]:
        copy.wait()
    for copy in sends_e:
        copy.wait_recv()
    send_weights(0, 3, (0, 1))
    for copy in sends_a:
        copy.wait_recv()
    for copy in sends_o2:
        copy.wait_recv()
    wd_full = lambda: WD[...].reshape(width, half_ff)
    wgu_full = lambda: WGU[...].reshape(width, 2 * half_ff)
    lower, upper = pl.ds(0, nz // 2), pl.ds(nz // 2, nz // 2)
    across = [None, device(fs[1], z, c), device(fs[2], z, c), device(fs[3], z, c)]

    def second_hop(ref):
        return [net.send(ref.at[f, c], ref.at[f, c], across[k]) for k in (1, 2)]

    def third_hop(ref, k):
        part, to = ((lower, across[2]), (upper, across[1]))[k - 1]
        return net.send(ref.at[fs[k], c, part], ref.at[fs[k], c, part], to)

    arrive(chain_g)
    sends_g2 = second_hop(GA)
    forwards_g = [net.send(GA.at[f, c], GA.at[f, c], partner)]
    with jax.named_scope("proj"):
        part = dot_nt(AT[...].reshape(block, nz * 2 * HD), WO[...].reshape(width, nz * 2 * HD))
        PP[...] = part.reshape(2, hb, width)
    send_p = net.send(PP.at[other], PR, partner)
    x_own = X[c, z].astype(f32)
    gain_two = SMW[1:2, :].astype(f32)
    send_p.wait_recv()
    residual = x_own + PP[c] + PR[...]
    RES[...] = residual
    inverse_two = lax.rsqrt(jnp.mean(residual * residual, axis=1, keepdims=True) + epsilon)
    N2[f, c, z] = (residual * inverse_two * gain_two).astype(bf16)
    normed_two = N2[f, c, z]
    logits = dot_nt(SMW[16 : 16 + experts, :], normed_two)
    expert_at = lax.broadcasted_iota(jnp.int32, (experts, hb), 0)
    route = ec_ref[...]
    route = jnp.where(c == 0, route, pltpu.roll(route, 128 - hb, 1))
    picked = jnp.zeros((experts, hb), jnp.bool_)
    for j in range(chosen):
        picked = picked | (route[j : j + 1, 0:hb] == expert_at)
    peak = jnp.max(jnp.where(picked, logits, masked_score), axis=0, keepdims=True)
    weight = jnp.where(picked, jnp.exp(logits - peak), 0.0)
    gates = weight / jnp.sum(weight, axis=0, keepdims=True)
    GTB[f, c, z] = jnp.concatenate([gates, jnp.zeros((experts, 128 - hb), f32)], axis=1)
    view_n = [lambda at: N2.at[f, c, at], lambda at: GTB.at[f, c, at]]
    chain_n = line.pass_on(0, view_n)
    send_weights(0, 3, (2,))

    arrive(chain_n)
    chain_n = line.pass_on(1, view_n)
    send_weights(0, 2, (0,))
    arrive(chain_n)
    chain_n = line.pass_on(2, view_n)
    send_weights(0, 2, (1, 2))
    send_weights(0, 1)
    for k in (3, 2, 1):
        send_weights(1, k)
    sends_g3 = []
    for k in (1, 2):
        sends_g2[k - 1].wait_recv()
        sends_g3.append(third_hop(GA, k))
        forwards_g.append(net.send(GA.at[fs[k], c], GA.at[fs[k], c], partner))
    arrive(chain_n)
    sends_n2 = second_hop(N2)
    sends_t2 = [net.send(GTB.at[f, c], GTB.at[f, c], across[k]) for k in (1, 2, 3)]
    forwards_n = [net.send(N2.at[f, c], N2.at[f, c], partner)]
    forwards_t = [net.send(GTB.at[f, c], GTB.at[f, c], partner)]
    for copy in sends_g3:
        copy.wait_recv()
    forwards_g.append(net.send(GA.at[fs[3], c], GA.at[fs[3], c], partner))

    WGU[:, z, :, 0:unit] = SWG[:, z, :, 0:unit]
    WGU[:, z, :, unit : 2 * unit] = SWU[:, z, :, 0:unit]
    WGU[:, z, :, 2 * unit : 3 * unit] = SWG[:, z, :, unit : 2 * unit]
    WGU[:, z, :, 3 * unit : 4 * unit] = SWU[:, z, :, unit : 2 * unit]
    WD[:, z] = SWD[:, z]
    chosen_row = jnp.where(
        lax.broadcasted_iota(jnp.int32, (experts, 128), 0) == own, 1.0, 0.0
    ).astype(f32)
    sends_d, sends_b, exchange_b, exchange_m = [], {}, {}, {}
    low_half = z < nz // 2
    in_order = [jnp.where(low_half, 3, 0), jnp.where(low_half, 2, 1), zs[1], z]
    grads_z, grads_f = ([], []), ([], [])

    def send_grads(h, k):
        to = device(f, zs[k], c)
        grads_z[h].append(net.send(DGB.at[h, :, zs[k]], ZG.at[h, z], to))
        grads_z[h].append(net.send(DDB.at[h, :, zs[k]], ZD.at[h, z], to))

    def spread_grads(h):
        ZG[h, z] = DGB[h, :, z]
        ZD[h, z] = DDB[h, :, z]
        for copy in grads_z[h]:
            copy.wait_recv()
        for k in range(1, nf):
            grads_f[h].append(
                net.send(ZG.at[h, :, fs[k]], GUL.at[f, :, :, pl.ds(2 * h * unit, 2 * unit)], across[k])
            )
            grads_f[h].append(net.send(ZD.at[h, :, fs[k]], DDL.at[f, :, :, units(h)], across[k]))
        GUL[f, :, :, 2 * h * unit : 2 * (h + 1) * unit] = ZG[h, :, f]
        DDL[f, :, :, h * unit : (h + 1) * unit] = ZD[h, :, f]

    def expert_part(h, k):
        at_f = fs[k]
        tokens = N2[at_f].reshape(rows, width)
        grads = GA[at_f].reshape(rows, width)
        with jax.named_scope("gateup"):
            PSX[...] = dot_nn(tokens, WGU[:, :, :, 2 * h * unit : 2 * (h + 1) * unit].reshape(width, 2 * unit))
        with jax.named_scope("cotangent"):
            AA[...] = dot_nn(grads, WD[:, :, :, h * unit : (h + 1) * unit].reshape(width, unit))
        if h == 0:
            with jax.named_scope("gatecol"):
                for piece in range(2 * nz):
                    tile = GTB[at_f, piece // nz, piece % nz][:, 0:hb]
                    GC[k, piece * hb : (piece + 1) * hb, :] = dot_tn(tile, chosen_row, lax.Precision.HIGHEST)

        def expert_chunk(i, carry):
            at = pl.ds(pl.multiple_of(i * 64, 64), 64)
            gate_pre = PSX[at, 0:unit]
            up_pre = PSX[at, unit : 2 * unit]
            raw = AA[at, :]
            gate = GC[k, at, :]
            sigmoid = jax.nn.sigmoid(gate_pre)
            silu = gate_pre * sigmoid
            act = silu * up_pre
            PRD[at, :] = (act * raw).astype(bf16)
            H[k, at, h * unit : (h + 1) * unit] = (act * gate).astype(bf16)
            grad = raw * gate
            UG[k, at, 2 * h * unit : (2 * h + 1) * unit] = (
                grad * up_pre * sigmoid * (1.0 + gate_pre * (1.0 - sigmoid))
            ).astype(bf16)
            UG[k, at, (2 * h + 1) * unit : 2 * (h + 1) * unit] = (grad * silu).astype(bf16)
            return carry

        with jax.named_scope("chunk"):
            lax.fori_loop(0, rows // 64, expert_chunk, 0)
        if h == 1:
            with jax.named_scope("back"):
                BP[at_f] = dot_nt(UG[k], WGU[...].reshape(width, 2 * half_ff)).astype(bf16).reshape(2, nz, hb, width)
            exchange_b[k] = net.send(BP.at[at_f, other], BR.at[at_f], partner)
        with jax.named_scope("gdot"):
            dots = dot_nt(jnp.ones((8, unit), bf16), PRD[...])
            GDS[k] = dots if h == 0 else GDS[k] + dots
        if h == 1:
            for j in range(nz):
                for t in range(2):
                    to_z, to_c = zs[j], lax.rem(c + t, 2)
                    lanes = pl.ds(pl.multiple_of((to_c * (nz // 2) + lax.div(to_z, 2)) * 128, 128), 128)
                    if (k, j, t) != (0, 0, 0):
                        sends_d.append(
                            net.send(GDS.at[k, pl.ds(0, 1), lanes], GD.at[f, z, c, pl.ds(0, 1)], device(at_f, to_z, to_c))
                        )
                    else:
                        GD[f, z, c] = GDS[0, :, lanes]
            with jax.named_scope("mix"):
                MP[at_f] = dot_nt(H[k], WD[...].reshape(width, half_ff)).astype(bf16).reshape(2, nz, hb, width)
            exchange_m[k] = net.send(MP.at[at_f, other], MR.at[at_f], partner)
        with jax.named_scope("wgrad"):
            gate_up = dot_tn(UG[k, :, 2 * h * unit : 2 * (h + 1) * unit], tokens)
            down = dot_tn(H[k, :, h * unit : (h + 1) * unit], grads)
            first = k == (0, 3)[h]
            DGU[...] = gate_up if first else DGU[...] + gate_up
            DDT[...] = down if first else DDT[...] + down

    def shed(h):
        with jax.named_scope("transpose"):
            DGB[h] = jnp.transpose(DGU[...]).astype(bf16).reshape(nf, nz, shard, 2 * unit)
            DDB[h] = jnp.transpose(DDT[...]).astype(bf16).reshape(nf, nz, shard, unit)

    for copy in weights[0]:
        copy.wait_recv()
    for k in range(nf):
        if k == 1:
            sends_n3 = []
            for i in (1, 2):
                sends_n2[i - 1].wait_recv()
                sends_n3.append(third_hop(N2, i))
                forwards_n.append(net.send(N2.at[fs[i], c], N2.at[fs[i], c], partner))
                sends_t2[i - 1].wait_recv()
                forwards_t.append(net.send(GTB.at[fs[i], c], GTB.at[fs[i], c], partner))
        if k == 3:
            for copy in sends_n3:
                copy.wait_recv()
            forwards_n.append(net.send(N2.at[fs[k], c], N2.at[fs[k], c], partner))
            sends_t2[2].wait_recv()
            forwards_t.append(net.send(GTB.at[fs[k], c], GTB.at[fs[k], c], partner))
        forwards_g[k].wait_recv()
        forwards_n[k].wait_recv()
        forwards_t[k].wait_recv()
        expert_part(0, k)
    shed(0)
    for k in (3, 2, 1):
        send_grads(0, k)
    for copy in weights[1]:
        copy.wait_recv()
    own_half = ((lower, 1), (upper, 2))

    def spread(k, exchange, part, back, total, via, into, order):
        at_f = fs[k]
        exchange[k].wait_recv()
        if k == 0:
            total[...] = part[at_f, c].astype(f32) + back[at_f].astype(f32)
            return []
        if k == 3:
            part[at_f, c] = (part[at_f, c].astype(f32) + back[at_f].astype(f32)).astype(bf16)
            return [net.send(part.at[at_f, c, half_at], via.at[to - 1], across[to]) for half_at, to in own_half]
        return None

    def spread_near(k, firsts, part, back, via, into, order):
        at_f = fs[k]
        half_at, other_half = (upper, lower) if k == 1 else (lower, upper)
        firsts[2 - k].wait_recv()
        part[at_f, c, half_at] = (
            part[at_f, c, half_at].astype(f32) + back[at_f, half_at].astype(f32) + via[2 - k].astype(f32)
        ).astype(bf16)
        part[at_f, c, other_half] = (
            part[at_f, c, other_half].astype(f32) + back[at_f, other_half].astype(f32)
        ).astype(bf16)
        return [net.send(part.at[at_f, c, at], into.at[k - 1, at], across[k]) for at in order]

    sends_m = {}
    expert_part(1, 3)
    firsts_b = spread(3, exchange_b, BP, BR, BOWN, RBV, RB, in_order)
    firsts_m = spread(3, exchange_m, MP, MR, MOWN, RMV, RM, in_order)
    expert_part(1, 1)
    expert_part(1, 2)
    for k in (1, 2):
        exchange_b[k].wait_recv()
        sends_b[k] = spread_near(k, firsts_b, BP, BR, RBV, RB, in_order)
    expert_part(1, 0)
    for k in (1, 2):
        exchange_m[k].wait_recv()
        sends_m[k] = spread_near(k, firsts_m, MP, MR, RMV, RM, in_order)
    spread(0, exchange_b, BP, BR, BOWN, RBV, RB, in_order)
    spread(0, exchange_m, MP, MR, MOWN, RMV, RM, in_order)

    shed(1)
    send_grads(1, 3)

    for copy in sends_d:
        copy.wait_recv()
    dots = jnp.concatenate(
        [
            GD[e // nz, e % nz, 0][0:1, :] + GD[e // nz, e % nz, 1][0:1, :]
            for e in range(experts)
        ],
        axis=0,
    )
    dots = jnp.where(lax.rem(z, 2) == 0, dots, pltpu.roll(dots, 128 - hb, 1))[:, 0:hb]
    gates = GTB[f, c, z][:, 0:hb]
    logit_grad = gates * (dots - jnp.sum(gates * dots, axis=0, keepdims=True))
    router_t = SMW[16 : 16 + experts, :].astype(f32)
    SG[0:experts, :] = dot_nn(logit_grad, N2[f, c, z].astype(f32), lax.Precision.HIGHEST)
    GRES[...] = dot_tn(logit_grad, router_t, lax.Precision.HIGHEST)
    residual = RES[...]
    inverse_two = lax.rsqrt(jnp.mean(residual * residual, axis=1, keepdims=True) + epsilon)

    own_b, out_b, into_b = (lambda at: BOWN.at[at]), (lambda w, t: CO.at[w, t]), (lambda w, t: CI.at[w, t])

    def take_block(at):
        for k in (1, 2):
            sends_b[k][at].wait_recv()
            BOWN[in_order[at]] += RB[k - 1, in_order[at]].astype(f32)

    sums = []
    for t in range(nz):
        take_block(t)
        if t > 0:
            arrive(chain_b)
        if t < nz - 1:
            at_sums = len(net.copies)
            chain_b = line.add_on(t, own_b, out_b, into_b)
            sums.extend(range(at_sums, len(net.copies)))
    line.finish(BOWN.at[z], into_b)

    grad_two = BOWN[z] + GRES[...]
    scaled = grad_two * gain_two
    grad_res = (
        GA[f, c, z].astype(f32)
        + inverse_two * scaled
        - residual * (inverse_two * inverse_two * inverse_two) * jnp.mean(scaled * residual, axis=1, keepdims=True)
    )
    GRES[...] = grad_res
    RL[c] = grad_res.astype(bf16)
    send_r = net.send(RL.at[c], RL.at[c], partner)
    gain_term = jnp.sum(grad_two * residual * inverse_two, axis=0, keepdims=True)
    SG[experts : experts + 8, :] = jnp.broadcast_to(gain_term, (8, width))
    wide = width // nf
    block_lanes = lambda at: pl.ds(pl.multiple_of(at * wide, 128), wide)
    sends_sg = [net.send(SG.at[:, block_lanes(fs[k])], SGF.at[k - 1], device(fs[k], z, c)) for k in range(1, nf)]
    send_r.wait_recv()
    low = RL[...].reshape(block, width)
    with jax.named_scope("attgrad"):
        AGS[...] = dot_nn(low, WO[...].reshape(width, nz * 2 * HD)).astype(bf16).reshape(2, hb, nz * 2 * HD)
    sends_ag = [
        net.send(
            AGS.at[:, :, pl.ds(pl.multiple_of(zs[k] * 2 * HD, 2 * HD), 2 * HD)],
            AGR.at[:, z],
            device(f, zs[k], c),
        )
        for k in range(1, nz)
    ]
    AGR[:, z] = AGS[:, :, columns]
    for k in (1, 2):
        for at in range(nz):
            sends_m[k][at].wait_recv()
        MOWN[...] += RM[k - 1].astype(f32)
    own_m, out_m, into_m = (lambda at: MOWN.at[at]), (lambda w, t: MO.at[w, t]), (lambda w, t: MI.at[w, t])
    chain_m = line.add_on(0, own_m, out_m, into_m)
    send_grads(1, 2)
    send_grads(1, 1)
    with jax.named_scope("outgrad"):
        DWO[...] = (
            dot_tn(low, AT[...].reshape(block, nz * 2 * HD))
            .astype(bf16)
            .reshape(nf, nz, shard, nz * 2 * HD)
        )
    sends_wo = [net.send(DWO.at[fs[k]], RWO.at[k - 1], device(fs[k], z, c)) for k in range(1, nf)]

    for copy in sends_ag:
        copy.wait_recv()

    def backward(i, carry):
        at = pl.ds(pl.multiple_of(i * step, step), step)
        at_c, at_z = lax.div(2 * i, nz), lax.rem(2 * i, nz)
        grad = AGR[at_c, pl.ds(at_z, 2)].reshape(step, 2 * HD)
        out = ATT[at_c, pl.ds(at_z, 2)].reshape(step, 2 * HD)
        both = grad.astype(f32) * out.astype(f32)
        pieces = []
        for r in range(2):
            delta = jnp.sum(both[:, r * HD : (r + 1) * HD], axis=1, keepdims=True)
            prob_grad = dot_nt(grad[:, r * HD : (r + 1) * HD], V[...])
            probs = PSC[r, at, :].astype(f32)
            score_grad = (probs * (prob_grad - delta) * scale).astype(bf16)
            DS[r, at, :] = score_grad
            pieces.append(dot_nn(score_grad, K[...]))
        DQ[at, :] = jnp.concatenate(pieces, axis=1)
        return carry

    with jax.named_scope("attback"):
        lax.fori_loop(0, rows // step, backward, 0)
    with jax.named_scope("kvgrad"):
        grads = AGR[...].reshape(rows, 2 * HD)
        key_t = dot_tn(Q[:, 0:HD], DS[0]) + dot_tn(Q[:, HD : 2 * HD], DS[1])
        value_t = dot_tn(grads[:, 0:HD], PSC[0]) + dot_tn(grads[:, HD : 2 * HD], PSC[1])
        kv_grad = jnp.transpose(jnp.concatenate([key_t, value_t], axis=0))
        cosine, sine = CT[...], ST[...]
        q_grad = DQ[...]
        DQKV[:, 0 : 2 * HD] = (q_grad * cosine - swapped(q_grad) * sine).astype(bf16)
        DQKV[:, 2 * HD : 4 * HD] = jnp.where(
            is_key, kv_grad * cosine - swapped(kv_grad) * sine, kv_grad
        ).astype(bf16)
    with jax.named_scope("ingrad"):
        NG[...] = dot_nt(DQKV[...], WQ[...].reshape(width, 4 * HD)).astype(bf16).reshape(2, nz, hb, width)
    send_ng = net.send(NG.at[other], NR, partner)
    arrive(chain_m)
    chain_m = line.add_on(1, own_m, out_m, into_m)
    with jax.named_scope("qkvgrad"):
        DWQ[...] = (
            jnp.transpose(dot_tn(DQKV[...], N1[...])).astype(bf16).reshape(nf, nz, shard, 4 * HD)
        )
    sends_wq = [net.send(DWQ.at[fs[k]], RWQ.at[k - 1], device(fs[k], z, c)) for k in range(1, nf)]
    small = SG[:, block_lanes(f)]
    for k in range(1, nf):
        sends_sg[k - 1].wait_recv()
        small = small + SGF[k - 1]
    SGT[...] = small
    pair_lanes = lambda at: pl.ds(pl.multiple_of(lax.div(at, 2) * 128, 128), 128)
    sends_sz = [net.send(SGT.at[:, pair_lanes(zs[k])], SGZ.at[k - 1], device(f, zs[k], c)) for k in range(1, nz)]
    send_ng.wait_recv()
    net.drain(sums)
    BOWN[...] = NG[c].astype(f32) + NR[...].astype(f32)
    chain_g1 = line.add_on(0, own_b, out_b, into_b)
    arrive(chain_m)
    chain_m = line.add_on(2, own_m, out_m, into_m)
    arrive(chain_g1)
    chain_g1 = line.add_on(1, own_b, out_b, into_b)

    spread_grads(0)
    arrive(chain_g1)
    chain_g1 = line.add_on(2, own_b, out_b, into_b)

    total = DWO[f].astype(f32)
    for k in range(1, nf):
        sends_wo[k - 1].wait_recv()
        total = total + RWO[k - 1].astype(f32)
    ZWO[...] = total.astype(bf16)
    sends_wo2 = [net.send(ZWO.at[zs[k]], LWO.at[z], device(f, zs[k], c)) for k in range(1, nz)]
    LWO[z] = ZWO[z]
    total = DWQ[f].astype(f32)
    for k in range(1, nf):
        sends_wq[k - 1].wait_recv()
        total = total + RWQ[k - 1].astype(f32)
    ZWQ[...] = total.astype(bf16)
    sends_wq2 = [net.send(ZWQ.at[zs[k]], LWQ.at[z], device(f, zs[k], c)) for k in range(1, nz)]
    LWQ[z] = ZWQ[z]
    spread_grads(1)
    small = SGT[:, pair_lanes(z)]
    for k in range(1, nz):
        sends_sz[k - 1].wait_recv()
        small = small + SGZ[k - 1]
    SGP[0] = small
    send_sp = net.send(SGP.at[0], SGP.at[1], partner)
    arrive(chain_g1)
    line.finish(BOWN.at[z], into_b)
    grad_one = BOWN[z]
    gain_one = SMW[0:1, :].astype(f32)
    x_own = X[c, z].astype(f32)
    inverse = lax.rsqrt(jnp.mean(x_own * x_own, axis=1, keepdims=True) + epsilon)
    gain_term = jnp.sum(grad_one * x_own * inverse, axis=0, keepdims=True)
    SG1[0] = jnp.broadcast_to(gain_term, (8, width))
    send_g1 = net.send(SG1.at[0], SG1.at[1], partner)
    scaled = grad_one * gain_one
    EXG[c] = (
        GRES[...]
        + inverse * scaled
        - x_own * (inverse * inverse * inverse) * jnp.mean(scaled * x_own, axis=1, keepdims=True)
    )
    send_ig = net.send(EXG.at[c], EXG.at[c], partner)
    send_g1.wait_recv()
    SG1P[...] = SG1[0] + SG1[1]
    lanes_of = lambda df, dz: pl.ds(pl.multiple_of((df * (nz // 2) + lax.div(dz, 2)) * 128, 128), 128)
    sends_g1 = [
        net.send(SG1P.at[pl.ds(0, 1), lanes_of(fs[i], zs[j])], RSG1.at[f, z, pl.ds(0, 1)], device(fs[i], zs[j], c))
        for i, j in same
    ]
    RSG1[f, z] = SG1P[:, lanes_of(f, z)]

    arrive(chain_m)
    line.finish(MOWN.at[z], into_m)
    EXB[c] = (RES[...] + MOWN[z]).astype(bf16)
    send_bo = net.send(EXB.at[c], EXB.at[c], partner)
    send_sp.wait_recv()
    small_out[...] = SGP[0] + SGP[1]
    for copy in sends_wo2:
        copy.wait_recv()
    total = LWO[0].astype(f32)
    for j in range(1, nz):
        total = total + LWO[j].astype(f32)
    dwo_out[...] = total
    for copy in sends_wq2:
        copy.wait_recv()
    dqkv_out[...] = LWQ[...]
    for copy in grads_f[0] + grads_f[1]:
        copy.wait_recv()
    outs = [
        pltpu.make_async_copy(GUL, dgu_out, local_sems.at[8]),
        pltpu.make_async_copy(DDL, dd_out, local_sems.at[9]),
    ]
    for copy in outs:
        copy.start()
    for copy in sends_g1:
        copy.wait_recv()
    small = jnp.zeros((1, 128), f32)
    for i in range(nf):
        for j in range(nz):
            small = small + RSG1[i, j, 0:1]
    gain_out[...] = jnp.broadcast_to(small, (8, 128))
    send_bo.wait_recv()
    block_out[...] = EXB[...].reshape(block, width)
    send_ig.wait_recv()
    input_grad[...] = EXG[...].reshape(block, width)
    for copy in outs:
        copy.wait()
    net.drain()


def finish_kernel(
    dims, block_ref, input_ref, small_ref, gain_ref, dqkv_ref, dwo_ref, dgu_ref, dd_ref,
    block_out, input_out, gain1_out, q_out, k_out, v_out, o_out, gain2_out, router_out, gate_out, up_out, down_out,
):
    nz, experts, half_ff, shard = dims
    block_out[...] = block_ref[...]
    input_out[...] = input_ref[...]
    unit = half_ff // 2
    for h in range(2):
        gate_out[:, :, h * unit : (h + 1) * unit] = dgu_ref[:, :, 2 * h * unit : (2 * h + 1) * unit].astype(f32)
        up_out[:, :, h * unit : (h + 1) * unit] = dgu_ref[:, :, (2 * h + 1) * unit : 2 * (h + 1) * unit].astype(f32)
    down_out[...] = dd_ref[...].astype(f32)
    even = lax.rem(lax.axis_index("ctx"), 2) == 0
    pick = lambda v: jnp.where(even, v, pltpu.roll(v, 128 - shard, 1))[:, 0:shard]

    def once():
        gain1_out[...] = pick(gain_ref[...])[0:1]
        small = pick(small_ref[...])
        router_out[...] = small[0:experts]
        gain2_out[...] = small[experts : experts + 1]
        o_out[...] = dwo_ref[...]
        for j in range(nz):
            q_out[:, 2 * HD * j : 2 * HD * (j + 1)] = dqkv_ref[j, :, 0 : 2 * HD].astype(f32)
        for at, ref in ((2, k_out), (3, v_out)):
            ref[...] = jnp.concatenate(
                [dqkv_ref[j, :, at * HD : (at + 1) * HD].astype(f32) for j in range(nz)], axis=1
            )

    pl.when(pl.program_id(0) == 0)(once)


def fast_local(
    nf, nz,
    hidden_in, out_grad, attention_gain, query_weight, key_weight, value_weight, output_weight,
    expert_gain, router_weight, gate_weight, up_weight, down_weight, doc_lengths, expert_choice,
):
    block, width = hidden_in.shape[1], hidden_in.shape[2]
    hb = block // 2
    experts, shard, half_ff = gate_weight.shape
    ndoc, chosen = doc_lengths.shape[1], expert_choice.shape[2]
    rows = nz * block
    halfway = HD // 2
    frequency = np.float32(rope_base) ** (-np.arange(halfway, dtype=np.float32) / np.float32(halfway))
    frequency = jnp.asarray(np.tile(np.tile(frequency, 4)[None], (8, 1)).astype(np.float32))

    vm = pl.BlockSpec(memory_space=pltpu.VMEM)
    anywhere = pl.BlockSpec(memory_space=pl.ANY)
    shape = lambda s, d: jax.ShapeDtypeStruct(s, d)
    W = nz * 2 * HD
    scratch = dict(
        WP=((nz, shard, 4 * HD), bf16), SMT=((32, 128), bf16),
        X=((2, nz, hb, width), bf16), WQ=((nf, nz, shard, 4 * HD), bf16), WO=((nf, nz, shard, W), bf16),
        SMB=((nf, nz, 32, 128), bf16), SMW=((32, width), bf16), N1=((rows, width), bf16),
        CT=((rows, 128), f32), ST=((rows, 128), f32), SEGC=((rows, 1), jnp.int32), POSC=((rows, 1), jnp.int32),
        Q=((rows, 2 * HD), bf16), K=((rows, HD), bf16), V=((rows, HD), bf16), PSC=((2, rows, rows), bf16),
        ATT=((2, nz, hb, 2 * HD), bf16), AT=((2, hb, W), bf16), PP=((2, hb, width), f32), PR=((hb, width), f32),
        RES=((hb, width), f32),
        N2=((nf, 2, nz, hb, width), bf16), GTB=((nf, 2, nz, experts, 128), f32), GA=((nf, 2, nz, hb, width), bf16),
        WGU=((nf, nz, shard, 2 * half_ff), bf16), WD=((nf, nz, shard, half_ff), bf16),
        SWG=((nf, nz, shard, half_ff), bf16), SWU=((nf, nz, shard, half_ff), bf16), SWD=((nf, nz, shard, half_ff), bf16),
        AA=((rows, half_ff // 2), f32), PSX=((rows, half_ff), f32), GC=((nf, rows, 128), f32),
        H=((nf, rows, half_ff), bf16), UG=((nf, rows, 2 * half_ff), bf16), PRD=((rows, half_ff // 2), bf16),
        MP=((nf, 2, nz, hb, width), bf16), MR=((nf, nz, hb, width), bf16),
        BP=((nf, 2, nz, hb, width), bf16), BR=((nf, nz, hb, width), bf16),
        DGU=((half_ff, width), f32), DDT=((half_ff // 2, width), f32),
        GDS=((nf, 8, rows), f32), GD=((nf, nz, 2, 8, 128), f32),
        RB=((2, nz, hb, width), bf16), RM=((2, nz, hb, width), bf16),
        RBV=((2, nz // 2, hb, width), bf16), RMV=((2, nz // 2, hb, width), bf16),
        BOWN=((nz, hb, width), f32), MOWN=((nz, hb, width), f32),
        CO=((2, nz - 1, hb, width), bf16), CI=((2, nz - 1, hb, width), bf16),
        MO=((2, nz - 1, hb, width), bf16), MI=((2, nz - 1, hb, width), bf16),
        DGB=((2, nf, nz, shard, half_ff), bf16), GUL=((nf, nz, shard, 2 * half_ff), bf16), ZG=((2, nz, nf, shard, half_ff), bf16),
        DDB=((2, nf, nz, shard, half_ff // 2), bf16), DDL=((nf, nz, shard, half_ff), bf16), ZD=((2, nz, nf, shard, half_ff // 2), bf16),
        SG=((experts + 8, width), f32), SGF=((nf - 1, experts + 8, width // nf), f32),
        SGT=((experts + 8, width // nf), f32), SGZ=((nz - 1, experts + 8, 128), f32), SGP=((2, experts + 8, 128), f32),
        GRES=((hb, width), f32), RL=((2, hb, width), bf16),
        AGS=((2, hb, W), bf16), AGR=((2, nz, hb, 2 * HD), bf16),
        DWO=((nf, nz, shard, W), bf16), RWO=((nf - 1, nz, shard, W), bf16),
        ZWO=((nz, shard, W), bf16), LWO=((nz, shard, W), bf16),
        DS=((2, rows, rows), bf16), DQ=((rows, 2 * HD), f32),
        DQKV=((rows, 4 * HD), bf16), NG=((2, nz, hb, width), bf16), NR=((nz, hb, width), bf16),
        DWQ=((nf, nz, shard, 4 * HD), bf16), RWQ=((nf - 1, nz, shard, 4 * HD), bf16),
        ZWQ=((nz, shard, 4 * HD), bf16), LWQ=((nz, shard, 4 * HD), bf16),
        SG1=((2, 8, width), f32), SG1P=((8, width), f32), RSG1=((nf, nz, 8, 128), f32),
        EXB=((2, hb, width), bf16), EXG=((2, hb, width), f32),
    )
    slots = 320
    out = pl.pallas_call(
        functools.partial(layer_kernel, (nf, nz, hb, width, experts, half_ff, ndoc, chosen)),
        name="layer",
        out_shape=(
            shape((block, width), bf16), shape((block, width), f32), shape((experts + 8, 128), f32),
            shape((8, 128), f32), shape((nz, shard, 4 * HD), bf16), shape((shard, W), f32),
            shape((nf, nz, shard, 2 * half_ff), bf16), shape((nf, nz, shard, half_ff), bf16),
        ),
        in_specs=[anywhere] * 2 + [vm] * 3 + [anywhere] + [vm] * 3 + [anywhere] * 3
        + [pl.BlockSpec(memory_space=pltpu.SMEM), vm, vm],
        out_specs=(vm,) * 6 + (anywhere,) * 2,
        scratch_shapes=[pltpu.VMEM(s, d) for s, d in scratch.values()]
        + [pltpu.SemaphoreType.DMA((slots,)), pltpu.SemaphoreType.DMA((slots,)), pltpu.SemaphoreType.DMA((10,))],
        compiler_params=pltpu.CompilerParams(
            collective_id=0, has_side_effects=True, vmem_limit_bytes=67043328
        ),
    )(
        hidden_in[0], out_grad[0], query_weight, key_weight, value_weight, output_weight,
        attention_gain[None], expert_gain[None], router_weight.T, gate_weight, up_weight, down_weight,
        doc_lengths, expert_choice[0].T, frequency,
    )
    steps = nz
    some = lambda *s: pl.BlockSpec(s, lambda i: (i,) + (0,) * (len(s) - 1))
    whole = lambda *s: pl.BlockSpec(s, lambda i: (0,) * len(s))
    per = nf * nz // steps
    out = pl.pallas_call(
        functools.partial(finish_kernel, (nz, experts, half_ff, shard)),
        name="finish",
        grid=(steps,),
        out_shape=(
            shape((block, width), bf16), shape((block, width), f32), shape((1, shard), f32),
            shape((shard, nz * 2 * HD), f32), shape((shard, nz * HD), f32), shape((shard, nz * HD), f32),
            shape((shard, W), f32), shape((1, shard), f32), shape((experts, shard), f32),
            shape((experts, shard, half_ff), f32), shape((experts, shard, half_ff), f32),
            shape((experts, shard, half_ff), f32),
        ),
        in_specs=[
            some(block // steps, width), some(block // steps, width), whole(experts + 8, 128), whole(8, 128),
            whole(nz, shard, 4 * HD), whole(shard, W), some(per, shard, 2 * half_ff), some(per, shard, half_ff),
        ],
        out_specs=(
            some(block // steps, width), some(block // steps, width), whole(1, shard),
            whole(shard, nz * 2 * HD), whole(shard, nz * HD), whole(shard, nz * HD), whole(shard, W), whole(1, shard),
            whole(experts, shard), some(per, shard, half_ff), some(per, shard, half_ff), some(per, shard, half_ff),
        ),
        compiler_params=pltpu.CompilerParams(vmem_limit_bytes=33554432),
    )(*out[:6], out[6].reshape(experts, shard, 2 * half_ff), out[7].reshape(experts, shard, half_ff))
    block_out, input_grad, gain1, q, k, v, o, gain2, router, gate, up, down = out
    return (
        block_out[None], input_grad[None], gain1[0], q, k, v, o, gain2[0], router.T, gate, up, down,
    )


def fits(mesh, args):
    nf, nz, nc = mesh.shape["fsdp"], mesh.shape["ctx"], mesh.shape["tp"]
    hidden, query, key, gate = args[0], args[3], args[4], args[9]
    width, block = hidden.shape[2], hidden.shape[1] // nz
    return (
        nc == 2
        and nz == 4
        and nf == 4
        and hidden.shape[0] == nf
        and gate.shape[0] == nf * nz
        and gate.shape[0] == 16
        and width == 64 * nf * nz
        and block == 128
        and query.shape[1] == 2 * HD * nz * nc
        and key.shape[1] == HD * nz * nc
        and HD == 64
    )


def solution(mesh):
    in_specs = (
        P("fsdp", "ctx", None),
        P("fsdp", "ctx", None),
        P(("fsdp", "ctx")),
        P(("fsdp", "ctx"), "tp"),
        P(("fsdp", "ctx"), "tp"),
        P(("fsdp", "ctx"), "tp"),
        P(("fsdp", "ctx"), "tp"),
        P(("fsdp", "ctx")),
        P(("fsdp", "ctx"), None),
        P(None, ("fsdp", "ctx"), "tp"),
        P(None, ("fsdp", "ctx"), "tp"),
        P(None, ("fsdp", "ctx"), "tp"),
        P("fsdp", None),
        P("fsdp", "ctx", None),
    )
    out_specs = (
        P("fsdp", "ctx", None),
        P("fsdp", "ctx", None),
        P(("fsdp", "ctx")),
        P(("fsdp", "ctx"), "tp"),
        P(("fsdp", "ctx"), "tp"),
        P(("fsdp", "ctx"), "tp"),
        P(("fsdp", "ctx"), "tp"),
        P(("fsdp", "ctx")),
        P(("fsdp", "ctx"), None),
        P(None, ("fsdp", "ctx"), "tp"),
        P(None, ("fsdp", "ctx"), "tp"),
        P(None, ("fsdp", "ctx"), "tp"),
    )

    def step(*args):
        body = local
        if fits(mesh, args):
            body = functools.partial(fast_local, mesh.shape["fsdp"], mesh.shape["ctx"])
        return jax.shard_map(
            body, mesh=mesh, in_specs=in_specs, out_specs=out_specs, check_vma=False
        )(*args)

    return step
```

```python
import functools

import jax
import jax.numpy as jnp
import numpy as np
from jax import lax
from jax.experimental import pallas as pl
from jax.experimental.pallas import tpu as pltpu
from jax.sharding import PartitionSpec as P

HD = 64


epsilon = 1e-05
rope_base = 10000.0
masked_score = -1e30
highest = lax.Precision.HIGHEST


def doc_layout(lengths, positions):
    ends = jnp.cumsum(lengths)
    after = (positions[:, None] >= ends[None, :]).astype(jnp.int32)
    segment = jnp.sum(after, axis=1)
    offset = positions - jnp.sum(after * lengths[None, :], axis=1)
    return (segment, offset)


def rope_tables(offset):
    halfway = HD // 2
    frequency = rope_base ** (-jnp.arange(halfway, dtype=jnp.float32) / halfway)
    angle = offset.astype(jnp.float32)[:, None] * frequency[None, :]
    return (jnp.cos(angle), jnp.sin(angle))


def rotate(vectors, cosine, sine):
    halfway = vectors.shape[-1] // 2
    former = vectors[..., :halfway]
    latter = vectors[..., halfway:]
    cosine = cosine[:, None, :]
    sine = sine[:, None, :]
    return jnp.concatenate(
        [former * cosine - latter * sine, latter * cosine + former * sine], axis=-1
    )


def rotate_back(grads, cosine, sine):
    halfway = grads.shape[-1] // 2
    former = grads[..., :halfway]
    latter = grads[..., halfway:]
    cosine = cosine[:, None, :]
    sine = sine[:, None, :]
    return jnp.concatenate(
        [former * cosine + latter * sine, latter * cosine - former * sine], axis=-1
    )


def norm_forward(values, gain):
    inverse = lax.rsqrt(jnp.mean(values * values, axis=-1, keepdims=True) + epsilon)
    return (values * inverse * gain.astype(jnp.float32), inverse)


def norm_backward(values, inverse, gain, grad_normed):
    scaled = grad_normed * gain.astype(jnp.float32)
    grad_values = inverse * scaled - values * inverse**3 * jnp.mean(
        scaled * values, axis=-1, keepdims=True
    )
    grad_gain = jnp.sum(grad_normed * values * inverse, axis=0)
    return (grad_values, grad_gain)


def dispatch(route, experts, capacity):
    flat = route.reshape(-1)
    onehot = (flat[:, None] == jnp.arange(experts, dtype=jnp.int32)[None, :]).astype(jnp.int32)
    rank = jnp.sum((jnp.cumsum(onehot, axis=0) - onehot) * onehot, axis=1)
    slot = flat * capacity + rank
    pairs = flat.shape[0]
    owner = (
        jnp.zeros((experts * capacity,), jnp.int32).at[slot].set(jnp.arange(pairs, dtype=jnp.int32))
    )
    filled = jnp.zeros((experts * capacity,), jnp.int32).at[slot].set(1) > 0
    return (slot, owner, filled)


def expert_math(slot_inputs, slot_grads, gate_full, up_full, down_full):
    gate_pre = jnp.einsum(
        "gsd,gdf->gsf", slot_inputs, gate_full, preferred_element_type=jnp.float32
    )
    up_pre = jnp.einsum("gsd,gdf->gsf", slot_inputs, up_full, preferred_element_type=jnp.float32)
    sigmoid = jax.nn.sigmoid(gate_pre)
    activated = (gate_pre * sigmoid * up_pre).astype(jnp.bfloat16)
    expert_out = jnp.einsum(
        "gsf,gdf->gsd", activated, down_full, preferred_element_type=jnp.float32
    )
    act_grad = jnp.einsum("gsd,gdf->gsf", slot_grads, down_full, preferred_element_type=jnp.float32)
    gate_pre_grad = (act_grad * up_pre * sigmoid * (1.0 + gate_pre * (1.0 - sigmoid))).astype(
        jnp.bfloat16
    )
    up_pre_grad = (act_grad * gate_pre * sigmoid).astype(jnp.bfloat16)
    down_term = jnp.einsum(
        "gsd,gsf->gdf", slot_grads, activated, preferred_element_type=jnp.float32
    )
    gate_term = jnp.einsum(
        "gsd,gsf->gdf", slot_inputs, gate_pre_grad, preferred_element_type=jnp.float32
    )
    up_term = jnp.einsum(
        "gsd,gsf->gdf", slot_inputs, up_pre_grad, preferred_element_type=jnp.float32
    )
    slot_back = jnp.einsum(
        "gsf,gdf->gsd", gate_pre_grad, gate_full, preferred_element_type=jnp.float32
    ) + jnp.einsum("gsf,gdf->gsd", up_pre_grad, up_full, preferred_element_type=jnp.float32)
    return (expert_out, slot_back, gate_term, up_term, down_term)


def local(
    hidden_in,
    out_grad,
    attention_gain,
    query_weight,
    key_weight,
    value_weight,
    output_weight,
    expert_gain,
    router_weight,
    gate_weight,
    up_weight,
    down_weight,
    doc_lengths,
    expert_choice,
):
    block = hidden_in.shape[1]
    experts = gate_weight.shape[0]
    capacity = block * 3 // 4
    chosen_count = expert_choice.shape[2]
    context_count = lax.axis_size("ctx")
    scale = HD ** (-0.5)
    position = lax.axis_index("ctx") * block + jnp.arange(block, dtype=jnp.int32)
    lengths = doc_lengths[0]
    segment, offset = doc_layout(lengths, position)
    cosine, sine = rope_tables(offset)
    gain_one, query_full, key_full, value_full, output_full, gain_two, router_full = (
        lax.all_gather(attention_gain, ("fsdp", "ctx"), axis=0, tiled=True),
        lax.all_gather(query_weight, ("fsdp", "ctx"), axis=0, tiled=True),
        lax.all_gather(key_weight, ("fsdp", "ctx"), axis=0, tiled=True),
        lax.all_gather(value_weight, ("fsdp", "ctx"), axis=0, tiled=True),
        lax.all_gather(output_weight, ("fsdp", "ctx"), axis=0, tiled=True),
        lax.all_gather(expert_gain, ("fsdp", "ctx"), axis=0, tiled=True),
        lax.all_gather(router_weight, ("fsdp", "ctx"), axis=0, tiled=True),
    )
    inputs = hidden_in[0].astype(jnp.float32)
    normed_one, inverse_one = norm_forward(inputs, gain_one)
    normed_one = normed_one.astype(jnp.bfloat16)
    heads_local = query_full.shape[1] // HD
    groups_local = key_full.shape[1] // HD
    ratio = heads_local // groups_local
    query = rotate(
        jnp.dot(normed_one, query_full, preferred_element_type=jnp.float32).reshape(
            block, heads_local, HD
        ),
        cosine,
        sine,
    ).astype(jnp.bfloat16)
    keys = rotate(
        jnp.dot(normed_one, key_full, preferred_element_type=jnp.float32).reshape(
            block, groups_local, HD
        ),
        cosine,
        sine,
    ).astype(jnp.bfloat16)
    values = jnp.dot(normed_one, value_full, preferred_element_type=jnp.float32).astype(
        jnp.bfloat16
    )
    query_grouped = query.reshape(block, groups_local, ratio, HD)

    def allowed_mask(key_start, count):
        key_position = key_start + jnp.arange(count, dtype=jnp.int32)
        key_segment, unused = doc_layout(lengths, key_position)
        return (segment[:, None] == key_segment[None, :]) & (
            key_position[None, :] <= position[:, None]
        )

    def forward_update(state, key_block, value_block, allowed):
        peak, total, accum = state
        mask = allowed[:, None, None, :]
        scores = (
            jnp.einsum(
                "qgrd,kgd->qgrk", query_grouped, key_block, preferred_element_type=jnp.float32
            )
            * scale
        )
        scores = jnp.where(mask, scores, masked_score)
        new_peak = jnp.maximum(peak, jnp.max(scores, axis=3))
        weights = jnp.where(mask, jnp.exp(scores - new_peak[..., None]), 0.0)
        rescale = jnp.exp(peak - new_peak)
        total = total * rescale + jnp.sum(weights, axis=3)
        accum = accum * rescale[..., None] + jnp.einsum(
            "qgrk,kgd->qgrd", weights, value_block.astype(jnp.float32), precision=highest
        )
        return (new_peak, total, accum)

    travel = (keys.reshape(block, groups_local * HD), values)
    initial = (
        jnp.full((block, groups_local, ratio), masked_score, jnp.float32),
        jnp.zeros((block, groups_local, ratio), jnp.float32),
        jnp.zeros((block, groups_local, ratio, HD), jnp.float32),
    )
    state = initial
    key_piece = lax.all_gather(travel[0], "ctx", axis=0, tiled=True)
    value_piece = lax.all_gather(travel[1], "ctx", axis=0, tiled=True)
    pieces = key_piece.shape[0] // block
    key_blocks = key_piece.reshape(pieces, block, groups_local, HD)
    value_blocks = value_piece.reshape(pieces, block, groups_local, HD)
    starts = block * jnp.arange(pieces, dtype=jnp.int32)

    def visit(carry, item):
        key_block, value_block, key_start = item
        allowed = allowed_mask(key_start, block)
        return (forward_update(carry, key_block, value_block, allowed), None)

    state, unused = lax.scan(visit, state, (key_blocks, value_blocks, starts))
    peak, total, accum = state
    attended = (accum / total[..., None]).reshape(block, heads_local * HD).astype(jnp.bfloat16)
    log_total = peak + jnp.log(total)
    projected = lax.psum(jnp.dot(attended, output_full.T, preferred_element_type=jnp.float32), "tp")
    residual = inputs + projected
    normed_two, inverse_two = norm_forward(residual, gain_two)
    normed_two = normed_two.astype(jnp.bfloat16)
    route = expert_choice[0]
    logits = jnp.dot(normed_two, router_full, preferred_element_type=jnp.float32)
    gates = jax.nn.softmax(jnp.take_along_axis(logits, route, axis=1), axis=1)
    slot, owner, filled = dispatch(route, experts, capacity)
    token_of = owner // chosen_count
    grad_out = out_grad[0].astype(jnp.float32)
    slot_inputs = jnp.where(filled[:, None], normed_two[token_of], 0).reshape(experts, capacity, -1)
    slot_gate = jnp.where(filled, gates.reshape(-1)[owner], 0.0)
    slot_grads = (
        (grad_out[token_of] * slot_gate[:, None])
        .astype(jnp.bfloat16)
        .reshape(experts, capacity, -1)
    )
    gate_full, up_full, down_full = (
        lax.all_gather(gate_weight, ("fsdp", "ctx"), axis=1, tiled=True),
        lax.all_gather(up_weight, ("fsdp", "ctx"), axis=1, tiled=True),
        lax.all_gather(down_weight, ("fsdp", "ctx"), axis=1, tiled=True),
    )
    expert_out, slot_back, gate_term, up_term, down_term = expert_math(
        slot_inputs, slot_grads, gate_full, up_full, down_full
    )
    gate_share, up_share, down_share = (
        lax.psum_scatter(gate_term, ("fsdp", "ctx"), scatter_dimension=1, tiled=True),
        lax.psum_scatter(up_term, ("fsdp", "ctx"), scatter_dimension=1, tiled=True),
        lax.psum_scatter(down_term, ("fsdp", "ctx"), scatter_dimension=1, tiled=True),
    )
    pair_out = expert_out.reshape(experts * capacity, -1)[slot].reshape(block, chosen_count, -1)
    pair_back = slot_back.reshape(experts * capacity, -1)[slot].reshape(block, chosen_count, -1)
    mixed_part = jnp.sum(gates[..., None] * pair_out, axis=1)
    gate_dot_part = jnp.sum(pair_out * grad_out[:, None, :], axis=2)
    moe_part = jnp.sum(pair_back, axis=1)
    mixed, gate_dot, moe_input = (
        lax.psum(mixed_part.astype(jnp.bfloat16), "tp").astype(jnp.float32),
        lax.psum(gate_dot_part.astype(jnp.bfloat16), "tp").astype(jnp.float32),
        lax.psum(moe_part.astype(jnp.bfloat16), "tp").astype(jnp.float32),
    )
    block_out = (residual + mixed).astype(jnp.bfloat16)[None]
    chosen_grad = gates * (gate_dot - jnp.sum(gates * gate_dot, axis=1, keepdims=True))
    picked = (route[..., None] == jnp.arange(experts, dtype=jnp.int32)[None, None, :]).astype(
        jnp.float32
    )
    logit_grad = jnp.sum(picked * chosen_grad[..., None], axis=1)
    router_term = jnp.dot(normed_two.astype(jnp.float32).T, logit_grad, precision=highest)
    router_input = jnp.dot(logit_grad, router_full.astype(jnp.float32).T, precision=highest)
    grad_residual_norm, gain_two_term = norm_backward(
        residual, inverse_two, gain_two, moe_input + router_input
    )
    grad_residual = grad_out + grad_residual_norm
    residual_low = grad_residual.astype(jnp.bfloat16)
    attended_grad = jnp.dot(residual_low, output_full, preferred_element_type=jnp.float32).astype(
        jnp.bfloat16
    )
    output_term = jnp.dot(residual_low.T, attended, preferred_element_type=jnp.float32)
    delta = jnp.sum(
        (attended_grad.astype(jnp.float32) * attended.astype(jnp.float32)).reshape(
            block, groups_local, ratio, HD
        ),
        axis=3,
    )
    grad_grouped = attended_grad.reshape(block, groups_local, ratio, HD)
    back_keys, back_values = (
        lax.all_gather(travel[0], "ctx", axis=0, tiled=True),
        lax.all_gather(travel[1], "ctx", axis=0, tiled=True),
    )
    key_blocks = back_keys.reshape(context_count, block, groups_local, HD)
    value_blocks = back_values.reshape(context_count, block, groups_local, HD)
    starts = block * jnp.arange(context_count, dtype=jnp.int32)

    def backward_update(grad_query, key_block, value_block, allowed):
        mask = allowed[:, None, None, :]
        scores = (
            jnp.einsum(
                "qgrd,kgd->qgrk", query_grouped, key_block, preferred_element_type=jnp.float32
            )
            * scale
        )
        probs = jnp.where(mask, jnp.exp(scores - log_total[..., None]), 0.0)
        value_grad = jnp.einsum(
            "qgrk,qgrd->kgd",
            probs.astype(jnp.bfloat16),
            grad_grouped,
            preferred_element_type=jnp.float32,
        )
        prob_grad = jnp.einsum(
            "qgrd,kgd->qgrk", grad_grouped, value_block, preferred_element_type=jnp.float32
        )
        score_grad = (probs * (prob_grad - delta[..., None]) * scale).astype(jnp.bfloat16)
        grad_query = grad_query + jnp.einsum(
            "qgrk,kgd->qgrd", score_grad, key_block, preferred_element_type=jnp.float32
        )
        key_grad = jnp.einsum(
            "qgrk,qgrd->kgd", score_grad, query_grouped, preferred_element_type=jnp.float32
        )
        return (grad_query, key_grad.reshape(block, -1), value_grad.reshape(block, -1))

    def backward_visit(grad_query, item):
        key_block, value_block, key_start = item
        allowed = allowed_mask(key_start, block)
        grad_query, key_grad, value_grad = backward_update(
            grad_query, key_block, value_block, allowed
        )
        return (grad_query, (key_grad, value_grad))

    grad_query, (key_grads, value_grads) = lax.scan(
        backward_visit,
        jnp.zeros((block, groups_local, ratio, HD), jnp.float32),
        (key_blocks, value_blocks, starts),
    )
    own_key_grad, own_value_grad = (
        lax.psum_scatter(
            key_grads.reshape(context_count * block, -1).astype(jnp.bfloat16),
            "ctx",
            scatter_dimension=0,
            tiled=True,
        ).astype(jnp.float32),
        lax.psum_scatter(
            value_grads.reshape(context_count * block, -1).astype(jnp.bfloat16),
            "ctx",
            scatter_dimension=0,
            tiled=True,
        ).astype(jnp.float32),
    )
    query_grad = (
        rotate_back(grad_query.reshape(block, heads_local, HD), cosine, sine)
        .reshape(block, -1)
        .astype(jnp.bfloat16)
    )
    key_grad = (
        rotate_back(own_key_grad.reshape(block, groups_local, HD), cosine, sine)
        .reshape(block, -1)
        .astype(jnp.bfloat16)
    )
    value_grad = own_value_grad.astype(jnp.bfloat16)
    input_part = jnp.dot(query_grad, query_full.T, preferred_element_type=jnp.float32)
    input_part = input_part + jnp.dot(key_grad, key_full.T, preferred_element_type=jnp.float32)
    input_part = input_part + jnp.dot(value_grad, value_full.T, preferred_element_type=jnp.float32)
    normed_one_grad = lax.psum(input_part.astype(jnp.bfloat16), "tp").astype(jnp.float32)
    grad_input_norm, gain_one_term = norm_backward(inputs, inverse_one, gain_one, normed_one_grad)
    input_grad = (grad_residual + grad_input_norm)[None]
    query_term = jnp.dot(normed_one.T, query_grad, preferred_element_type=jnp.float32)
    key_term = jnp.dot(normed_one.T, key_grad, preferred_element_type=jnp.float32)
    value_term = jnp.dot(normed_one.T, value_grad, preferred_element_type=jnp.float32)
    (
        gain_one_share,
        query_share,
        key_share,
        value_share,
        output_share,
        gain_two_share,
        router_share,
    ) = (
        lax.psum_scatter(gain_one_term, ("fsdp", "ctx"), scatter_dimension=0, tiled=True),
        lax.psum_scatter(query_term, ("fsdp", "ctx"), scatter_dimension=0, tiled=True),
        lax.psum_scatter(key_term, ("fsdp", "ctx"), scatter_dimension=0, tiled=True),
        lax.psum_scatter(value_term, ("fsdp", "ctx"), scatter_dimension=0, tiled=True),
        lax.psum_scatter(output_term, ("fsdp", "ctx"), scatter_dimension=0, tiled=True),
        lax.psum_scatter(gain_two_term, ("fsdp", "ctx"), scatter_dimension=0, tiled=True),
        lax.psum_scatter(router_term, ("fsdp", "ctx"), scatter_dimension=0, tiled=True),
    )
    return (
        block_out,
        input_grad,
        gain_one_share,
        query_share,
        key_share,
        value_share,
        output_share,
        gain_two_share,
        router_share,
        gate_share,
        up_share,
        down_share,
    )


MESH = pl.DeviceIdType.MESH
f32 = jnp.float32
bf16 = jnp.bfloat16


def dot_nn(a, b, precision=None):
    return lax.dot_general(a, b, (((1,), (0,)), ((), ())), precision=precision, preferred_element_type=f32)


def dot_nt(a, b, precision=None):
    return lax.dot_general(a, b, (((1,), (1,)), ((), ())), precision=precision, preferred_element_type=f32)


def dot_tn(a, b, precision=None):
    return lax.dot_general(a, b, (((0,), (0,)), ((), ())), precision=precision, preferred_element_type=f32)


class Net:
    def __init__(self, send_sems, recv_sems):
        self.send_sems, self.recv_sems, self.copies, self.left = send_sems, recv_sems, [], set()
        self.slots, self.free_send, self.free_recv = [], [], []
        self.top_send = self.top_recv = 0

    def make(self, source, target, device, sends=None):
        if self.free_send:
            send_at = self.free_send.pop(0)
        else:
            send_at, self.top_send = self.top_send, self.top_send + 1
        if self.free_recv:
            recv_at = self.free_recv.pop(0)
        else:
            recv_at, self.top_recv = self.top_recv, self.top_recv + 1
        assert max(send_at + 1 - self.send_sems.shape[0], recv_at + 1 - self.recv_sems.shape[0]) <= 0
        copy = pltpu.make_async_remote_copy(
            src_ref=source,
            dst_ref=target,
            send_sem=self.send_sems.at[send_at],
            recv_sem=self.recv_sems.at[recv_at],
            device_id=device,
            device_id_type=MESH,
        )
        self.copies.append((copy, sends))
        self.slots.append((send_at, recv_at))
        return copy

    def send(self, source, target, device):
        copy = self.make(source, target, device)
        copy.start()
        return copy

    def free(self, among):
        self.free_recv.extend(self.slots[at][1] for at in among)

    def numbers(self, *groups):
        found = []
        for group in groups:
            if isinstance(group, list):
                found += self.numbers(*group)
            else:
                copy = group[0] if isinstance(group, tuple) else group
                found += [at for at, (one, sends) in enumerate(self.copies) if one is copy]
        return found

    def drain(self, among=None):
        for at, (copy, sends) in enumerate(self.copies):
            if at in self.left or (among is not None and at not in among):
                continue
            self.left.add(at)
            self.free_send.append(self.slots[at][0])
            if sends is None:
                copy.wait_send()
            else:
                pl.when(sends)(copy.wait_send)


class Line:
    def __init__(self, net, z, nz, device):
        self.net, self.z, self.nz, self.device = net, z, nz, device

    def both(self):
        z, nz = self.z, self.nz
        right, left = self.device(lax.min(z + 1, nz - 1)), self.device(lax.max(z - 1, 0))
        return ((z, right), (nz - 1 - z, left))

    def pass_on(self, step, views):
        copies = []
        for way, (rank, target) in enumerate(self.both()):
            sends = (rank >= step) & (rank < self.nz - 1)
            arrives = rank >= step + 1
            block = lax.clamp(0, self.z - step if way == 0 else self.z + step, self.nz - 1)
            for view in views:
                copy = self.net.make(view(block), view(block), target, sends)
                pl.when(sends)(copy.start)
                copies.append((copy, arrives))
        return copies

    def add_on(self, step, own, out, into):
        copies = []
        for way, (rank, target) in enumerate(self.both()):
            sends = rank <= step
            arrives = (rank >= 1) & (rank - 1 <= step)
            dest = self.nz - 1 - step + rank
            dest = lax.clamp(0, dest if way == 0 else self.nz - 1 - dest, self.nz - 1)
            copy = self.net.make(out(way, step), into(way, step), target, sends)

            def prepare():
                out(way, step)[...] = own(dest)[...].astype(bf16)
                if step > 0:

                    def add():
                        out(way, step)[...] = (own(dest)[...] + into(way, step - 1)[...].astype(f32)).astype(bf16)

                    pl.when(rank >= 1)(add)
                copy.start()

            pl.when(sends)(prepare)
            copies.append((copy, arrives))
        return copies

    def finish(self, total, into):
        for way, (rank, target) in enumerate(self.both()):

            def add():
                total[...] += into(way, self.nz - 2)[...].astype(f32)

            pl.when(rank >= 1)(add)


def arrive(copies):
    for copy, arrives in copies:
        pl.when(arrives)(copy.wait_recv)


def layer_kernel(
    dims,
    x_ref, g_ref, wq_ref, wk_ref, wv_ref, wo_ref, ga_ref, ge_ref, rt_ref, wg_ref, wu_ref, wd_ref, dl_ref, ec_ref,
    fr_ref,
    block_out, input_grad, small_out, gain_out, dqkv_out, dwo_out, dgu_out, dd_out,
    WP, SMT, X, WQ, WO, SMB, SMW, N1, CT, ST, SEGC, POSC, Q, K, V, PSC, ATT, AT, PP, PR, RES,
    N2, GTB, GA, WGU, WD, SWG, SWU, SWD, AA, PSX, GC, H, UG, PRD, MP, MR, BP, BR, DGU, DDT, GDS, GD,
    RB, RM, RBV, RMV, BOWN, MOWN, CO, CI, MO, MI, DGB, GUL, ZG, DDB, DDL, ZD, SG, SGF, SGT, SGZ, SGP, GRES, RL,
    AGS, AGR, DWO, RWO, ZWO, LWO, DS, DQ, DQKV, NG, NR, DWQ, RWQ, ZWQ, LWQ,
    SG1, SG1P, RSG1, EXB, EXG,
    send_sems, recv_sems, local_sems,
):
    nf, nz, hb, width, experts, half_ff, ndoc, chosen = dims
    rows = 2 * nz * hb
    half = nz * hb
    block = 2 * hb
    shard = width // (nf * nz)
    f, z, c = lax.axis_index("fsdp"), lax.axis_index("ctx"), lax.axis_index("tp")
    other = 1 - c
    own = f * nz + z
    net = Net(send_sems, recv_sems)
    device = lambda df, dz, core: {"fsdp": df, "ctx": dz, "tp": core}
    partner = device(f, z, other)
    line = Line(net, z, nz, lambda dz: device(f, dz, c))
    zs = [z, z + 1 - 2 * lax.rem(z, 2), lax.rem(z + 2, 4), 3 - z]
    fs = [f, f + 1 - 2 * lax.rem(f, 2), lax.rem(f + 2, 4), 3 - f]
    everyone = [(i, j, k) for k in range(2) for i in range(nf) for j in range(nz) if (i, j, k) != (0, 0, 0)]
    others = [device(fs[i], zs[j], lax.rem(c + k, 2)) for i, j, k in everyone]
    same = [(i, 0) for i in range(1, nf)] + [(i, j) for i in range(nf) for j in (3, 1, 2)]

    mine = pl.ds(pl.multiple_of(c * hb, hb), hb)
    loads = [
        pltpu.make_async_copy(x_ref.at[mine], X.at[c, z], local_sems.at[0]),
        pltpu.make_async_copy(g_ref.at[mine], GA.at[f, c, z], local_sems.at[1]),
        pltpu.make_async_copy(wo_ref, WO.at[f, z], local_sems.at[2]),
    ]
    row_experts = lambda at: pl.ds(at * nz, nz)
    shards = ((wg_ref, SWG), (wu_ref, SWU), (wd_ref, SWD))
    loads += [
        pltpu.make_async_copy(ref.at[row_experts(f)], staged.at[f], local_sems.at[3 + at])
        for at, (ref, staged) in enumerate(shards)
    ]
    unit = half_ff // 2
    units = lambda h: pl.ds(h * unit, unit)
    for copy in loads:
        copy.start()
    barrier = pltpu.get_barrier_semaphore()
    for peer in others:
        pl.semaphore_signal(barrier, inc=1, device_id=peer, device_id_type=MESH)

    for j in range(nz):
        WP[j, :, 0 : 2 * HD] = wq_ref[:, 2 * HD * j : 2 * HD * (j + 1)]
        WP[j, :, 2 * HD : 4 * HD] = jnp.concatenate(
            [wk_ref[:, HD * j : HD * (j + 1)], wv_ref[:, HD * j : HD * (j + 1)]], axis=1
        )
    base = jnp.concatenate(
        [ga_ref[...].astype(f32), ge_ref[...].astype(f32), jnp.zeros((14, shard), f32), rt_ref[...].astype(f32)],
        axis=0,
    )
    in_half = (lax.broadcasted_iota(jnp.int32, (32, 128), 1) < shard) == (lax.rem(z, 2) == 0)
    SMT[...] = jnp.where(in_half, jnp.concatenate([base, base], axis=1), 0.0).astype(bf16)
    SMB[f, z] = SMT[...]
    WQ[f, z] = WP[z]
    pl.semaphore_wait(barrier, len(others))

    wd_full = lambda: WD[...].reshape(width, half_ff)
    wgu_full = lambda: WGU[...].reshape(width, 2 * half_ff)
    lower, upper = pl.ds(0, nz // 2), pl.ds(nz // 2, nz // 2)
    across = [None, device(fs[1], z, c), device(fs[2], z, c), device(fs[3], z, c)]

    def second_hop(ref):
        return [net.send(ref.at[f, c], ref.at[f, c], across[k]) for k in (1, 2)]

    def third_hop(ref, k):
        part, to = ((lower, across[2]), (upper, across[1]))[k - 1]
        return net.send(ref.at[fs[k], c, part], ref.at[fs[k], c, part], to)

    sends_q = [net.send(WP.at[zs[k]], WQ.at[f, z], device(f, zs[k], c)) for k in range(1, nz)]
    sends_s = [net.send(SMT, SMB.at[f, z], device(f, zs[k], c)) for k in range(1, nz)]
    loads[0].wait()
    sends_x = [net.send(X.at[c, z], X.at[c, z], device(f, zs[k], c)) for k in range(1, nz)]
    forwards_x = [net.send(X.at[c, z], X.at[c, z], partner)]
    loads[2].wait()
    sends_o = [net.send(WO.at[f, z], WO.at[f, z], device(f, zs[k], c)) for k in range(1, nz)]
    loads[1].wait()
    view_g = [lambda at: GA.at[f, c, at]]
    chain_g = line.pass_on(0, view_g)
    chains = [chain_g]
    weights = ([], [], [])

    def send_row(k, at):
        ref, staged = shards[at]
        return net.send(ref.at[row_experts(fs[k])], staged.at[f], device(fs[k], z, c))

    sends_e = [[send_row(k, at) for k in (1, 2)] for at in range(3)]

    def send_weights(k, *what):
        for at in what:
            staged, into, lanes, target = (
                (SWG, WGU, units(0), units(0)),
                (SWU, WGU, units(0), units(1)),
                (SWG, WGU, units(1), units(2)),
                (SWU, WGU, units(1), units(3)),
                (SWD, WD, pl.ds(0, half_ff), pl.ds(0, half_ff)),
            )[at]
            weights[at // 2].append(
                net.send(staged.at[:, zs[k], :, lanes], into.at[:, z, :, target], device(f, zs[k], c))
            )

    def places(shape, dim):
        at = lax.broadcasted_iota(jnp.int32, shape, dim)
        core_at, rest = lax.div(at, half), lax.rem(at, half)
        return lax.div(rest, hb) * block + core_at * hb + lax.rem(rest, hb)

    def layout(position):
        segment = jnp.zeros_like(position)
        start = jnp.zeros_like(position)
        end = jnp.int32(0)
        for i in range(ndoc):
            length = dl_ref[0, i]
            end = end + length
            after = jnp.where(position >= end, 1, 0)
            segment = segment + after
            start = start + after * length
        return segment, position - start

    lane = lax.broadcasted_iota(jnp.int32, (1, 2 * HD), 1)
    former = lax.rem(lane, HD) < HD // 2
    is_key = lane < HD

    with jax.named_scope("tables0"):
        pos_col = places((rows, 1), 0)
        seg_col, offset = layout(pos_col)
        POSC[...] = pos_col
        SEGC[...] = seg_col
        pos_row = places((1, rows), 1)
        seg_row, unused = layout(pos_row)

    def swapped(v):
        return jnp.where(former, pltpu.roll(v, 2 * HD - HD // 2, 1), pltpu.roll(v, HD // 2, 1))

    for copy in sends_q:
        copy.wait_recv()
    sends_q2 = [net.send(WQ.at[f], WQ.at[f], device(fs[k], z, c)) for k in range(1, nf)]
    for copy in sends_s:
        copy.wait_recv()
    sends_s2 = [net.send(SMB.at[f], SMB.at[f], device(fs[k], z, c)) for k in range(1, nf)]
    for at in (0, 1):
        sends_e[at].append(send_row(3, at))
    with jax.named_scope("tables1"):
        angle = offset.astype(f32) * fr_ref[0:1, :]
        CT[...] = jnp.cos(angle)
        ST[...] = jnp.where(former, -1.0, 1.0) * jnp.sin(angle)
    for copy in sends_s2:
        copy.wait_recv()
    for pair in range(nf * nz // 2):
        at_f, at_z = pair // (nz // 2), 2 * (pair % (nz // 2))
        SMW[:, 128 * pair : 128 * pair + 128] = SMB[at_f, at_z] + SMB[at_f, at_z + 1]

    def norm_block(at_c, at_z):
        v = X[at_c, at_z].astype(f32)
        inverse = lax.rsqrt(jnp.mean(v * v, axis=1, keepdims=True) + epsilon)
        at = pl.ds(pl.multiple_of((at_c * nz + at_z) * hb, hb), hb)
        N1[at, :] = (v * inverse * SMW[0:1, :].astype(f32)).astype(bf16)

    norm_block(c, z)
    for k in range(1, nz):
        sends_x[k - 1].wait_recv()
        forwards_x.append(net.send(X.at[c, zs[k]], X.at[c, zs[k]], partner))
        norm_block(c, zs[k])
    for k in range(nz):
        forwards_x[k].wait_recv()
        norm_block(other, zs[k])
    for copy in sends_q2:
        copy.wait_recv()
    with jax.named_scope("qkv"):
        projected = dot_nn(N1[...], WQ[...].reshape(width, 4 * HD))
        cosine, sine = CT[...], ST[...]
        q_part, kv_part = projected[:, : 2 * HD], projected[:, 2 * HD :]
        Q[...] = (q_part * cosine + swapped(q_part) * sine).astype(bf16)
        kv = jnp.where(is_key, kv_part * cosine + swapped(kv_part) * sine, kv_part).astype(bf16)
        K[...] = kv[:, :HD]
        V[...] = kv[:, HD:]
    for copy in sends_o:
        copy.wait_recv()
    sends_o2 = [net.send(WO.at[f], WO.at[f], across[k]) for k in (1, 2)]
    sends_e[2].append(send_row(3, 2))

    scale = HD ** (-0.5)
    step = 2 * hb

    def attend(i, carry):
        at = pl.ds(pl.multiple_of(i * step, step), step)
        mask = (SEGC[at, :] == seg_row) & (pos_row <= POSC[at, :])
        q = Q[at, :]
        pieces = []
        for r in range(2):
            scores = dot_nt(q[:, r * HD : (r + 1) * HD], K[...]) * scale
            scores = jnp.where(mask, scores, masked_score)
            peak = jnp.max(scores, axis=1, keepdims=True)
            weights = jnp.where(mask, jnp.exp(scores - peak), 0.0)
            total = jnp.sum(weights, axis=1, keepdims=True)
            pieces.append(dot_nn(weights.astype(bf16), V[...]) / total)
            PSC[r, at, :] = (weights / total).astype(bf16)
        out = jnp.concatenate(pieces, axis=1).astype(bf16)
        at_c, at_z = lax.div(2 * i, nz), lax.rem(2 * i, nz)
        ATT[at_c, pl.ds(at_z, 2)] = out.reshape(2, hb, 2 * HD)
        return carry

    with jax.named_scope("attend"):
        lax.fori_loop(0, rows // step, attend, 0)
    columns = pl.ds(pl.multiple_of(z * 2 * HD, 2 * HD), 2 * HD)
    sends_a = [
        net.send(ATT.at[:, zs[k]], AT.at[:, :, columns], device(f, zs[k], c)) for k in range(1, nz)
    ]
    AT[:, :, columns] = ATT[:, z]
    for k in (1, 2):
        part, to = ((lower, across[2]), (upper, across[1]))[k - 1]
        sends_o2[k - 1].wait_recv()
        sends_o2.append(net.send(WO.at[fs[k], part], WO.at[fs[k], part], to))
    arrive(chain_g)
    chain_g = line.pass_on(1, view_g)
    chains.append(chain_g)
    for copy in loads[3:]:
        copy.wait()
    for copy in sends_e[0] + sends_e[1]:
        copy.wait_recv()
    send_weights(3, 0, 1)
    for copy in sends_a + sends_o2[2:]:
        copy.wait_recv()

    with jax.named_scope("proj"):
        part = dot_nt(AT[...].reshape(block, nz * 2 * HD), WO[...].reshape(width, nz * 2 * HD))
        PP[...] = part.reshape(2, hb, width)
    send_p = net.send(PP.at[other], PR, partner)
    arrive(chain_g)
    chain_g = line.pass_on(2, view_g)
    chains.append(chain_g)
    x_own = X[c, z].astype(f32)
    gain_two = SMW[1:2, :].astype(f32)
    send_p.wait_recv()
    residual = x_own + PP[c] + PR[...]
    RES[...] = residual
    inverse_two = lax.rsqrt(jnp.mean(residual * residual, axis=1, keepdims=True) + epsilon)
    N2[f, c, z] = (residual * inverse_two * gain_two).astype(bf16)
    normed_two = N2[f, c, z]
    logits = dot_nt(SMW[16 : 16 + experts, :], normed_two)
    expert_at = lax.broadcasted_iota(jnp.int32, (experts, hb), 0)
    route = ec_ref[...]
    route = jnp.where(c == 0, route, pltpu.roll(route, 128 - hb, 1))
    picked = jnp.zeros((experts, hb), jnp.bool_)
    for j in range(chosen):
        picked = picked | (route[j : j + 1, 0:hb] == expert_at)
    peak = jnp.max(jnp.where(picked, logits, masked_score), axis=0, keepdims=True)
    weight = jnp.where(picked, jnp.exp(logits - peak), 0.0)
    gates = weight / jnp.sum(weight, axis=0, keepdims=True)
    GTB[f, c, z] = jnp.concatenate([gates, jnp.zeros((experts, 128 - hb), f32)], axis=1)
    view_n = [lambda at: N2.at[f, c, at], lambda at: GTB.at[f, c, at]]
    early = net.numbers(
        sends_q, sends_s, sends_x, forwards_x, sends_o, sends_e[:2], sends_q2, sends_s2, sends_o2, sends_a, chains[:2], send_p
    )
    chain_n = line.pass_on(0, view_n)
    chains = [chains[2], chain_n]
    send_weights(2, 0)

    arrive(chain_g)
    sends_g2 = second_hop(GA)
    forwards_g = [net.send(GA.at[f, c], GA.at[f, c], partner)]
    arrive(chain_n)
    chain_n = line.pass_on(1, view_n)
    chains.append(chain_n)
    send_weights(2, 1)
    arrive(chain_n)
    chain_n = line.pass_on(2, view_n)
    chains.append(chain_n)
    send_weights(1, 0, 1)
    for copy in sends_e[2]:
        copy.wait_recv()
    for k in (3, 2, 1):
        send_weights(k, 4)
    sends_g3 = []
    for k in (1, 2):
        sends_g2[k - 1].wait_recv()
        sends_g3.append(third_hop(GA, k))
        forwards_g.append(net.send(GA.at[fs[k], c], GA.at[fs[k], c], partner))
    arrive(chain_n)
    sends_n2 = second_hop(N2)
    sends_t2 = [net.send(GTB.at[f, c], GTB.at[f, c], across[k]) for k in (1, 2, 3)]
    forwards_n = [net.send(N2.at[f, c], N2.at[f, c], partner)]
    forwards_t = [net.send(GTB.at[f, c], GTB.at[f, c], partner)]
    for k in (3, 2, 1):
        send_weights(k, 2, 3)
    before = range(len(net.copies) - 20)

    WGU[:, z, :, 0:unit] = SWG[:, z, :, 0:unit]
    WGU[:, z, :, unit : 2 * unit] = SWU[:, z, :, 0:unit]
    WGU[:, z, :, 2 * unit : 3 * unit] = SWG[:, z, :, unit : 2 * unit]
    WGU[:, z, :, 3 * unit : 4 * unit] = SWU[:, z, :, unit : 2 * unit]
    WD[:, z] = SWD[:, z]
    chosen_row = jnp.where(
        lax.broadcasted_iota(jnp.int32, (experts, 128), 0) == own, 1.0, 0.0
    ).astype(f32)
    sends_d, sends_b, exchange_b, exchange_m = [], {}, {}, {}
    low_half = z < nz // 2
    in_order = [jnp.where(low_half, 3, 0), jnp.where(low_half, 2, 1), zs[1], z]
    grads_z, grads_f = ([], []), ([], [])

    def send_grads(h, k):
        to = device(f, zs[k], c)
        grads_z[h].append(net.send(DGB.at[h, :, zs[k]], ZG.at[h, z], to))
        grads_z[h].append(net.send(DDB.at[h, :, zs[k]], ZD.at[h, z], to))

    def spread_grads(h):
        ZG[h, z] = DGB[h, :, z]
        ZD[h, z] = DDB[h, :, z]
        for copy in grads_z[h]:
            copy.wait_recv()
        for k in range(1, nf):
            grads_f[h].append(
                net.send(ZG.at[h, :, fs[k]], GUL.at[f, :, :, pl.ds(2 * h * unit, 2 * unit)], across[k])
            )
            grads_f[h].append(net.send(ZD.at[h, :, fs[k]], DDL.at[f, :, :, units(h)], across[k]))
        GUL[f, :, :, 2 * h * unit : 2 * (h + 1) * unit] = ZG[h, :, f]
        DDL[f, :, :, h * unit : (h + 1) * unit] = ZD[h, :, f]

    def expert_part(h, k):
        at_f = fs[k]
        tokens = N2[at_f].reshape(rows, width)
        with jax.named_scope("gateup"):
            PSX[...] = dot_nn(tokens, WGU[:, :, :, 2 * h * unit : 2 * (h + 1) * unit].reshape(width, 2 * unit))
        if h == 0:
            with jax.named_scope("gatecol"):
                for piece in range(2 * nz):
                    tile = GTB[at_f, piece // nz, piece % nz][:, 0:hb]
                    GC[k, piece * hb : (piece + 1) * hb, :] = dot_tn(tile, chosen_row, lax.Precision.HIGHEST)

        def expert_chunk(i, carry):
            at = pl.ds(pl.multiple_of(i * 64, 64), 64)
            gate_pre = PSX[at, 0:unit]
            up_pre = PSX[at, unit : 2 * unit]
            raw = AA[k, at, h * unit : (h + 1) * unit]
            gate = GC[k, at, :]
            sigmoid = jax.nn.sigmoid(gate_pre)
            silu = gate_pre * sigmoid
            act = silu * up_pre
            PRD[at, :] = (act * raw).astype(bf16)
            H[k, at, h * unit : (h + 1) * unit] = (act * gate).astype(bf16)
            grad = raw * gate
            UG[k, at, 2 * h * unit : (2 * h + 1) * unit] = (
                grad * up_pre * sigmoid * (1.0 + gate_pre * (1.0 - sigmoid))
            ).astype(bf16)
            UG[k, at, (2 * h + 1) * unit : 2 * (h + 1) * unit] = (grad * silu).astype(bf16)
            return carry

        with jax.named_scope("chunk"):
            lax.fori_loop(0, rows // 64, expert_chunk, 0)
        if h == 1:
            with jax.named_scope("back"):
                BP[at_f] = dot_nt(UG[k], WGU[...].reshape(width, 2 * half_ff)).astype(bf16).reshape(2, nz, hb, width)
            exchange_b[k] = net.send(BP.at[at_f, other], BR.at[at_f], partner)
        with jax.named_scope("gdot"):
            dots = dot_nt(jnp.ones((8, unit), bf16), PRD[...])
            GDS[k] = dots if h == 0 else GDS[k] + dots
        if h == 1:
            for j in range(nz):
                for t in range(2):
                    to_z, to_c = zs[j], lax.rem(c + t, 2)
                    lanes = pl.ds(pl.multiple_of((to_c * (nz // 2) + lax.div(to_z, 2)) * 128, 128), 128)
                    if (k, j, t) != (0, 0, 0):
                        sends_d.append(
                            net.send(GDS.at[k, pl.ds(0, 1), lanes], GD.at[f, z, c, pl.ds(0, 1)], device(at_f, to_z, to_c))
                        )
                    else:
                        GD[f, z, c] = GDS[0, :, lanes]

    def mix(k):
        with jax.named_scope("mix"):
            MP[fs[k]] = dot_nt(H[k], WD[...].reshape(width, half_ff)).astype(bf16).reshape(2, nz, hb, width)
        exchange_m[k] = net.send(MP.at[fs[k], other], MR.at[fs[k]], partner)

    def weight_terms(h, k):
        with jax.named_scope("wgrad"):
            gate_up = dot_tn(UG[k, :, 2 * h * unit : 2 * (h + 1) * unit], N2[fs[k]].reshape(rows, width))
            down = dot_tn(H[k, :, h * unit : (h + 1) * unit], GA[fs[k]].reshape(rows, width))
            first = k == (0, 3)[h]
            DGU[...] = gate_up if first else DGU[...] + gate_up
            DDT[...] = down if first else DDT[...] + down

    def shed(h):
        with jax.named_scope("transpose"):
            DGB[h] = jnp.transpose(DGU[...]).astype(bf16).reshape(nf, nz, shard, 2 * unit)
            DDB[h] = jnp.transpose(DDT[...]).astype(bf16).reshape(nf, nz, shard, unit)

    def cotangent(k):
        forwards_g[k].wait_recv()
        with jax.named_scope("cotangent"):
            AA[k] = dot_nn(GA[fs[k]].reshape(rows, width), WD[...].reshape(width, half_ff))

    net.drain(before)
    for copy in weights[2]:
        copy.wait_recv()
    for k in range(nf - 1):
        cotangent(k)
    for copy in weights[0]:
        copy.wait_recv()
    for k in range(nf):
        if k == 1:
            sends_n3 = []
            for i in (1, 2):
                sends_n2[i - 1].wait_recv()
                sends_n3.append(third_hop(N2, i))
                forwards_n.append(net.send(N2.at[fs[i], c], N2.at[fs[i], c], partner))
                sends_t2[i - 1].wait_recv()
                forwards_t.append(net.send(GTB.at[fs[i], c], GTB.at[fs[i], c], partner))
            for copy in sends_g3:
                copy.wait_recv()
            forwards_g.append(net.send(GA.at[fs[3], c], GA.at[fs[3], c], partner))
        if k == 3:
            cotangent(k)
            for copy in sends_n3:
                copy.wait_recv()
            forwards_n.append(net.send(N2.at[fs[k], c], N2.at[fs[k], c], partner))
            sends_t2[2].wait_recv()
            forwards_t.append(net.send(GTB.at[fs[k], c], GTB.at[fs[k], c], partner))
        forwards_n[k].wait_recv()
        forwards_t[k].wait_recv()
        expert_part(0, k)
        weight_terms(0, k)
    shed(0)
    for k in (3, 2, 1):
        send_grads(0, k)
    for copy in weights[1]:
        copy.wait_recv()
    own_half = ((lower, 1), (upper, 2))

    def spread(k, exchange, part, back, total, via, into, order):
        at_f = fs[k]
        exchange[k].wait_recv()
        if k == 0:
            total[...] = part[at_f, c].astype(f32) + back[at_f].astype(f32)
            return []
        if k == 3:
            part[at_f, c] = (part[at_f, c].astype(f32) + back[at_f].astype(f32)).astype(bf16)
            return [net.send(part.at[at_f, c, half_at], via.at[to - 1], across[to]) for half_at, to in own_half]
        return None

    def spread_near(k, firsts, part, back, via, into, order):
        at_f = fs[k]
        half_at, other_half = (upper, lower) if k == 1 else (lower, upper)
        firsts[2 - k].wait_recv()
        part[at_f, c, half_at] = (
            part[at_f, c, half_at].astype(f32) + back[at_f, half_at].astype(f32) + via[2 - k].astype(f32)
        ).astype(bf16)
        part[at_f, c, other_half] = (
            part[at_f, c, other_half].astype(f32) + back[at_f, other_half].astype(f32)
        ).astype(bf16)
        return [net.send(part.at[at_f, c, at], into.at[k - 1, at], across[k]) for at in order]

    sends_m = {}
    middle = net.numbers(
        sends_e[2:], sends_g2, sends_g3, forwards_g, *weights, chains, sends_n2, sends_n3, sends_t2,
        forwards_n, forwards_t,
    )
    net.free(early)
    expert_part(1, 3)
    weight_terms(1, 3)
    mix(3)
    firsts_b = spread(3, exchange_b, BP, BR, BOWN, RBV, RB, in_order)
    for k in (1, 2, 0):
        expert_part(1, k)
    for k in (1, 2):
        exchange_b[k].wait_recv()
        sends_b[k] = spread_near(k, firsts_b, BP, BR, RBV, RB, in_order)
    spread(0, exchange_b, BP, BR, BOWN, RBV, RB, in_order)
    firsts_m = spread(3, exchange_m, MP, MR, MOWN, RMV, RM, in_order)
    for k in (1, 2, 0):
        mix(k)
        weight_terms(1, k)

    expert_copies = len(net.copies)
    shed(1)

    def dots_back():
        for copy in sends_d:
            copy.wait_recv()
        dots = jnp.concatenate(
            [
                GD[e // nz, e % nz, 0][0:1, :] + GD[e // nz, e % nz, 1][0:1, :]
                for e in range(experts)
            ],
            axis=0,
        )
        dots = jnp.where(lax.rem(z, 2) == 0, dots, pltpu.roll(dots, 128 - hb, 1))[:, 0:hb]
        gates = GTB[f, c, z][:, 0:hb]
        logit_grad = gates * (dots - jnp.sum(gates * dots, axis=0, keepdims=True))
        router_t = SMW[16 : 16 + experts, :].astype(f32)
        SG[0:experts, :] = dot_nn(logit_grad, N2[f, c, z].astype(f32), lax.Precision.HIGHEST)
        GRES[...] = dot_tn(logit_grad, router_t, lax.Precision.HIGHEST)

    own_b, out_b, into_b = (lambda at: BOWN.at[at]), (lambda w, t: CO.at[w, t]), (lambda w, t: CI.at[w, t])

    def take_block(at):
        for k in (1, 2):
            sends_b[k][at].wait_recv()
            BOWN[in_order[at]] += RB[k - 1, in_order[at]].astype(f32)

    sums = []
    for t in range(nz):
        take_block(t)
        if t > 0:
            arrive(chain_b)
        if t < nz - 1:
            at_sums = len(net.copies)
            chain_b = line.add_on(t, own_b, out_b, into_b)
            sums.extend(range(at_sums, len(net.copies)))
        if t == 0:
            dots_back()
    line.finish(BOWN.at[z], into_b)
    net.free(middle)

    residual = RES[...]
    inverse_two = lax.rsqrt(jnp.mean(residual * residual, axis=1, keepdims=True) + epsilon)
    grad_two = BOWN[z] + GRES[...]
    scaled = grad_two * gain_two
    grad_res = (
        GA[f, c, z].astype(f32)
        + inverse_two * scaled
        - residual * (inverse_two * inverse_two * inverse_two) * jnp.mean(scaled * residual, axis=1, keepdims=True)
    )
    GRES[...] = grad_res
    RL[c] = grad_res.astype(bf16)
    send_r = net.send(RL.at[c], RL.at[c], partner)
    for k in (1, 2):
        exchange_m[k].wait_recv()
        sends_m[k] = spread_near(k, firsts_m, MP, MR, RMV, RM, in_order)
    spread(0, exchange_m, MP, MR, MOWN, RMV, RM, in_order)
    gain_term = jnp.sum(grad_two * residual * inverse_two, axis=0, keepdims=True)
    SG[experts : experts + 8, :] = jnp.broadcast_to(gain_term, (8, width))
    wide = width // nf
    block_lanes = lambda at: pl.ds(pl.multiple_of(at * wide, 128), wide)
    sends_sg = [net.send(SG.at[:, block_lanes(fs[k])], SGF.at[k - 1], device(fs[k], z, c)) for k in range(1, nf)]
    send_r.wait_recv()
    low = RL[...].reshape(block, width)
    with jax.named_scope("attgrad"):
        AGS[...] = dot_nn(low, WO[...].reshape(width, nz * 2 * HD)).astype(bf16).reshape(2, hb, nz * 2 * HD)
    sends_ag = [
        net.send(
            AGS.at[:, :, pl.ds(pl.multiple_of(zs[k] * 2 * HD, 2 * HD), 2 * HD)],
            AGR.at[:, z],
            device(f, zs[k], c),
        )
        for k in range(1, nz)
    ]
    AGR[:, z] = AGS[:, :, columns]
    for k in (1, 3, 2):
        send_grads(1, k)
    with jax.named_scope("outgrad"):
        DWO[...] = (
            dot_tn(low, AT[...].reshape(block, nz * 2 * HD))
            .astype(bf16)
            .reshape(nf, nz, shard, nz * 2 * HD)
        )
    sends_wo = [net.send(DWO.at[fs[k]], RWO.at[k - 1], device(fs[k], z, c)) for k in range(1, nf)]

    net.drain(range(expert_copies))
    for copy in sends_ag:
        copy.wait_recv()

    def backward(i, carry):
        at = pl.ds(pl.multiple_of(i * step, step), step)
        at_c, at_z = lax.div(2 * i, nz), lax.rem(2 * i, nz)
        grad = AGR[at_c, pl.ds(at_z, 2)].reshape(step, 2 * HD)
        out = ATT[at_c, pl.ds(at_z, 2)].reshape(step, 2 * HD)
        both = grad.astype(f32) * out.astype(f32)
        pieces = []
        for r in range(2):
            delta = jnp.sum(both[:, r * HD : (r + 1) * HD], axis=1, keepdims=True)
            prob_grad = dot_nt(grad[:, r * HD : (r + 1) * HD], V[...])
            probs = PSC[r, at, :].astype(f32)
            score_grad = (probs * (prob_grad - delta) * scale).astype(bf16)
            DS[r, at, :] = score_grad
            pieces.append(dot_nn(score_grad, K[...]))
        DQ[at, :] = jnp.concatenate(pieces, axis=1)
        return carry

    with jax.named_scope("attback"):
        lax.fori_loop(0, rows // step, backward, 0)
    with jax.named_scope("kvgrad"):
        grads = AGR[...].reshape(rows, 2 * HD)
        key_t = dot_tn(Q[:, 0:HD], DS[0]) + dot_tn(Q[:, HD : 2 * HD], DS[1])
        value_t = dot_tn(grads[:, 0:HD], PSC[0]) + dot_tn(grads[:, HD : 2 * HD], PSC[1])
        kv_grad = jnp.transpose(jnp.concatenate([key_t, value_t], axis=0))
        cosine, sine = CT[...], ST[...]
        q_grad = DQ[...]
        DQKV[:, 0 : 2 * HD] = (q_grad * cosine - swapped(q_grad) * sine).astype(bf16)
        DQKV[:, 2 * HD : 4 * HD] = jnp.where(
            is_key, kv_grad * cosine - swapped(kv_grad) * sine, kv_grad
        ).astype(bf16)
    with jax.named_scope("ingrad"):
        NG[...] = dot_nt(DQKV[...], WQ[...].reshape(width, 4 * HD)).astype(bf16).reshape(2, nz, hb, width)
    send_ng = net.send(NG.at[other], NR, partner)
    with jax.named_scope("qkvgrad"):
        DWQ[...] = (
            jnp.transpose(dot_tn(DQKV[...], N1[...])).astype(bf16).reshape(nf, nz, shard, 4 * HD)
        )
    sends_wq = [net.send(DWQ.at[fs[k]], RWQ.at[k - 1], device(fs[k], z, c)) for k in range(1, nf)]
    small = SG[:, block_lanes(f)]
    for k in range(1, nf):
        sends_sg[k - 1].wait_recv()
        small = small + SGF[k - 1]
    SGT[...] = small
    pair_lanes = lambda at: pl.ds(pl.multiple_of(lax.div(at, 2) * 128, 128), 128)
    sends_sz = [net.send(SGT.at[:, pair_lanes(zs[k])], SGZ.at[k - 1], device(f, zs[k], c)) for k in range(1, nz)]
    send_ng.wait_recv()
    net.drain(sums)
    BOWN[...] = NG[c].astype(f32) + NR[...].astype(f32)
    chain_g1 = line.add_on(0, own_b, out_b, into_b)
    for k in (1, 2):
        for at in range(nz):
            sends_m[k][at].wait_recv()
        MOWN[...] += RM[k - 1].astype(f32)
    own_m, out_m, into_m = (lambda at: MOWN.at[at]), (lambda w, t: MO.at[w, t]), (lambda w, t: MI.at[w, t])
    chain_m = line.add_on(0, own_m, out_m, into_m)
    arrive(chain_g1)
    chain_g1 = line.add_on(1, own_b, out_b, into_b)
    arrive(chain_m)
    chain_m = line.add_on(1, own_m, out_m, into_m)
    spread_grads(0)
    arrive(chain_g1)
    chain_g1 = line.add_on(2, own_b, out_b, into_b)
    arrive(chain_m)
    chain_m = line.add_on(2, own_m, out_m, into_m)

    total = DWO[f].astype(f32)
    for k in range(1, nf):
        sends_wo[k - 1].wait_recv()
        total = total + RWO[k - 1].astype(f32)
    ZWO[...] = total.astype(bf16)
    sends_wo2 = [net.send(ZWO.at[zs[k]], LWO.at[z], device(f, zs[k], c)) for k in range(1, nz)]
    LWO[z] = ZWO[z]
    total = DWQ[f].astype(f32)
    for k in range(1, nf):
        sends_wq[k - 1].wait_recv()
        total = total + RWQ[k - 1].astype(f32)
    ZWQ[...] = total.astype(bf16)
    sends_wq2 = [net.send(ZWQ.at[zs[k]], LWQ.at[z], device(f, zs[k], c)) for k in range(1, nz)]
    LWQ[z] = ZWQ[z]
    arrive(chain_g1)
    line.finish(BOWN.at[z], into_b)
    grad_one = BOWN[z]
    gain_one = SMW[0:1, :].astype(f32)
    x_own = X[c, z].astype(f32)
    inverse = lax.rsqrt(jnp.mean(x_own * x_own, axis=1, keepdims=True) + epsilon)
    gain_term = jnp.sum(grad_one * x_own * inverse, axis=0, keepdims=True)
    SG1[0] = jnp.broadcast_to(gain_term, (8, width))
    send_g1 = net.send(SG1.at[0], SG1.at[1], partner)
    scaled = grad_one * gain_one
    EXG[c] = (
        GRES[...]
        + inverse * scaled
        - x_own * (inverse * inverse * inverse) * jnp.mean(scaled * x_own, axis=1, keepdims=True)
    )
    send_ig = net.send(EXG.at[c], EXG.at[c], partner)
    small = SGT[:, pair_lanes(z)]
    for k in range(1, nz):
        sends_sz[k - 1].wait_recv()
        small = small + SGZ[k - 1]
    SGP[0] = small
    send_sp = net.send(SGP.at[0], SGP.at[1], partner)
    net.drain(range(expert_copies))
    send_g1.wait_recv()
    SG1P[...] = SG1[0] + SG1[1]
    lanes_of = lambda df, dz: pl.ds(pl.multiple_of((df * (nz // 2) + lax.div(dz, 2)) * 128, 128), 128)
    sends_g1 = [
        net.send(SG1P.at[pl.ds(0, 1), lanes_of(fs[i], zs[j])], RSG1.at[f, z, pl.ds(0, 1)], device(fs[i], zs[j], c))
        for i, j in same
    ]
    RSG1[f, z] = SG1P[:, lanes_of(f, z)]

    spread_grads(1)
    arrive(chain_m)
    line.finish(MOWN.at[z], into_m)
    EXB[c] = (RES[...] + MOWN[z]).astype(bf16)
    send_bo = net.send(EXB.at[c], EXB.at[c], partner)
    send_sp.wait_recv()
    small_out[...] = SGP[0] + SGP[1]
    for copy in sends_wo2:
        copy.wait_recv()
    total = LWO[0].astype(f32)
    for j in range(1, nz):
        total = total + LWO[j].astype(f32)
    dwo_out[...] = total
    outs = []

    def leave(source, target):
        copy = pltpu.make_async_copy(source, target, local_sems.at[6 + len(outs)])
        copy.start()
        outs.append(copy)

    for copy in sends_wq2:
        copy.wait_recv()
    leave(LWQ, dqkv_out)
    send_bo.wait_recv()
    leave(EXB, block_out)
    send_ig.wait_recv()
    leave(EXG, input_grad)
    for copy in sends_g1:
        copy.wait_recv()
    small = jnp.zeros((1, 128), f32)
    for i in range(nf):
        for j in range(nz):
            small = small + RSG1[i, j, 0:1]
    gain_out[...] = jnp.broadcast_to(small, (8, 128))
    for copy in grads_f[0] + grads_f[1]:
        copy.wait_recv()
    leave(GUL, dgu_out)
    leave(DDL, dd_out)
    with jax.named_scope("drain"):
        net.drain()
    with jax.named_scope("outs"):
        for copy in outs:
            copy.wait()


def finish_kernel(
    dims, block_ref, input_ref, small_ref, gain_ref, dqkv_ref, dwo_ref, dgu_ref, dd_ref,
    block_out, input_out, gain1_out, q_out, k_out, v_out, o_out, gain2_out, router_out, gate_out, up_out, down_out,
):
    nz, experts, half_ff, shard = dims
    block_out[...] = block_ref[...]
    input_out[...] = input_ref[...]
    unit = half_ff // 2
    for h in range(2):
        gate_out[:, :, h * unit : (h + 1) * unit] = dgu_ref[:, :, 2 * h * unit : (2 * h + 1) * unit].astype(f32)
        up_out[:, :, h * unit : (h + 1) * unit] = dgu_ref[:, :, (2 * h + 1) * unit : 2 * (h + 1) * unit].astype(f32)
    down_out[...] = dd_ref[...].astype(f32)
    even = lax.rem(lax.axis_index("ctx"), 2) == 0
    pick = lambda v: jnp.where(even, v, pltpu.roll(v, 128 - shard, 1))[:, 0:shard]

    def once():
        gain1_out[...] = pick(gain_ref[...])[0:1]
        small = pick(small_ref[...])
        router_out[...] = small[0:experts]
        gain2_out[...] = small[experts : experts + 1]
        o_out[...] = dwo_ref[...]
        for j in range(nz):
            q_out[:, 2 * HD * j : 2 * HD * (j + 1)] = dqkv_ref[j, :, 0 : 2 * HD].astype(f32)
        for at, ref in ((2, k_out), (3, v_out)):
            ref[...] = jnp.concatenate(
                [dqkv_ref[j, :, at * HD : (at + 1) * HD].astype(f32) for j in range(nz)], axis=1
            )

    pl.when(pl.program_id(0) == 0)(once)


def fast_local(
    nf, nz,
    hidden_in, out_grad, attention_gain, query_weight, key_weight, value_weight, output_weight,
    expert_gain, router_weight, gate_weight, up_weight, down_weight, doc_lengths, expert_choice,
):
    block, width = hidden_in.shape[1], hidden_in.shape[2]
    hb = block // 2
    experts, shard, half_ff = gate_weight.shape
    ndoc, chosen = doc_lengths.shape[1], expert_choice.shape[2]
    rows = nz * block
    halfway = HD // 2
    frequency = np.float32(rope_base) ** (-np.arange(halfway, dtype=np.float32) / np.float32(halfway))
    frequency = jnp.asarray(np.tile(np.tile(frequency, 4)[None], (8, 1)).astype(np.float32))

    vm = pl.BlockSpec(memory_space=pltpu.VMEM)
    anywhere = pl.BlockSpec(memory_space=pl.ANY)
    shape = lambda s, d: jax.ShapeDtypeStruct(s, d)
    W = nz * 2 * HD
    scratch = dict(
        WP=((nz, shard, 4 * HD), bf16), SMT=((32, 128), bf16),
        X=((2, nz, hb, width), bf16), WQ=((nf, nz, shard, 4 * HD), bf16), WO=((nf, nz, shard, W), bf16),
        SMB=((nf, nz, 32, 128), bf16), SMW=((32, width), bf16), N1=((rows, width), bf16),
        CT=((rows, 128), f32), ST=((rows, 128), f32), SEGC=((rows, 1), jnp.int32), POSC=((rows, 1), jnp.int32),
        Q=((rows, 2 * HD), bf16), K=((rows, HD), bf16), V=((rows, HD), bf16), PSC=((2, rows, rows), bf16),
        ATT=((2, nz, hb, 2 * HD), bf16), AT=((2, hb, W), bf16), PP=((2, hb, width), f32), PR=((hb, width), f32),
        RES=((hb, width), f32),
        N2=((nf, 2, nz, hb, width), bf16), GTB=((nf, 2, nz, experts, 128), f32), GA=((nf, 2, nz, hb, width), bf16),
        WGU=((nf, nz, shard, 2 * half_ff), bf16), WD=((nf, nz, shard, half_ff), bf16),
        SWG=((nf, nz, shard, half_ff), bf16), SWU=((nf, nz, shard, half_ff), bf16), SWD=((nf, nz, shard, half_ff), bf16),
        AA=((nf, rows, half_ff), f32), PSX=((rows, half_ff), f32), GC=((nf, rows, 128), f32),
        H=((nf, rows, half_ff), bf16), UG=((nf, rows, 2 * half_ff), bf16), PRD=((rows, half_ff // 2), bf16),
        MP=((nf, 2, nz, hb, width), bf16), MR=((nf, nz, hb, width), bf16),
        BP=((nf, 2, nz, hb, width), bf16), BR=((nf, nz, hb, width), bf16),
        DGU=((half_ff, width), f32), DDT=((half_ff // 2, width), f32),
        GDS=((nf, 8, rows), f32), GD=((nf, nz, 2, 8, 128), f32),
        RB=((2, nz, hb, width), bf16), RM=((2, nz, hb, width), bf16),
        RBV=((2, nz // 2, hb, width), bf16), RMV=((2, nz // 2, hb, width), bf16),
        BOWN=((nz, hb, width), f32), MOWN=((nz, hb, width), f32),
        CO=((2, nz - 1, hb, width), bf16), CI=((2, nz - 1, hb, width), bf16),
        MO=((2, nz - 1, hb, width), bf16), MI=((2, nz - 1, hb, width), bf16),
        DGB=((2, nf, nz, shard, half_ff), bf16), GUL=((nf, nz, shard, 2 * half_ff), bf16), ZG=((2, nz, nf, shard, half_ff), bf16),
        DDB=((2, nf, nz, shard, half_ff // 2), bf16), DDL=((nf, nz, shard, half_ff), bf16), ZD=((2, nz, nf, shard, half_ff // 2), bf16),
        SG=((experts + 8, width), f32), SGF=((nf - 1, experts + 8, width // nf), f32),
        SGT=((experts + 8, width // nf), f32), SGZ=((nz - 1, experts + 8, 128), f32), SGP=((2, experts + 8, 128), f32),
        GRES=((hb, width), f32), RL=((2, hb, width), bf16),
        AGS=((2, hb, W), bf16), AGR=((2, nz, hb, 2 * HD), bf16),
        DWO=((nf, nz, shard, W), bf16), RWO=((nf - 1, nz, shard, W), bf16),
        ZWO=((nz, shard, W), bf16), LWO=((nz, shard, W), bf16),
        DS=((2, rows, rows), bf16), DQ=((rows, 2 * HD), f32),
        DQKV=((rows, 4 * HD), bf16), NG=((2, nz, hb, width), bf16), NR=((nz, hb, width), bf16),
        DWQ=((nf, nz, shard, 4 * HD), bf16), RWQ=((nf - 1, nz, shard, 4 * HD), bf16),
        ZWQ=((nz, shard, 4 * HD), bf16), LWQ=((nz, shard, 4 * HD), bf16),
        SG1=((2, 8, width), f32), SG1P=((8, width), f32), RSG1=((nf, nz, 8, 128), f32),
        EXB=((2, hb, width), bf16), EXG=((2, hb, width), f32),
    )
    slots = (136, 160)
    out = pl.pallas_call(
        functools.partial(layer_kernel, (nf, nz, hb, width, experts, half_ff, ndoc, chosen)),
        name="layer",
        out_shape=(
            shape((2, hb, width), bf16), shape((2, hb, width), f32), shape((experts + 8, 128), f32),
            shape((8, 128), f32), shape((nz, shard, 4 * HD), bf16), shape((shard, W), f32),
            shape((nf, nz, shard, 2 * half_ff), bf16), shape((nf, nz, shard, half_ff), bf16),
        ),
        in_specs=[anywhere] * 2 + [vm] * 3 + [anywhere] + [vm] * 3 + [anywhere] * 3
        + [pl.BlockSpec(memory_space=pltpu.SMEM), vm, vm],
        out_specs=(anywhere,) * 2 + (vm,) * 2 + (anywhere, vm) + (anywhere,) * 2,
        scratch_shapes=[pltpu.VMEM(s, d) for s, d in scratch.values()]
        + [pltpu.SemaphoreType.DMA((slots[0],)), pltpu.SemaphoreType.DMA((slots[1],)), pltpu.SemaphoreType.DMA((11,))],
        compiler_params=pltpu.CompilerParams(
            collective_id=0, has_side_effects=True, vmem_limit_bytes=67043328
        ),
    )(
        hidden_in[0], out_grad[0], query_weight, key_weight, value_weight, output_weight,
        attention_gain[None], expert_gain[None], router_weight.T, gate_weight, up_weight, down_weight,
        doc_lengths, expert_choice[0].T, frequency,
    )
    steps = nz // 2
    some = lambda *s: pl.BlockSpec(s, lambda i: (i,) + (0,) * (len(s) - 1))
    whole = lambda *s: pl.BlockSpec(s, lambda i: (0,) * len(s))
    per = nf * nz // steps
    out = pl.pallas_call(
        functools.partial(finish_kernel, (nz, experts, half_ff, shard)),
        name="finish",
        grid=(steps,),
        out_shape=(
            shape((block, width), bf16), shape((block, width), f32), shape((1, shard), f32),
            shape((shard, nz * 2 * HD), f32), shape((shard, nz * HD), f32), shape((shard, nz * HD), f32),
            shape((shard, W), f32), shape((1, shard), f32), shape((experts, shard), f32),
            shape((experts, shard, half_ff), f32), shape((experts, shard, half_ff), f32),
            shape((experts, shard, half_ff), f32),
        ),
        in_specs=[
            some(block // steps, width), some(block // steps, width), whole(experts + 8, 128), whole(8, 128),
            whole(nz, shard, 4 * HD), whole(shard, W), some(per, shard, 2 * half_ff), some(per, shard, half_ff),
        ],
        out_specs=(
            some(block // steps, width), some(block // steps, width), whole(1, shard),
            whole(shard, nz * 2 * HD), whole(shard, nz * HD), whole(shard, nz * HD), whole(shard, W), whole(1, shard),
            whole(experts, shard), some(per, shard, half_ff), some(per, shard, half_ff), some(per, shard, half_ff),
        ),
        compiler_params=pltpu.CompilerParams(vmem_limit_bytes=67043328),
    )(out[0].reshape(block, width), out[1].reshape(block, width), *out[2:6], out[6].reshape(experts, shard, 2 * half_ff), out[7].reshape(experts, shard, half_ff))
    block_out, input_grad, gain1, q, k, v, o, gain2, router, gate, up, down = out
    return (
        block_out[None], input_grad[None], gain1[0], q, k, v, o, gain2[0], router.T, gate, up, down,
    )


def fits(mesh, args):
    nf, nz, nc = mesh.shape["fsdp"], mesh.shape["ctx"], mesh.shape["tp"]
    hidden, query, key, gate = args[0], args[3], args[4], args[9]
    width, block = hidden.shape[2], hidden.shape[1] // nz
    return (
        nc == 2
        and nz == 4
        and nf == 4
        and hidden.shape[0] == nf
        and gate.shape[0] == nf * nz
        and gate.shape[0] == 16
        and width == 64 * nf * nz
        and block == 128
        and query.shape[1] == 2 * HD * nz * nc
        and key.shape[1] == HD * nz * nc
        and HD == 64
    )


def solution(mesh):
    in_specs = (
        P("fsdp", "ctx", None),
        P("fsdp", "ctx", None),
        P(("fsdp", "ctx")),
        P(("fsdp", "ctx"), "tp"),
        P(("fsdp", "ctx"), "tp"),
        P(("fsdp", "ctx"), "tp"),
        P(("fsdp", "ctx"), "tp"),
        P(("fsdp", "ctx")),
        P(("fsdp", "ctx"), None),
        P(None, ("fsdp", "ctx"), "tp"),
        P(None, ("fsdp", "ctx"), "tp"),
        P(None, ("fsdp", "ctx"), "tp"),
        P("fsdp", None),
        P("fsdp", "ctx", None),
    )
    out_specs = (
        P("fsdp", "ctx", None),
        P("fsdp", "ctx", None),
        P(("fsdp", "ctx")),
        P(("fsdp", "ctx"), "tp"),
        P(("fsdp", "ctx"), "tp"),
        P(("fsdp", "ctx"), "tp"),
        P(("fsdp", "ctx"), "tp"),
        P(("fsdp", "ctx")),
        P(("fsdp", "ctx"), None),
        P(None, ("fsdp", "ctx"), "tp"),
        P(None, ("fsdp", "ctx"), "tp"),
        P(None, ("fsdp", "ctx"), "tp"),
    )

    def step(*args):
        body = local
        if fits(mesh, args):
            body = functools.partial(fast_local, mesh.shape["fsdp"], mesh.shape["ctx"])
        return jax.shard_map(
            body, mesh=mesh, in_specs=in_specs, out_specs=out_specs, check_vma=False
        )(*args)

    return step
```

```python
import functools

import jax
import jax.numpy as jnp
import numpy as np
from jax import lax
from jax.experimental import pallas as pl
from jax.experimental.pallas import tpu as pltpu
from jax.sharding import PartitionSpec as P

HD = 64


epsilon = 1e-05
rope_base = 10000.0
masked_score = -1e30
highest = lax.Precision.HIGHEST


def doc_layout(lengths, positions):
    ends = jnp.cumsum(lengths)
    after = (positions[:, None] >= ends[None, :]).astype(jnp.int32)
    segment = jnp.sum(after, axis=1)
    offset = positions - jnp.sum(after * lengths[None, :], axis=1)
    return (segment, offset)


def rope_tables(offset):
    halfway = HD // 2
    frequency = rope_base ** (-jnp.arange(halfway, dtype=jnp.float32) / halfway)
    angle = offset.astype(jnp.float32)[:, None] * frequency[None, :]
    return (jnp.cos(angle), jnp.sin(angle))


def rotate(vectors, cosine, sine):
    halfway = vectors.shape[-1] // 2
    former = vectors[..., :halfway]
    latter = vectors[..., halfway:]
    cosine = cosine[:, None, :]
    sine = sine[:, None, :]
    return jnp.concatenate(
        [former * cosine - latter * sine, latter * cosine + former * sine], axis=-1
    )


def rotate_back(grads, cosine, sine):
    halfway = grads.shape[-1] // 2
    former = grads[..., :halfway]
    latter = grads[..., halfway:]
    cosine = cosine[:, None, :]
    sine = sine[:, None, :]
    return jnp.concatenate(
        [former * cosine + latter * sine, latter * cosine - former * sine], axis=-1
    )


def norm_forward(values, gain):
    inverse = lax.rsqrt(jnp.mean(values * values, axis=-1, keepdims=True) + epsilon)
    return (values * inverse * gain.astype(jnp.float32), inverse)


def norm_backward(values, inverse, gain, grad_normed):
    scaled = grad_normed * gain.astype(jnp.float32)
    grad_values = inverse * scaled - values * inverse**3 * jnp.mean(
        scaled * values, axis=-1, keepdims=True
    )
    grad_gain = jnp.sum(grad_normed * values * inverse, axis=0)
    return (grad_values, grad_gain)


def dispatch(route, experts, capacity):
    flat = route.reshape(-1)
    onehot = (flat[:, None] == jnp.arange(experts, dtype=jnp.int32)[None, :]).astype(jnp.int32)
    rank = jnp.sum((jnp.cumsum(onehot, axis=0) - onehot) * onehot, axis=1)
    slot = flat * capacity + rank
    pairs = flat.shape[0]
    owner = (
        jnp.zeros((experts * capacity,), jnp.int32).at[slot].set(jnp.arange(pairs, dtype=jnp.int32))
    )
    filled = jnp.zeros((experts * capacity,), jnp.int32).at[slot].set(1) > 0
    return (slot, owner, filled)


def expert_math(slot_inputs, slot_grads, gate_full, up_full, down_full):
    gate_pre = jnp.einsum(
        "gsd,gdf->gsf", slot_inputs, gate_full, preferred_element_type=jnp.float32
    )
    up_pre = jnp.einsum("gsd,gdf->gsf", slot_inputs, up_full, preferred_element_type=jnp.float32)
    sigmoid = jax.nn.sigmoid(gate_pre)
    activated = (gate_pre * sigmoid * up_pre).astype(jnp.bfloat16)
    expert_out = jnp.einsum(
        "gsf,gdf->gsd", activated, down_full, preferred_element_type=jnp.float32
    )
    act_grad = jnp.einsum("gsd,gdf->gsf", slot_grads, down_full, preferred_element_type=jnp.float32)
    gate_pre_grad = (act_grad * up_pre * sigmoid * (1.0 + gate_pre * (1.0 - sigmoid))).astype(
        jnp.bfloat16
    )
    up_pre_grad = (act_grad * gate_pre * sigmoid).astype(jnp.bfloat16)
    down_term = jnp.einsum(
        "gsd,gsf->gdf", slot_grads, activated, preferred_element_type=jnp.float32
    )
    gate_term = jnp.einsum(
        "gsd,gsf->gdf", slot_inputs, gate_pre_grad, preferred_element_type=jnp.float32
    )
    up_term = jnp.einsum(
        "gsd,gsf->gdf", slot_inputs, up_pre_grad, preferred_element_type=jnp.float32
    )
    slot_back = jnp.einsum(
        "gsf,gdf->gsd", gate_pre_grad, gate_full, preferred_element_type=jnp.float32
    ) + jnp.einsum("gsf,gdf->gsd", up_pre_grad, up_full, preferred_element_type=jnp.float32)
    return (expert_out, slot_back, gate_term, up_term, down_term)


def local(
    hidden_in,
    out_grad,
    attention_gain,
    query_weight,
    key_weight,
    value_weight,
    output_weight,
    expert_gain,
    router_weight,
    gate_weight,
    up_weight,
    down_weight,
    doc_lengths,
    expert_choice,
):
    block = hidden_in.shape[1]
    experts = gate_weight.shape[0]
    capacity = block * 3 // 4
    chosen_count = expert_choice.shape[2]
    context_count = lax.axis_size("ctx")
    scale = HD ** (-0.5)
    position = lax.axis_index("ctx") * block + jnp.arange(block, dtype=jnp.int32)
    lengths = doc_lengths[0]
    segment, offset = doc_layout(lengths, position)
    cosine, sine = rope_tables(offset)
    gain_one, query_full, key_full, value_full, output_full, gain_two, router_full = (
        lax.all_gather(attention_gain, ("fsdp", "ctx"), axis=0, tiled=True),
        lax.all_gather(query_weight, ("fsdp", "ctx"), axis=0, tiled=True),
        lax.all_gather(key_weight, ("fsdp", "ctx"), axis=0, tiled=True),
        lax.all_gather(value_weight, ("fsdp", "ctx"), axis=0, tiled=True),
        lax.all_gather(output_weight, ("fsdp", "ctx"), axis=0, tiled=True),
        lax.all_gather(expert_gain, ("fsdp", "ctx"), axis=0, tiled=True),
        lax.all_gather(router_weight, ("fsdp", "ctx"), axis=0, tiled=True),
    )
    inputs = hidden_in[0].astype(jnp.float32)
    normed_one, inverse_one = norm_forward(inputs, gain_one)
    normed_one = normed_one.astype(jnp.bfloat16)
    heads_local = query_full.shape[1] // HD
    groups_local = key_full.shape[1] // HD
    ratio = heads_local // groups_local
    query = rotate(
        jnp.dot(normed_one, query_full, preferred_element_type=jnp.float32).reshape(
            block, heads_local, HD
        ),
        cosine,
        sine,
    ).astype(jnp.bfloat16)
    keys = rotate(
        jnp.dot(normed_one, key_full, preferred_element_type=jnp.float32).reshape(
            block, groups_local, HD
        ),
        cosine,
        sine,
    ).astype(jnp.bfloat16)
    values = jnp.dot(normed_one, value_full, preferred_element_type=jnp.float32).astype(
        jnp.bfloat16
    )
    query_grouped = query.reshape(block, groups_local, ratio, HD)

    def allowed_mask(key_start, count):
        key_position = key_start + jnp.arange(count, dtype=jnp.int32)
        key_segment, unused = doc_layout(lengths, key_position)
        return (segment[:, None] == key_segment[None, :]) & (
            key_position[None, :] <= position[:, None]
        )

    def forward_update(state, key_block, value_block, allowed):
        peak, total, accum = state
        mask = allowed[:, None, None, :]
        scores = (
            jnp.einsum(
                "qgrd,kgd->qgrk", query_grouped, key_block, preferred_element_type=jnp.float32
            )
            * scale
        )
        scores = jnp.where(mask, scores, masked_score)
        new_peak = jnp.maximum(peak, jnp.max(scores, axis=3))
        weights = jnp.where(mask, jnp.exp(scores - new_peak[..., None]), 0.0)
        rescale = jnp.exp(peak - new_peak)
        total = total * rescale + jnp.sum(weights, axis=3)
        accum = accum * rescale[..., None] + jnp.einsum(
            "qgrk,kgd->qgrd", weights, value_block.astype(jnp.float32), precision=highest
        )
        return (new_peak, total, accum)

    travel = (keys.reshape(block, groups_local * HD), values)
    initial = (
        jnp.full((block, groups_local, ratio), masked_score, jnp.float32),
        jnp.zeros((block, groups_local, ratio), jnp.float32),
        jnp.zeros((block, groups_local, ratio, HD), jnp.float32),
    )
    state = initial
    key_piece = lax.all_gather(travel[0], "ctx", axis=0, tiled=True)
    value_piece = lax.all_gather(travel[1], "ctx", axis=0, tiled=True)
    pieces = key_piece.shape[0] // block
    key_blocks = key_piece.reshape(pieces, block, groups_local, HD)
    value_blocks = value_piece.reshape(pieces, block, groups_local, HD)
    starts = block * jnp.arange(pieces, dtype=jnp.int32)

    def visit(carry, item):
        key_block, value_block, key_start = item
        allowed = allowed_mask(key_start, block)
        return (forward_update(carry, key_block, value_block, allowed), None)

    state, unused = lax.scan(visit, state, (key_blocks, value_blocks, starts))
    peak, total, accum = state
    attended = (accum / total[..., None]).reshape(block, heads_local * HD).astype(jnp.bfloat16)
    log_total = peak + jnp.log(total)
    projected = lax.psum(jnp.dot(attended, output_full.T, preferred_element_type=jnp.float32), "tp")
    residual = inputs + projected
    normed_two, inverse_two = norm_forward(residual, gain_two)
    normed_two = normed_two.astype(jnp.bfloat16)
    route = expert_choice[0]
    logits = jnp.dot(normed_two, router_full, preferred_element_type=jnp.float32)
    gates = jax.nn.softmax(jnp.take_along_axis(logits, route, axis=1), axis=1)
    slot, owner, filled = dispatch(route, experts, capacity)
    token_of = owner // chosen_count
    grad_out = out_grad[0].astype(jnp.float32)
    slot_inputs = jnp.where(filled[:, None], normed_two[token_of], 0).reshape(experts, capacity, -1)
    slot_gate = jnp.where(filled, gates.reshape(-1)[owner], 0.0)
    slot_grads = (
        (grad_out[token_of] * slot_gate[:, None])
        .astype(jnp.bfloat16)
        .reshape(experts, capacity, -1)
    )
    gate_full, up_full, down_full = (
        lax.all_gather(gate_weight, ("fsdp", "ctx"), axis=1, tiled=True),
        lax.all_gather(up_weight, ("fsdp", "ctx"), axis=1, tiled=True),
        lax.all_gather(down_weight, ("fsdp", "ctx"), axis=1, tiled=True),
    )
    expert_out, slot_back, gate_term, up_term, down_term = expert_math(
        slot_inputs, slot_grads, gate_full, up_full, down_full
    )
    gate_share, up_share, down_share = (
        lax.psum_scatter(gate_term, ("fsdp", "ctx"), scatter_dimension=1, tiled=True),
        lax.psum_scatter(up_term, ("fsdp", "ctx"), scatter_dimension=1, tiled=True),
        lax.psum_scatter(down_term, ("fsdp", "ctx"), scatter_dimension=1, tiled=True),
    )
    pair_out = expert_out.reshape(experts * capacity, -1)[slot].reshape(block, chosen_count, -1)
    pair_back = slot_back.reshape(experts * capacity, -1)[slot].reshape(block, chosen_count, -1)
    mixed_part = jnp.sum(gates[..., None] * pair_out, axis=1)
    gate_dot_part = jnp.sum(pair_out * grad_out[:, None, :], axis=2)
    moe_part = jnp.sum(pair_back, axis=1)
    mixed, gate_dot, moe_input = (
        lax.psum(mixed_part.astype(jnp.bfloat16), "tp").astype(jnp.float32),
        lax.psum(gate_dot_part.astype(jnp.bfloat16), "tp").astype(jnp.float32),
        lax.psum(moe_part.astype(jnp.bfloat16), "tp").astype(jnp.float32),
    )
    block_out = (residual + mixed).astype(jnp.bfloat16)[None]
    chosen_grad = gates * (gate_dot - jnp.sum(gates * gate_dot, axis=1, keepdims=True))
    picked = (route[..., None] == jnp.arange(experts, dtype=jnp.int32)[None, None, :]).astype(
        jnp.float32
    )
    logit_grad = jnp.sum(picked * chosen_grad[..., None], axis=1)
    router_term = jnp.dot(normed_two.astype(jnp.float32).T, logit_grad, precision=highest)
    router_input = jnp.dot(logit_grad, router_full.astype(jnp.float32).T, precision=highest)
    grad_residual_norm, gain_two_term = norm_backward(
        residual, inverse_two, gain_two, moe_input + router_input
    )
    grad_residual = grad_out + grad_residual_norm
    residual_low = grad_residual.astype(jnp.bfloat16)
    attended_grad = jnp.dot(residual_low, output_full, preferred_element_type=jnp.float32).astype(
        jnp.bfloat16
    )
    output_term = jnp.dot(residual_low.T, attended, preferred_element_type=jnp.float32)
    delta = jnp.sum(
        (attended_grad.astype(jnp.float32) * attended.astype(jnp.float32)).reshape(
            block, groups_local, ratio, HD
        ),
        axis=3,
    )
    grad_grouped = attended_grad.reshape(block, groups_local, ratio, HD)
    back_keys, back_values = (
        lax.all_gather(travel[0], "ctx", axis=0, tiled=True),
        lax.all_gather(travel[1], "ctx", axis=0, tiled=True),
    )
    key_blocks = back_keys.reshape(context_count, block, groups_local, HD)
    value_blocks = back_values.reshape(context_count, block, groups_local, HD)
    starts = block * jnp.arange(context_count, dtype=jnp.int32)

    def backward_update(grad_query, key_block, value_block, allowed):
        mask = allowed[:, None, None, :]
        scores = (
            jnp.einsum(
                "qgrd,kgd->qgrk", query_grouped, key_block, preferred_element_type=jnp.float32
            )
            * scale
        )
        probs = jnp.where(mask, jnp.exp(scores - log_total[..., None]), 0.0)
        value_grad = jnp.einsum(
            "qgrk,qgrd->kgd",
            probs.astype(jnp.bfloat16),
            grad_grouped,
            preferred_element_type=jnp.float32,
        )
        prob_grad = jnp.einsum(
            "qgrd,kgd->qgrk", grad_grouped, value_block, preferred_element_type=jnp.float32
        )
        score_grad = (probs * (prob_grad - delta[..., None]) * scale).astype(jnp.bfloat16)
        grad_query = grad_query + jnp.einsum(
            "qgrk,kgd->qgrd", score_grad, key_block, preferred_element_type=jnp.float32
        )
        key_grad = jnp.einsum(
            "qgrk,qgrd->kgd", score_grad, query_grouped, preferred_element_type=jnp.float32
        )
        return (grad_query, key_grad.reshape(block, -1), value_grad.reshape(block, -1))

    def backward_visit(grad_query, item):
        key_block, value_block, key_start = item
        allowed = allowed_mask(key_start, block)
        grad_query, key_grad, value_grad = backward_update(
            grad_query, key_block, value_block, allowed
        )
        return (grad_query, (key_grad, value_grad))

    grad_query, (key_grads, value_grads) = lax.scan(
        backward_visit,
        jnp.zeros((block, groups_local, ratio, HD), jnp.float32),
        (key_blocks, value_blocks, starts),
    )
    own_key_grad, own_value_grad = (
        lax.psum_scatter(
            key_grads.reshape(context_count * block, -1).astype(jnp.bfloat16),
            "ctx",
            scatter_dimension=0,
            tiled=True,
        ).astype(jnp.float32),
        lax.psum_scatter(
            value_grads.reshape(context_count * block, -1).astype(jnp.bfloat16),
            "ctx",
            scatter_dimension=0,
            tiled=True,
        ).astype(jnp.float32),
    )
    query_grad = (
        rotate_back(grad_query.reshape(block, heads_local, HD), cosine, sine)
        .reshape(block, -1)
        .astype(jnp.bfloat16)
    )
    key_grad = (
        rotate_back(own_key_grad.reshape(block, groups_local, HD), cosine, sine)
        .reshape(block, -1)
        .astype(jnp.bfloat16)
    )
    value_grad = own_value_grad.astype(jnp.bfloat16)
    input_part = jnp.dot(query_grad, query_full.T, preferred_element_type=jnp.float32)
    input_part = input_part + jnp.dot(key_grad, key_full.T, preferred_element_type=jnp.float32)
    input_part = input_part + jnp.dot(value_grad, value_full.T, preferred_element_type=jnp.float32)
    normed_one_grad = lax.psum(input_part.astype(jnp.bfloat16), "tp").astype(jnp.float32)
    grad_input_norm, gain_one_term = norm_backward(inputs, inverse_one, gain_one, normed_one_grad)
    input_grad = (grad_residual + grad_input_norm)[None]
    query_term = jnp.dot(normed_one.T, query_grad, preferred_element_type=jnp.float32)
    key_term = jnp.dot(normed_one.T, key_grad, preferred_element_type=jnp.float32)
    value_term = jnp.dot(normed_one.T, value_grad, preferred_element_type=jnp.float32)
    (
        gain_one_share,
        query_share,
        key_share,
        value_share,
        output_share,
        gain_two_share,
        router_share,
    ) = (
        lax.psum_scatter(gain_one_term, ("fsdp", "ctx"), scatter_dimension=0, tiled=True),
        lax.psum_scatter(query_term, ("fsdp", "ctx"), scatter_dimension=0, tiled=True),
        lax.psum_scatter(key_term, ("fsdp", "ctx"), scatter_dimension=0, tiled=True),
        lax.psum_scatter(value_term, ("fsdp", "ctx"), scatter_dimension=0, tiled=True),
        lax.psum_scatter(output_term, ("fsdp", "ctx"), scatter_dimension=0, tiled=True),
        lax.psum_scatter(gain_two_term, ("fsdp", "ctx"), scatter_dimension=0, tiled=True),
        lax.psum_scatter(router_term, ("fsdp", "ctx"), scatter_dimension=0, tiled=True),
    )
    return (
        block_out,
        input_grad,
        gain_one_share,
        query_share,
        key_share,
        value_share,
        output_share,
        gain_two_share,
        router_share,
        gate_share,
        up_share,
        down_share,
    )


MESH = pl.DeviceIdType.MESH
f32 = jnp.float32
bf16 = jnp.bfloat16


def dot_nn(a, b, precision=None):
    return lax.dot_general(a, b, (((1,), (0,)), ((), ())), precision=precision, preferred_element_type=f32)


def dot_nt(a, b, precision=None):
    return lax.dot_general(a, b, (((1,), (1,)), ((), ())), precision=precision, preferred_element_type=f32)


def dot_tn(a, b, precision=None):
    return lax.dot_general(a, b, (((0,), (0,)), ((), ())), precision=precision, preferred_element_type=f32)


class Net:
    def __init__(self, send_sems, recv_sems):
        self.send_sems, self.recv_sems, self.copies, self.left = send_sems, recv_sems, [], set()
        self.slots, self.free_send, self.free_recv = [], [], []
        self.top_send = self.top_recv = 0

    def make(self, source, target, device, sends=None):
        if self.free_send:
            send_at = self.free_send.pop(0)
        else:
            send_at, self.top_send = self.top_send, self.top_send + 1
        if self.free_recv:
            recv_at = self.free_recv.pop(0)
        else:
            recv_at, self.top_recv = self.top_recv, self.top_recv + 1
        assert max(send_at + 1 - self.send_sems.shape[0], recv_at + 1 - self.recv_sems.shape[0]) <= 0
        copy = pltpu.make_async_remote_copy(
            src_ref=source,
            dst_ref=target,
            send_sem=self.send_sems.at[send_at],
            recv_sem=self.recv_sems.at[recv_at],
            device_id=device,
            device_id_type=MESH,
        )
        self.copies.append((copy, sends))
        self.slots.append((send_at, recv_at))
        return copy

    def send(self, source, target, device):
        copy = self.make(source, target, device)
        copy.start()
        return copy

    def together(self, triples, whole):
        first = self.make(*triples[0])
        send_at, recv_at = self.slots[-1]
        first.start()
        for source, target, device in triples[1:]:
            pltpu.make_async_remote_copy(
                src_ref=source,
                dst_ref=target,
                send_sem=self.send_sems.at[send_at],
                recv_sem=self.recv_sems.at[recv_at],
                device_id=device,
                device_id_type=MESH,
            ).start()
        waits = Whole(
            pltpu.make_async_copy(whole, whole, self.send_sems.at[send_at]),
            pltpu.make_async_copy(whole, whole, self.recv_sems.at[recv_at]),
        )
        self.copies[-1] = (waits, None)
        return waits

    def free(self, among):
        self.free_recv.extend(self.slots[at][1] for at in among)

    def numbers(self, *groups):
        found = []
        for group in groups:
            if isinstance(group, list):
                found += self.numbers(*group)
            else:
                copy = group[0] if isinstance(group, tuple) else group
                found += [at for at, (one, sends) in enumerate(self.copies) if one is copy]
        return found

    def drain(self, among=None):
        for at, (copy, sends) in enumerate(self.copies):
            if at in self.left or (among is not None and at not in among):
                continue
            self.left.add(at)
            self.free_send.append(self.slots[at][0])
            if sends is None:
                copy.wait_send()
            else:
                pl.when(sends)(copy.wait_send)


class Whole:
    def __init__(self, sent, received):
        self.wait_send, self.wait_recv = sent.wait, received.wait


class Line:
    def __init__(self, net, z, nz, device):
        self.net, self.z, self.nz, self.device = net, z, nz, device

    def both(self):
        z, nz = self.z, self.nz
        right, left = self.device(lax.min(z + 1, nz - 1)), self.device(lax.max(z - 1, 0))
        return ((z, right), (nz - 1 - z, left))

    def pass_on(self, step, views):
        copies = []
        for way, (rank, target) in enumerate(self.both()):
            sends = (rank >= step) & (rank < self.nz - 1)
            arrives = rank >= step + 1
            block = lax.clamp(0, self.z - step if way == 0 else self.z + step, self.nz - 1)
            for view in views:
                copy = self.net.make(view(block), view(block), target, sends)
                pl.when(sends)(copy.start)
                copies.append((copy, arrives))
        return copies

    def add_on(self, step, own, out, into):
        copies = []
        for way, (rank, target) in enumerate(self.both()):
            sends = rank <= step
            arrives = (rank >= 1) & (rank - 1 <= step)
            dest = self.nz - 1 - step + rank
            dest = lax.clamp(0, dest if way == 0 else self.nz - 1 - dest, self.nz - 1)
            copy = self.net.make(out(way, step), into(way, step), target, sends)

            def prepare():
                out(way, step)[...] = own(dest)[...].astype(bf16)
                if step > 0:

                    def add():
                        out(way, step)[...] = (own(dest)[...] + into(way, step - 1)[...].astype(f32)).astype(bf16)

                    pl.when(rank >= 1)(add)
                copy.start()

            pl.when(sends)(prepare)
            copies.append((copy, arrives))
        return copies

    def finish(self, total, into):
        for way, (rank, target) in enumerate(self.both()):

            def add():
                total[...] += into(way, self.nz - 2)[...].astype(f32)

            pl.when(rank >= 1)(add)


def arrive(copies):
    for copy, arrives in copies:
        pl.when(arrives)(copy.wait_recv)


def layer_kernel(
    dims,
    x_ref, g_ref, wq_ref, wk_ref, wv_ref, wo_ref, ga_ref, ge_ref, rt_ref, wg_ref, wu_ref, wd_ref, dl_ref, ec_ref,
    fr_ref,
    block_out, input_grad, small_out, gain_out, dqkv_out, dwo_out, dgu_out, dd_out,
    WP, SMT, X, WQ, WO, SMB, SMW, N1, CT, ST, SEGC, POSC, Q, K, V, PSC, ATT, AT, PP, PR, RES,
    N2, GTB, GA, WGU, WD, SWG, SWU, SWD, AA, PSX, GC, H, UG, PRD, MP, MR, BP, BR, DGU, DDT, GDS, GD,
    RB, RM, RBV, RMV, BOWN, MOWN, CO, CI, MO, MI, DGB, GUL, ZG, DDB, DDL, ZD, SG, SGF, SGT, SGZ, SGP, GRES, RL,
    AGS, AGR, DWO, RWO, ZWO, LWO, DS, DQ, DQKV, NG, NR, DWQ, RWQ, ZWQ, LWQ,
    SGW, SG1, SG1P, RSG1, EXB, EXG,
    send_sems, recv_sems, local_sems,
):
    nf, nz, hb, width, experts, half_ff, ndoc, chosen = dims
    rows = 2 * nz * hb
    half = nz * hb
    block = 2 * hb
    shard = width // (nf * nz)
    f, z, c = lax.axis_index("fsdp"), lax.axis_index("ctx"), lax.axis_index("tp")
    other = 1 - c
    own = f * nz + z
    net = Net(send_sems, recv_sems)
    device = lambda df, dz, core: {"fsdp": df, "ctx": dz, "tp": core}
    partner = device(f, z, other)
    line = Line(net, z, nz, lambda dz: device(f, dz, c))
    zs = [z, z + 1 - 2 * lax.rem(z, 2), lax.rem(z + 2, 4), 3 - z]
    fs = [f, f + 1 - 2 * lax.rem(f, 2), lax.rem(f + 2, 4), 3 - f]
    everyone = [(i, j, k) for k in range(2) for i in range(nf) for j in range(nz) if (i, j, k) != (0, 0, 0)]
    others = [device(fs[i], zs[j], lax.rem(c + k, 2)) for i, j, k in everyone]
    same = [(i, 0) for i in range(1, nf)] + [(i, j) for i in range(nf) for j in (3, 1, 2)]

    mine = pl.ds(pl.multiple_of(c * hb, hb), hb)
    loads = [
        pltpu.make_async_copy(x_ref.at[mine], X.at[c, z], local_sems.at[0]),
        pltpu.make_async_copy(g_ref.at[mine], GA.at[f, c, z], local_sems.at[1]),
        pltpu.make_async_copy(wo_ref, WO.at[f, z], local_sems.at[2]),
    ]
    row_experts = lambda at: pl.ds(at * nz, nz)
    shards = ((wg_ref, SWG), (wu_ref, SWU), (wd_ref, SWD))
    loads += [
        pltpu.make_async_copy(ref.at[row_experts(f)], staged.at[f], local_sems.at[3 + at])
        for at, (ref, staged) in enumerate(shards)
    ]
    unit = half_ff // 2
    units = lambda h: pl.ds(h * unit, unit)
    for copy in loads:
        copy.start()
    barrier = pltpu.get_barrier_semaphore()
    for peer in others:
        pl.semaphore_signal(barrier, inc=1, device_id=peer, device_id_type=MESH)

    for j in range(nz):
        WP[j, :, 0 : 2 * HD] = wq_ref[:, 2 * HD * j : 2 * HD * (j + 1)]
        WP[j, :, 2 * HD : 4 * HD] = jnp.concatenate(
            [wk_ref[:, HD * j : HD * (j + 1)], wv_ref[:, HD * j : HD * (j + 1)]], axis=1
        )
    base = jnp.concatenate(
        [ga_ref[...].astype(f32), ge_ref[...].astype(f32), jnp.zeros((14, shard), f32), rt_ref[...].astype(f32)],
        axis=0,
    )
    in_half = (lax.broadcasted_iota(jnp.int32, (32, 128), 1) < shard) == (lax.rem(z, 2) == 0)
    SMT[...] = jnp.where(in_half, jnp.concatenate([base, base], axis=1), 0.0).astype(bf16)
    SMB[f, z] = SMT[...]
    WQ[f, z] = WP[z]
    pl.semaphore_wait(barrier, len(others))

    wd_full = lambda: WD[...].reshape(width, half_ff)
    wgu_full = lambda: WGU[...].reshape(width, 2 * half_ff)
    lower, upper = pl.ds(0, nz // 2), pl.ds(nz // 2, nz // 2)
    across = [None, device(fs[1], z, c), device(fs[2], z, c), device(fs[3], z, c)]

    def second_hop(ref):
        return [net.send(ref.at[f, c], ref.at[f, c], across[k]) for k in (1, 2)]

    def third_hop(ref, k):
        part, to = ((lower, across[2]), (upper, across[1]))[k - 1]
        return net.send(ref.at[fs[k], c, part], ref.at[fs[k], c, part], to)

    sends_q = [net.send(WP.at[zs[k]], WQ.at[f, z], device(f, zs[k], c)) for k in range(1, nz)]
    sends_s = [net.send(SMT, SMB.at[f, z], device(f, zs[k], c)) for k in range(1, nz)]
    loads[0].wait()
    sends_x = [net.send(X.at[c, z], X.at[c, z], device(f, zs[k], c)) for k in range(1, nz)]
    forwards_x = [net.send(X.at[c, z], X.at[c, z], partner)]
    loads[2].wait()
    sends_o = [net.send(WO.at[f, z], WO.at[f, z], device(f, zs[k], c)) for k in range(1, nz)]
    loads[1].wait()
    view_g = [lambda at: GA.at[f, c, at]]
    chain_g = line.pass_on(0, view_g)
    chains = [chain_g]
    weights = ([], [], [])

    def send_row(k, at):
        ref, staged = shards[at]
        return net.send(ref.at[row_experts(fs[k])], staged.at[f], device(fs[k], z, c))

    sends_e = [[send_row(k, at) for k in (1, 2)] for at in range(3)]

    def send_weights(k, *what):
        for at in what:
            staged, into, lanes, target = (
                (SWG, WGU, units(0), units(0)),
                (SWU, WGU, units(0), units(1)),
                (SWG, WGU, units(1), units(2)),
                (SWU, WGU, units(1), units(3)),
                (SWD, WD, pl.ds(0, half_ff), pl.ds(0, half_ff)),
            )[at]
            weights[at // 2].append(
                net.send(staged.at[:, zs[k], :, lanes], into.at[:, z, :, target], device(f, zs[k], c))
            )

    def places(shape, dim):
        at = lax.broadcasted_iota(jnp.int32, shape, dim)
        core_at, rest = lax.div(at, half), lax.rem(at, half)
        return lax.div(rest, hb) * block + core_at * hb + lax.rem(rest, hb)

    def layout(position):
        segment = jnp.zeros_like(position)
        start = jnp.zeros_like(position)
        end = jnp.int32(0)
        for i in range(ndoc):
            length = dl_ref[0, i]
            end = end + length
            after = jnp.where(position >= end, 1, 0)
            segment = segment + after
            start = start + after * length
        return segment, position - start

    lane = lax.broadcasted_iota(jnp.int32, (1, 2 * HD), 1)
    former = lax.rem(lane, HD) < HD // 2
    is_key = lane < HD

    with jax.named_scope("tables0"):
        pos_col = places((rows, 1), 0)
        seg_col, offset = layout(pos_col)
        POSC[...] = pos_col
        SEGC[...] = seg_col
        pos_row = places((1, rows), 1)
        seg_row, unused = layout(pos_row)

    def swapped(v):
        return jnp.where(former, pltpu.roll(v, 2 * HD - HD // 2, 1), pltpu.roll(v, HD // 2, 1))

    for copy in sends_q:
        copy.wait_recv()
    sends_q2 = [net.send(WQ.at[f], WQ.at[f], device(fs[k], z, c)) for k in range(1, nf)]
    for copy in sends_s:
        copy.wait_recv()
    sends_s2 = [net.send(SMB.at[f], SMB.at[f], device(fs[k], z, c)) for k in range(1, nf)]
    for at in (0, 1):
        sends_e[at].append(send_row(3, at))
    with jax.named_scope("tables1"):
        angle = offset.astype(f32) * fr_ref[0:1, :]
        CT[...] = jnp.cos(angle)
        ST[...] = jnp.where(former, -1.0, 1.0) * jnp.sin(angle)
    for copy in sends_s2:
        copy.wait_recv()
    for pair in range(nf * nz // 2):
        at_f, at_z = pair // (nz // 2), 2 * (pair % (nz // 2))
        SMW[:, 128 * pair : 128 * pair + 128] = SMB[at_f, at_z] + SMB[at_f, at_z + 1]

    def norm_block(at_c, at_z):
        v = X[at_c, at_z].astype(f32)
        inverse = lax.rsqrt(jnp.mean(v * v, axis=1, keepdims=True) + epsilon)
        at = pl.ds(pl.multiple_of((at_c * nz + at_z) * hb, hb), hb)
        N1[at, :] = (v * inverse * SMW[0:1, :].astype(f32)).astype(bf16)

    norm_block(c, z)
    for k in range(1, nz):
        sends_x[k - 1].wait_recv()
        forwards_x.append(net.send(X.at[c, zs[k]], X.at[c, zs[k]], partner))
        norm_block(c, zs[k])
    for k in range(nz):
        forwards_x[k].wait_recv()
        norm_block(other, zs[k])
    for copy in sends_q2:
        copy.wait_recv()
    with jax.named_scope("qkv"):
        projected = dot_nn(N1[...], WQ[...].reshape(width, 4 * HD))
        cosine, sine = CT[...], ST[...]
        q_part, kv_part = projected[:, : 2 * HD], projected[:, 2 * HD :]
        Q[...] = (q_part * cosine + swapped(q_part) * sine).astype(bf16)
        kv = jnp.where(is_key, kv_part * cosine + swapped(kv_part) * sine, kv_part).astype(bf16)
        K[...] = kv[:, :HD]
        V[...] = kv[:, HD:]
    for copy in sends_o:
        copy.wait_recv()
    sends_o2 = [net.send(WO.at[f], WO.at[f], across[k]) for k in (1, 2)]
    sends_e[2].append(send_row(3, 2))

    scale = HD ** (-0.5)
    step = 2 * hb

    def attend(i, carry):
        at = pl.ds(pl.multiple_of(i * step, step), step)
        mask = (SEGC[at, :] == seg_row) & (pos_row <= POSC[at, :])
        q = Q[at, :]
        pieces = []
        for r in range(2):
            scores = dot_nt(q[:, r * HD : (r + 1) * HD], K[...]) * scale
            scores = jnp.where(mask, scores, masked_score)
            peak = jnp.max(scores, axis=1, keepdims=True)
            weights = jnp.where(mask, jnp.exp(scores - peak), 0.0)
            total = jnp.sum(weights, axis=1, keepdims=True)
            pieces.append(dot_nn(weights.astype(bf16), V[...]) / total)
            PSC[r, at, :] = (weights / total).astype(bf16)
        out = jnp.concatenate(pieces, axis=1).astype(bf16)
        at_c, at_z = lax.div(2 * i, nz), lax.rem(2 * i, nz)
        ATT[at_c, pl.ds(at_z, 2)] = out.reshape(2, hb, 2 * HD)
        return carry

    with jax.named_scope("attend"):
        lax.fori_loop(0, rows // step, attend, 0)
    columns = pl.ds(pl.multiple_of(z * 2 * HD, 2 * HD), 2 * HD)
    sends_a = [
        net.send(ATT.at[:, zs[k]], AT.at[:, :, columns], device(f, zs[k], c)) for k in range(1, nz)
    ]
    AT[:, :, columns] = ATT[:, z]
    for k in (1, 2):
        part, to = ((lower, across[2]), (upper, across[1]))[k - 1]
        sends_o2[k - 1].wait_recv()
        sends_o2.append(net.send(WO.at[fs[k], part], WO.at[fs[k], part], to))
    arrive(chain_g)
    chain_g = line.pass_on(1, view_g)
    chains.append(chain_g)
    for copy in loads[3:]:
        copy.wait()
    for copy in sends_e[0] + sends_e[1]:
        copy.wait_recv()
    send_weights(3, 0, 1)
    for copy in sends_a + sends_o2[2:]:
        copy.wait_recv()

    with jax.named_scope("proj"):
        part = dot_nt(AT[...].reshape(block, nz * 2 * HD), WO[...].reshape(width, nz * 2 * HD))
        PP[...] = part.reshape(2, hb, width)
    send_p = net.send(PP.at[other], PR, partner)
    arrive(chain_g)
    chain_g = line.pass_on(2, view_g)
    chains.append(chain_g)
    x_own = X[c, z].astype(f32)
    gain_two = SMW[1:2, :].astype(f32)
    send_p.wait_recv()
    residual = x_own + PP[c] + PR[...]
    RES[...] = residual
    inverse_two = lax.rsqrt(jnp.mean(residual * residual, axis=1, keepdims=True) + epsilon)
    N2[f, c, z] = (residual * inverse_two * gain_two).astype(bf16)
    normed_two = N2[f, c, z]
    logits = dot_nt(SMW[16 : 16 + experts, :], normed_two)
    expert_at = lax.broadcasted_iota(jnp.int32, (experts, hb), 0)
    route = ec_ref[...]
    route = jnp.where(c == 0, route, pltpu.roll(route, 128 - hb, 1))
    picked = jnp.zeros((experts, hb), jnp.bool_)
    for j in range(chosen):
        picked = picked | (route[j : j + 1, 0:hb] == expert_at)
    peak = jnp.max(jnp.where(picked, logits, masked_score), axis=0, keepdims=True)
    weight = jnp.where(picked, jnp.exp(logits - peak), 0.0)
    gates = weight / jnp.sum(weight, axis=0, keepdims=True)
    GTB[f, c, z] = jnp.concatenate([gates, jnp.zeros((experts, 128 - hb), f32)], axis=1)
    view_n = [lambda at: N2.at[f, c, at], lambda at: GTB.at[f, c, at]]
    early = net.numbers(
        sends_q, sends_s, sends_x, forwards_x, sends_o, sends_e[:2], sends_q2, sends_s2, sends_o2, sends_a, chains[:2], send_p
    )
    chain_n = line.pass_on(0, view_n)
    chains = [chains[2], chain_n]
    send_weights(2, 0)

    arrive(chain_g)
    sends_g2 = second_hop(GA)
    forwards_g = [net.send(GA.at[f, c], GA.at[f, c], partner)]
    arrive(chain_n)
    chain_n = line.pass_on(1, view_n)
    chains.append(chain_n)
    send_weights(2, 1)
    arrive(chain_n)
    chain_n = line.pass_on(2, view_n)
    chains.append(chain_n)
    send_weights(1, 0, 1)
    for copy in sends_e[2]:
        copy.wait_recv()
    for k in (3, 2, 1):
        send_weights(k, 4)
    sends_g3 = []
    for k in (1, 2):
        sends_g2[k - 1].wait_recv()
        sends_g3.append(third_hop(GA, k))
        forwards_g.append(net.send(GA.at[fs[k], c], GA.at[fs[k], c], partner))
    arrive(chain_n)
    sends_n2 = second_hop(N2)
    sends_t2 = [net.send(GTB.at[f, c], GTB.at[f, c], across[k]) for k in (1, 2, 3)]
    forwards_n = [net.send(N2.at[f, c], N2.at[f, c], partner)]
    forwards_t = [net.send(GTB.at[f, c], GTB.at[f, c], partner)]
    for k in (3, 2, 1):
        send_weights(k, 2, 3)
    before = range(len(net.copies) - 20)

    WGU[:, z, :, 0:unit] = SWG[:, z, :, 0:unit]
    WGU[:, z, :, unit : 2 * unit] = SWU[:, z, :, 0:unit]
    WGU[:, z, :, 2 * unit : 3 * unit] = SWG[:, z, :, unit : 2 * unit]
    WGU[:, z, :, 3 * unit : 4 * unit] = SWU[:, z, :, unit : 2 * unit]
    WD[:, z] = SWD[:, z]
    chosen_row = jnp.where(
        lax.broadcasted_iota(jnp.int32, (experts, 128), 0) == own, 1.0, 0.0
    ).astype(f32)
    sends_d, sends_b, exchange_b, exchange_m = [], {}, {}, {}
    low_half = z < nz // 2
    in_order = [jnp.where(low_half, 3, 0), jnp.where(low_half, 2, 1), zs[1], z]
    grads_z, grads_f = ([], []), ([], [])

    def send_grads(h, k):
        to = device(f, zs[k], c)
        grads_z[h].append(net.send(DGB.at[h, :, zs[k]], ZG.at[h, z], to))
        grads_z[h].append(net.send(DDB.at[h, :, zs[k]], ZD.at[h, z], to))

    def spread_grads(h):
        ZG[h, z] = DGB[h, :, z]
        ZD[h, z] = DDB[h, :, z]
        for copy in grads_z[h]:
            copy.wait_recv()
        for k in range(1, nf):
            grads_f[h].append(
                net.send(ZG.at[h, :, fs[k]], GUL.at[f, :, :, pl.ds(2 * h * unit, 2 * unit)], across[k])
            )
            grads_f[h].append(net.send(ZD.at[h, :, fs[k]], DDL.at[f, :, :, units(h)], across[k]))
        GUL[f, :, :, 2 * h * unit : 2 * (h + 1) * unit] = ZG[h, :, f]
        DDL[f, :, :, h * unit : (h + 1) * unit] = ZD[h, :, f]

    def expert_part(h, k):
        at_f = fs[k]
        tokens = N2[at_f].reshape(rows, width)
        with jax.named_scope("gateup"):
            PSX[...] = dot_nn(tokens, WGU[:, :, :, 2 * h * unit : 2 * (h + 1) * unit].reshape(width, 2 * unit))
        if h == 0:
            with jax.named_scope("gatecol"):
                for piece in range(2 * nz):
                    tile = GTB[at_f, piece // nz, piece % nz][:, 0:hb]
                    GC[k, piece * hb : (piece + 1) * hb, :] = dot_tn(tile, chosen_row, lax.Precision.HIGHEST)

        def expert_chunk(i, carry):
            at = pl.ds(pl.multiple_of(i * 64, 64), 64)
            gate_pre = PSX[at, 0:unit]
            up_pre = PSX[at, unit : 2 * unit]
            raw = AA[k, at, h * unit : (h + 1) * unit]
            gate = GC[k, at, :]
            sigmoid = jax.nn.sigmoid(gate_pre)
            silu = gate_pre * sigmoid
            act = silu * up_pre
            PRD[at, :] = (act * raw).astype(bf16)
            H[k, at, h * unit : (h + 1) * unit] = (act * gate).astype(bf16)
            grad = raw * gate
            UG[k, at, 2 * h * unit : (2 * h + 1) * unit] = (
                grad * up_pre * sigmoid * (1.0 + gate_pre * (1.0 - sigmoid))
            ).astype(bf16)
            UG[k, at, (2 * h + 1) * unit : 2 * (h + 1) * unit] = (grad * silu).astype(bf16)
            return carry

        with jax.named_scope("chunk"):
            lax.fori_loop(0, rows // 64, expert_chunk, 0)
        if h == 1:
            with jax.named_scope("back"):
                BP[at_f] = dot_nt(UG[k], WGU[...].reshape(width, 2 * half_ff)).astype(bf16).reshape(2, nz, hb, width)
            exchange_b[k] = net.send(BP.at[at_f, other], BR.at[at_f], partner)
        with jax.named_scope("gdot"):
            dots = dot_nt(jnp.ones((8, unit), bf16), PRD[...])
            GDS[k] = dots if h == 0 else GDS[k] + dots
        if h == 1:
            sets = []
            for j in range(nz):
                for t in range(2):
                    to_z, to_c = zs[j], lax.rem(c + t, 2)
                    lanes = pl.ds(pl.multiple_of((to_c * (nz // 2) + lax.div(to_z, 2)) * 128, 128), 128)
                    if (k, j, t) != (0, 0, 0):
                        sets.append(
                            (GDS.at[k, pl.ds(0, 1), lanes], GD.at[f, z, c, pl.ds(0, 1)], device(at_f, to_z, to_c))
                        )
                    else:
                        GD[f, z, c] = GDS[0, :, lanes]
            sends_d.append(net.together(sets, SGW.at[pl.ds(0, len(sets))]))

    def mix(k):
        with jax.named_scope("mix"):
            MP[fs[k]] = dot_nt(H[k], WD[...].reshape(width, half_ff)).astype(bf16).reshape(2, nz, hb, width)
        exchange_m[k] = net.send(MP.at[fs[k], other], MR.at[fs[k]], partner)

    def weight_terms(h, k):
        with jax.named_scope("wgrad"):
            gate_up = dot_tn(UG[k, :, 2 * h * unit : 2 * (h + 1) * unit], N2[fs[k]].reshape(rows, width))
            down = dot_tn(H[k, :, h * unit : (h + 1) * unit], GA[fs[k]].reshape(rows, width))
            first = k == (0, 3)[h]
            DGU[...] = gate_up if first else DGU[...] + gate_up
            DDT[...] = down if first else DDT[...] + down

    def shed(h):
        with jax.named_scope("transpose"):
            DGB[h] = jnp.transpose(DGU[...]).astype(bf16).reshape(nf, nz, shard, 2 * unit)
            DDB[h] = jnp.transpose(DDT[...]).astype(bf16).reshape(nf, nz, shard, unit)

    def cotangent(k):
        forwards_g[k].wait_recv()
        with jax.named_scope("cotangent"):
            AA[k] = dot_nn(GA[fs[k]].reshape(rows, width), WD[...].reshape(width, half_ff))

    net.drain(before)
    for copy in weights[2]:
        copy.wait_recv()
    for k in range(nf - 1):
        cotangent(k)
    for copy in weights[0]:
        copy.wait_recv()
    for k in range(nf):
        if k == 1:
            sends_n3 = []
            for i in (1, 2):
                sends_n2[i - 1].wait_recv()
                sends_n3.append(third_hop(N2, i))
                forwards_n.append(net.send(N2.at[fs[i], c], N2.at[fs[i], c], partner))
                sends_t2[i - 1].wait_recv()
                forwards_t.append(net.send(GTB.at[fs[i], c], GTB.at[fs[i], c], partner))
            for copy in sends_g3:
                copy.wait_recv()
            forwards_g.append(net.send(GA.at[fs[3], c], GA.at[fs[3], c], partner))
        if k == 3:
            cotangent(k)
            for copy in sends_n3:
                copy.wait_recv()
            forwards_n.append(net.send(N2.at[fs[k], c], N2.at[fs[k], c], partner))
            sends_t2[2].wait_recv()
            forwards_t.append(net.send(GTB.at[fs[k], c], GTB.at[fs[k], c], partner))
        forwards_n[k].wait_recv()
        forwards_t[k].wait_recv()
        expert_part(0, k)
        weight_terms(0, k)
    shed(0)
    for k in (3, 2, 1):
        send_grads(0, k)
    for copy in weights[1]:
        copy.wait_recv()
    own_half = ((lower, 1), (upper, 2))

    def spread(k, exchange, part, back, total, via, into, order):
        at_f = fs[k]
        exchange[k].wait_recv()
        if k == 0:
            total[...] = part[at_f, c].astype(f32) + back[at_f].astype(f32)
            return []
        if k == 3:
            part[at_f, c] = (part[at_f, c].astype(f32) + back[at_f].astype(f32)).astype(bf16)
            return [net.send(part.at[at_f, c, half_at], via.at[to - 1], across[to]) for half_at, to in own_half]
        return None

    def spread_near(k, firsts, part, back, via, into, order):
        at_f = fs[k]
        half_at, other_half = (upper, lower) if k == 1 else (lower, upper)
        firsts[2 - k].wait_recv()
        part[at_f, c, half_at] = (
            part[at_f, c, half_at].astype(f32) + back[at_f, half_at].astype(f32) + via[2 - k].astype(f32)
        ).astype(bf16)
        part[at_f, c, other_half] = (
            part[at_f, c, other_half].astype(f32) + back[at_f, other_half].astype(f32)
        ).astype(bf16)
        return [net.send(part.at[at_f, c, at], into.at[k - 1, at], across[k]) for at in order]

    sends_m = {}
    middle = net.numbers(
        sends_e[2:], sends_g2, sends_g3, forwards_g, *weights, chains, sends_n2, sends_n3, sends_t2,
        forwards_n, forwards_t,
    )
    net.free(early)
    expert_part(1, 3)
    weight_terms(1, 3)
    mix(3)
    firsts_b = spread(3, exchange_b, BP, BR, BOWN, RBV, RB, in_order)
    for k in (1, 2, 0):
        expert_part(1, k)
    for k in (1, 2):
        exchange_b[k].wait_recv()
        sends_b[k] = spread_near(k, firsts_b, BP, BR, RBV, RB, in_order)
    spread(0, exchange_b, BP, BR, BOWN, RBV, RB, in_order)
    firsts_m = spread(3, exchange_m, MP, MR, MOWN, RMV, RM, in_order)
    for k in (1, 2, 0):
        mix(k)
        weight_terms(1, k)

    expert_copies = len(net.copies)
    shed(1)

    def dots_back():
        for copy in sends_d:
            copy.wait_recv()
        dots = jnp.concatenate(
            [
                GD[e // nz, e % nz, 0][0:1, :] + GD[e // nz, e % nz, 1][0:1, :]
                for e in range(experts)
            ],
            axis=0,
        )
        dots = jnp.where(lax.rem(z, 2) == 0, dots, pltpu.roll(dots, 128 - hb, 1))[:, 0:hb]
        gates = GTB[f, c, z][:, 0:hb]
        logit_grad = gates * (dots - jnp.sum(gates * dots, axis=0, keepdims=True))
        router_t = SMW[16 : 16 + experts, :].astype(f32)
        SG[0:experts, :] = dot_nn(logit_grad, N2[f, c, z].astype(f32), lax.Precision.HIGHEST)
        GRES[...] = dot_tn(logit_grad, router_t, lax.Precision.HIGHEST)

    own_b, out_b, into_b = (lambda at: BOWN.at[at]), (lambda w, t: CO.at[w, t]), (lambda w, t: CI.at[w, t])

    def take_block(at):
        for k in (1, 2):
            sends_b[k][at].wait_recv()
            BOWN[in_order[at]] += RB[k - 1, in_order[at]].astype(f32)

    sums = []
    for t in range(nz):
        take_block(t)
        if t > 0:
            arrive(chain_b)
        if t < nz - 1:
            at_sums = len(net.copies)
            chain_b = line.add_on(t, own_b, out_b, into_b)
            sums.extend(range(at_sums, len(net.copies)))
        if t == 0:
            dots_back()
        if t == 2:
            spread_grads(0)
    line.finish(BOWN.at[z], into_b)
    net.free(middle)

    residual = RES[...]
    inverse_two = lax.rsqrt(jnp.mean(residual * residual, axis=1, keepdims=True) + epsilon)
    grad_two = BOWN[z] + GRES[...]
    scaled = grad_two * gain_two
    grad_res = (
        GA[f, c, z].astype(f32)
        + inverse_two * scaled
        - residual * (inverse_two * inverse_two * inverse_two) * jnp.mean(scaled * residual, axis=1, keepdims=True)
    )
    GRES[...] = grad_res
    RL[c] = grad_res.astype(bf16)
    send_r = net.send(RL.at[c], RL.at[c], partner)
    gain_term = jnp.sum(grad_two * residual * inverse_two, axis=0, keepdims=True)
    SG[experts : experts + 8, :] = jnp.broadcast_to(gain_term, (8, width))
    wide = width // nf
    block_lanes = lambda at: pl.ds(pl.multiple_of(at * wide, 128), wide)
    sends_sg = [net.send(SG.at[:, block_lanes(fs[k])], SGF.at[k - 1], device(fs[k], z, c)) for k in range(1, nf)]
    for k in (1, 2):
        exchange_m[k].wait_recv()
        sends_m[k] = spread_near(k, firsts_m, MP, MR, RMV, RM, in_order)
    spread(0, exchange_m, MP, MR, MOWN, RMV, RM, in_order)
    send_r.wait_recv()
    low = RL[...].reshape(block, width)
    with jax.named_scope("attgrad"):
        AGS[...] = dot_nn(low, WO[...].reshape(width, nz * 2 * HD)).astype(bf16).reshape(2, hb, nz * 2 * HD)
    sends_ag = [
        net.send(
            AGS.at[:, :, pl.ds(pl.multiple_of(zs[k] * 2 * HD, 2 * HD), 2 * HD)],
            AGR.at[:, z],
            device(f, zs[k], c),
        )
        for k in range(1, nz)
    ]
    AGR[:, z] = AGS[:, :, columns]
    for k in (1, 3, 2):
        send_grads(1, k)
    with jax.named_scope("outgrad"):
        DWO[...] = (
            dot_tn(low, AT[...].reshape(block, nz * 2 * HD))
            .astype(bf16)
            .reshape(nf, nz, shard, nz * 2 * HD)
        )
    sends_wo = [net.send(DWO.at[fs[k]], RWO.at[k - 1], device(fs[k], z, c)) for k in range(1, nf)]

    net.drain(range(expert_copies))
    for copy in sends_ag:
        copy.wait_recv()

    def backward(i, carry):
        at = pl.ds(pl.multiple_of(i * step, step), step)
        at_c, at_z = lax.div(2 * i, nz), lax.rem(2 * i, nz)
        grad = AGR[at_c, pl.ds(at_z, 2)].reshape(step, 2 * HD)
        out = ATT[at_c, pl.ds(at_z, 2)].reshape(step, 2 * HD)
        both = grad.astype(f32) * out.astype(f32)
        pieces = []
        for r in range(2):
            delta = jnp.sum(both[:, r * HD : (r + 1) * HD], axis=1, keepdims=True)
            prob_grad = dot_nt(grad[:, r * HD : (r + 1) * HD], V[...])
            probs = PSC[r, at, :].astype(f32)
            score_grad = (probs * (prob_grad - delta) * scale).astype(bf16)
            DS[r, at, :] = score_grad
            pieces.append(dot_nn(score_grad, K[...]))
        DQ[at, :] = jnp.concatenate(pieces, axis=1)
        return carry

    with jax.named_scope("attback"):
        lax.fori_loop(0, rows // step, backward, 0)
    with jax.named_scope("kvgrad"):
        grads = AGR[...].reshape(rows, 2 * HD)
        key_t = dot_tn(Q[:, 0:HD], DS[0]) + dot_tn(Q[:, HD : 2 * HD], DS[1])
        value_t = dot_tn(grads[:, 0:HD], PSC[0]) + dot_tn(grads[:, HD : 2 * HD], PSC[1])
        kv_grad = jnp.transpose(jnp.concatenate([key_t, value_t], axis=0))
        cosine, sine = CT[...], ST[...]
        q_grad = DQ[...]
        DQKV[:, 0 : 2 * HD] = (q_grad * cosine - swapped(q_grad) * sine).astype(bf16)
        DQKV[:, 2 * HD : 4 * HD] = jnp.where(
            is_key, kv_grad * cosine - swapped(kv_grad) * sine, kv_grad
        ).astype(bf16)
    with jax.named_scope("ingrad"):
        NG[...] = dot_nt(DQKV[...], WQ[...].reshape(width, 4 * HD)).astype(bf16).reshape(2, nz, hb, width)
    send_ng = net.send(NG.at[other], NR, partner)
    with jax.named_scope("qkvgrad"):
        DWQ[...] = (
            jnp.transpose(dot_tn(DQKV[...], N1[...])).astype(bf16).reshape(nf, nz, shard, 4 * HD)
        )
    sends_wq = [net.send(DWQ.at[fs[k]], RWQ.at[k - 1], device(fs[k], z, c)) for k in range(1, nf)]
    send_ng.wait_recv()
    net.drain(sums)
    BOWN[...] = NG[c].astype(f32) + NR[...].astype(f32)
    chain_g1 = line.add_on(0, own_b, out_b, into_b)
    for k in (1, 2):
        for at in range(nz):
            sends_m[k][at].wait_recv()
        MOWN[...] += RM[k - 1].astype(f32)
    own_m, out_m, into_m = (lambda at: MOWN.at[at]), (lambda w, t: MO.at[w, t]), (lambda w, t: MI.at[w, t])
    chain_m = line.add_on(0, own_m, out_m, into_m)
    arrive(chain_g1)
    chain_g1 = line.add_on(1, own_b, out_b, into_b)
    arrive(chain_m)
    chain_m = line.add_on(1, own_m, out_m, into_m)
    arrive(chain_g1)
    chain_g1 = line.add_on(2, own_b, out_b, into_b)
    arrive(chain_m)
    chain_m = line.add_on(2, own_m, out_m, into_m)

    arrive(chain_g1)
    line.finish(BOWN.at[z], into_b)
    grad_one = BOWN[z]
    gain_one = SMW[0:1, :].astype(f32)
    x_own = X[c, z].astype(f32)
    inverse = lax.rsqrt(jnp.mean(x_own * x_own, axis=1, keepdims=True) + epsilon)
    gain_term = jnp.sum(grad_one * x_own * inverse, axis=0, keepdims=True)
    SG1[0] = jnp.broadcast_to(gain_term, (8, width))
    send_g1 = net.send(SG1.at[0], SG1.at[1], partner)
    scaled = grad_one * gain_one
    EXG[c] = (
        GRES[...]
        + inverse * scaled
        - x_own * (inverse * inverse * inverse) * jnp.mean(scaled * x_own, axis=1, keepdims=True)
    )
    send_ig = net.send(EXG.at[c], EXG.at[c], partner)
    small = SG[:, block_lanes(f)]
    for k in range(1, nf):
        sends_sg[k - 1].wait_recv()
        small = small + SGF[k - 1]
    SGT[...] = small
    pair_lanes = lambda at: pl.ds(pl.multiple_of(lax.div(at, 2) * 128, 128), 128)
    sends_sz = [net.send(SGT.at[:, pair_lanes(zs[k])], SGZ.at[k - 1], device(f, zs[k], c)) for k in range(1, nz)]
    total = DWO[f].astype(f32)
    for k in range(1, nf):
        sends_wo[k - 1].wait_recv()
        total = total + RWO[k - 1].astype(f32)
    ZWO[...] = total.astype(bf16)
    sends_wo2 = [net.send(ZWO.at[zs[k]], LWO.at[z], device(f, zs[k], c)) for k in range(1, nz)]
    LWO[z] = ZWO[z]
    total = DWQ[f].astype(f32)
    for k in range(1, nf):
        sends_wq[k - 1].wait_recv()
        total = total + RWQ[k - 1].astype(f32)
    ZWQ[...] = total.astype(bf16)
    sends_wq2 = [net.send(ZWQ.at[zs[k]], LWQ.at[z], device(f, zs[k], c)) for k in range(1, nz)]
    LWQ[z] = ZWQ[z]
    small = SGT[:, pair_lanes(z)]
    for k in range(1, nz):
        sends_sz[k - 1].wait_recv()
        small = small + SGZ[k - 1]
    SGP[0] = small
    send_sp = net.send(SGP.at[0], SGP.at[1], partner)
    net.drain(range(expert_copies))
    send_g1.wait_recv()
    SG1P[...] = SG1[0] + SG1[1]
    lanes_of = lambda df, dz: pl.ds(pl.multiple_of((df * (nz // 2) + lax.div(dz, 2)) * 128, 128), 128)
    sets = [
        (SG1P.at[pl.ds(0, 1), lanes_of(fs[i], zs[j])], RSG1.at[f, z, pl.ds(0, 1)], device(fs[i], zs[j], c))
        for i, j in same
    ]
    sends_g1 = [net.together(sets, SGW.at[pl.ds(0, len(sets))])]
    RSG1[f, z] = SG1P[:, lanes_of(f, z)]

    spread_grads(1)
    arrive(chain_m)
    line.finish(MOWN.at[z], into_m)
    EXB[c] = (RES[...] + MOWN[z]).astype(bf16)
    send_bo = net.send(EXB.at[c], EXB.at[c], partner)
    send_sp.wait_recv()
    small_out[...] = SGP[0] + SGP[1]
    for copy in sends_wo2:
        copy.wait_recv()
    total = LWO[0].astype(f32)
    for j in range(1, nz):
        total = total + LWO[j].astype(f32)
    dwo_out[...] = total
    outs = []

    def leave(source, target):
        copy = pltpu.make_async_copy(source, target, local_sems.at[6 + len(outs)])
        copy.start()
        outs.append(copy)

    for copy in sends_wq2:
        copy.wait_recv()
    leave(LWQ, dqkv_out)
    send_bo.wait_recv()
    leave(EXB, block_out)
    send_ig.wait_recv()
    leave(EXG, input_grad)
    for copy in sends_g1:
        copy.wait_recv()
    small = jnp.zeros((1, 128), f32)
    for i in range(nf):
        for j in range(nz):
            small = small + RSG1[i, j, 0:1]
    gain_out[...] = jnp.broadcast_to(small, (8, 128))
    for copy in grads_f[0] + grads_f[1]:
        copy.wait_recv()
    leave(GUL, dgu_out)
    leave(DDL, dd_out)
    with jax.named_scope("drain"):
        net.drain()
    with jax.named_scope("outs"):
        for copy in outs:
            copy.wait()


def finish_kernel(
    dims, block_ref, input_ref, small_ref, gain_ref, dqkv_ref, dwo_ref, dgu_ref, dd_ref,
    block_out, input_out, gain1_out, q_out, k_out, v_out, o_out, gain2_out, router_out, gate_out, up_out, down_out,
):
    nz, experts, half_ff, shard = dims
    block_out[...] = block_ref[...]
    input_out[...] = input_ref[...]
    unit = half_ff // 2
    for h in range(2):
        gate_out[:, :, h * unit : (h + 1) * unit] = dgu_ref[:, :, 2 * h * unit : (2 * h + 1) * unit].astype(f32)
        up_out[:, :, h * unit : (h + 1) * unit] = dgu_ref[:, :, (2 * h + 1) * unit : 2 * (h + 1) * unit].astype(f32)
    down_out[...] = dd_ref[...].astype(f32)
    even = lax.rem(lax.axis_index("ctx"), 2) == 0
    pick = lambda v: jnp.where(even, v, pltpu.roll(v, 128 - shard, 1))[:, 0:shard]

    def once():
        gain1_out[...] = pick(gain_ref[...])[0:1]
        small = pick(small_ref[...])
        router_out[...] = small[0:experts]
        gain2_out[...] = small[experts : experts + 1]
        o_out[...] = dwo_ref[...]
        for j in range(nz):
            q_out[:, 2 * HD * j : 2 * HD * (j + 1)] = dqkv_ref[j, :, 0 : 2 * HD].astype(f32)
        for at, ref in ((2, k_out), (3, v_out)):
            ref[...] = jnp.concatenate(
                [dqkv_ref[j, :, at * HD : (at + 1) * HD].astype(f32) for j in range(nz)], axis=1
            )

    pl.when(pl.program_id(0) == 0)(once)


def fast_local(
    nf, nz,
    hidden_in, out_grad, attention_gain, query_weight, key_weight, value_weight, output_weight,
    expert_gain, router_weight, gate_weight, up_weight, down_weight, doc_lengths, expert_choice,
):
    block, width = hidden_in.shape[1], hidden_in.shape[2]
    hb = block // 2
    experts, shard, half_ff = gate_weight.shape
    ndoc, chosen = doc_lengths.shape[1], expert_choice.shape[2]
    rows = nz * block
    halfway = HD // 2
    frequency = np.float32(rope_base) ** (-np.arange(halfway, dtype=np.float32) / np.float32(halfway))
    frequency = jnp.asarray(np.tile(np.tile(frequency, 4)[None], (8, 1)).astype(np.float32))

    vm = pl.BlockSpec(memory_space=pltpu.VMEM)
    anywhere = pl.BlockSpec(memory_space=pl.ANY)
    shape = lambda s, d: jax.ShapeDtypeStruct(s, d)
    W = nz * 2 * HD
    scratch = dict(
        WP=((nz, shard, 4 * HD), bf16), SMT=((32, 128), bf16),
        X=((2, nz, hb, width), bf16), WQ=((nf, nz, shard, 4 * HD), bf16), WO=((nf, nz, shard, W), bf16),
        SMB=((nf, nz, 32, 128), bf16), SMW=((32, width), bf16), N1=((rows, width), bf16),
        CT=((rows, 128), f32), ST=((rows, 128), f32), SEGC=((rows, 1), jnp.int32), POSC=((rows, 1), jnp.int32),
        Q=((rows, 2 * HD), bf16), K=((rows, HD), bf16), V=((rows, HD), bf16), PSC=((2, rows, rows), bf16),
        ATT=((2, nz, hb, 2 * HD), bf16), AT=((2, hb, W), bf16), PP=((2, hb, width), f32), PR=((hb, width), f32),
        RES=((hb, width), f32),
        N2=((nf, 2, nz, hb, width), bf16), GTB=((nf, 2, nz, experts, 128), f32), GA=((nf, 2, nz, hb, width), bf16),
        WGU=((nf, nz, shard, 2 * half_ff), bf16), WD=((nf, nz, shard, half_ff), bf16),
        SWG=((nf, nz, shard, half_ff), bf16), SWU=((nf, nz, shard, half_ff), bf16), SWD=((nf, nz, shard, half_ff), bf16),
        AA=((nf, rows, half_ff), f32), PSX=((rows, half_ff), f32), GC=((nf, rows, 128), f32),
        H=((nf, rows, half_ff), bf16), UG=((nf, rows, 2 * half_ff), bf16), PRD=((rows, half_ff // 2), bf16),
        MP=((nf, 2, nz, hb, width), bf16), MR=((nf, nz, hb, width), bf16),
        BP=((nf, 2, nz, hb, width), bf16), BR=((nf, nz, hb, width), bf16),
        DGU=((half_ff, width), f32), DDT=((half_ff // 2, width), f32),
        GDS=((nf, 8, rows), f32), GD=((nf, nz, 2, 8, 128), f32),
        RB=((2, nz, hb, width), bf16), RM=((2, nz, hb, width), bf16),
        RBV=((2, nz // 2, hb, width), bf16), RMV=((2, nz // 2, hb, width), bf16),
        BOWN=((nz, hb, width), f32), MOWN=((nz, hb, width), f32),
        CO=((2, nz - 1, hb, width), bf16), CI=((2, nz - 1, hb, width), bf16),
        MO=((2, nz - 1, hb, width), bf16), MI=((2, nz - 1, hb, width), bf16),
        DGB=((2, nf, nz, shard, half_ff), bf16), GUL=((nf, nz, shard, 2 * half_ff), bf16), ZG=((2, nz, nf, shard, half_ff), bf16),
        DDB=((2, nf, nz, shard, half_ff // 2), bf16), DDL=((nf, nz, shard, half_ff), bf16), ZD=((2, nz, nf, shard, half_ff // 2), bf16),
        SG=((experts + 8, width), f32), SGF=((nf - 1, experts + 8, width // nf), f32),
        SGT=((experts + 8, width // nf), f32), SGZ=((nz - 1, experts + 8, 128), f32), SGP=((2, experts + 8, 128), f32),
        GRES=((hb, width), f32), RL=((2, hb, width), bf16),
        AGS=((2, hb, W), bf16), AGR=((2, nz, hb, 2 * HD), bf16),
        DWO=((nf, nz, shard, W), bf16), RWO=((nf - 1, nz, shard, W), bf16),
        ZWO=((nz, shard, W), bf16), LWO=((nz, shard, W), bf16),
        DS=((2, rows, rows), bf16), DQ=((rows, 2 * HD), f32),
        DQKV=((rows, 4 * HD), bf16), NG=((2, nz, hb, width), bf16), NR=((nz, hb, width), bf16),
        DWQ=((nf, nz, shard, 4 * HD), bf16), RWQ=((nf - 1, nz, shard, 4 * HD), bf16),
        ZWQ=((nz, shard, 4 * HD), bf16), LWQ=((nz, shard, 4 * HD), bf16),
        SGW=((16, 128), f32), SG1=((2, 8, width), f32), SG1P=((8, width), f32), RSG1=((nf, nz, 8, 128), f32),
        EXB=((2, hb, width), bf16), EXG=((2, hb, width), f32),
    )
    slots = (96, 104)
    out = pl.pallas_call(
        functools.partial(layer_kernel, (nf, nz, hb, width, experts, half_ff, ndoc, chosen)),
        name="layer",
        out_shape=(
            shape((2, hb, width), bf16), shape((2, hb, width), f32), shape((experts + 8, 128), f32),
            shape((8, 128), f32), shape((nz, shard, 4 * HD), bf16), shape((shard, W), f32),
            shape((nf, nz, shard, 2 * half_ff), bf16), shape((nf, nz, shard, half_ff), bf16),
        ),
        in_specs=[anywhere] * 2 + [vm] * 3 + [anywhere] + [vm] * 3 + [anywhere] * 3
        + [pl.BlockSpec(memory_space=pltpu.SMEM), vm, vm],
        out_specs=(anywhere,) * 2 + (vm,) * 2 + (anywhere, vm) + (anywhere,) * 2,
        scratch_shapes=[pltpu.VMEM(s, d) for s, d in scratch.values()]
        + [pltpu.SemaphoreType.DMA((slots[0],)), pltpu.SemaphoreType.DMA((slots[1],)), pltpu.SemaphoreType.DMA((11,))],
        compiler_params=pltpu.CompilerParams(
            collective_id=0, has_side_effects=True, vmem_limit_bytes=67043328
        ),
    )(
        hidden_in[0], out_grad[0], query_weight, key_weight, value_weight, output_weight,
        attention_gain[None], expert_gain[None], router_weight.T, gate_weight, up_weight, down_weight,
        doc_lengths, expert_choice[0].T, frequency,
    )
    steps = nz // 2
    some = lambda *s: pl.BlockSpec(s, lambda i: (i,) + (0,) * (len(s) - 1))
    whole = lambda *s: pl.BlockSpec(s, lambda i: (0,) * len(s))
    per = nf * nz // steps
    out = pl.pallas_call(
        functools.partial(finish_kernel, (nz, experts, half_ff, shard)),
        name="finish",
        grid=(steps,),
        out_shape=(
            shape((block, width), bf16), shape((block, width), f32), shape((1, shard), f32),
            shape((shard, nz * 2 * HD), f32), shape((shard, nz * HD), f32), shape((shard, nz * HD), f32),
            shape((shard, W), f32), shape((1, shard), f32), shape((experts, shard), f32),
            shape((experts, shard, half_ff), f32), shape((experts, shard, half_ff), f32),
            shape((experts, shard, half_ff), f32),
        ),
        in_specs=[
            some(block // steps, width), some(block // steps, width), whole(experts + 8, 128), whole(8, 128),
            whole(nz, shard, 4 * HD), whole(shard, W), some(per, shard, 2 * half_ff), some(per, shard, half_ff),
        ],
        out_specs=(
            some(block // steps, width), some(block // steps, width), whole(1, shard),
            whole(shard, nz * 2 * HD), whole(shard, nz * HD), whole(shard, nz * HD), whole(shard, W), whole(1, shard),
            whole(experts, shard), some(per, shard, half_ff), some(per, shard, half_ff), some(per, shard, half_ff),
        ),
        compiler_params=pltpu.CompilerParams(vmem_limit_bytes=67043328),
    )(out[0].reshape(block, width), out[1].reshape(block, width), *out[2:6], out[6].reshape(experts, shard, 2 * half_ff), out[7].reshape(experts, shard, half_ff))
    block_out, input_grad, gain1, q, k, v, o, gain2, router, gate, up, down = out
    return (
        block_out[None], input_grad[None], gain1[0], q, k, v, o, gain2[0], router.T, gate, up, down,
    )


def fits(mesh, args):
    nf, nz, nc = mesh.shape["fsdp"], mesh.shape["ctx"], mesh.shape["tp"]
    hidden, query, key, gate = args[0], args[3], args[4], args[9]
    width, block = hidden.shape[2], hidden.shape[1] // nz
    return (
        nc == 2
        and nz == 4
        and nf == 4
        and hidden.shape[0] == nf
        and gate.shape[0] == nf * nz
        and gate.shape[0] == 16
        and width == 64 * nf * nz
        and block == 128
        and query.shape[1] == 2 * HD * nz * nc
        and key.shape[1] == HD * nz * nc
        and HD == 64
    )


def solution(mesh):
    in_specs = (
        P("fsdp", "ctx", None),
        P("fsdp", "ctx", None),
        P(("fsdp", "ctx")),
        P(("fsdp", "ctx"), "tp"),
        P(("fsdp", "ctx"), "tp"),
        P(("fsdp", "ctx"), "tp"),
        P(("fsdp", "ctx"), "tp"),
        P(("fsdp", "ctx")),
        P(("fsdp", "ctx"), None),
        P(None, ("fsdp", "ctx"), "tp"),
        P(None, ("fsdp", "ctx"), "tp"),
        P(None, ("fsdp", "ctx"), "tp"),
        P("fsdp", None),
        P("fsdp", "ctx", None),
    )
    out_specs = (
        P("fsdp", "ctx", None),
        P("fsdp", "ctx", None),
        P(("fsdp", "ctx")),
        P(("fsdp", "ctx"), "tp"),
        P(("fsdp", "ctx"), "tp"),
        P(("fsdp", "ctx"), "tp"),
        P(("fsdp", "ctx"), "tp"),
        P(("fsdp", "ctx")),
        P(("fsdp", "ctx"), None),
        P(None, ("fsdp", "ctx"), "tp"),
        P(None, ("fsdp", "ctx"), "tp"),
        P(None, ("fsdp", "ctx"), "tp"),
    )

    def step(*args):
        body = local
        if fits(mesh, args):
            body = functools.partial(fast_local, mesh.shape["fsdp"], mesh.shape["ctx"])
        return jax.shard_map(
            body, mesh=mesh, in_specs=in_specs, out_specs=out_specs, check_vma=False
        )(*args)

    return step
```

```python
import functools

import jax
import jax.numpy as jnp
import numpy as np
from jax import lax
from jax.experimental import pallas as pl
from jax.experimental.pallas import tpu as pltpu
from jax.sharding import PartitionSpec as P

HD = 64


epsilon = 1e-05
rope_base = 10000.0
masked_score = -1e30
highest = lax.Precision.HIGHEST


def doc_layout(lengths, positions):
    ends = jnp.cumsum(lengths)
    after = (positions[:, None] >= ends[None, :]).astype(jnp.int32)
    segment = jnp.sum(after, axis=1)
    offset = positions - jnp.sum(after * lengths[None, :], axis=1)
    return (segment, offset)


def rope_tables(offset):
    halfway = HD // 2
    frequency = rope_base ** (-jnp.arange(halfway, dtype=jnp.float32) / halfway)
    angle = offset.astype(jnp.float32)[:, None] * frequency[None, :]
    return (jnp.cos(angle), jnp.sin(angle))


def rotate(vectors, cosine, sine):
    halfway = vectors.shape[-1] // 2
    former = vectors[..., :halfway]
    latter = vectors[..., halfway:]
    cosine = cosine[:, None, :]
    sine = sine[:, None, :]
    return jnp.concatenate(
        [former * cosine - latter * sine, latter * cosine + former * sine], axis=-1
    )


def rotate_back(grads, cosine, sine):
    halfway = grads.shape[-1] // 2
    former = grads[..., :halfway]
    latter = grads[..., halfway:]
    cosine = cosine[:, None, :]
    sine = sine[:, None, :]
    return jnp.concatenate(
        [former * cosine + latter * sine, latter * cosine - former * sine], axis=-1
    )


def norm_forward(values, gain):
    inverse = lax.rsqrt(jnp.mean(values * values, axis=-1, keepdims=True) + epsilon)
    return (values * inverse * gain.astype(jnp.float32), inverse)


def norm_backward(values, inverse, gain, grad_normed):
    scaled = grad_normed * gain.astype(jnp.float32)
    grad_values = inverse * scaled - values * inverse**3 * jnp.mean(
        scaled * values, axis=-1, keepdims=True
    )
    grad_gain = jnp.sum(grad_normed * values * inverse, axis=0)
    return (grad_values, grad_gain)


def dispatch(route, experts, capacity):
    flat = route.reshape(-1)
    onehot = (flat[:, None] == jnp.arange(experts, dtype=jnp.int32)[None, :]).astype(jnp.int32)
    rank = jnp.sum((jnp.cumsum(onehot, axis=0) - onehot) * onehot, axis=1)
    slot = flat * capacity + rank
    pairs = flat.shape[0]
    owner = (
        jnp.zeros((experts * capacity,), jnp.int32).at[slot].set(jnp.arange(pairs, dtype=jnp.int32))
    )
    filled = jnp.zeros((experts * capacity,), jnp.int32).at[slot].set(1) > 0
    return (slot, owner, filled)


def expert_math(slot_inputs, slot_grads, gate_full, up_full, down_full):
    gate_pre = jnp.einsum(
        "gsd,gdf->gsf", slot_inputs, gate_full, preferred_element_type=jnp.float32
    )
    up_pre = jnp.einsum("gsd,gdf->gsf", slot_inputs, up_full, preferred_element_type=jnp.float32)
    sigmoid = jax.nn.sigmoid(gate_pre)
    activated = (gate_pre * sigmoid * up_pre).astype(jnp.bfloat16)
    expert_out = jnp.einsum(
        "gsf,gdf->gsd", activated, down_full, preferred_element_type=jnp.float32
    )
    act_grad = jnp.einsum("gsd,gdf->gsf", slot_grads, down_full, preferred_element_type=jnp.float32)
    gate_pre_grad = (act_grad * up_pre * sigmoid * (1.0 + gate_pre * (1.0 - sigmoid))).astype(
        jnp.bfloat16
    )
    up_pre_grad = (act_grad * gate_pre * sigmoid).astype(jnp.bfloat16)
    down_term = jnp.einsum(
        "gsd,gsf->gdf", slot_grads, activated, preferred_element_type=jnp.float32
    )
    gate_term = jnp.einsum(
        "gsd,gsf->gdf", slot_inputs, gate_pre_grad, preferred_element_type=jnp.float32
    )
    up_term = jnp.einsum(
        "gsd,gsf->gdf", slot_inputs, up_pre_grad, preferred_element_type=jnp.float32
    )
    slot_back = jnp.einsum(
        "gsf,gdf->gsd", gate_pre_grad, gate_full, preferred_element_type=jnp.float32
    ) + jnp.einsum("gsf,gdf->gsd", up_pre_grad, up_full, preferred_element_type=jnp.float32)
    return (expert_out, slot_back, gate_term, up_term, down_term)


def local(
    hidden_in,
    out_grad,
    attention_gain,
    query_weight,
    key_weight,
    value_weight,
    output_weight,
    expert_gain,
    router_weight,
    gate_weight,
    up_weight,
    down_weight,
    doc_lengths,
    expert_choice,
):
    block = hidden_in.shape[1]
    experts = gate_weight.shape[0]
    capacity = block * 3 // 4
    chosen_count = expert_choice.shape[2]
    context_count = lax.axis_size("ctx")
    scale = HD ** (-0.5)
    position = lax.axis_index("ctx") * block + jnp.arange(block, dtype=jnp.int32)
    lengths = doc_lengths[0]
    segment, offset = doc_layout(lengths, position)
    cosine, sine = rope_tables(offset)
    gain_one, query_full, key_full, value_full, output_full, gain_two, router_full = (
        lax.all_gather(attention_gain, ("fsdp", "ctx"), axis=0, tiled=True),
        lax.all_gather(query_weight, ("fsdp", "ctx"), axis=0, tiled=True),
        lax.all_gather(key_weight, ("fsdp", "ctx"), axis=0, tiled=True),
        lax.all_gather(value_weight, ("fsdp", "ctx"), axis=0, tiled=True),
        lax.all_gather(output_weight, ("fsdp", "ctx"), axis=0, tiled=True),
        lax.all_gather(expert_gain, ("fsdp", "ctx"), axis=0, tiled=True),
        lax.all_gather(router_weight, ("fsdp", "ctx"), axis=0, tiled=True),
    )
    inputs = hidden_in[0].astype(jnp.float32)
    normed_one, inverse_one = norm_forward(inputs, gain_one)
    normed_one = normed_one.astype(jnp.bfloat16)
    heads_local = query_full.shape[1] // HD
    groups_local = key_full.shape[1] // HD
    ratio = heads_local // groups_local
    query = rotate(
        jnp.dot(normed_one, query_full, preferred_element_type=jnp.float32).reshape(
            block, heads_local, HD
        ),
        cosine,
        sine,
    ).astype(jnp.bfloat16)
    keys = rotate(
        jnp.dot(normed_one, key_full, preferred_element_type=jnp.float32).reshape(
            block, groups_local, HD
        ),
        cosine,
        sine,
    ).astype(jnp.bfloat16)
    values = jnp.dot(normed_one, value_full, preferred_element_type=jnp.float32).astype(
        jnp.bfloat16
    )
    query_grouped = query.reshape(block, groups_local, ratio, HD)

    def allowed_mask(key_start, count):
        key_position = key_start + jnp.arange(count, dtype=jnp.int32)
        key_segment, unused = doc_layout(lengths, key_position)
        return (segment[:, None] == key_segment[None, :]) & (
            key_position[None, :] <= position[:, None]
        )

    def forward_update(state, key_block, value_block, allowed):
        peak, total, accum = state
        mask = allowed[:, None, None, :]
        scores = (
            jnp.einsum(
                "qgrd,kgd->qgrk", query_grouped, key_block, preferred_element_type=jnp.float32
            )
            * scale
        )
        scores = jnp.where(mask, scores, masked_score)
        new_peak = jnp.maximum(peak, jnp.max(scores, axis=3))
        weights = jnp.where(mask, jnp.exp(scores - new_peak[..., None]), 0.0)
        rescale = jnp.exp(peak - new_peak)
        total = total * rescale + jnp.sum(weights, axis=3)
        accum = accum * rescale[..., None] + jnp.einsum(
            "qgrk,kgd->qgrd", weights, value_block.astype(jnp.float32), precision=highest
        )
        return (new_peak, total, accum)

    travel = (keys.reshape(block, groups_local * HD), values)
    initial = (
        jnp.full((block, groups_local, ratio), masked_score, jnp.float32),
        jnp.zeros((block, groups_local, ratio), jnp.float32),
        jnp.zeros((block, groups_local, ratio, HD), jnp.float32),
    )
    state = initial
    key_piece = lax.all_gather(travel[0], "ctx", axis=0, tiled=True)
    value_piece = lax.all_gather(travel[1], "ctx", axis=0, tiled=True)
    pieces = key_piece.shape[0] // block
    key_blocks = key_piece.reshape(pieces, block, groups_local, HD)
    value_blocks = value_piece.reshape(pieces, block, groups_local, HD)
    starts = block * jnp.arange(pieces, dtype=jnp.int32)

    def visit(carry, item):
        key_block, value_block, key_start = item
        allowed = allowed_mask(key_start, block)
        return (forward_update(carry, key_block, value_block, allowed), None)

    state, unused = lax.scan(visit, state, (key_blocks, value_blocks, starts))
    peak, total, accum = state
    attended = (accum / total[..., None]).reshape(block, heads_local * HD).astype(jnp.bfloat16)
    log_total = peak + jnp.log(total)
    projected = lax.psum(jnp.dot(attended, output_full.T, preferred_element_type=jnp.float32), "tp")
    residual = inputs + projected
    normed_two, inverse_two = norm_forward(residual, gain_two)
    normed_two = normed_two.astype(jnp.bfloat16)
    route = expert_choice[0]
    logits = jnp.dot(normed_two, router_full, preferred_element_type=jnp.float32)
    gates = jax.nn.softmax(jnp.take_along_axis(logits, route, axis=1), axis=1)
    slot, owner, filled = dispatch(route, experts, capacity)
    token_of = owner // chosen_count
    grad_out = out_grad[0].astype(jnp.float32)
    slot_inputs = jnp.where(filled[:, None], normed_two[token_of], 0).reshape(experts, capacity, -1)
    slot_gate = jnp.where(filled, gates.reshape(-1)[owner], 0.0)
    slot_grads = (
        (grad_out[token_of] * slot_gate[:, None])
        .astype(jnp.bfloat16)
        .reshape(experts, capacity, -1)
    )
    gate_full, up_full, down_full = (
        lax.all_gather(gate_weight, ("fsdp", "ctx"), axis=1, tiled=True),
        lax.all_gather(up_weight, ("fsdp", "ctx"), axis=1, tiled=True),
        lax.all_gather(down_weight, ("fsdp", "ctx"), axis=1, tiled=True),
    )
    expert_out, slot_back, gate_term, up_term, down_term = expert_math(
        slot_inputs, slot_grads, gate_full, up_full, down_full
    )
    gate_share, up_share, down_share = (
        lax.psum_scatter(gate_term, ("fsdp", "ctx"), scatter_dimension=1, tiled=True),
        lax.psum_scatter(up_term, ("fsdp", "ctx"), scatter_dimension=1, tiled=True),
        lax.psum_scatter(down_term, ("fsdp", "ctx"), scatter_dimension=1, tiled=True),
    )
    pair_out = expert_out.reshape(experts * capacity, -1)[slot].reshape(block, chosen_count, -1)
    pair_back = slot_back.reshape(experts * capacity, -1)[slot].reshape(block, chosen_count, -1)
    mixed_part = jnp.sum(gates[..., None] * pair_out, axis=1)
    gate_dot_part = jnp.sum(pair_out * grad_out[:, None, :], axis=2)
    moe_part = jnp.sum(pair_back, axis=1)
    mixed, gate_dot, moe_input = (
        lax.psum(mixed_part.astype(jnp.bfloat16), "tp").astype(jnp.float32),
        lax.psum(gate_dot_part.astype(jnp.bfloat16), "tp").astype(jnp.float32),
        lax.psum(moe_part.astype(jnp.bfloat16), "tp").astype(jnp.float32),
    )
    block_out = (residual + mixed).astype(jnp.bfloat16)[None]
    chosen_grad = gates * (gate_dot - jnp.sum(gates * gate_dot, axis=1, keepdims=True))
    picked = (route[..., None] == jnp.arange(experts, dtype=jnp.int32)[None, None, :]).astype(
        jnp.float32
    )
    logit_grad = jnp.sum(picked * chosen_grad[..., None], axis=1)
    router_term = jnp.dot(normed_two.astype(jnp.float32).T, logit_grad, precision=highest)
    router_input = jnp.dot(logit_grad, router_full.astype(jnp.float32).T, precision=highest)
    grad_residual_norm, gain_two_term = norm_backward(
        residual, inverse_two, gain_two, moe_input + router_input
    )
    grad_residual = grad_out + grad_residual_norm
    residual_low = grad_residual.astype(jnp.bfloat16)
    attended_grad = jnp.dot(residual_low, output_full, preferred_element_type=jnp.float32).astype(
        jnp.bfloat16
    )
    output_term = jnp.dot(residual_low.T, attended, preferred_element_type=jnp.float32)
    delta = jnp.sum(
        (attended_grad.astype(jnp.float32) * attended.astype(jnp.float32)).reshape(
            block, groups_local, ratio, HD
        ),
        axis=3,
    )
    grad_grouped = attended_grad.reshape(block, groups_local, ratio, HD)
    back_keys, back_values = (
        lax.all_gather(travel[0], "ctx", axis=0, tiled=True),
        lax.all_gather(travel[1], "ctx", axis=0, tiled=True),
    )
    key_blocks = back_keys.reshape(context_count, block, groups_local, HD)
    value_blocks = back_values.reshape(context_count, block, groups_local, HD)
    starts = block * jnp.arange(context_count, dtype=jnp.int32)

    def backward_update(grad_query, key_block, value_block, allowed):
        mask = allowed[:, None, None, :]
        scores = (
            jnp.einsum(
                "qgrd,kgd->qgrk", query_grouped, key_block, preferred_element_type=jnp.float32
            )
            * scale
        )
        probs = jnp.where(mask, jnp.exp(scores - log_total[..., None]), 0.0)
        value_grad = jnp.einsum(
            "qgrk,qgrd->kgd",
            probs.astype(jnp.bfloat16),
            grad_grouped,
            preferred_element_type=jnp.float32,
        )
        prob_grad = jnp.einsum(
            "qgrd,kgd->qgrk", grad_grouped, value_block, preferred_element_type=jnp.float32
        )
        score_grad = (probs * (prob_grad - delta[..., None]) * scale).astype(jnp.bfloat16)
        grad_query = grad_query + jnp.einsum(
            "qgrk,kgd->qgrd", score_grad, key_block, preferred_element_type=jnp.float32
        )
        key_grad = jnp.einsum(
            "qgrk,qgrd->kgd", score_grad, query_grouped, preferred_element_type=jnp.float32
        )
        return (grad_query, key_grad.reshape(block, -1), value_grad.reshape(block, -1))

    def backward_visit(grad_query, item):
        key_block, value_block, key_start = item
        allowed = allowed_mask(key_start, block)
        grad_query, key_grad, value_grad = backward_update(
            grad_query, key_block, value_block, allowed
        )
        return (grad_query, (key_grad, value_grad))

    grad_query, (key_grads, value_grads) = lax.scan(
        backward_visit,
        jnp.zeros((block, groups_local, ratio, HD), jnp.float32),
        (key_blocks, value_blocks, starts),
    )
    own_key_grad, own_value_grad = (
        lax.psum_scatter(
            key_grads.reshape(context_count * block, -1).astype(jnp.bfloat16),
            "ctx",
            scatter_dimension=0,
            tiled=True,
        ).astype(jnp.float32),
        lax.psum_scatter(
            value_grads.reshape(context_count * block, -1).astype(jnp.bfloat16),
            "ctx",
            scatter_dimension=0,
            tiled=True,
        ).astype(jnp.float32),
    )
    query_grad = (
        rotate_back(grad_query.reshape(block, heads_local, HD), cosine, sine)
        .reshape(block, -1)
        .astype(jnp.bfloat16)
    )
    key_grad = (
        rotate_back(own_key_grad.reshape(block, groups_local, HD), cosine, sine)
        .reshape(block, -1)
        .astype(jnp.bfloat16)
    )
    value_grad = own_value_grad.astype(jnp.bfloat16)
    input_part = jnp.dot(query_grad, query_full.T, preferred_element_type=jnp.float32)
    input_part = input_part + jnp.dot(key_grad, key_full.T, preferred_element_type=jnp.float32)
    input_part = input_part + jnp.dot(value_grad, value_full.T, preferred_element_type=jnp.float32)
    normed_one_grad = lax.psum(input_part.astype(jnp.bfloat16), "tp").astype(jnp.float32)
    grad_input_norm, gain_one_term = norm_backward(inputs, inverse_one, gain_one, normed_one_grad)
    input_grad = (grad_residual + grad_input_norm)[None]
    query_term = jnp.dot(normed_one.T, query_grad, preferred_element_type=jnp.float32)
    key_term = jnp.dot(normed_one.T, key_grad, preferred_element_type=jnp.float32)
    value_term = jnp.dot(normed_one.T, value_grad, preferred_element_type=jnp.float32)
    (
        gain_one_share,
        query_share,
        key_share,
        value_share,
        output_share,
        gain_two_share,
        router_share,
    ) = (
        lax.psum_scatter(gain_one_term, ("fsdp", "ctx"), scatter_dimension=0, tiled=True),
        lax.psum_scatter(query_term, ("fsdp", "ctx"), scatter_dimension=0, tiled=True),
        lax.psum_scatter(key_term, ("fsdp", "ctx"), scatter_dimension=0, tiled=True),
        lax.psum_scatter(value_term, ("fsdp", "ctx"), scatter_dimension=0, tiled=True),
        lax.psum_scatter(output_term, ("fsdp", "ctx"), scatter_dimension=0, tiled=True),
        lax.psum_scatter(gain_two_term, ("fsdp", "ctx"), scatter_dimension=0, tiled=True),
        lax.psum_scatter(router_term, ("fsdp", "ctx"), scatter_dimension=0, tiled=True),
    )
    return (
        block_out,
        input_grad,
        gain_one_share,
        query_share,
        key_share,
        value_share,
        output_share,
        gain_two_share,
        router_share,
        gate_share,
        up_share,
        down_share,
    )


MESH = pl.DeviceIdType.MESH
f32 = jnp.float32
bf16 = jnp.bfloat16


def dot_nn(a, b, precision=None):
    return lax.dot_general(a, b, (((1,), (0,)), ((), ())), precision=precision, preferred_element_type=f32)


def dot_nt(a, b, precision=None):
    return lax.dot_general(a, b, (((1,), (1,)), ((), ())), precision=precision, preferred_element_type=f32)


def dot_tn(a, b, precision=None):
    return lax.dot_general(a, b, (((0,), (0,)), ((), ())), precision=precision, preferred_element_type=f32)


class Net:
    def __init__(self, send_sems, recv_sems):
        self.send_sems, self.recv_sems, self.copies, self.left = send_sems, recv_sems, [], set()
        self.slots, self.free_send, self.free_recv = [], [], []
        self.top_send = self.top_recv = 0

    def make(self, source, target, device, sends=None):
        if self.free_send:
            send_at = self.free_send.pop(0)
        else:
            send_at, self.top_send = self.top_send, self.top_send + 1
        if self.free_recv:
            recv_at = self.free_recv.pop(0)
        else:
            recv_at, self.top_recv = self.top_recv, self.top_recv + 1
        assert max(send_at + 1 - self.send_sems.shape[0], recv_at + 1 - self.recv_sems.shape[0]) <= 0
        copy = pltpu.make_async_remote_copy(
            src_ref=source,
            dst_ref=target,
            send_sem=self.send_sems.at[send_at],
            recv_sem=self.recv_sems.at[recv_at],
            device_id=device,
            device_id_type=MESH,
        )
        self.copies.append((copy, sends))
        self.slots.append((send_at, recv_at))
        return copy

    def send(self, source, target, device):
        copy = self.make(source, target, device)
        copy.start()
        return copy

    def together(self, triples, whole):
        first = self.make(*triples[0])
        send_at, recv_at = self.slots[-1]
        first.start()
        for source, target, device in triples[1:]:
            pltpu.make_async_remote_copy(
                src_ref=source,
                dst_ref=target,
                send_sem=self.send_sems.at[send_at],
                recv_sem=self.recv_sems.at[recv_at],
                device_id=device,
                device_id_type=MESH,
            ).start()
        waits = Whole(
            pltpu.make_async_copy(whole, whole, self.send_sems.at[send_at]),
            pltpu.make_async_copy(whole, whole, self.recv_sems.at[recv_at]),
        )
        self.copies[-1] = (waits, None)
        return waits

    def free(self, among):
        self.free_recv.extend(self.slots[at][1] for at in among)

    def numbers(self, *groups):
        found = []
        for group in groups:
            if isinstance(group, list):
                found += self.numbers(*group)
            else:
                copy = group[0] if isinstance(group, tuple) else group
                found += [at for at, (one, sends) in enumerate(self.copies) if one is copy]
        return found

    def drain(self, among=None):
        for at, (copy, sends) in enumerate(self.copies):
            if at in self.left or (among is not None and at not in among):
                continue
            self.left.add(at)
            self.free_send.append(self.slots[at][0])
            if sends is None:
                copy.wait_send()
            else:
                pl.when(sends)(copy.wait_send)


class Whole:
    def __init__(self, sent, received):
        self.wait_send, self.wait_recv = sent.wait, received.wait


class Line:
    def __init__(self, net, z, nz, device):
        self.net, self.z, self.nz, self.device = net, z, nz, device

    def both(self):
        z, nz = self.z, self.nz
        right, left = self.device(lax.min(z + 1, nz - 1)), self.device(lax.max(z - 1, 0))
        return ((z, right), (nz - 1 - z, left))

    def pass_on(self, step, views):
        copies = []
        for way, (rank, target) in enumerate(self.both()):
            sends = (rank >= step) & (rank < self.nz - 1)
            arrives = rank >= step + 1
            block = lax.clamp(0, self.z - step if way == 0 else self.z + step, self.nz - 1)
            for view in views:
                copy = self.net.make(view(block), view(block), target, sends)
                pl.when(sends)(copy.start)
                copies.append((copy, arrives))
        return copies

    def add_on(self, step, own, out, into):
        copies = []
        for way, (rank, target) in enumerate(self.both()):
            sends = rank <= step
            arrives = (rank >= 1) & (rank - 1 <= step)
            dest = self.nz - 1 - step + rank
            dest = lax.clamp(0, dest if way == 0 else self.nz - 1 - dest, self.nz - 1)
            copy = self.net.make(out(way, step), into(way, step), target, sends)

            def prepare():
                out(way, step)[...] = own(dest)[...].astype(bf16)
                if step > 0:

                    def add():
                        out(way, step)[...] = (own(dest)[...] + into(way, step - 1)[...].astype(f32)).astype(bf16)

                    pl.when(rank >= 1)(add)
                copy.start()

            pl.when(sends)(prepare)
            copies.append((copy, arrives))
        return copies

    def finish(self, total, into):
        for way, (rank, target) in enumerate(self.both()):

            def add():
                total[...] += into(way, self.nz - 2)[...].astype(f32)

            pl.when(rank >= 1)(add)


def arrive(copies):
    for copy, arrives in copies:
        pl.when(arrives)(copy.wait_recv)


def layer_kernel(
    dims,
    x_ref, g_ref, wq_ref, wk_ref, wv_ref, wo_ref, ga_ref, ge_ref, rt_ref, wg_ref, wu_ref, wd_ref, dl_ref, ec_ref,
    fr_ref,
    block_out, input_grad, small_out, gain_out, dqkv_out, dwo_out, dgu_out, dd_out,
    WP, SMT, X, WQ, WO, SMB, SMW, N1, CT, ST, SEGC, POSC, Q, K, V, PSC, ATT, AT, PP, PR, RES,
    N2, GTB, GA, WGU, WD, SWG, SWU, SWD, AA, PSX, GC, H, UG, PRD, MP, MR, BP, BR, DGU, DDT, GDS, GD,
    RB, RM, RBV, RMV, BOWN, MOWN, CO, CI, MO, MI, DGB, GUL, ZG, DDB, DDL, ZD, SG, SGF, SGT, SGZ, SGP, GRES, RL,
    AGS, AGR, DWO, RWO, ZWO, LWO, DS, DQ, DQKV, NG, NR, DWQ, RWQ, ZWQ, LWQ,
    SMO, GNO, DWF, SGW, SG1, SG1P, RSG1, EXB, EXG,
    send_sems, recv_sems, local_sems,
):
    nf, nz, hb, width, experts, half_ff, ndoc, chosen = dims
    rows = 2 * nz * hb
    half = nz * hb
    block = 2 * hb
    shard = width // (nf * nz)
    f, z, c = lax.axis_index("fsdp"), lax.axis_index("ctx"), lax.axis_index("tp")
    other = 1 - c
    own = f * nz + z
    net = Net(send_sems, recv_sems)
    device = lambda df, dz, core: {"fsdp": df, "ctx": dz, "tp": core}
    partner = device(f, z, other)
    line = Line(net, z, nz, lambda dz: device(f, dz, c))
    zs = [z, z + 1 - 2 * lax.rem(z, 2), lax.rem(z + 2, 4), 3 - z]
    fs = [f, f + 1 - 2 * lax.rem(f, 2), lax.rem(f + 2, 4), 3 - f]
    everyone = [(i, j, k) for k in range(2) for i in range(nf) for j in range(nz) if (i, j, k) != (0, 0, 0)]
    others = [device(fs[i], zs[j], lax.rem(c + k, 2)) for i, j, k in everyone]
    same = [(i, 0) for i in range(1, nf)] + [(i, j) for i in range(nf) for j in (3, 1, 2)]

    mine = pl.ds(pl.multiple_of(c * hb, hb), hb)
    loads = [
        pltpu.make_async_copy(x_ref.at[mine], X.at[c, z], local_sems.at[0]),
        pltpu.make_async_copy(g_ref.at[mine], GA.at[f, c, z], local_sems.at[1]),
        pltpu.make_async_copy(wo_ref, WO.at[f, z], local_sems.at[2]),
    ]
    row_experts = lambda at: pl.ds(at * nz, nz)
    shards = ((wg_ref, SWG), (wu_ref, SWU), (wd_ref, SWD))
    loads += [
        pltpu.make_async_copy(ref.at[row_experts(f)], staged.at[f], local_sems.at[3 + at])
        for at, (ref, staged) in enumerate(shards)
    ]
    unit = half_ff // 2
    units = lambda h: pl.ds(h * unit, unit)
    for copy in loads:
        copy.start()
    barrier = pltpu.get_barrier_semaphore()
    for peer in others:
        pl.semaphore_signal(barrier, inc=1, device_id=peer, device_id_type=MESH)

    for j in range(nz):
        WP[j, :, 0 : 2 * HD] = wq_ref[:, 2 * HD * j : 2 * HD * (j + 1)]
        WP[j, :, 2 * HD : 4 * HD] = jnp.concatenate(
            [wk_ref[:, HD * j : HD * (j + 1)], wv_ref[:, HD * j : HD * (j + 1)]], axis=1
        )
    base = jnp.concatenate(
        [ga_ref[...].astype(f32), ge_ref[...].astype(f32), jnp.zeros((14, shard), f32), rt_ref[...].astype(f32)],
        axis=0,
    )
    in_half = (lax.broadcasted_iota(jnp.int32, (32, 128), 1) < shard) == (lax.rem(z, 2) == 0)
    SMT[...] = jnp.where(in_half, jnp.concatenate([base, base], axis=1), 0.0).astype(bf16)
    SMB[f, z] = SMT[...]
    WQ[f, z] = WP[z]
    pl.semaphore_wait(barrier, len(others))

    wd_full = lambda: WD[...].reshape(width, half_ff)
    wgu_full = lambda: WGU[...].reshape(width, 2 * half_ff)
    lower, upper = pl.ds(0, nz // 2), pl.ds(nz // 2, nz // 2)
    across = [None, device(fs[1], z, c), device(fs[2], z, c), device(fs[3], z, c)]

    def second_hop(ref):
        return [net.send(ref.at[f, c], ref.at[f, c], across[k]) for k in (1, 2)]

    def third_hop(ref, k):
        part, to = ((lower, across[2]), (upper, across[1]))[k - 1]
        return net.send(ref.at[fs[k], c, part], ref.at[fs[k], c, part], to)

    sends_q = [net.send(WP.at[zs[k]], WQ.at[f, z], device(f, zs[k], c)) for k in range(1, nz)]
    sends_s = [net.send(SMT, SMB.at[f, z], device(f, zs[k], c)) for k in range(1, nz)]
    loads[0].wait()
    sends_x = [net.send(X.at[c, z], X.at[c, z], device(f, zs[k], c)) for k in range(1, nz)]
    forwards_x = [net.send(X.at[c, z], X.at[c, z], partner)]
    loads[2].wait()
    sends_o = [net.send(WO.at[f, z], WO.at[f, z], device(f, zs[k], c)) for k in range(1, nz)]
    loads[1].wait()
    view_g = [lambda at: GA.at[f, c, at]]
    chain_g = line.pass_on(0, view_g)
    chains = [chain_g]
    weights = ([], [], [])

    def send_row(k, at):
        ref, staged = shards[at]
        return net.send(ref.at[row_experts(fs[k])], staged.at[f], device(fs[k], z, c))

    sends_e = [[send_row(k, at) for k in (1, 2)] for at in range(3)]

    def send_weights(k, *what):
        for at in what:
            staged, into, lanes, target = (
                (SWG, WGU, units(0), units(0)),
                (SWU, WGU, units(0), units(1)),
                (SWG, WGU, units(1), units(2)),
                (SWU, WGU, units(1), units(3)),
                (SWD, WD, pl.ds(0, half_ff), pl.ds(0, half_ff)),
            )[at]
            weights[at // 2].append(
                net.send(staged.at[:, zs[k], :, lanes], into.at[:, z, :, target], device(f, zs[k], c))
            )

    def places(shape, dim):
        at = lax.broadcasted_iota(jnp.int32, shape, dim)
        core_at, rest = lax.div(at, half), lax.rem(at, half)
        return lax.div(rest, hb) * block + core_at * hb + lax.rem(rest, hb)

    def layout(position):
        segment = jnp.zeros_like(position)
        start = jnp.zeros_like(position)
        end = jnp.int32(0)
        for i in range(ndoc):
            length = dl_ref[0, i]
            end = end + length
            after = jnp.where(position >= end, 1, 0)
            segment = segment + after
            start = start + after * length
        return segment, position - start

    lane = lax.broadcasted_iota(jnp.int32, (1, 2 * HD), 1)
    former = lax.rem(lane, HD) < HD // 2
    is_key = lane < HD

    with jax.named_scope("tables0"):
        pos_col = places((rows, 1), 0)
        seg_col, offset = layout(pos_col)
        POSC[...] = pos_col
        SEGC[...] = seg_col
        pos_row = places((1, rows), 1)
        seg_row, unused = layout(pos_row)

    def swapped(v):
        return jnp.where(former, pltpu.roll(v, 2 * HD - HD // 2, 1), pltpu.roll(v, HD // 2, 1))

    for copy in sends_q:
        copy.wait_recv()
    sends_q2 = [net.send(WQ.at[f], WQ.at[f], device(fs[k], z, c)) for k in range(1, nf)]
    for copy in sends_s:
        copy.wait_recv()
    sends_s2 = [net.send(SMB.at[f], SMB.at[f], device(fs[k], z, c)) for k in range(1, nf)]
    for at in (0, 1):
        sends_e[at].append(send_row(3, at))
    with jax.named_scope("tables1"):
        angle = offset.astype(f32) * fr_ref[0:1, :]
        CT[...] = jnp.cos(angle)
        ST[...] = jnp.where(former, -1.0, 1.0) * jnp.sin(angle)
    for copy in sends_s2:
        copy.wait_recv()
    for pair in range(nf * nz // 2):
        at_f, at_z = pair // (nz // 2), 2 * (pair % (nz // 2))
        SMW[:, 128 * pair : 128 * pair + 128] = SMB[at_f, at_z] + SMB[at_f, at_z + 1]

    def norm_block(at_c, at_z):
        v = X[at_c, at_z].astype(f32)
        inverse = lax.rsqrt(jnp.mean(v * v, axis=1, keepdims=True) + epsilon)
        at = pl.ds(pl.multiple_of((at_c * nz + at_z) * hb, hb), hb)
        N1[at, :] = (v * inverse * SMW[0:1, :].astype(f32)).astype(bf16)

    norm_block(c, z)
    for k in range(1, nz):
        sends_x[k - 1].wait_recv()
        forwards_x.append(net.send(X.at[c, zs[k]], X.at[c, zs[k]], partner))
        norm_block(c, zs[k])
    for k in range(nz):
        forwards_x[k].wait_recv()
        norm_block(other, zs[k])
    for copy in sends_q2:
        copy.wait_recv()
    with jax.named_scope("qkv"):
        projected = dot_nn(N1[...], WQ[...].reshape(width, 4 * HD))
        cosine, sine = CT[...], ST[...]
        q_part, kv_part = projected[:, : 2 * HD], projected[:, 2 * HD :]
        Q[...] = (q_part * cosine + swapped(q_part) * sine).astype(bf16)
        kv = jnp.where(is_key, kv_part * cosine + swapped(kv_part) * sine, kv_part).astype(bf16)
        K[...] = kv[:, :HD]
        V[...] = kv[:, HD:]
    for copy in sends_o:
        copy.wait_recv()
    sends_o2 = [net.send(WO.at[f], WO.at[f], across[k]) for k in (1, 2, 3)]
    sends_e[2].append(send_row(3, 2))

    scale = HD ** (-0.5)
    step = 2 * hb

    def attend(i, carry):
        at = pl.ds(pl.multiple_of(i * step, step), step)
        mask = (SEGC[at, :] == seg_row) & (pos_row <= POSC[at, :])
        q = Q[at, :]
        pieces = []
        for r in range(2):
            scores = dot_nt(q[:, r * HD : (r + 1) * HD], K[...]) * scale
            scores = jnp.where(mask, scores, masked_score)
            peak = jnp.max(scores, axis=1, keepdims=True)
            weights = jnp.where(mask, jnp.exp(scores - peak), 0.0)
            total = jnp.sum(weights, axis=1, keepdims=True)
            pieces.append(dot_nn(weights.astype(bf16), V[...]) / total)
            PSC[r, at, :] = (weights / total).astype(bf16)
        out = jnp.concatenate(pieces, axis=1).astype(bf16)
        at_c, at_z = lax.div(2 * i, nz), lax.rem(2 * i, nz)
        ATT[at_c, pl.ds(at_z, 2)] = out.reshape(2, hb, 2 * HD)
        return carry

    with jax.named_scope("attend"):
        lax.fori_loop(0, rows // step, attend, 0)
    columns = pl.ds(pl.multiple_of(z * 2 * HD, 2 * HD), 2 * HD)
    sends_a = [
        net.send(ATT.at[:, zs[k]], AT.at[:, :, columns], device(f, zs[k], c)) for k in range(1, nz)
    ]
    AT[:, :, columns] = ATT[:, z]
    arrive(chain_g)
    chain_g = line.pass_on(1, view_g)
    chains.append(chain_g)
    for copy in loads[3:]:
        copy.wait()
    for copy in sends_e[0] + sends_e[1]:
        copy.wait_recv()
    send_weights(3, 0, 1)
    for copy in sends_a + sends_o2:
        copy.wait_recv()

    with jax.named_scope("proj"):
        part = dot_nt(AT[...].reshape(block, nz * 2 * HD), WO[...].reshape(width, nz * 2 * HD))
        PP[...] = part.reshape(2, hb, width)
    send_p = net.send(PP.at[other], PR, partner)
    arrive(chain_g)
    chain_g = line.pass_on(2, view_g)
    chains.append(chain_g)
    x_own = X[c, z].astype(f32)
    gain_two = SMW[1:2, :].astype(f32)
    send_p.wait_recv()
    residual = x_own + PP[c] + PR[...]
    RES[...] = residual
    inverse_two = lax.rsqrt(jnp.mean(residual * residual, axis=1, keepdims=True) + epsilon)
    N2[f, c, z] = (residual * inverse_two * gain_two).astype(bf16)
    normed_two = N2[f, c, z]
    logits = dot_nt(SMW[16 : 16 + experts, :], normed_two)
    expert_at = lax.broadcasted_iota(jnp.int32, (experts, hb), 0)
    route = ec_ref[...]
    route = jnp.where(c == 0, route, pltpu.roll(route, 128 - hb, 1))
    picked = jnp.zeros((experts, hb), jnp.bool_)
    for j in range(chosen):
        picked = picked | (route[j : j + 1, 0:hb] == expert_at)
    peak = jnp.max(jnp.where(picked, logits, masked_score), axis=0, keepdims=True)
    weight = jnp.where(picked, jnp.exp(logits - peak), 0.0)
    gates = weight / jnp.sum(weight, axis=0, keepdims=True)
    GTB[f, c, z] = jnp.concatenate([gates, jnp.zeros((experts, 128 - hb), f32)], axis=1)
    view_n = [lambda at: N2.at[f, c, at], lambda at: GTB.at[f, c, at]]
    early = net.numbers(
        sends_q, sends_s, sends_x, forwards_x, sends_o, sends_e[:2], sends_q2, sends_s2, sends_o2, sends_a, chains[:2], send_p
    )
    chain_n = line.pass_on(0, view_n)
    chains = [chains[2], chain_n]
    send_weights(2, 0)

    arrive(chain_g)
    sends_g2 = second_hop(GA)
    forwards_g = [net.send(GA.at[f, c], GA.at[f, c], partner)]
    arrive(chain_n)
    chain_n = line.pass_on(1, view_n)
    chains.append(chain_n)
    send_weights(2, 1)
    arrive(chain_n)
    chain_n = line.pass_on(2, view_n)
    chains.append(chain_n)
    send_weights(1, 0, 1)
    for copy in sends_e[2]:
        copy.wait_recv()
    for k in (3, 2, 1):
        send_weights(k, 4)
    sends_g3 = []
    for k in (1, 2):
        sends_g2[k - 1].wait_recv()
        sends_g3.append(third_hop(GA, k))
        forwards_g.append(net.send(GA.at[fs[k], c], GA.at[fs[k], c], partner))
    arrive(chain_n)
    sends_n2 = second_hop(N2)
    sends_t2 = [net.send(GTB.at[f, c], GTB.at[f, c], across[k]) for k in (1, 2, 3)]
    forwards_n = [net.send(N2.at[f, c], N2.at[f, c], partner)]
    forwards_t = [net.send(GTB.at[f, c], GTB.at[f, c], partner)]
    for k in (3, 2, 1):
        send_weights(k, 2, 3)
    before = range(len(net.copies) - 20)

    WGU[:, z, :, 0:unit] = SWG[:, z, :, 0:unit]
    WGU[:, z, :, unit : 2 * unit] = SWU[:, z, :, 0:unit]
    WGU[:, z, :, 2 * unit : 3 * unit] = SWG[:, z, :, unit : 2 * unit]
    WGU[:, z, :, 3 * unit : 4 * unit] = SWU[:, z, :, unit : 2 * unit]
    WD[:, z] = SWD[:, z]
    chosen_row = jnp.where(
        lax.broadcasted_iota(jnp.int32, (experts, 128), 0) == own, 1.0, 0.0
    ).astype(f32)
    sends_d, sends_b, exchange_b, exchange_m = [], {}, {}, {}
    low_half = z < nz // 2
    in_order = [jnp.where(low_half, 3, 0), jnp.where(low_half, 2, 1), zs[1], z]
    grads_z, grads_f = ([], []), ([], [])

    def send_grads(h, k):
        to = device(f, zs[k], c)
        grads_z[h].append(net.send(DGB.at[h, :, zs[k]], ZG.at[h, z], to))
        grads_z[h].append(net.send(DDB.at[h, :, zs[k]], ZD.at[h, z], to))

    def spread_grads(h):
        ZG[h, z] = DGB[h, :, z]
        ZD[h, z] = DDB[h, :, z]
        for copy in grads_z[h]:
            copy.wait_recv()
        for k in range(1, nf):
            grads_f[h].append(
                net.send(ZG.at[h, :, fs[k]], GUL.at[f, :, :, pl.ds(2 * h * unit, 2 * unit)], across[k])
            )
            grads_f[h].append(net.send(ZD.at[h, :, fs[k]], DDL.at[f, :, :, units(h)], across[k]))
        GUL[f, :, :, 2 * h * unit : 2 * (h + 1) * unit] = ZG[h, :, f]
        DDL[f, :, :, h * unit : (h + 1) * unit] = ZD[h, :, f]

    def expert_part(h, k):
        at_f = fs[k]
        tokens = N2[at_f].reshape(rows, width)
        with jax.named_scope("gateup"):
            PSX[...] = dot_nn(tokens, WGU[:, :, :, 2 * h * unit : 2 * (h + 1) * unit].reshape(width, 2 * unit))
        if h == 0:
            with jax.named_scope("gatecol"):
                for piece in range(2 * nz):
                    tile = GTB[at_f, piece // nz, piece % nz][:, 0:hb]
                    GC[k, piece * hb : (piece + 1) * hb, :] = dot_tn(tile, chosen_row, lax.Precision.HIGHEST)

        def expert_chunk(i, carry):
            at = pl.ds(pl.multiple_of(i * 64, 64), 64)
            gate_pre = PSX[at, 0:unit]
            up_pre = PSX[at, unit : 2 * unit]
            raw = AA[k, at, h * unit : (h + 1) * unit]
            gate = GC[k, at, :]
            sigmoid = jax.nn.sigmoid(gate_pre)
            silu = gate_pre * sigmoid
            act = silu * up_pre
            PRD[at, :] = (act * raw).astype(bf16)
            H[k, at, h * unit : (h + 1) * unit] = (act * gate).astype(bf16)
            grad = raw * gate
            UG[k, at, 2 * h * unit : (2 * h + 1) * unit] = (
                grad * up_pre * sigmoid * (1.0 + gate_pre * (1.0 - sigmoid))
            ).astype(bf16)
            UG[k, at, (2 * h + 1) * unit : 2 * (h + 1) * unit] = (grad * silu).astype(bf16)
            return carry

        with jax.named_scope("chunk"):
            lax.fori_loop(0, rows // 64, expert_chunk, 0)
        if h == 1:
            with jax.named_scope("back"):
                BP[at_f] = dot_nt(UG[k], WGU[...].reshape(width, 2 * half_ff)).astype(bf16).reshape(2, nz, hb, width)
            exchange_b[k] = net.send(BP.at[at_f, other], BR.at[at_f], partner)
        with jax.named_scope("gdot"):
            dots = dot_nt(jnp.ones((8, unit), bf16), PRD[...])
            GDS[k] = dots if h == 0 else GDS[k] + dots
        if h == 1:
            sets = []
            for j in range(nz):
                for t in range(2):
                    to_z, to_c = zs[j], lax.rem(c + t, 2)
                    lanes = pl.ds(pl.multiple_of((to_c * (nz // 2) + lax.div(to_z, 2)) * 128, 128), 128)
                    if (k, j, t) != (0, 0, 0):
                        sets.append(
                            (GDS.at[k, pl.ds(0, 1), lanes], GD.at[f, z, c, pl.ds(0, 1)], device(at_f, to_z, to_c))
                        )
                    else:
                        GD[f, z, c] = GDS[0, :, lanes]
            sends_d.append(net.together(sets, SGW.at[pl.ds(0, len(sets))]))

    def mix(k):
        with jax.named_scope("mix"):
            MP[fs[k]] = dot_nt(H[k], WD[...].reshape(width, half_ff)).astype(bf16).reshape(2, nz, hb, width)
        exchange_m[k] = net.send(MP.at[fs[k], other], MR.at[fs[k]], partner)

    def weight_terms(h, k):
        with jax.named_scope("wgrad"):
            gate_up = dot_tn(UG[k, :, 2 * h * unit : 2 * (h + 1) * unit], N2[fs[k]].reshape(rows, width))
            down = dot_tn(H[k, :, h * unit : (h + 1) * unit], GA[fs[k]].reshape(rows, width))
            first = k == (0, 3)[h]
            DGU[...] = gate_up if first else DGU[...] + gate_up
            DDT[...] = down if first else DDT[...] + down

    def shed(h):
        with jax.named_scope("transpose"):
            DGB[h] = jnp.transpose(DGU[...]).astype(bf16).reshape(nf, nz, shard, 2 * unit)
            DDB[h] = jnp.transpose(DDT[...]).astype(bf16).reshape(nf, nz, shard, unit)

    def cotangent(k):
        forwards_g[k].wait_recv()
        with jax.named_scope("cotangent"):
            AA[k] = dot_nn(GA[fs[k]].reshape(rows, width), WD[...].reshape(width, half_ff))

    net.drain(before)
    for copy in weights[2]:
        copy.wait_recv()
    for k in range(nf - 1):
        cotangent(k)
    for copy in weights[0]:
        copy.wait_recv()
    for k in range(nf):
        if k == 1:
            sends_n3 = []
            for i in (1, 2):
                sends_n2[i - 1].wait_recv()
                sends_n3.append(third_hop(N2, i))
                forwards_n.append(net.send(N2.at[fs[i], c], N2.at[fs[i], c], partner))
                sends_t2[i - 1].wait_recv()
                forwards_t.append(net.send(GTB.at[fs[i], c], GTB.at[fs[i], c], partner))
            for copy in sends_g3:
                copy.wait_recv()
            forwards_g.append(net.send(GA.at[fs[3], c], GA.at[fs[3], c], partner))
        if k == 3:
            cotangent(k)
            for copy in sends_n3:
                copy.wait_recv()
            forwards_n.append(net.send(N2.at[fs[k], c], N2.at[fs[k], c], partner))
            sends_t2[2].wait_recv()
            forwards_t.append(net.send(GTB.at[fs[k], c], GTB.at[fs[k], c], partner))
        forwards_n[k].wait_recv()
        forwards_t[k].wait_recv()
        expert_part(0, k)
        weight_terms(0, k)
    shed(0)
    for k in (3, 2, 1):
        send_grads(0, k)
    for copy in weights[1]:
        copy.wait_recv()
    own_half = ((lower, 1), (upper, 2))

    def spread(k, exchange, part, back, total, via, into, order):
        at_f = fs[k]
        exchange[k].wait_recv()
        if k == 0:
            total[...] = part[at_f, c].astype(f32) + back[at_f].astype(f32)
            return []
        if k == 3:
            part[at_f, c] = (part[at_f, c].astype(f32) + back[at_f].astype(f32)).astype(bf16)
            return [net.send(part.at[at_f, c, half_at], via.at[to - 1], across[to]) for half_at, to in own_half]
        return None

    def spread_near(k, firsts, part, back, via, into, order):
        at_f = fs[k]
        half_at, other_half = (upper, lower) if k == 1 else (lower, upper)
        firsts[2 - k].wait_recv()
        part[at_f, c, half_at] = (
            part[at_f, c, half_at].astype(f32) + back[at_f, half_at].astype(f32) + via[2 - k].astype(f32)
        ).astype(bf16)
        part[at_f, c, other_half] = (
            part[at_f, c, other_half].astype(f32) + back[at_f, other_half].astype(f32)
        ).astype(bf16)
        return [net.send(part.at[at_f, c, at], into.at[k - 1, at], across[k]) for at in order]

    sends_m = {}
    middle = net.numbers(
        sends_e[2:], sends_g2, sends_g3, forwards_g, *weights, chains, sends_n2, sends_n3, sends_t2,
        forwards_n, forwards_t,
    )
    net.free(early)
    expert_part(1, 3)
    weight_terms(1, 3)
    mix(3)
    firsts_b = spread(3, exchange_b, BP, BR, BOWN, RBV, RB, in_order)
    for k in (1, 2, 0):
        expert_part(1, k)
    for k in (1, 2):
        exchange_b[k].wait_recv()
        sends_b[k] = spread_near(k, firsts_b, BP, BR, RBV, RB, in_order)
    spread(0, exchange_b, BP, BR, BOWN, RBV, RB, in_order)
    firsts_m = spread(3, exchange_m, MP, MR, MOWN, RMV, RM, in_order)
    for k in (1, 2, 0):
        mix(k)
        weight_terms(1, k)

    expert_copies = len(net.copies)
    shed(1)

    def dots_back():
        for copy in sends_d:
            copy.wait_recv()
        dots = jnp.concatenate(
            [
                GD[e // nz, e % nz, 0][0:1, :] + GD[e // nz, e % nz, 1][0:1, :]
                for e in range(experts)
            ],
            axis=0,
        )
        dots = jnp.where(lax.rem(z, 2) == 0, dots, pltpu.roll(dots, 128 - hb, 1))[:, 0:hb]
        gates = GTB[f, c, z][:, 0:hb]
        logit_grad = gates * (dots - jnp.sum(gates * dots, axis=0, keepdims=True))
        router_t = SMW[16 : 16 + experts, :].astype(f32)
        SG[0:experts, :] = dot_nn(logit_grad, N2[f, c, z].astype(f32), lax.Precision.HIGHEST)
        GRES[...] = dot_tn(logit_grad, router_t, lax.Precision.HIGHEST)

    own_b, out_b, into_b = (lambda at: BOWN.at[at]), (lambda w, t: CO.at[w, t]), (lambda w, t: CI.at[w, t])

    def take_block(at):
        for k in (1, 2):
            sends_b[k][at].wait_recv()
            BOWN[in_order[at]] += RB[k - 1, in_order[at]].astype(f32)

    sums = []
    for t in range(nz):
        take_block(t)
        if t > 0:
            arrive(chain_b)
        if t < nz - 1:
            at_sums = len(net.copies)
            chain_b = line.add_on(t, own_b, out_b, into_b)
            sums.extend(range(at_sums, len(net.copies)))
        if t == 0:
            dots_back()
        if t == 2:
            spread_grads(0)
    line.finish(BOWN.at[z], into_b)
    net.free(middle)

    residual = RES[...]
    inverse_two = lax.rsqrt(jnp.mean(residual * residual, axis=1, keepdims=True) + epsilon)
    grad_two = BOWN[z] + GRES[...]
    scaled = grad_two * gain_two
    grad_res = (
        GA[f, c, z].astype(f32)
        + inverse_two * scaled
        - residual * (inverse_two * inverse_two * inverse_two) * jnp.mean(scaled * residual, axis=1, keepdims=True)
    )
    GRES[...] = grad_res
    RL[c] = grad_res.astype(bf16)
    send_r = net.send(RL.at[c], RL.at[c], partner)
    gain_term = jnp.sum(grad_two * residual * inverse_two, axis=0, keepdims=True)
    SG[experts : experts + 8, :] = jnp.broadcast_to(gain_term, (8, width))
    wide = width // nf
    block_lanes = lambda at: pl.ds(pl.multiple_of(at * wide, 128), wide)
    sends_sg = [net.send(SG.at[:, block_lanes(fs[k])], SGF.at[k - 1], device(fs[k], z, c)) for k in range(1, nf)]
    send_r.wait_recv()
    low = RL[...].reshape(block, width)
    with jax.named_scope("attgrad"):
        AGS[...] = dot_nn(low, WO[...].reshape(width, nz * 2 * HD)).astype(bf16).reshape(2, hb, nz * 2 * HD)
    sends_ag = [
        net.send(
            AGS.at[:, :, pl.ds(pl.multiple_of(zs[k] * 2 * HD, 2 * HD), 2 * HD)],
            AGR.at[:, z],
            device(f, zs[k], c),
        )
        for k in range(1, nz)
    ]
    AGR[:, z] = AGS[:, :, columns]
    for k in (1, 2):
        exchange_m[k].wait_recv()
        sends_m[k] = spread_near(k, firsts_m, MP, MR, RMV, RM, in_order)
    spread(0, exchange_m, MP, MR, MOWN, RMV, RM, in_order)
    for k in (1, 3, 2):
        send_grads(1, k)
    with jax.named_scope("outgrad"):
        DWO[...] = (
            dot_tn(low, AT[...].reshape(block, nz * 2 * HD))
            .astype(bf16)
            .reshape(nf, nz, shard, nz * 2 * HD)
        )
    sends_wo = [net.send(DWO.at[fs[k]], RWO.at[k - 1], device(fs[k], z, c)) for k in range(1, nf)]

    net.drain(range(expert_copies))
    for copy in sends_ag:
        copy.wait_recv()

    def backward(i, carry):
        at = pl.ds(pl.multiple_of(i * step, step), step)
        at_c, at_z = lax.div(2 * i, nz), lax.rem(2 * i, nz)
        grad = AGR[at_c, pl.ds(at_z, 2)].reshape(step, 2 * HD)
        out = ATT[at_c, pl.ds(at_z, 2)].reshape(step, 2 * HD)
        both = grad.astype(f32) * out.astype(f32)
        pieces = []
        for r in range(2):
            delta = jnp.sum(both[:, r * HD : (r + 1) * HD], axis=1, keepdims=True)
            prob_grad = dot_nt(grad[:, r * HD : (r + 1) * HD], V[...])
            probs = PSC[r, at, :].astype(f32)
            score_grad = (probs * (prob_grad - delta) * scale).astype(bf16)
            DS[r, at, :] = score_grad
            pieces.append(dot_nn(score_grad, K[...]))
        DQ[at, :] = jnp.concatenate(pieces, axis=1)
        return carry

    with jax.named_scope("attback"):
        lax.fori_loop(0, rows // step, backward, 0)
    with jax.named_scope("kvgrad"):
        grads = AGR[...].reshape(rows, 2 * HD)
        key_t = dot_tn(Q[:, 0:HD], DS[0]) + dot_tn(Q[:, HD : 2 * HD], DS[1])
        value_t = dot_tn(grads[:, 0:HD], PSC[0]) + dot_tn(grads[:, HD : 2 * HD], PSC[1])
        kv_grad = jnp.transpose(jnp.concatenate([key_t, value_t], axis=0))
        cosine, sine = CT[...], ST[...]
        q_grad = DQ[...]
        DQKV[:, 0 : 2 * HD] = (q_grad * cosine - swapped(q_grad) * sine).astype(bf16)
        DQKV[:, 2 * HD : 4 * HD] = jnp.where(
            is_key, kv_grad * cosine - swapped(kv_grad) * sine, kv_grad
        ).astype(bf16)
    with jax.named_scope("ingrad"):
        NG[...] = dot_nt(DQKV[...], WQ[...].reshape(width, 4 * HD)).astype(bf16).reshape(2, nz, hb, width)
    send_ng = net.send(NG.at[other], NR, partner)
    with jax.named_scope("qkvgrad"):
        DWQ[...] = (
            jnp.transpose(dot_tn(DQKV[...], N1[...])).astype(bf16).reshape(nf, nz, shard, 4 * HD)
        )
    sends_wq = [net.send(DWQ.at[fs[k]], RWQ.at[k - 1], device(fs[k], z, c)) for k in range(1, nf)]
    send_ng.wait_recv()
    net.drain(sums)
    BOWN[...] = NG[c].astype(f32) + NR[...].astype(f32)
    chain_g1 = line.add_on(0, own_b, out_b, into_b)
    for k in (1, 2):
        for at in range(nz):
            sends_m[k][at].wait_recv()
        MOWN[...] += RM[k - 1].astype(f32)
    own_m, out_m, into_m = (lambda at: MOWN.at[at]), (lambda w, t: MO.at[w, t]), (lambda w, t: MI.at[w, t])
    chain_m = line.add_on(0, own_m, out_m, into_m)
    arrive(chain_g1)
    chain_g1 = line.add_on(1, own_b, out_b, into_b)
    arrive(chain_m)
    chain_m = line.add_on(1, own_m, out_m, into_m)
    arrive(chain_g1)
    chain_g1 = line.add_on(2, own_b, out_b, into_b)
    arrive(chain_m)
    chain_m = line.add_on(2, own_m, out_m, into_m)

    arrive(chain_g1)
    line.finish(BOWN.at[z], into_b)
    grad_one = BOWN[z]
    gain_one = SMW[0:1, :].astype(f32)
    x_own = X[c, z].astype(f32)
    inverse = lax.rsqrt(jnp.mean(x_own * x_own, axis=1, keepdims=True) + epsilon)
    gain_term = jnp.sum(grad_one * x_own * inverse, axis=0, keepdims=True)
    SG1[0] = jnp.broadcast_to(gain_term, (8, width))
    send_g1 = net.send(SG1.at[0], SG1.at[1], partner)
    scaled = grad_one * gain_one
    EXG[c] = (
        GRES[...]
        + inverse * scaled
        - x_own * (inverse * inverse * inverse) * jnp.mean(scaled * x_own, axis=1, keepdims=True)
    )
    send_ig = net.send(EXG.at[c], EXG.at[c], partner)
    small = SG[:, block_lanes(f)]
    for k in range(1, nf):
        sends_sg[k - 1].wait_recv()
        small = small + SGF[k - 1]
    SGT[...] = small
    pair_lanes = lambda at: pl.ds(pl.multiple_of(lax.div(at, 2) * 128, 128), 128)
    sends_sz = [net.send(SGT.at[:, pair_lanes(zs[k])], SGZ.at[k - 1], device(f, zs[k], c)) for k in range(1, nz)]
    total = DWO[f].astype(f32)
    for k in range(1, nf):
        sends_wo[k - 1].wait_recv()
        total = total + RWO[k - 1].astype(f32)
    ZWO[...] = total.astype(bf16)
    sends_wo2 = [net.send(ZWO.at[zs[k]], LWO.at[z], device(f, zs[k], c)) for k in range(1, nz)]
    LWO[z] = ZWO[z]
    total = DWQ[f].astype(f32)
    for k in range(1, nf):
        sends_wq[k - 1].wait_recv()
        total = total + RWQ[k - 1].astype(f32)
    ZWQ[...] = total.astype(bf16)
    sends_wq2 = [net.send(ZWQ.at[zs[k]], LWQ.at[z], device(f, zs[k], c)) for k in range(1, nz)]
    LWQ[z] = ZWQ[z]
    small = SGT[:, pair_lanes(z)]
    for k in range(1, nz):
        sends_sz[k - 1].wait_recv()
        small = small + SGZ[k - 1]
    SGP[0] = small
    send_sp = net.send(SGP.at[0], SGP.at[1], partner)
    net.drain(range(expert_copies))
    send_g1.wait_recv()
    SG1P[...] = SG1[0] + SG1[1]
    lanes_of = lambda df, dz: pl.ds(pl.multiple_of((df * (nz // 2) + lax.div(dz, 2)) * 128, 128), 128)
    sets = [
        (SG1P.at[pl.ds(0, 1), lanes_of(fs[i], zs[j])], RSG1.at[f, z, pl.ds(0, 1)], device(fs[i], zs[j], c))
        for i, j in same
    ]
    sends_g1 = [net.together(sets, SGW.at[pl.ds(0, len(sets))])]
    RSG1[f, z] = SG1P[:, lanes_of(f, z)]

    spread_grads(1)
    arrive(chain_m)
    line.finish(MOWN.at[z], into_m)
    EXB[c] = (RES[...] + MOWN[z]).astype(bf16)
    send_bo = net.send(EXB.at[c], EXB.at[c], partner)
    outs = []

    def leave(source, target):
        copy = pltpu.make_async_copy(source, target, local_sems.at[6 + len(outs)])
        copy.start()
        outs.append(copy)

    send_sp.wait_recv()
    SMO[...] = SGP[0] + SGP[1]
    leave(SMO, small_out)
    for copy in sends_wo2:
        copy.wait_recv()
    total = LWO[0].astype(f32)
    for j in range(1, nz):
        total = total + LWO[j].astype(f32)
    DWF[...] = total
    leave(DWF, dwo_out)
    for copy in sends_wq2:
        copy.wait_recv()
    leave(LWQ, dqkv_out)
    send_bo.wait_recv()
    leave(EXB, block_out)
    send_ig.wait_recv()
    leave(EXG, input_grad)
    for copy in sends_g1:
        copy.wait_recv()
    small = jnp.zeros((1, 128), f32)
    for i in range(nf):
        for j in range(nz):
            small = small + RSG1[i, j, 0:1]
    GNO[...] = jnp.broadcast_to(small, (8, 128))
    leave(GNO, gain_out)
    for copy in grads_f[0] + grads_f[1]:
        copy.wait_recv()
    leave(GUL, dgu_out)
    leave(DDL, dd_out)
    with jax.named_scope("drain"):
        net.drain()
    with jax.named_scope("outs"):
        for copy in outs:
            copy.wait()


def finish_kernel(
    dims, block_ref, input_ref, small_ref, gain_ref, dqkv_ref, dwo_ref, dgu_ref, dd_ref,
    block_out, input_out, gain1_out, q_out, k_out, v_out, o_out, gain2_out, router_out, gate_out, up_out, down_out,
):
    nz, experts, half_ff, shard = dims
    block_out[...] = block_ref[...]
    input_out[...] = input_ref[...]
    unit = half_ff // 2
    for h in range(2):
        gate_out[:, :, h * unit : (h + 1) * unit] = dgu_ref[:, :, 2 * h * unit : (2 * h + 1) * unit].astype(f32)
        up_out[:, :, h * unit : (h + 1) * unit] = dgu_ref[:, :, (2 * h + 1) * unit : 2 * (h + 1) * unit].astype(f32)
    down_out[...] = dd_ref[...].astype(f32)
    even = lax.rem(lax.axis_index("ctx"), 2) == 0
    pick = lambda v: jnp.where(even, v, pltpu.roll(v, 128 - shard, 1))[:, 0:shard]

    def once():
        gain1_out[...] = pick(gain_ref[...])[0:1]
        small = pick(small_ref[...])
        router_out[...] = small[0:experts]
        gain2_out[...] = small[experts : experts + 1]
        o_out[...] = dwo_ref[...]
        for j in range(nz):
            q_out[:, 2 * HD * j : 2 * HD * (j + 1)] = dqkv_ref[j, :, 0 : 2 * HD].astype(f32)
        for at, ref in ((2, k_out), (3, v_out)):
            ref[...] = jnp.concatenate(
                [dqkv_ref[j, :, at * HD : (at + 1) * HD].astype(f32) for j in range(nz)], axis=1
            )

    pl.when(pl.program_id(0) == 0)(once)


def fast_local(
    nf, nz,
    hidden_in, out_grad, attention_gain, query_weight, key_weight, value_weight, output_weight,
    expert_gain, router_weight, gate_weight, up_weight, down_weight, doc_lengths, expert_choice,
):
    block, width = hidden_in.shape[1], hidden_in.shape[2]
    hb = block // 2
    experts, shard, half_ff = gate_weight.shape
    ndoc, chosen = doc_lengths.shape[1], expert_choice.shape[2]
    rows = nz * block
    halfway = HD // 2
    frequency = np.float32(rope_base) ** (-np.arange(halfway, dtype=np.float32) / np.float32(halfway))
    frequency = jnp.asarray(np.tile(np.tile(frequency, 4)[None], (8, 1)).astype(np.float32))

    vm = pl.BlockSpec(memory_space=pltpu.VMEM)
    anywhere = pl.BlockSpec(memory_space=pl.ANY)
    shape = lambda s, d: jax.ShapeDtypeStruct(s, d)
    W = nz * 2 * HD
    scratch = dict(
        WP=((nz, shard, 4 * HD), bf16), SMT=((32, 128), bf16),
        X=((2, nz, hb, width), bf16), WQ=((nf, nz, shard, 4 * HD), bf16), WO=((nf, nz, shard, W), bf16),
        SMB=((nf, nz, 32, 128), bf16), SMW=((32, width), bf16), N1=((rows, width), bf16),
        CT=((rows, 128), f32), ST=((rows, 128), f32), SEGC=((rows, 1), jnp.int32), POSC=((rows, 1), jnp.int32),
        Q=((rows, 2 * HD), bf16), K=((rows, HD), bf16), V=((rows, HD), bf16), PSC=((2, rows, rows), bf16),
        ATT=((2, nz, hb, 2 * HD), bf16), AT=((2, hb, W), bf16), PP=((2, hb, width), f32), PR=((hb, width), f32),
        RES=((hb, width), f32),
        N2=((nf, 2, nz, hb, width), bf16), GTB=((nf, 2, nz, experts, 128), f32), GA=((nf, 2, nz, hb, width), bf16),
        WGU=((nf, nz, shard, 2 * half_ff), bf16), WD=((nf, nz, shard, half_ff), bf16),
        SWG=((nf, nz, shard, half_ff), bf16), SWU=((nf, nz, shard, half_ff), bf16), SWD=((nf, nz, shard, half_ff), bf16),
        AA=((nf, rows, half_ff), f32), PSX=((rows, half_ff), f32), GC=((nf, rows, 128), f32),
        H=((nf, rows, half_ff), bf16), UG=((nf, rows, 2 * half_ff), bf16), PRD=((rows, half_ff // 2), bf16),
        MP=((nf, 2, nz, hb, width), bf16), MR=((nf, nz, hb, width), bf16),
        BP=((nf, 2, nz, hb, width), bf16), BR=((nf, nz, hb, width), bf16),
        DGU=((half_ff, width), f32), DDT=((half_ff // 2, width), f32),
        GDS=((nf, 8, rows), f32), GD=((nf, nz, 2, 8, 128), f32),
        RB=((2, nz, hb, width), bf16), RM=((2, nz, hb, width), bf16),
        RBV=((2, nz // 2, hb, width), bf16), RMV=((2, nz // 2, hb, width), bf16),
        BOWN=((nz, hb, width), f32), MOWN=((nz, hb, width), f32),
        CO=((2, nz - 1, hb, width), bf16), CI=((2, nz - 1, hb, width), bf16),
        MO=((2, nz - 1, hb, width), bf16), MI=((2, nz - 1, hb, width), bf16),
        DGB=((2, nf, nz, shard, half_ff), bf16), GUL=((nf, nz, shard, 2 * half_ff), bf16), ZG=((2, nz, nf, shard, half_ff), bf16),
        DDB=((2, nf, nz, shard, half_ff // 2), bf16), DDL=((nf, nz, shard, half_ff), bf16), ZD=((2, nz, nf, shard, half_ff // 2), bf16),
        SG=((experts + 8, width), f32), SGF=((nf - 1, experts + 8, width // nf), f32),
        SGT=((experts + 8, width // nf), f32), SGZ=((nz - 1, experts + 8, 128), f32), SGP=((2, experts + 8, 128), f32),
        GRES=((hb, width), f32), RL=((2, hb, width), bf16),
        AGS=((2, hb, W), bf16), AGR=((2, nz, hb, 2 * HD), bf16),
        DWO=((nf, nz, shard, W), bf16), RWO=((nf - 1, nz, shard, W), bf16),
        ZWO=((nz, shard, W), bf16), LWO=((nz, shard, W), bf16),
        DS=((2, rows, rows), bf16), DQ=((rows, 2 * HD), f32),
        DQKV=((rows, 4 * HD), bf16), NG=((2, nz, hb, width), bf16), NR=((nz, hb, width), bf16),
        DWQ=((nf, nz, shard, 4 * HD), bf16), RWQ=((nf - 1, nz, shard, 4 * HD), bf16),
        ZWQ=((nz, shard, 4 * HD), bf16), LWQ=((nz, shard, 4 * HD), bf16),
        SMO=((experts + 8, 128), f32), GNO=((8, 128), f32), DWF=((shard, W), f32), SGW=((16, 128), f32), SG1=((2, 8, width), f32), SG1P=((8, width), f32), RSG1=((nf, nz, 8, 128), f32),
        EXB=((2, hb, width), bf16), EXG=((2, hb, width), f32),
    )
    slots = (96, 104)
    out = pl.pallas_call(
        functools.partial(layer_kernel, (nf, nz, hb, width, experts, half_ff, ndoc, chosen)),
        name="layer",
        out_shape=(
            shape((2, hb, width), bf16), shape((2, hb, width), f32), shape((experts + 8, 128), f32),
            shape((8, 128), f32), shape((nz, shard, 4 * HD), bf16), shape((shard, W), f32),
            shape((nf, nz, shard, 2 * half_ff), bf16), shape((nf, nz, shard, half_ff), bf16),
        ),
        in_specs=[anywhere] * 2 + [vm] * 3 + [anywhere] + [vm] * 3 + [anywhere] * 3
        + [pl.BlockSpec(memory_space=pltpu.SMEM), vm, vm],
        out_specs=(anywhere,) * 8,
        scratch_shapes=[pltpu.VMEM(s, d) for s, d in scratch.values()]
        + [pltpu.SemaphoreType.DMA((slots[0],)), pltpu.SemaphoreType.DMA((slots[1],)), pltpu.SemaphoreType.DMA((14,))],
        compiler_params=pltpu.CompilerParams(
            collective_id=0, has_side_effects=True, vmem_limit_bytes=67043328
        ),
    )(
        hidden_in[0], out_grad[0], query_weight, key_weight, value_weight, output_weight,
        attention_gain[None], expert_gain[None], router_weight.T, gate_weight, up_weight, down_weight,
        doc_lengths, expert_choice[0].T, frequency,
    )
    steps = nz // 2
    some = lambda *s: pl.BlockSpec(s, lambda i: (i,) + (0,) * (len(s) - 1))
    whole = lambda *s: pl.BlockSpec(s, lambda i: (0,) * len(s))
    per = nf * nz // steps
    out = pl.pallas_call(
        functools.partial(finish_kernel, (nz, experts, half_ff, shard)),
        name="finish",
        grid=(steps,),
        out_shape=(
            shape((block, width), bf16), shape((block, width), f32), shape((1, shard), f32),
            shape((shard, nz * 2 * HD), f32), shape((shard, nz * HD), f32), shape((shard, nz * HD), f32),
            shape((shard, W), f32), shape((1, shard), f32), shape((experts, shard), f32),
            shape((experts, shard, half_ff), f32), shape((experts, shard, half_ff), f32),
            shape((experts, shard, half_ff), f32),
        ),
        in_specs=[
            some(block // steps, width), some(block // steps, width), whole(experts + 8, 128), whole(8, 128),
            whole(nz, shard, 4 * HD), whole(shard, W), some(per, shard, 2 * half_ff), some(per, shard, half_ff),
        ],
        out_specs=(
            some(block // steps, width), some(block // steps, width), whole(1, shard),
            whole(shard, nz * 2 * HD), whole(shard, nz * HD), whole(shard, nz * HD), whole(shard, W), whole(1, shard),
            whole(experts, shard), some(per, shard, half_ff), some(per, shard, half_ff), some(per, shard, half_ff),
        ),
        compiler_params=pltpu.CompilerParams(vmem_limit_bytes=67043328),
    )(out[0].reshape(block, width), out[1].reshape(block, width), *out[2:6], out[6].reshape(experts, shard, 2 * half_ff), out[7].reshape(experts, shard, half_ff))
    block_out, input_grad, gain1, q, k, v, o, gain2, router, gate, up, down = out
    return (
        block_out[None], input_grad[None], gain1[0], q, k, v, o, gain2[0], router.T, gate, up, down,
    )


def fits(mesh, args):
    nf, nz, nc = mesh.shape["fsdp"], mesh.shape["ctx"], mesh.shape["tp"]
    hidden, query, key, gate = args[0], args[3], args[4], args[9]
    width, block = hidden.shape[2], hidden.shape[1] // nz
    return (
        nc == 2
        and nz == 4
        and nf == 4
        and hidden.shape[0] == nf
        and gate.shape[0] == nf * nz
        and gate.shape[0] == 16
        and width == 64 * nf * nz
        and block == 128
        and query.shape[1] == 2 * HD * nz * nc
        and key.shape[1] == HD * nz * nc
        and HD == 64
    )


def solution(mesh):
    in_specs = (
        P("fsdp", "ctx", None),
        P("fsdp", "ctx", None),
        P(("fsdp", "ctx")),
        P(("fsdp", "ctx"), "tp"),
        P(("fsdp", "ctx"), "tp"),
        P(("fsdp", "ctx"), "tp"),
        P(("fsdp", "ctx"), "tp"),
        P(("fsdp", "ctx")),
        P(("fsdp", "ctx"), None),
        P(None, ("fsdp", "ctx"), "tp"),
        P(None, ("fsdp", "ctx"), "tp"),
        P(None, ("fsdp", "ctx"), "tp"),
        P("fsdp", None),
        P("fsdp", "ctx", None),
    )
    out_specs = (
        P("fsdp", "ctx", None),
        P("fsdp", "ctx", None),
        P(("fsdp", "ctx")),
        P(("fsdp", "ctx"), "tp"),
        P(("fsdp", "ctx"), "tp"),
        P(("fsdp", "ctx"), "tp"),
        P(("fsdp", "ctx"), "tp"),
        P(("fsdp", "ctx")),
        P(("fsdp", "ctx"), None),
        P(None, ("fsdp", "ctx"), "tp"),
        P(None, ("fsdp", "ctx"), "tp"),
        P(None, ("fsdp", "ctx"), "tp"),
    )

    def step(*args):
        body = local
        if fits(mesh, args):
            body = functools.partial(fast_local, mesh.shape["fsdp"], mesh.shape["ctx"])
        return jax.shard_map(
            body, mesh=mesh, in_specs=in_specs, out_specs=out_specs, check_vma=False
        )(*args)

    return step
```

```python
import functools

import jax
import jax.numpy as jnp
import numpy as np
from jax import lax
from jax.experimental import pallas as pl
from jax.experimental.pallas import tpu as pltpu
from jax.sharding import PartitionSpec as P

HD = 64


epsilon = 1e-05
rope_base = 10000.0
masked_score = -1e30
highest = lax.Precision.HIGHEST


def doc_layout(lengths, positions):
    ends = jnp.cumsum(lengths)
    after = (positions[:, None] >= ends[None, :]).astype(jnp.int32)
    segment = jnp.sum(after, axis=1)
    offset = positions - jnp.sum(after * lengths[None, :], axis=1)
    return (segment, offset)


def rope_tables(offset):
    halfway = HD // 2
    frequency = rope_base ** (-jnp.arange(halfway, dtype=jnp.float32) / halfway)
    angle = offset.astype(jnp.float32)[:, None] * frequency[None, :]
    return (jnp.cos(angle), jnp.sin(angle))


def rotate(vectors, cosine, sine):
    halfway = vectors.shape[-1] // 2
    former = vectors[..., :halfway]
    latter = vectors[..., halfway:]
    cosine = cosine[:, None, :]
    sine = sine[:, None, :]
    return jnp.concatenate(
        [former * cosine - latter * sine, latter * cosine + former * sine], axis=-1
    )


def rotate_back(grads, cosine, sine):
    halfway = grads.shape[-1] // 2
    former = grads[..., :halfway]
    latter = grads[..., halfway:]
    cosine = cosine[:, None, :]
    sine = sine[:, None, :]
    return jnp.concatenate(
        [former * cosine + latter * sine, latter * cosine - former * sine], axis=-1
    )


def norm_forward(values, gain):
    inverse = lax.rsqrt(jnp.mean(values * values, axis=-1, keepdims=True) + epsilon)
    return (values * inverse * gain.astype(jnp.float32), inverse)


def norm_backward(values, inverse, gain, grad_normed):
    scaled = grad_normed * gain.astype(jnp.float32)
    grad_values = inverse * scaled - values * inverse**3 * jnp.mean(
        scaled * values, axis=-1, keepdims=True
    )
    grad_gain = jnp.sum(grad_normed * values * inverse, axis=0)
    return (grad_values, grad_gain)


def dispatch(route, experts, capacity):
    flat = route.reshape(-1)
    onehot = (flat[:, None] == jnp.arange(experts, dtype=jnp.int32)[None, :]).astype(jnp.int32)
    rank = jnp.sum((jnp.cumsum(onehot, axis=0) - onehot) * onehot, axis=1)
    slot = flat * capacity + rank
    pairs = flat.shape[0]
    owner = (
        jnp.zeros((experts * capacity,), jnp.int32).at[slot].set(jnp.arange(pairs, dtype=jnp.int32))
    )
    filled = jnp.zeros((experts * capacity,), jnp.int32).at[slot].set(1) > 0
    return (slot, owner, filled)


def expert_math(slot_inputs, slot_grads, gate_full, up_full, down_full):
    gate_pre = jnp.einsum(
        "gsd,gdf->gsf", slot_inputs, gate_full, preferred_element_type=jnp.float32
    )
    up_pre = jnp.einsum("gsd,gdf->gsf", slot_inputs, up_full, preferred_element_type=jnp.float32)
    sigmoid = jax.nn.sigmoid(gate_pre)
    activated = (gate_pre * sigmoid * up_pre).astype(jnp.bfloat16)
    expert_out = jnp.einsum(
        "gsf,gdf->gsd", activated, down_full, preferred_element_type=jnp.float32
    )
    act_grad = jnp.einsum("gsd,gdf->gsf", slot_grads, down_full, preferred_element_type=jnp.float32)
    gate_pre_grad = (act_grad * up_pre * sigmoid * (1.0 + gate_pre * (1.0 - sigmoid))).astype(
        jnp.bfloat16
    )
    up_pre_grad = (act_grad * gate_pre * sigmoid).astype(jnp.bfloat16)
    down_term = jnp.einsum(
        "gsd,gsf->gdf", slot_grads, activated, preferred_element_type=jnp.float32
    )
    gate_term = jnp.einsum(
        "gsd,gsf->gdf", slot_inputs, gate_pre_grad, preferred_element_type=jnp.float32
    )
    up_term = jnp.einsum(
        "gsd,gsf->gdf", slot_inputs, up_pre_grad, preferred_element_type=jnp.float32
    )
    slot_back = jnp.einsum(
        "gsf,gdf->gsd", gate_pre_grad, gate_full, preferred_element_type=jnp.float32
    ) + jnp.einsum("gsf,gdf->gsd", up_pre_grad, up_full, preferred_element_type=jnp.float32)
    return (expert_out, slot_back, gate_term, up_term, down_term)


def local(
    hidden_in,
    out_grad,
    attention_gain,
    query_weight,
    key_weight,
    value_weight,
    output_weight,
    expert_gain,
    router_weight,
    gate_weight,
    up_weight,
    down_weight,
    doc_lengths,
    expert_choice,
):
    block = hidden_in.shape[1]
    experts = gate_weight.shape[0]
    capacity = block * 3 // 4
    chosen_count = expert_choice.shape[2]
    context_count = lax.axis_size("ctx")
    scale = HD ** (-0.5)
    position = lax.axis_index("ctx") * block + jnp.arange(block, dtype=jnp.int32)
    lengths = doc_lengths[0]
    segment, offset = doc_layout(lengths, position)
    cosine, sine = rope_tables(offset)
    gain_one, query_full, key_full, value_full, output_full, gain_two, router_full = (
        lax.all_gather(attention_gain, ("fsdp", "ctx"), axis=0, tiled=True),
        lax.all_gather(query_weight, ("fsdp", "ctx"), axis=0, tiled=True),
        lax.all_gather(key_weight, ("fsdp", "ctx"), axis=0, tiled=True),
        lax.all_gather(value_weight, ("fsdp", "ctx"), axis=0, tiled=True),
        lax.all_gather(output_weight, ("fsdp", "ctx"), axis=0, tiled=True),
        lax.all_gather(expert_gain, ("fsdp", "ctx"), axis=0, tiled=True),
        lax.all_gather(router_weight, ("fsdp", "ctx"), axis=0, tiled=True),
    )
    inputs = hidden_in[0].astype(jnp.float32)
    normed_one, inverse_one = norm_forward(inputs, gain_one)
    normed_one = normed_one.astype(jnp.bfloat16)
    heads_local = query_full.shape[1] // HD
    groups_local = key_full.shape[1] // HD
    ratio = heads_local // groups_local
    query = rotate(
        jnp.dot(normed_one, query_full, preferred_element_type=jnp.float32).reshape(
            block, heads_local, HD
        ),
        cosine,
        sine,
    ).astype(jnp.bfloat16)
    keys = rotate(
        jnp.dot(normed_one, key_full, preferred_element_type=jnp.float32).reshape(
            block, groups_local, HD
        ),
        cosine,
        sine,
    ).astype(jnp.bfloat16)
    values = jnp.dot(normed_one, value_full, preferred_element_type=jnp.float32).astype(
        jnp.bfloat16
    )
    query_grouped = query.reshape(block, groups_local, ratio, HD)

    def allowed_mask(key_start, count):
        key_position = key_start + jnp.arange(count, dtype=jnp.int32)
        key_segment, unused = doc_layout(lengths, key_position)
        return (segment[:, None] == key_segment[None, :]) & (
            key_position[None, :] <= position[:, None]
        )

    def forward_update(state, key_block, value_block, allowed):
        peak, total, accum = state
        mask = allowed[:, None, None, :]
        scores = (
            jnp.einsum(
                "qgrd,kgd->qgrk", query_grouped, key_block, preferred_element_type=jnp.float32
            )
            * scale
        )
        scores = jnp.where(mask, scores, masked_score)
        new_peak = jnp.maximum(peak, jnp.max(scores, axis=3))
        weights = jnp.where(mask, jnp.exp(scores - new_peak[..., None]), 0.0)
        rescale = jnp.exp(peak - new_peak)
        total = total * rescale + jnp.sum(weights, axis=3)
        accum = accum * rescale[..., None] + jnp.einsum(
            "qgrk,kgd->qgrd", weights, value_block.astype(jnp.float32), precision=highest
        )
        return (new_peak, total, accum)

    travel = (keys.reshape(block, groups_local * HD), values)
    initial = (
        jnp.full((block, groups_local, ratio), masked_score, jnp.float32),
        jnp.zeros((block, groups_local, ratio), jnp.float32),
        jnp.zeros((block, groups_local, ratio, HD), jnp.float32),
    )
    state = initial
    key_piece = lax.all_gather(travel[0], "ctx", axis=0, tiled=True)
    value_piece = lax.all_gather(travel[1], "ctx", axis=0, tiled=True)
    pieces = key_piece.shape[0] // block
    key_blocks = key_piece.reshape(pieces, block, groups_local, HD)
    value_blocks = value_piece.reshape(pieces, block, groups_local, HD)
    starts = block * jnp.arange(pieces, dtype=jnp.int32)

    def visit(carry, item):
        key_block, value_block, key_start = item
        allowed = allowed_mask(key_start, block)
        return (forward_update(carry, key_block, value_block, allowed), None)

    state, unused = lax.scan(visit, state, (key_blocks, value_blocks, starts))
    peak, total, accum = state
    attended = (accum / total[..., None]).reshape(block, heads_local * HD).astype(jnp.bfloat16)
    log_total = peak + jnp.log(total)
    projected = lax.psum(jnp.dot(attended, output_full.T, preferred_element_type=jnp.float32), "tp")
    residual = inputs + projected
    normed_two, inverse_two = norm_forward(residual, gain_two)
    normed_two = normed_two.astype(jnp.bfloat16)
    route = expert_choice[0]
    logits = jnp.dot(normed_two, router_full, preferred_element_type=jnp.float32)
    gates = jax.nn.softmax(jnp.take_along_axis(logits, route, axis=1), axis=1)
    slot, owner, filled = dispatch(route, experts, capacity)
    token_of = owner // chosen_count
    grad_out = out_grad[0].astype(jnp.float32)
    slot_inputs = jnp.where(filled[:, None], normed_two[token_of], 0).reshape(experts, capacity, -1)
    slot_gate = jnp.where(filled, gates.reshape(-1)[owner], 0.0)
    slot_grads = (
        (grad_out[token_of] * slot_gate[:, None])
        .astype(jnp.bfloat16)
        .reshape(experts, capacity, -1)
    )
    gate_full, up_full, down_full = (
        lax.all_gather(gate_weight, ("fsdp", "ctx"), axis=1, tiled=True),
        lax.all_gather(up_weight, ("fsdp", "ctx"), axis=1, tiled=True),
        lax.all_gather(down_weight, ("fsdp", "ctx"), axis=1, tiled=True),
    )
    expert_out, slot_back, gate_term, up_term, down_term = expert_math(
        slot_inputs, slot_grads, gate_full, up_full, down_full
    )
    gate_share, up_share, down_share = (
        lax.psum_scatter(gate_term, ("fsdp", "ctx"), scatter_dimension=1, tiled=True),
        lax.psum_scatter(up_term, ("fsdp", "ctx"), scatter_dimension=1, tiled=True),
        lax.psum_scatter(down_term, ("fsdp", "ctx"), scatter_dimension=1, tiled=True),
    )
    pair_out = expert_out.reshape(experts * capacity, -1)[slot].reshape(block, chosen_count, -1)
    pair_back = slot_back.reshape(experts * capacity, -1)[slot].reshape(block, chosen_count, -1)
    mixed_part = jnp.sum(gates[..., None] * pair_out, axis=1)
    gate_dot_part = jnp.sum(pair_out * grad_out[:, None, :], axis=2)
    moe_part = jnp.sum(pair_back, axis=1)
    mixed, gate_dot, moe_input = (
        lax.psum(mixed_part.astype(jnp.bfloat16), "tp").astype(jnp.float32),
        lax.psum(gate_dot_part.astype(jnp.bfloat16), "tp").astype(jnp.float32),
        lax.psum(moe_part.astype(jnp.bfloat16), "tp").astype(jnp.float32),
    )
    block_out = (residual + mixed).astype(jnp.bfloat16)[None]
    chosen_grad = gates * (gate_dot - jnp.sum(gates * gate_dot, axis=1, keepdims=True))
    picked = (route[..., None] == jnp.arange(experts, dtype=jnp.int32)[None, None, :]).astype(
        jnp.float32
    )
    logit_grad = jnp.sum(picked * chosen_grad[..., None], axis=1)
    router_term = jnp.dot(normed_two.astype(jnp.float32).T, logit_grad, precision=highest)
    router_input = jnp.dot(logit_grad, router_full.astype(jnp.float32).T, precision=highest)
    grad_residual_norm, gain_two_term = norm_backward(
        residual, inverse_two, gain_two, moe_input + router_input
    )
    grad_residual = grad_out + grad_residual_norm
    residual_low = grad_residual.astype(jnp.bfloat16)
    attended_grad = jnp.dot(residual_low, output_full, preferred_element_type=jnp.float32).astype(
        jnp.bfloat16
    )
    output_term = jnp.dot(residual_low.T, attended, preferred_element_type=jnp.float32)
    delta = jnp.sum(
        (attended_grad.astype(jnp.float32) * attended.astype(jnp.float32)).reshape(
            block, groups_local, ratio, HD
        ),
        axis=3,
    )
    grad_grouped = attended_grad.reshape(block, groups_local, ratio, HD)
    back_keys, back_values = (
        lax.all_gather(travel[0], "ctx", axis=0, tiled=True),
        lax.all_gather(travel[1], "ctx", axis=0, tiled=True),
    )
    key_blocks = back_keys.reshape(context_count, block, groups_local, HD)
    value_blocks = back_values.reshape(context_count, block, groups_local, HD)
    starts = block * jnp.arange(context_count, dtype=jnp.int32)

    def backward_update(grad_query, key_block, value_block, allowed):
        mask = allowed[:, None, None, :]
        scores = (
            jnp.einsum(
                "qgrd,kgd->qgrk", query_grouped, key_block, preferred_element_type=jnp.float32
            )
            * scale
        )
        probs = jnp.where(mask, jnp.exp(scores - log_total[..., None]), 0.0)
        value_grad = jnp.einsum(
            "qgrk,qgrd->kgd",
            probs.astype(jnp.bfloat16),
            grad_grouped,
            preferred_element_type=jnp.float32,
        )
        prob_grad = jnp.einsum(
            "qgrd,kgd->qgrk", grad_grouped, value_block, preferred_element_type=jnp.float32
        )
        score_grad = (probs * (prob_grad - delta[..., None]) * scale).astype(jnp.bfloat16)
        grad_query = grad_query + jnp.einsum(
            "qgrk,kgd->qgrd", score_grad, key_block, preferred_element_type=jnp.float32
        )
        key_grad = jnp.einsum(
            "qgrk,qgrd->kgd", score_grad, query_grouped, preferred_element_type=jnp.float32
        )
        return (grad_query, key_grad.reshape(block, -1), value_grad.reshape(block, -1))

    def backward_visit(grad_query, item):
        key_block, value_block, key_start = item
        allowed = allowed_mask(key_start, block)
        grad_query, key_grad, value_grad = backward_update(
            grad_query, key_block, value_block, allowed
        )
        return (grad_query, (key_grad, value_grad))

    grad_query, (key_grads, value_grads) = lax.scan(
        backward_visit,
        jnp.zeros((block, groups_local, ratio, HD), jnp.float32),
        (key_blocks, value_blocks, starts),
    )
    own_key_grad, own_value_grad = (
        lax.psum_scatter(
            key_grads.reshape(context_count * block, -1).astype(jnp.bfloat16),
            "ctx",
            scatter_dimension=0,
            tiled=True,
        ).astype(jnp.float32),
        lax.psum_scatter(
            value_grads.reshape(context_count * block, -1).astype(jnp.bfloat16),
            "ctx",
            scatter_dimension=0,
            tiled=True,
        ).astype(jnp.float32),
    )
    query_grad = (
        rotate_back(grad_query.reshape(block, heads_local, HD), cosine, sine)
        .reshape(block, -1)
        .astype(jnp.bfloat16)
    )
    key_grad = (
        rotate_back(own_key_grad.reshape(block, groups_local, HD), cosine, sine)
        .reshape(block, -1)
        .astype(jnp.bfloat16)
    )
    value_grad = own_value_grad.astype(jnp.bfloat16)
    input_part = jnp.dot(query_grad, query_full.T, preferred_element_type=jnp.float32)
    input_part = input_part + jnp.dot(key_grad, key_full.T, preferred_element_type=jnp.float32)
    input_part = input_part + jnp.dot(value_grad, value_full.T, preferred_element_type=jnp.float32)
    normed_one_grad = lax.psum(input_part.astype(jnp.bfloat16), "tp").astype(jnp.float32)
    grad_input_norm, gain_one_term = norm_backward(inputs, inverse_one, gain_one, normed_one_grad)
    input_grad = (grad_residual + grad_input_norm)[None]
    query_term = jnp.dot(normed_one.T, query_grad, preferred_element_type=jnp.float32)
    key_term = jnp.dot(normed_one.T, key_grad, preferred_element_type=jnp.float32)
    value_term = jnp.dot(normed_one.T, value_grad, preferred_element_type=jnp.float32)
    (
        gain_one_share,
        query_share,
        key_share,
        value_share,
        output_share,
        gain_two_share,
        router_share,
    ) = (
        lax.psum_scatter(gain_one_term, ("fsdp", "ctx"), scatter_dimension=0, tiled=True),
        lax.psum_scatter(query_term, ("fsdp", "ctx"), scatter_dimension=0, tiled=True),
        lax.psum_scatter(key_term, ("fsdp", "ctx"), scatter_dimension=0, tiled=True),
        lax.psum_scatter(value_term, ("fsdp", "ctx"), scatter_dimension=0, tiled=True),
        lax.psum_scatter(output_term, ("fsdp", "ctx"), scatter_dimension=0, tiled=True),
        lax.psum_scatter(gain_two_term, ("fsdp", "ctx"), scatter_dimension=0, tiled=True),
        lax.psum_scatter(router_term, ("fsdp", "ctx"), scatter_dimension=0, tiled=True),
    )
    return (
        block_out,
        input_grad,
        gain_one_share,
        query_share,
        key_share,
        value_share,
        output_share,
        gain_two_share,
        router_share,
        gate_share,
        up_share,
        down_share,
    )


MESH = pl.DeviceIdType.MESH
f32 = jnp.float32
bf16 = jnp.bfloat16


def dot_nn(a, b, precision=None):
    return lax.dot_general(a, b, (((1,), (0,)), ((), ())), precision=precision, preferred_element_type=f32)


def dot_nt(a, b, precision=None):
    return lax.dot_general(a, b, (((1,), (1,)), ((), ())), precision=precision, preferred_element_type=f32)


def dot_tn(a, b, precision=None):
    return lax.dot_general(a, b, (((0,), (0,)), ((), ())), precision=precision, preferred_element_type=f32)


class Net:
    def __init__(self, send_sems, recv_sems):
        self.send_sems, self.recv_sems, self.copies, self.left = send_sems, recv_sems, [], set()
        self.slots, self.free_send, self.free_recv = [], [], []
        self.top_send = self.top_recv = 0

    def make(self, source, target, device, sends=None):
        if self.free_send:
            send_at = self.free_send.pop(0)
        else:
            send_at, self.top_send = self.top_send, self.top_send + 1
        if self.free_recv:
            recv_at = self.free_recv.pop(0)
        else:
            recv_at, self.top_recv = self.top_recv, self.top_recv + 1
        assert max(send_at + 1 - self.send_sems.shape[0], recv_at + 1 - self.recv_sems.shape[0]) <= 0
        copy = pltpu.make_async_remote_copy(
            src_ref=source,
            dst_ref=target,
            send_sem=self.send_sems.at[send_at],
            recv_sem=self.recv_sems.at[recv_at],
            device_id=device,
            device_id_type=MESH,
        )
        self.copies.append((copy, sends))
        self.slots.append((send_at, recv_at))
        return copy

    def send(self, source, target, device):
        copy = self.make(source, target, device)
        copy.start()
        return copy

    def together(self, triples, whole):
        first = self.make(*triples[0])
        send_at, recv_at = self.slots[-1]
        first.start()
        for source, target, device in triples[1:]:
            pltpu.make_async_remote_copy(
                src_ref=source,
                dst_ref=target,
                send_sem=self.send_sems.at[send_at],
                recv_sem=self.recv_sems.at[recv_at],
                device_id=device,
                device_id_type=MESH,
            ).start()
        waits = Whole(
            pltpu.make_async_copy(whole, whole, self.send_sems.at[send_at]),
            pltpu.make_async_copy(whole, whole, self.recv_sems.at[recv_at]),
        )
        self.copies[-1] = (waits, None)
        return waits

    def free(self, among):
        self.free_recv.extend(self.slots[at][1] for at in among)

    def numbers(self, *groups):
        found = []
        for group in groups:
            if isinstance(group, list):
                found += self.numbers(*group)
            else:
                copy = group[0] if isinstance(group, tuple) else group
                found += [at for at, (one, sends) in enumerate(self.copies) if one is copy]
        return found

    def drain(self, among=None):
        for at, (copy, sends) in enumerate(self.copies):
            if at in self.left or (among is not None and at not in among):
                continue
            self.left.add(at)
            self.free_send.append(self.slots[at][0])
            if sends is None:
                copy.wait_send()
            else:
                pl.when(sends)(copy.wait_send)


class Whole:
    def __init__(self, sent, received):
        self.wait_send, self.wait_recv = sent.wait, received.wait


class Line:
    def __init__(self, net, z, nz, device):
        self.net, self.z, self.nz, self.device = net, z, nz, device

    def both(self):
        z, nz = self.z, self.nz
        right, left = self.device(lax.min(z + 1, nz - 1)), self.device(lax.max(z - 1, 0))
        return ((z, right), (nz - 1 - z, left))

    def pass_on(self, step, views):
        copies = []
        for way, (rank, target) in enumerate(self.both()):
            sends = (rank >= step) & (rank < self.nz - 1)
            arrives = rank >= step + 1
            block = lax.clamp(0, self.z - step if way == 0 else self.z + step, self.nz - 1)
            for view in views:
                copy = self.net.make(view(block), view(block), target, sends)
                pl.when(sends)(copy.start)
                copies.append((copy, arrives))
        return copies

    def add_on(self, step, own, out, into):
        copies = []
        for way, (rank, target) in enumerate(self.both()):
            sends = rank <= step
            arrives = (rank >= 1) & (rank - 1 <= step)
            dest = self.nz - 1 - step + rank
            dest = lax.clamp(0, dest if way == 0 else self.nz - 1 - dest, self.nz - 1)
            copy = self.net.make(out(way, step), into(way, step), target, sends)

            def prepare():
                out(way, step)[...] = own(dest)[...].astype(bf16)
                if step > 0:

                    def add():
                        out(way, step)[...] = (own(dest)[...] + into(way, step - 1)[...].astype(f32)).astype(bf16)

                    pl.when(rank >= 1)(add)
                copy.start()

            pl.when(sends)(prepare)
            copies.append((copy, arrives))
        return copies

    def finish(self, total, into):
        for way, (rank, target) in enumerate(self.both()):

            def add():
                total[...] += into(way, self.nz - 2)[...].astype(f32)

            pl.when(rank >= 1)(add)


def arrive(copies):
    for copy, arrives in copies:
        pl.when(arrives)(copy.wait_recv)


def layer_kernel(
    dims,
    x_ref, g_ref, wq_ref, wk_ref, wv_ref, wo_ref, ga_ref, ge_ref, rt_ref, wg_ref, wu_ref, wd_ref, dl_ref, ec_ref,
    fr_ref,
    block_out, input_grad, small_out, gain_out, dqkv_out, dwo_out, dgu_out, dd_out,
    WP, SMT, X, WQ, WO, SMB, SMW, N1, CT, ST, SEGC, POSC, Q, K, V, PSC, ATT, AT, PP, PR, RES,
    N2, GTB, GA, WGU, WD, SWG, SWU, SWD, AA, PSX, GC, H, UG, PRD, MP, MR, BP, BR, DGU, DDT, GDS, GD,
    RB, RM, RBV, RMV, BOWN, MOWN, CO, CI, MO, MI, DGB, GUL, ZG, DDB, DDL, ZD, SG, SGF, SGT, SGZ, SGP, GRES, RL,
    AGS, AGR, DWO, RWO, ZWO, LWO, DS, DQ, DQKV, NG, NR, DWQ, RWQ, ZWQ, LWQ,
    SMO, GNO, DWF, SGW, SG1, SG1P, RSG1, EXB, EXG,
    send_sems, recv_sems, local_sems,
):
    nf, nz, hb, width, experts, half_ff, ndoc, chosen = dims
    rows = 2 * nz * hb
    half = nz * hb
    block = 2 * hb
    shard = width // (nf * nz)
    f, z, c = lax.axis_index("fsdp"), lax.axis_index("ctx"), lax.axis_index("tp")
    other = 1 - c
    own = f * nz + z
    net = Net(send_sems, recv_sems)
    device = lambda df, dz, core: {"fsdp": df, "ctx": dz, "tp": core}
    partner = device(f, z, other)
    line = Line(net, z, nz, lambda dz: device(f, dz, c))
    zs = [z, z + 1 - 2 * lax.rem(z, 2), lax.rem(z + 2, 4), 3 - z]
    fs = [f, f + 1 - 2 * lax.rem(f, 2), lax.rem(f + 2, 4), 3 - f]
    everyone = [(i, j, k) for k in range(2) for i in range(nf) for j in range(nz) if (i, j, k) != (0, 0, 0)]
    others = [device(fs[i], zs[j], lax.rem(c + k, 2)) for i, j, k in everyone]
    same = [(i, 0) for i in range(1, nf)] + [(i, j) for i in range(nf) for j in (3, 1, 2)]

    mine = pl.ds(pl.multiple_of(c * hb, hb), hb)
    loads = [
        pltpu.make_async_copy(x_ref.at[mine], X.at[c, z], local_sems.at[0]),
        pltpu.make_async_copy(g_ref.at[mine], GA.at[f, c, z], local_sems.at[1]),
        pltpu.make_async_copy(wo_ref, WO.at[f, z], local_sems.at[2]),
    ]
    row_experts = lambda at: pl.ds(at * nz, nz)
    shards = ((wg_ref, SWG), (wu_ref, SWU), (wd_ref, SWD))
    loads += [
        pltpu.make_async_copy(ref.at[row_experts(f)], staged.at[f], local_sems.at[3 + at])
        for at, (ref, staged) in enumerate(shards)
    ]
    unit = half_ff // 2
    units = lambda h: pl.ds(h * unit, unit)
    for copy in loads:
        copy.start()
    barrier = pltpu.get_barrier_semaphore()
    for peer in others:
        pl.semaphore_signal(barrier, inc=1, device_id=peer, device_id_type=MESH)

    for j in range(nz):
        WP[j, :, 0 : 2 * HD] = wq_ref[:, 2 * HD * j : 2 * HD * (j + 1)]
        WP[j, :, 2 * HD : 4 * HD] = jnp.concatenate(
            [wk_ref[:, HD * j : HD * (j + 1)], wv_ref[:, HD * j : HD * (j + 1)]], axis=1
        )
    base = jnp.concatenate(
        [ga_ref[...].astype(f32), ge_ref[...].astype(f32), jnp.zeros((14, shard), f32), rt_ref[...].astype(f32)],
        axis=0,
    )
    in_half = (lax.broadcasted_iota(jnp.int32, (32, 128), 1) < shard) == (lax.rem(z, 2) == 0)
    SMT[...] = jnp.where(in_half, jnp.concatenate([base, base], axis=1), 0.0).astype(bf16)
    SMB[f, z] = SMT[...]
    WQ[f, z] = WP[z]
    pl.semaphore_wait(barrier, len(others))

    wd_full = lambda: WD[...].reshape(width, half_ff)
    wgu_full = lambda: WGU[...].reshape(width, 2 * half_ff)
    lower, upper = pl.ds(0, nz // 2), pl.ds(nz // 2, nz // 2)
    across = [None, device(fs[1], z, c), device(fs[2], z, c), device(fs[3], z, c)]

    def second_hop(ref):
        return [net.send(ref.at[f, c], ref.at[f, c], across[k]) for k in (1, 2)]

    def third_hop(ref, k):
        part, to = ((lower, across[2]), (upper, across[1]))[k - 1]
        return net.send(ref.at[fs[k], c, part], ref.at[fs[k], c, part], to)

    sends_q = [net.send(WP.at[zs[k]], WQ.at[f, z], device(f, zs[k], c)) for k in range(1, nz)]
    sends_s = [net.send(SMT, SMB.at[f, z], device(f, zs[k], c)) for k in range(1, nz)]
    loads[0].wait()
    sends_x = [net.send(X.at[c, z], X.at[c, z], device(f, zs[k], c)) for k in range(1, nz)]
    forwards_x = [net.send(X.at[c, z], X.at[c, z], partner)]
    loads[2].wait()
    sends_o = [net.send(WO.at[f, z], WO.at[f, z], device(f, zs[k], c)) for k in range(1, nz)]
    loads[1].wait()
    view_g = [lambda at: GA.at[f, c, at]]
    chain_g = line.pass_on(0, view_g)
    chains = [chain_g]
    weights = ([], [], [])

    def send_row(k, at):
        ref, staged = shards[at]
        return net.send(ref.at[row_experts(fs[k])], staged.at[f], device(fs[k], z, c))

    sends_e = [[send_row(k, at) for k in (1, 2)] for at in range(3)]

    def send_weights(k, *what):
        for at in what:
            staged, into, lanes, target = (
                (SWG, WGU, units(0), units(0)),
                (SWU, WGU, units(0), units(1)),
                (SWG, WGU, units(1), units(2)),
                (SWU, WGU, units(1), units(3)),
                (SWD, WD, pl.ds(0, half_ff), pl.ds(0, half_ff)),
            )[at]
            weights[at // 2].append(
                net.send(staged.at[:, zs[k], :, lanes], into.at[:, z, :, target], device(f, zs[k], c))
            )

    def places(shape, dim):
        at = lax.broadcasted_iota(jnp.int32, shape, dim)
        core_at, rest = lax.div(at, half), lax.rem(at, half)
        return lax.div(rest, hb) * block + core_at * hb + lax.rem(rest, hb)

    def layout(position):
        segment = jnp.zeros_like(position)
        start = jnp.zeros_like(position)
        end = jnp.int32(0)
        for i in range(ndoc):
            length = dl_ref[0, i]
            end = end + length
            after = jnp.where(position >= end, 1, 0)
            segment = segment + after
            start = start + after * length
        return segment, position - start

    lane = lax.broadcasted_iota(jnp.int32, (1, 2 * HD), 1)
    former = lax.rem(lane, HD) < HD // 2
    is_key = lane < HD

    with jax.named_scope("tables0"):
        pos_col = places((rows, 1), 0)
        seg_col, offset = layout(pos_col)
        POSC[...] = pos_col
        SEGC[...] = seg_col
        pos_row = places((1, rows), 1)
        seg_row, unused = layout(pos_row)

    def swapped(v):
        return jnp.where(former, pltpu.roll(v, 2 * HD - HD // 2, 1), pltpu.roll(v, HD // 2, 1))

    for copy in sends_q:
        copy.wait_recv()
    sends_q2 = [net.send(WQ.at[f], WQ.at[f], device(fs[k], z, c)) for k in range(1, nf)]
    for copy in sends_s:
        copy.wait_recv()
    sends_s2 = [net.send(SMB.at[f], SMB.at[f], device(fs[k], z, c)) for k in range(1, nf)]
    for at in (0, 1):
        sends_e[at].append(send_row(3, at))
    with jax.named_scope("tables1"):
        angle = offset.astype(f32) * fr_ref[0:1, :]
        CT[...] = jnp.cos(angle)
        ST[...] = jnp.where(former, -1.0, 1.0) * jnp.sin(angle)
    for copy in sends_s2:
        copy.wait_recv()
    for pair in range(nf * nz // 2):
        at_f, at_z = pair // (nz // 2), 2 * (pair % (nz // 2))
        SMW[:, 128 * pair : 128 * pair + 128] = SMB[at_f, at_z] + SMB[at_f, at_z + 1]

    def norm_block(at_c, at_z):
        v = X[at_c, at_z].astype(f32)
        inverse = lax.rsqrt(jnp.mean(v * v, axis=1, keepdims=True) + epsilon)
        at = pl.ds(pl.multiple_of((at_c * nz + at_z) * hb, hb), hb)
        N1[at, :] = (v * inverse * SMW[0:1, :].astype(f32)).astype(bf16)

    norm_block(c, z)
    for k in range(1, nz):
        sends_x[k - 1].wait_recv()
        forwards_x.append(net.send(X.at[c, zs[k]], X.at[c, zs[k]], partner))
        norm_block(c, zs[k])
    for k in range(nz):
        forwards_x[k].wait_recv()
        norm_block(other, zs[k])
    for copy in sends_q2:
        copy.wait_recv()
    with jax.named_scope("qkv"):
        projected = dot_nn(N1[...], WQ[...].reshape(width, 4 * HD))
        cosine, sine = CT[...], ST[...]
        q_part, kv_part = projected[:, : 2 * HD], projected[:, 2 * HD :]
        Q[...] = (q_part * cosine + swapped(q_part) * sine).astype(bf16)
        kv = jnp.where(is_key, kv_part * cosine + swapped(kv_part) * sine, kv_part).astype(bf16)
        K[...] = kv[:, :HD]
        V[...] = kv[:, HD:]
    for copy in sends_o:
        copy.wait_recv()
    sends_o2 = [net.send(WO.at[f], WO.at[f], across[k]) for k in (1, 2, 3)]
    sends_e[2].append(send_row(3, 2))

    scale = HD ** (-0.5)
    step = 2 * hb

    def attend(i, carry):
        at = pl.ds(pl.multiple_of(i * step, step), step)
        mask = (SEGC[at, :] == seg_row) & (pos_row <= POSC[at, :])
        q = Q[at, :]
        pieces = []
        for r in range(2):
            scores = dot_nt(q[:, r * HD : (r + 1) * HD], K[...]) * scale
            scores = jnp.where(mask, scores, masked_score)
            peak = jnp.max(scores, axis=1, keepdims=True)
            weights = jnp.where(mask, jnp.exp(scores - peak), 0.0)
            total = jnp.sum(weights, axis=1, keepdims=True)
            pieces.append(dot_nn(weights.astype(bf16), V[...]) / total)
            PSC[r, at, :] = (weights / total).astype(bf16)
        out = jnp.concatenate(pieces, axis=1).astype(bf16)
        at_c, at_z = lax.div(2 * i, nz), lax.rem(2 * i, nz)
        ATT[at_c, pl.ds(at_z, 2)] = out.reshape(2, hb, 2 * HD)
        return carry

    with jax.named_scope("attend"):
        lax.fori_loop(0, rows // step, attend, 0)
    columns = pl.ds(pl.multiple_of(z * 2 * HD, 2 * HD), 2 * HD)
    sends_a = [
        net.send(ATT.at[:, zs[k]], AT.at[:, :, columns], device(f, zs[k], c)) for k in range(1, nz)
    ]
    AT[:, :, columns] = ATT[:, z]
    arrive(chain_g)
    chain_g = line.pass_on(1, view_g)
    chains.append(chain_g)
    for copy in loads[3:]:
        copy.wait()
    for copy in sends_e[0] + sends_e[1]:
        copy.wait_recv()
    send_weights(3, 0, 1)
    for copy in sends_a + sends_o2:
        copy.wait_recv()

    with jax.named_scope("proj"):
        part = dot_nt(AT[...].reshape(block, nz * 2 * HD), WO[...].reshape(width, nz * 2 * HD))
        PP[...] = part.reshape(2, hb, width)
    send_p = net.send(PP.at[other], PR, partner)
    arrive(chain_g)
    chain_g = line.pass_on(2, view_g)
    chains.append(chain_g)
    x_own = X[c, z].astype(f32)
    gain_two = SMW[1:2, :].astype(f32)
    send_p.wait_recv()
    residual = x_own + PP[c] + PR[...]
    RES[...] = residual
    inverse_two = lax.rsqrt(jnp.mean(residual * residual, axis=1, keepdims=True) + epsilon)
    N2[f, c, z] = (residual * inverse_two * gain_two).astype(bf16)
    normed_two = N2[f, c, z]
    logits = dot_nt(SMW[16 : 16 + experts, :], normed_two)
    expert_at = lax.broadcasted_iota(jnp.int32, (experts, hb), 0)
    route = ec_ref[...]
    route = jnp.where(c == 0, route, pltpu.roll(route, 128 - hb, 1))
    picked = jnp.zeros((experts, hb), jnp.bool_)
    for j in range(chosen):
        picked = picked | (route[j : j + 1, 0:hb] == expert_at)
    peak = jnp.max(jnp.where(picked, logits, masked_score), axis=0, keepdims=True)
    weight = jnp.where(picked, jnp.exp(logits - peak), 0.0)
    gates = weight / jnp.sum(weight, axis=0, keepdims=True)
    GTB[f, c, z] = jnp.concatenate([gates, jnp.zeros((experts, 128 - hb), f32)], axis=1)
    view_n = [lambda at: N2.at[f, c, at], lambda at: GTB.at[f, c, at]]
    early = net.numbers(
        sends_q, sends_s, sends_x, forwards_x, sends_o, sends_e[:2], sends_q2, sends_s2, sends_o2, sends_a, chains[:2], send_p
    )
    chain_n = line.pass_on(0, view_n)
    chains = [chains[2], chain_n]
    send_weights(2, 0)

    arrive(chain_g)
    sends_g2 = second_hop(GA)
    forwards_g = [net.send(GA.at[f, c], GA.at[f, c], partner)]
    arrive(chain_n)
    chain_n = line.pass_on(1, view_n)
    chains.append(chain_n)
    send_weights(2, 1)
    arrive(chain_n)
    chain_n = line.pass_on(2, view_n)
    chains.append(chain_n)
    send_weights(1, 0, 1)
    for copy in sends_e[2]:
        copy.wait_recv()
    for k in (3, 2, 1):
        send_weights(k, 4)
    for k in (3, 2, 1):
        send_weights(k, 2, 3)
    sends_g3 = []
    for k in (1, 2):
        sends_g2[k - 1].wait_recv()
        sends_g3.append(third_hop(GA, k))
        forwards_g.append(net.send(GA.at[fs[k], c], GA.at[fs[k], c], partner))
    arrive(chain_n)
    sends_n2 = second_hop(N2)
    sends_t2 = [net.send(GTB.at[f, c], GTB.at[f, c], across[k]) for k in (1, 2, 3)]
    forwards_n = [net.send(N2.at[f, c], N2.at[f, c], partner)]
    forwards_t = [net.send(GTB.at[f, c], GTB.at[f, c], partner)]
    before = range(len(net.copies) - 20)

    WGU[:, z, :, 0:unit] = SWG[:, z, :, 0:unit]
    WGU[:, z, :, unit : 2 * unit] = SWU[:, z, :, 0:unit]
    WGU[:, z, :, 2 * unit : 3 * unit] = SWG[:, z, :, unit : 2 * unit]
    WGU[:, z, :, 3 * unit : 4 * unit] = SWU[:, z, :, unit : 2 * unit]
    WD[:, z] = SWD[:, z]
    chosen_row = jnp.where(
        lax.broadcasted_iota(jnp.int32, (experts, 128), 0) == own, 1.0, 0.0
    ).astype(f32)
    sends_d, sends_b, exchange_b, exchange_m = [], {}, {}, {}
    low_half = z < nz // 2
    in_order = [jnp.where(low_half, 3, 0), jnp.where(low_half, 2, 1), zs[1], z]
    grads_z, grads_f = ([], []), ([], [])

    def send_grads(h, k):
        to = device(f, zs[k], c)
        grads_z[h].append(net.send(DGB.at[h, :, zs[k]], ZG.at[h, z], to))
        grads_z[h].append(net.send(DDB.at[h, :, zs[k]], ZD.at[h, z], to))

    def spread_grads(h):
        ZG[h, z] = DGB[h, :, z]
        ZD[h, z] = DDB[h, :, z]
        for copy in grads_z[h]:
            copy.wait_recv()
        for k in range(1, nf):
            grads_f[h].append(
                net.send(ZG.at[h, :, fs[k]], GUL.at[f, :, :, pl.ds(2 * h * unit, 2 * unit)], across[k])
            )
            grads_f[h].append(net.send(ZD.at[h, :, fs[k]], DDL.at[f, :, :, units(h)], across[k]))
        GUL[f, :, :, 2 * h * unit : 2 * (h + 1) * unit] = ZG[h, :, f]
        DDL[f, :, :, h * unit : (h + 1) * unit] = ZD[h, :, f]

    def expert_part(h, k):
        at_f = fs[k]
        tokens = N2[at_f].reshape(rows, width)
        with jax.named_scope("gateup"):
            PSX[...] = dot_nn(tokens, WGU[:, :, :, 2 * h * unit : 2 * (h + 1) * unit].reshape(width, 2 * unit))
        if h == 0:
            with jax.named_scope("gatecol"):
                for piece in range(2 * nz):
                    tile = GTB[at_f, piece // nz, piece % nz][:, 0:hb]
                    GC[k, piece * hb : (piece + 1) * hb, :] = dot_tn(tile, chosen_row, lax.Precision.HIGHEST)

        def expert_chunk(i, carry):
            at = pl.ds(pl.multiple_of(i * 64, 64), 64)
            gate_pre = PSX[at, 0:unit]
            up_pre = PSX[at, unit : 2 * unit]
            raw = AA[k, at, h * unit : (h + 1) * unit]
            gate = GC[k, at, :]
            sigmoid = jax.nn.sigmoid(gate_pre)
            silu = gate_pre * sigmoid
            act = silu * up_pre
            PRD[at, :] = (act * raw).astype(bf16)
            H[k, at, h * unit : (h + 1) * unit] = (act * gate).astype(bf16)
            grad = raw * gate
            UG[k, at, 2 * h * unit : (2 * h + 1) * unit] = (
                grad * up_pre * sigmoid * (1.0 + gate_pre * (1.0 - sigmoid))
            ).astype(bf16)
            UG[k, at, (2 * h + 1) * unit : 2 * (h + 1) * unit] = (grad * silu).astype(bf16)
            return carry

        with jax.named_scope("chunk"):
            lax.fori_loop(0, rows // 64, expert_chunk, 0)
        if h == 1:
            with jax.named_scope("back"):
                BP[at_f] = dot_nt(UG[k], WGU[...].reshape(width, 2 * half_ff)).astype(bf16).reshape(2, nz, hb, width)
            exchange_b[k] = net.send(BP.at[at_f, other], BR.at[at_f], partner)
        with jax.named_scope("gdot"):
            dots = dot_nt(jnp.ones((8, unit), bf16), PRD[...])
            GDS[k] = dots if h == 0 else GDS[k] + dots
        if h == 1:
            sets = []
            for j in range(nz):
                for t in range(2):
                    to_z, to_c = zs[j], lax.rem(c + t, 2)
                    lanes = pl.ds(pl.multiple_of((to_c * (nz // 2) + lax.div(to_z, 2)) * 128, 128), 128)
                    if (k, j, t) != (0, 0, 0):
                        sets.append(
                            (GDS.at[k, pl.ds(0, 1), lanes], GD.at[f, z, c, pl.ds(0, 1)], device(at_f, to_z, to_c))
                        )
                    else:
                        GD[f, z, c] = GDS[0, :, lanes]
            sends_d.append(net.together(sets, SGW.at[pl.ds(0, len(sets))]))

    def mix(k):
        with jax.named_scope("mix"):
            MP[fs[k]] = dot_nt(H[k], WD[...].reshape(width, half_ff)).astype(bf16).reshape(2, nz, hb, width)
        exchange_m[k] = net.send(MP.at[fs[k], other], MR.at[fs[k]], partner)

    def weight_terms(h, k):
        with jax.named_scope("wgrad"):
            gate_up = dot_tn(UG[k, :, 2 * h * unit : 2 * (h + 1) * unit], N2[fs[k]].reshape(rows, width))
            down = dot_tn(H[k, :, h * unit : (h + 1) * unit], GA[fs[k]].reshape(rows, width))
            first = k == (0, 3)[h]
            DGU[...] = gate_up if first else DGU[...] + gate_up
            DDT[...] = down if first else DDT[...] + down

    def shed(h):
        with jax.named_scope("transpose"):
            DGB[h] = jnp.transpose(DGU[...]).astype(bf16).reshape(nf, nz, shard, 2 * unit)
            DDB[h] = jnp.transpose(DDT[...]).astype(bf16).reshape(nf, nz, shard, unit)

    def cotangent(k):
        forwards_g[k].wait_recv()
        with jax.named_scope("cotangent"):
            AA[k] = dot_nn(GA[fs[k]].reshape(rows, width), WD[...].reshape(width, half_ff))

    net.drain(before)
    for copy in weights[2]:
        copy.wait_recv()
    for k in range(nf - 1):
        cotangent(k)
    for copy in weights[0]:
        copy.wait_recv()
    for k in range(nf):
        if k == 1:
            sends_n3 = []
            for i in (1, 2):
                sends_n2[i - 1].wait_recv()
                sends_n3.append(third_hop(N2, i))
                forwards_n.append(net.send(N2.at[fs[i], c], N2.at[fs[i], c], partner))
                sends_t2[i - 1].wait_recv()
                forwards_t.append(net.send(GTB.at[fs[i], c], GTB.at[fs[i], c], partner))
            for copy in sends_g3:
                copy.wait_recv()
            forwards_g.append(net.send(GA.at[fs[3], c], GA.at[fs[3], c], partner))
        if k == 3:
            cotangent(k)
            for copy in sends_n3:
                copy.wait_recv()
            forwards_n.append(net.send(N2.at[fs[k], c], N2.at[fs[k], c], partner))
            sends_t2[2].wait_recv()
            forwards_t.append(net.send(GTB.at[fs[k], c], GTB.at[fs[k], c], partner))
        forwards_n[k].wait_recv()
        forwards_t[k].wait_recv()
        expert_part(0, k)
        weight_terms(0, k)
    shed(0)
    for k in (3, 2, 1):
        send_grads(0, k)
    for copy in weights[1]:
        copy.wait_recv()
    own_half = ((lower, 1), (upper, 2))

    def spread(k, exchange, part, back, total, via, into, order):
        at_f = fs[k]
        exchange[k].wait_recv()
        if k == 0:
            total[...] = part[at_f, c].astype(f32) + back[at_f].astype(f32)
            return []
        if k == 3:
            part[at_f, c] = (part[at_f, c].astype(f32) + back[at_f].astype(f32)).astype(bf16)
            return [net.send(part.at[at_f, c, half_at], via.at[to - 1], across[to]) for half_at, to in own_half]
        return None

    def spread_near(k, firsts, part, back, via, into, order):
        at_f = fs[k]
        half_at, other_half = (upper, lower) if k == 1 else (lower, upper)
        firsts[2 - k].wait_recv()
        part[at_f, c, half_at] = (
            part[at_f, c, half_at].astype(f32) + back[at_f, half_at].astype(f32) + via[2 - k].astype(f32)
        ).astype(bf16)
        part[at_f, c, other_half] = (
            part[at_f, c, other_half].astype(f32) + back[at_f, other_half].astype(f32)
        ).astype(bf16)
        return [net.send(part.at[at_f, c, at], into.at[k - 1, at], across[k]) for at in order]

    sends_m = {}
    middle = net.numbers(
        sends_e[2:], sends_g2, sends_g3, forwards_g, *weights, chains, sends_n2, sends_n3, sends_t2,
        forwards_n, forwards_t,
    )
    net.free(early)
    expert_part(1, 3)
    weight_terms(1, 3)
    mix(3)
    firsts_b = spread(3, exchange_b, BP, BR, BOWN, RBV, RB, in_order)
    for k in (1, 2, 0):
        expert_part(1, k)
    for k in (1, 2):
        exchange_b[k].wait_recv()
        sends_b[k] = spread_near(k, firsts_b, BP, BR, RBV, RB, in_order)
    spread(0, exchange_b, BP, BR, BOWN, RBV, RB, in_order)
    firsts_m = spread(3, exchange_m, MP, MR, MOWN, RMV, RM, in_order)
    for k in (1, 2, 0):
        mix(k)
        weight_terms(1, k)

    expert_copies = len(net.copies)
    shed(1)

    def dots_back():
        for copy in sends_d:
            copy.wait_recv()
        dots = jnp.concatenate(
            [
                GD[e // nz, e % nz, 0][0:1, :] + GD[e // nz, e % nz, 1][0:1, :]
                for e in range(experts)
            ],
            axis=0,
        )
        dots = jnp.where(lax.rem(z, 2) == 0, dots, pltpu.roll(dots, 128 - hb, 1))[:, 0:hb]
        gates = GTB[f, c, z][:, 0:hb]
        logit_grad = gates * (dots - jnp.sum(gates * dots, axis=0, keepdims=True))
        router_t = SMW[16 : 16 + experts, :].astype(f32)
        SG[0:experts, :] = dot_nn(logit_grad, N2[f, c, z].astype(f32), lax.Precision.HIGHEST)
        GRES[...] = dot_tn(logit_grad, router_t, lax.Precision.HIGHEST)

    own_b, out_b, into_b = (lambda at: BOWN.at[at]), (lambda w, t: CO.at[w, t]), (lambda w, t: CI.at[w, t])

    def take_block(at):
        for k in (1, 2):
            sends_b[k][at].wait_recv()
            BOWN[in_order[at]] += RB[k - 1, in_order[at]].astype(f32)

    sums = []
    for t in range(nz):
        take_block(t)
        if t > 0:
            arrive(chain_b)
        if t < nz - 1:
            at_sums = len(net.copies)
            chain_b = line.add_on(t, own_b, out_b, into_b)
            sums.extend(range(at_sums, len(net.copies)))
        if t == 0:
            dots_back()
        if t == 2:
            spread_grads(0)
    line.finish(BOWN.at[z], into_b)
    net.free(middle)

    residual = RES[...]
    inverse_two = lax.rsqrt(jnp.mean(residual * residual, axis=1, keepdims=True) + epsilon)
    grad_two = BOWN[z] + GRES[...]
    scaled = grad_two * gain_two
    grad_res = (
        GA[f, c, z].astype(f32)
        + inverse_two * scaled
        - residual * (inverse_two * inverse_two * inverse_two) * jnp.mean(scaled * residual, axis=1, keepdims=True)
    )
    GRES[...] = grad_res
    RL[c] = grad_res.astype(bf16)
    send_r = net.send(RL.at[c], RL.at[c], partner)
    gain_term = jnp.sum(grad_two * residual * inverse_two, axis=0, keepdims=True)
    SG[experts : experts + 8, :] = jnp.broadcast_to(gain_term, (8, width))
    wide = width // nf
    block_lanes = lambda at: pl.ds(pl.multiple_of(at * wide, 128), wide)
    sends_sg = [net.send(SG.at[:, block_lanes(fs[k])], SGF.at[k - 1], device(fs[k], z, c)) for k in range(1, nf)]
    send_r.wait_recv()
    low = RL[...].reshape(block, width)
    with jax.named_scope("attgrad"):
        AGS[...] = dot_nn(low, WO[...].reshape(width, nz * 2 * HD)).astype(bf16).reshape(2, hb, nz * 2 * HD)
    sends_ag = [
        net.send(
            AGS.at[:, :, pl.ds(pl.multiple_of(zs[k] * 2 * HD, 2 * HD), 2 * HD)],
            AGR.at[:, z],
            device(f, zs[k], c),
        )
        for k in range(1, nz)
    ]
    AGR[:, z] = AGS[:, :, columns]
    for k in (1, 2):
        exchange_m[k].wait_recv()
        sends_m[k] = spread_near(k, firsts_m, MP, MR, RMV, RM, in_order)
    spread(0, exchange_m, MP, MR, MOWN, RMV, RM, in_order)
    for k in (1, 3, 2):
        send_grads(1, k)
    with jax.named_scope("outgrad"):
        DWO[...] = (
            dot_tn(low, AT[...].reshape(block, nz * 2 * HD))
            .astype(bf16)
            .reshape(nf, nz, shard, nz * 2 * HD)
        )
    sends_wo = [net.send(DWO.at[fs[k]], RWO.at[k - 1], device(fs[k], z, c)) for k in range(1, nf)]

    net.drain(range(expert_copies))
    for copy in sends_ag:
        copy.wait_recv()

    def backward(i, carry):
        at = pl.ds(pl.multiple_of(i * step, step), step)
        at_c, at_z = lax.div(2 * i, nz), lax.rem(2 * i, nz)
        grad = AGR[at_c, pl.ds(at_z, 2)].reshape(step, 2 * HD)
        out = ATT[at_c, pl.ds(at_z, 2)].reshape(step, 2 * HD)
        both = grad.astype(f32) * out.astype(f32)
        pieces = []
        for r in range(2):
            delta = jnp.sum(both[:, r * HD : (r + 1) * HD], axis=1, keepdims=True)
            prob_grad = dot_nt(grad[:, r * HD : (r + 1) * HD], V[...])
            probs = PSC[r, at, :].astype(f32)
            score_grad = (probs * (prob_grad - delta) * scale).astype(bf16)
            DS[r, at, :] = score_grad
            pieces.append(dot_nn(score_grad, K[...]))
        DQ[at, :] = jnp.concatenate(pieces, axis=1)
        return carry

    with jax.named_scope("attback"):
        lax.fori_loop(0, rows // step, backward, 0)
    with jax.named_scope("kvgrad"):
        grads = AGR[...].reshape(rows, 2 * HD)
        key_t = dot_tn(Q[:, 0:HD], DS[0]) + dot_tn(Q[:, HD : 2 * HD], DS[1])
        value_t = dot_tn(grads[:, 0:HD], PSC[0]) + dot_tn(grads[:, HD : 2 * HD], PSC[1])
        kv_grad = jnp.transpose(jnp.concatenate([key_t, value_t], axis=0))
        cosine, sine = CT[...], ST[...]
        q_grad = DQ[...]
        DQKV[:, 0 : 2 * HD] = (q_grad * cosine - swapped(q_grad) * sine).astype(bf16)
        DQKV[:, 2 * HD : 4 * HD] = jnp.where(
            is_key, kv_grad * cosine - swapped(kv_grad) * sine, kv_grad
        ).astype(bf16)
    with jax.named_scope("ingrad"):
        NG[...] = dot_nt(DQKV[...], WQ[...].reshape(width, 4 * HD)).astype(bf16).reshape(2, nz, hb, width)
    send_ng = net.send(NG.at[other], NR, partner)
    with jax.named_scope("qkvgrad"):
        DWQ[...] = (
            jnp.transpose(dot_tn(DQKV[...], N1[...])).astype(bf16).reshape(nf, nz, shard, 4 * HD)
        )
    sends_wq = [net.send(DWQ.at[fs[k]], RWQ.at[k - 1], device(fs[k], z, c)) for k in range(1, nf)]
    send_ng.wait_recv()
    net.drain(sums)
    BOWN[...] = NG[c].astype(f32) + NR[...].astype(f32)
    chain_g1 = line.add_on(0, own_b, out_b, into_b)
    for k in (1, 2):
        for at in range(nz):
            sends_m[k][at].wait_recv()
        MOWN[...] += RM[k - 1].astype(f32)
    own_m, out_m, into_m = (lambda at: MOWN.at[at]), (lambda w, t: MO.at[w, t]), (lambda w, t: MI.at[w, t])
    chain_m = line.add_on(0, own_m, out_m, into_m)
    arrive(chain_g1)
    chain_g1 = line.add_on(1, own_b, out_b, into_b)
    arrive(chain_m)
    chain_m = line.add_on(1, own_m, out_m, into_m)
    arrive(chain_g1)
    chain_g1 = line.add_on(2, own_b, out_b, into_b)
    arrive(chain_m)
    chain_m = line.add_on(2, own_m, out_m, into_m)

    arrive(chain_g1)
    line.finish(BOWN.at[z], into_b)
    grad_one = BOWN[z]
    gain_one = SMW[0:1, :].astype(f32)
    x_own = X[c, z].astype(f32)
    inverse = lax.rsqrt(jnp.mean(x_own * x_own, axis=1, keepdims=True) + epsilon)
    gain_term = jnp.sum(grad_one * x_own * inverse, axis=0, keepdims=True)
    SG1[0] = jnp.broadcast_to(gain_term, (8, width))
    send_g1 = net.send(SG1.at[0], SG1.at[1], partner)
    scaled = grad_one * gain_one
    EXG[c] = (
        GRES[...]
        + inverse * scaled
        - x_own * (inverse * inverse * inverse) * jnp.mean(scaled * x_own, axis=1, keepdims=True)
    )
    send_ig = net.send(EXG.at[c], EXG.at[c], partner)
    small = SG[:, block_lanes(f)]
    for k in range(1, nf):
        sends_sg[k - 1].wait_recv()
        small = small + SGF[k - 1]
    SGT[...] = small
    pair_lanes = lambda at: pl.ds(pl.multiple_of(lax.div(at, 2) * 128, 128), 128)
    sends_sz = [net.send(SGT.at[:, pair_lanes(zs[k])], SGZ.at[k - 1], device(f, zs[k], c)) for k in range(1, nz)]
    total = DWO[f].astype(f32)
    for k in range(1, nf):
        sends_wo[k - 1].wait_recv()
        total = total + RWO[k - 1].astype(f32)
    ZWO[...] = total.astype(bf16)
    sends_wo2 = [net.send(ZWO.at[zs[k]], LWO.at[z], device(f, zs[k], c)) for k in range(1, nz)]
    LWO[z] = ZWO[z]
    total = DWQ[f].astype(f32)
    for k in range(1, nf):
        sends_wq[k - 1].wait_recv()
        total = total + RWQ[k - 1].astype(f32)
    ZWQ[...] = total.astype(bf16)
    sends_wq2 = [net.send(ZWQ.at[zs[k]], LWQ.at[z], device(f, zs[k], c)) for k in range(1, nz)]
    LWQ[z] = ZWQ[z]
    small = SGT[:, pair_lanes(z)]
    for k in range(1, nz):
        sends_sz[k - 1].wait_recv()
        small = small + SGZ[k - 1]
    SGP[0] = small
    send_sp = net.send(SGP.at[0], SGP.at[1], partner)
    net.drain(range(expert_copies))
    send_g1.wait_recv()
    SG1P[...] = SG1[0] + SG1[1]
    lanes_of = lambda df, dz: pl.ds(pl.multiple_of((df * (nz // 2) + lax.div(dz, 2)) * 128, 128), 128)
    sets = [
        (SG1P.at[pl.ds(0, 1), lanes_of(fs[i], zs[j])], RSG1.at[f, z, pl.ds(0, 1)], device(fs[i], zs[j], c))
        for i, j in same
    ]
    sends_g1 = [net.together(sets, SGW.at[pl.ds(0, len(sets))])]
    RSG1[f, z] = SG1P[:, lanes_of(f, z)]

    spread_grads(1)
    arrive(chain_m)
    line.finish(MOWN.at[z], into_m)
    EXB[c] = (RES[...] + MOWN[z]).astype(bf16)
    send_bo = net.send(EXB.at[c], EXB.at[c], partner)
    outs = []

    def leave(source, target):
        copy = pltpu.make_async_copy(source, target, local_sems.at[6 + len(outs)])
        copy.start()
        outs.append(copy)

    send_sp.wait_recv()
    SMO[...] = SGP[0] + SGP[1]
    leave(SMO, small_out)
    for copy in sends_wo2:
        copy.wait_recv()
    total = LWO[0].astype(f32)
    for j in range(1, nz):
        total = total + LWO[j].astype(f32)
    DWF[...] = total
    leave(DWF, dwo_out)
    for copy in sends_wq2:
        copy.wait_recv()
    leave(LWQ, dqkv_out)
    send_bo.wait_recv()
    leave(EXB, block_out)
    send_ig.wait_recv()
    leave(EXG, input_grad)
    for copy in sends_g1:
        copy.wait_recv()
    small = jnp.zeros((1, 128), f32)
    for i in range(nf):
        for j in range(nz):
            small = small + RSG1[i, j, 0:1]
    GNO[...] = jnp.broadcast_to(small, (8, 128))
    leave(GNO, gain_out)
    for copy in grads_f[0] + grads_f[1]:
        copy.wait_recv()
    leave(GUL, dgu_out)
    leave(DDL, dd_out)
    with jax.named_scope("drain"):
        net.drain()
    with jax.named_scope("outs"):
        for copy in outs:
            copy.wait()


def finish_kernel(
    dims, block_ref, input_ref, small_ref, gain_ref, dqkv_ref, dwo_ref, dgu_ref, dd_ref,
    block_out, input_out, gain1_out, q_out, k_out, v_out, o_out, gain2_out, router_out, gate_out, up_out, down_out,
):
    nz, experts, half_ff, shard = dims
    block_out[...] = block_ref[...]
    input_out[...] = input_ref[...]
    unit = half_ff // 2
    for h in range(2):
        gate_out[:, :, h * unit : (h + 1) * unit] = dgu_ref[:, :, 2 * h * unit : (2 * h + 1) * unit].astype(f32)
        up_out[:, :, h * unit : (h + 1) * unit] = dgu_ref[:, :, (2 * h + 1) * unit : 2 * (h + 1) * unit].astype(f32)
    down_out[...] = dd_ref[...].astype(f32)
    even = lax.rem(lax.axis_index("ctx"), 2) == 0
    pick = lambda v: jnp.where(even, v, pltpu.roll(v, 128 - shard, 1))[:, 0:shard]

    def once():
        gain1_out[...] = pick(gain_ref[...])[0:1]
        small = pick(small_ref[...])
        router_out[...] = small[0:experts]
        gain2_out[...] = small[experts : experts + 1]
        o_out[...] = dwo_ref[...]
        for j in range(nz):
            q_out[:, 2 * HD * j : 2 * HD * (j + 1)] = dqkv_ref[j, :, 0 : 2 * HD].astype(f32)
        for at, ref in ((2, k_out), (3, v_out)):
            ref[...] = jnp.concatenate(
                [dqkv_ref[j, :, at * HD : (at + 1) * HD].astype(f32) for j in range(nz)], axis=1
            )

    pl.when(pl.program_id(0) == 0)(once)


def fast_local(
    nf, nz,
    hidden_in, out_grad, attention_gain, query_weight, key_weight, value_weight, output_weight,
    expert_gain, router_weight, gate_weight, up_weight, down_weight, doc_lengths, expert_choice,
):
    block, width = hidden_in.shape[1], hidden_in.shape[2]
    hb = block // 2
    experts, shard, half_ff = gate_weight.shape
    ndoc, chosen = doc_lengths.shape[1], expert_choice.shape[2]
    rows = nz * block
    halfway = HD // 2
    frequency = np.float32(rope_base) ** (-np.arange(halfway, dtype=np.float32) / np.float32(halfway))
    frequency = jnp.asarray(np.tile(np.tile(frequency, 4)[None], (8, 1)).astype(np.float32))

    vm = pl.BlockSpec(memory_space=pltpu.VMEM)
    anywhere = pl.BlockSpec(memory_space=pl.ANY)
    shape = lambda s, d: jax.ShapeDtypeStruct(s, d)
    W = nz * 2 * HD
    scratch = dict(
        WP=((nz, shard, 4 * HD), bf16), SMT=((32, 128), bf16),
        X=((2, nz, hb, width), bf16), WQ=((nf, nz, shard, 4 * HD), bf16), WO=((nf, nz, shard, W), bf16),
        SMB=((nf, nz, 32, 128), bf16), SMW=((32, width), bf16), N1=((rows, width), bf16),
        CT=((rows, 128), f32), ST=((rows, 128), f32), SEGC=((rows, 1), jnp.int32), POSC=((rows, 1), jnp.int32),
        Q=((rows, 2 * HD), bf16), K=((rows, HD), bf16), V=((rows, HD), bf16), PSC=((2, rows, rows), bf16),
        ATT=((2, nz, hb, 2 * HD), bf16), AT=((2, hb, W), bf16), PP=((2, hb, width), f32), PR=((hb, width), f32),
        RES=((hb, width), f32),
        N2=((nf, 2, nz, hb, width), bf16), GTB=((nf, 2, nz, experts, 128), f32), GA=((nf, 2, nz, hb, width), bf16),
        WGU=((nf, nz, shard, 2 * half_ff), bf16), WD=((nf, nz, shard, half_ff), bf16),
        SWG=((nf, nz, shard, half_ff), bf16), SWU=((nf, nz, shard, half_ff), bf16), SWD=((nf, nz, shard, half_ff), bf16),
        AA=((nf, rows, half_ff), f32), PSX=((rows, half_ff), f32), GC=((nf, rows, 128), f32),
        H=((nf, rows, half_ff), bf16), UG=((nf, rows, 2 * half_ff), bf16), PRD=((rows, half_ff // 2), bf16),
        MP=((nf, 2, nz, hb, width), bf16), MR=((nf, nz, hb, width), bf16),
        BP=((nf, 2, nz, hb, width), bf16), BR=((nf, nz, hb, width), bf16),
        DGU=((half_ff, width), f32), DDT=((half_ff // 2, width), f32),
        GDS=((nf, 8, rows), f32), GD=((nf, nz, 2, 8, 128), f32),
        RB=((2, nz, hb, width), bf16), RM=((2, nz, hb, width), bf16),
        RBV=((2, nz // 2, hb, width), bf16), RMV=((2, nz // 2, hb, width), bf16),
        BOWN=((nz, hb, width), f32), MOWN=((nz, hb, width), f32),
        CO=((2, nz - 1, hb, width), bf16), CI=((2, nz - 1, hb, width), bf16),
        MO=((2, nz - 1, hb, width), bf16), MI=((2, nz - 1, hb, width), bf16),
        DGB=((2, nf, nz, shard, half_ff), bf16), GUL=((nf, nz, shard, 2 * half_ff), bf16), ZG=((2, nz, nf, shard, half_ff), bf16),
        DDB=((2, nf, nz, shard, half_ff // 2), bf16), DDL=((nf, nz, shard, half_ff), bf16), ZD=((2, nz, nf, shard, half_ff // 2), bf16),
        SG=((experts + 8, width), f32), SGF=((nf - 1, experts + 8, width // nf), f32),
        SGT=((experts + 8, width // nf), f32), SGZ=((nz - 1, experts + 8, 128), f32), SGP=((2, experts + 8, 128), f32),
        GRES=((hb, width), f32), RL=((2, hb, width), bf16),
        AGS=((2, hb, W), bf16), AGR=((2, nz, hb, 2 * HD), bf16),
        DWO=((nf, nz, shard, W), bf16), RWO=((nf - 1, nz, shard, W), bf16),
        ZWO=((nz, shard, W), bf16), LWO=((nz, shard, W), bf16),
        DS=((2, rows, rows), bf16), DQ=((rows, 2 * HD), f32),
        DQKV=((rows, 4 * HD), bf16), NG=((2, nz, hb, width), bf16), NR=((nz, hb, width), bf16),
        DWQ=((nf, nz, shard, 4 * HD), bf16), RWQ=((nf - 1, nz, shard, 4 * HD), bf16),
        ZWQ=((nz, shard, 4 * HD), bf16), LWQ=((nz, shard, 4 * HD), bf16),
        SMO=((experts + 8, 128), f32), GNO=((8, 128), f32), DWF=((shard, W), f32), SGW=((16, 128), f32), SG1=((2, 8, width), f32), SG1P=((8, width), f32), RSG1=((nf, nz, 8, 128), f32),
        EXB=((2, hb, width), bf16), EXG=((2, hb, width), f32),
    )
    slots = (96, 104)
    out = pl.pallas_call(
        functools.partial(layer_kernel, (nf, nz, hb, width, experts, half_ff, ndoc, chosen)),
        name="layer",
        out_shape=(
            shape((2, hb, width), bf16), shape((2, hb, width), f32), shape((experts + 8, 128), f32),
            shape((8, 128), f32), shape((nz, shard, 4 * HD), bf16), shape((shard, W), f32),
            shape((nf, nz, shard, 2 * half_ff), bf16), shape((nf, nz, shard, half_ff), bf16),
        ),
        in_specs=[anywhere] * 2 + [vm] * 3 + [anywhere] + [vm] * 3 + [anywhere] * 3
        + [pl.BlockSpec(memory_space=pltpu.SMEM), vm, vm],
        out_specs=(anywhere,) * 8,
        scratch_shapes=[pltpu.VMEM(s, d) for s, d in scratch.values()]
        + [pltpu.SemaphoreType.DMA((slots[0],)), pltpu.SemaphoreType.DMA((slots[1],)), pltpu.SemaphoreType.DMA((14,))],
        compiler_params=pltpu.CompilerParams(
            collective_id=0, has_side_effects=True, vmem_limit_bytes=67043328
        ),
    )(
        hidden_in[0], out_grad[0], query_weight, key_weight, value_weight, output_weight,
        attention_gain[None], expert_gain[None], router_weight.T, gate_weight, up_weight, down_weight,
        doc_lengths, expert_choice[0].T, frequency,
    )
    steps = nz // 2
    some = lambda *s: pl.BlockSpec(s, lambda i: (i,) + (0,) * (len(s) - 1))
    whole = lambda *s: pl.BlockSpec(s, lambda i: (0,) * len(s))
    per = nf * nz // steps
    out = pl.pallas_call(
        functools.partial(finish_kernel, (nz, experts, half_ff, shard)),
        name="finish",
        grid=(steps,),
        out_shape=(
            shape((block, width), bf16), shape((block, width), f32), shape((1, shard), f32),
            shape((shard, nz * 2 * HD), f32), shape((shard, nz * HD), f32), shape((shard, nz * HD), f32),
            shape((shard, W), f32), shape((1, shard), f32), shape((experts, shard), f32),
            shape((experts, shard, half_ff), f32), shape((experts, shard, half_ff), f32),
            shape((experts, shard, half_ff), f32),
        ),
        in_specs=[
            some(block // steps, width), some(block // steps, width), whole(experts + 8, 128), whole(8, 128),
            whole(nz, shard, 4 * HD), whole(shard, W), some(per, shard, 2 * half_ff), some(per, shard, half_ff),
        ],
        out_specs=(
            some(block // steps, width), some(block // steps, width), whole(1, shard),
            whole(shard, nz * 2 * HD), whole(shard, nz * HD), whole(shard, nz * HD), whole(shard, W), whole(1, shard),
            whole(experts, shard), some(per, shard, half_ff), some(per, shard, half_ff), some(per, shard, half_ff),
        ),
        compiler_params=pltpu.CompilerParams(vmem_limit_bytes=67043328),
    )(out[0].reshape(block, width), out[1].reshape(block, width), *out[2:6], out[6].reshape(experts, shard, 2 * half_ff), out[7].reshape(experts, shard, half_ff))
    block_out, input_grad, gain1, q, k, v, o, gain2, router, gate, up, down = out
    return (
        block_out[None], input_grad[None], gain1[0], q, k, v, o, gain2[0], router.T, gate, up, down,
    )


def fits(mesh, args):
    nf, nz, nc = mesh.shape["fsdp"], mesh.shape["ctx"], mesh.shape["tp"]
    hidden, query, key, gate = args[0], args[3], args[4], args[9]
    width, block = hidden.shape[2], hidden.shape[1] // nz
    return (
        nc == 2
        and nz == 4
        and nf == 4
        and hidden.shape[0] == nf
        and gate.shape[0] == nf * nz
        and gate.shape[0] == 16
        and width == 64 * nf * nz
        and block == 128
        and query.shape[1] == 2 * HD * nz * nc
        and key.shape[1] == HD * nz * nc
        and HD == 64
    )


def solution(mesh):
    in_specs = (
        P("fsdp", "ctx", None),
        P("fsdp", "ctx", None),
        P(("fsdp", "ctx")),
        P(("fsdp", "ctx"), "tp"),
        P(("fsdp", "ctx"), "tp"),
        P(("fsdp", "ctx"), "tp"),
        P(("fsdp", "ctx"), "tp"),
        P(("fsdp", "ctx")),
        P(("fsdp", "ctx"), None),
        P(None, ("fsdp", "ctx"), "tp"),
        P(None, ("fsdp", "ctx"), "tp"),
        P(None, ("fsdp", "ctx"), "tp"),
        P("fsdp", None),
        P("fsdp", "ctx", None),
    )
    out_specs = (
        P("fsdp", "ctx", None),
        P("fsdp", "ctx", None),
        P(("fsdp", "ctx")),
        P(("fsdp", "ctx"), "tp"),
        P(("fsdp", "ctx"), "tp"),
        P(("fsdp", "ctx"), "tp"),
        P(("fsdp", "ctx"), "tp"),
        P(("fsdp", "ctx")),
        P(("fsdp", "ctx"), None),
        P(None, ("fsdp", "ctx"), "tp"),
        P(None, ("fsdp", "ctx"), "tp"),
        P(None, ("fsdp", "ctx"), "tp"),
    )

    def step(*args):
        body = local
        if fits(mesh, args):
            body = functools.partial(fast_local, mesh.shape["fsdp"], mesh.shape["ctx"])
        return jax.shard_map(
            body, mesh=mesh, in_specs=in_specs, out_specs=out_specs, check_vma=False
        )(*args)

    return step
```
